32 devices in a mesh: dp: 8 (over z, y), fsdp: 4 (over x, core).
Axes of the slice: x: 2, y: 2, z: 4, core: 2. Of those that a mesh axis runs over, the one named last changes fastest.
Arguments:
- hidden: bfloat16 [32768, 1536], P(('dp', 'fsdp')), may hold values from -6 to 6
- grad_out: bfloat16 [32768, 1536], P(('dp', 'fsdp')), may hold values from -6 to 6
- segment_ids: int32 [32768], P(('dp', 'fsdp')), may hold values from 0 to 189, as said below
- w_zx: bfloat16 [1536, 6144], P(('dp', 'fsdp')), may hold values from -0.15625 to 0.15625
- w_bc: bfloat16 [1536, 256], P(('dp', 'fsdp')), may hold values from -0.15625 to 0.15625
- w_dt: bfloat16 [1536, 48], P(('dp', 'fsdp')), may hold values from -0.15625 to 0.15625
- w_out: bfloat16 [3072, 1536], P(('dp', 'fsdp')), may hold values from -0.109375 to 0.109375
- conv_params: bfloat16 [5, 3328], P(None, ('dp', 'fsdp')), may hold values from -3 to 3
- norm_gain: bfloat16 [1536], P(('dp', 'fsdp')), may hold values from 0.5 to 1.5
- gate_gain: bfloat16 [3072], P(('dp', 'fsdp')), may hold values from 0.5 to 1.5
- head_params: float32 [3, 48], replicated, may hold values from -7 to 3, as said below
Outputs:
- output: bfloat16 [32768, 1536], P(('dp', 'fsdp'))
- grad_input: bfloat16 [32768, 1536], P(('dp', 'fsdp'))
- grad_w_zx: float32 [1536, 6144], P(('dp', 'fsdp'))
- grad_w_bc: float32 [1536, 256], P(('dp', 'fsdp'))
- grad_w_dt: float32 [1536, 48], P(('dp', 'fsdp'))
- grad_w_out: float32 [3072, 1536], P(('dp', 'fsdp'))
- grad_conv: float32 [5, 3328], P(None, ('dp', 'fsdp'))
- grad_norm_gain: float32 [1536], P(('dp', 'fsdp'))
- grad_gate_gain: float32 [3072], P(('dp', 'fsdp'))
- grad_heads: float32 [3, 48], replicated
The draws below stay inside these ranges and needn't reach their ends.
Inputs may be any that keep to these rules, and one draw needn't show every extreme that they name: `segment_ids`: ids never fall along the array and a new id begins at every multiple of 512 positions. The first block of 512 positions holds one sequence that fills it; every other block holds exactly 3 sequences of uneven lengths, whose boundaries fall anywhere inside the block, so the largest id is 189. `head_params`: row 0 is the log of a positive decay rate, row 1 a step bias, row 2 a skip weight.
All inputs are finite; a program needn't handle non-finite values.
Results may differ from the reference program's by a relative error of at most 0.012.
Values may be sent and summed in bfloat16 or wider, within the bound.
A program may use at most 448 MiB of HBM per device.

```python
import math
import jax
import jax.numpy as jnp
from jax import lax

D = 1536
H = 48
N = 128
K = 4
GROUP = 256
SLOT = 512
E = 3072
TOKENS = 32768


def draw_segment_ids(key, part):
    blocks = TOKENS // SLOT
    scores = jax.random.randint(key, (blocks, SLOT - 1), 0, 65536) * SLOT + jnp.arange(1, SLOT)[None, :]
    second = jnp.sort(scores, axis=1)[:, 1:2]
    extra = (scores <= second) & (jnp.arange(blocks)[:, None] > 0)
    starts = jnp.concatenate([jnp.ones((blocks, 1), jnp.int32), extra.astype(jnp.int32)], axis=1)
    return (jnp.cumsum(starts.reshape(TOKENS)) - 1).astype(jnp.int32)


def draw_head_params(key, part):
    first_key, second_key, third_key = jax.random.split(key, 3)
    a_log = jnp.log(jax.random.uniform(first_key, (H,), jnp.float32, 1.0, 16.0))
    step_size = jnp.exp(jax.random.uniform(second_key, (H,), jnp.float32, math.log(0.001), math.log(0.1)))
    step_bias = step_size + jnp.log(-jnp.expm1(-step_size))
    skip_weight = jax.random.uniform(third_key, (H,), jnp.float32, 0.5, 1.5)
    return jnp.stack([a_log, step_bias, skip_weight]).astype(jnp.float32)


def raised(array, own_key, source, target, blocks, factor):
    def block_of(position):
        return (jnp.arange(array.shape[position]) // (array.shape[position] // blocks)).reshape((-1,) + (1,) * (array.ndim - 1 - position))

    first = jax.random.permutation(own_key, blocks)[block_of(target)]
    far = (block_of(target) + blocks // 2) % blocks
    return jnp.where((block_of(source) == first) | (block_of(source) == far), factor * array, array)


def block_scale(rng, shape, cuts, smallest, top_value):
    level = 1.0
    for axis_at, shards_of in cuts:
        draws = jax.random.uniform(jax.random.fold_in(jax.random.fold_in(rng, 6), axis_at), (shards_of,), jnp.float32, smallest / len(cuts), top_value / len(cuts))
        level = level * jnp.repeat(jnp.exp(draws), shape[axis_at] // shards_of).reshape((-1,) + (1,) * (len(shape) - 1 - axis_at))
    return level


def bell_draw(rng, shape, scale, bound, shards=(), kind=jnp.bfloat16):
    result = scale * jax.random.normal(rng, shape, jnp.float32)
    if shards:
        result = result * block_scale(rng, shape, shards, -0.22, 0.18)
    return jnp.clip(result, -bound, bound).astype(kind)


def gaussian_with(rng, extent, scale, most, cuts, heavy, held_as=jnp.bfloat16):
    values = scale * jax.random.normal(rng, extent, jnp.float32)
    if cuts:
        values = values * block_scale(rng, extent, cuts, -0.22, 0.18)
    return jnp.clip(raised(values, jax.random.fold_in(rng, 3), *heavy), -most, most).astype(held_as)


def setup_inputs(seed: int = 0) -> dict:
    arg_keys = jax.random.split(jax.random.key(seed), 12)
    hidden = gaussian_with(arg_keys[0], (TOKENS, D), 1.0, 6.0, ((0, 32),), (0, 1, 32, 2.75))
    grad_out = bell_draw(arg_keys[1], (TOKENS, D), 1.0, 6.0, ((0, 32),))
    segment_ids = draw_segment_ids(jax.random.fold_in(arg_keys[11], 71), 0)
    w_zx = bell_draw(arg_keys[3], (D, 2 * E), D ** -0.5, 0.15625, ((0, 32),))
    w_bc = bell_draw(arg_keys[4], (D, 2 * N), D ** -0.5, 0.15625, ((0, 32),))
    w_dt = bell_draw(arg_keys[5], (D, H), D ** -0.5, 0.15625, ((0, 32),))
    w_out = bell_draw(arg_keys[6], (E, D), E ** -0.5, 0.109375, ((0, 32),))
    conv_params = bell_draw(arg_keys[7], (K + 1, E + 2 * N), K ** -0.5, 3.0, ((1, 32),))
    norm_gain = jnp.clip(1.0 + 0.1 * jax.random.normal(arg_keys[8], (D,), jnp.float32), 0.5, 1.5).astype(jnp.bfloat16)
    gate_gain = jnp.clip(1.0 + 0.1 * jax.random.normal(arg_keys[9], (E,), jnp.float32), 0.5, 1.5).astype(jnp.bfloat16)
    head_params = draw_head_params(jax.random.fold_in(arg_keys[11], 71), 0)
    return {"hidden": hidden, "grad_out": grad_out, "segment_ids": segment_ids, "w_zx": w_zx, "w_bc": w_bc, "w_dt": w_dt, "w_out": w_out, "conv_params": conv_params, "norm_gain": norm_gain, "gate_gain": gate_gain, "head_params": head_params}


EPS = 1e-05
HIGHEST = lax.Precision.HIGHEST

def pre_norm(rows, gain):
    return rows * lax.rsqrt(lax.optimization_barrier(jnp.mean(rows * rows, axis=-1, keepdims=True)) + EPS) * gain

def causal_conv(signal, taps_bias, seg):
    width_taps = taps_bias.shape[0] - 1
    length = signal.shape[0]
    summed = taps_bias[width_taps] + taps_bias[width_taps - 1] * signal
    for offset in range(1, width_taps):
        moved = jnp.pad(signal, ((offset, 0), (0, 0)))[:length]
        earlier = jnp.pad(seg, (offset, 0), constant_values=-1)[:length]
        summed = summed + taps_bias[width_taps - 1 - offset] * jnp.where((earlier == seg)[:, None], moved, 0.0)
    return summed

def group_step(carried, sliced):
    head_x, b_rows, c_rows, step_sizes, decays, seg_rows, prev_id = sliced
    cumul = jnp.cumsum(decays, axis=0)
    length = seg_rows.shape[0]
    places = jnp.arange(length)
    allowed = (places[:, None] >= places[None, :]) & (seg_rows[:, None] == seg_rows[None, :])
    cumul_t = cumul.T
    spread = cumul_t[:, :, None] - cumul_t[:, None, :]
    within = jnp.where(allowed[None], jnp.exp(jnp.where(allowed[None], spread, 0.0)), 0.0)
    scores = jnp.einsum('in,jn->ij', c_rows, b_rows, precision=HIGHEST)
    mixing = within * scores[None] * step_sizes.T[:, None, :]
    inner = jnp.einsum('hij,jhp->ihp', mixing, head_x, precision=HIGHEST)
    entering = jnp.where((seg_rows == prev_id)[:, None], jnp.exp(cumul), 0.0)
    outer = jnp.einsum('in,hpn->ihp', c_rows, carried, precision=HIGHEST) * entering[:, :, None]
    leaving = jnp.where((seg_rows == seg_rows[-1])[:, None], jnp.exp(cumul[-1][None, :] - cumul), 0.0) * step_sizes
    kept_part = jnp.where(seg_rows[-1] == prev_id, jnp.exp(cumul[-1]), 0.0)
    updated = carried * kept_part[:, None, None] + jnp.einsum('jh,jhp,jn->hpn', leaving, head_x, b_rows, precision=HIGHEST)
    return (updated, inner + outer)

def mixer(zx_part, bc_part, dt_part, conv_part, heads, gate_scale, seg):
    width = gate_scale.shape[0]
    head_count = heads.shape[1]
    head_size = width // head_count
    state_size = bc_part.shape[1] // 2
    length = zx_part.shape[0]
    gate_part = zx_part[:, :width]
    joined = jnp.concatenate([zx_part[:, width:], bc_part], axis=1)
    activated = jax.nn.silu(causal_conv(joined, conv_part, seg))
    head_x = activated[:, :width].reshape(length, head_count, head_size)
    b_rows = activated[:, width:width + state_size]
    c_rows = activated[:, width + state_size:]
    step_sizes = jax.nn.softplus(dt_part + heads[1])
    decays = -jnp.exp(heads[0]) * step_sizes
    blocks = length // GROUP
    prev_ids = jnp.concatenate([jnp.full((1,), -1, jnp.int32), seg[GROUP - 1:length - 1:GROUP].astype(jnp.int32)])
    initial = jnp.zeros((head_count, head_size, state_size), head_x.dtype)
    sliced = (head_x.reshape(blocks, GROUP, head_count, head_size), b_rows.reshape(blocks, GROUP, state_size), c_rows.reshape(blocks, GROUP, state_size), step_sizes.reshape(blocks, GROUP, head_count), decays.reshape(blocks, GROUP, head_count), seg.reshape(blocks, GROUP), prev_ids)
    final_state, scanned = lax.scan(jax.checkpoint(group_step), initial, sliced)
    scan_y = scanned.reshape(length, head_count, head_size) + heads[2][None, :, None] * head_x
    gated = scan_y.reshape(length, width) * jax.nn.silu(gate_part)
    return gated * lax.rsqrt(lax.optimization_barrier(jnp.mean(gated * gated, axis=-1, keepdims=True)) + EPS) * gate_scale

def layer_forward(rows, seg, weights, heads):
    w_zx, w_bc, w_dt, w_out, conv_params, norm_gain, gate_gain = weights
    rows_f = rows.astype(jnp.float32)
    normed, norm_back = jax.vjp(pre_norm, rows_f, norm_gain.astype(jnp.float32))
    normed_bf = normed.astype(jnp.bfloat16)
    zx_bf = lax.optimization_barrier(jnp.dot(normed_bf, w_zx, preferred_element_type=jnp.float32).astype(jnp.bfloat16))
    bc_bf = lax.optimization_barrier(jnp.dot(normed_bf, w_bc, preferred_element_type=jnp.float32).astype(jnp.bfloat16))
    dt_bf = lax.optimization_barrier(jnp.dot(normed_bf, w_dt, preferred_element_type=jnp.float32).astype(jnp.bfloat16))

    def local_mixer(zx_part, bc_part, dt_part, conv_part, head_part, gate_scale):
        return mixer(zx_part, bc_part, dt_part, conv_part, head_part, gate_scale, seg)
    mixed, mixer_back = jax.vjp(local_mixer, zx_bf.astype(jnp.float32), bc_bf.astype(jnp.float32), dt_bf.astype(jnp.float32), conv_params.astype(jnp.float32), heads, gate_gain.astype(jnp.float32))
    mixed_bf = mixed.astype(jnp.bfloat16)
    output = (rows_f + jnp.dot(mixed_bf, w_out, preferred_element_type=jnp.float32)).astype(jnp.bfloat16)
    return (output, (normed_bf, mixed_bf, norm_back, mixer_back))

def layer_backward(cotangent, saved, weights):
    w_zx, w_bc, w_dt, w_out, conv_params, norm_gain, gate_gain = weights
    normed_bf, mixed_bf, norm_back, mixer_back = saved
    back_mixed = jnp.dot(cotangent, w_out.T, preferred_element_type=jnp.float32)
    grad_out_w = jnp.dot(mixed_bf.T, cotangent, preferred_element_type=jnp.float32)
    d_zx, d_bc, d_dt, d_conv, d_heads, d_gate = mixer_back(back_mixed)
    d_zx_bf = d_zx.astype(jnp.bfloat16)
    d_bc_bf = d_bc.astype(jnp.bfloat16)
    d_dt_bf = d_dt.astype(jnp.bfloat16)
    grad_zx = jnp.dot(normed_bf.T, d_zx_bf, preferred_element_type=jnp.float32)
    grad_bc = jnp.dot(normed_bf.T, d_bc_bf, preferred_element_type=jnp.float32)
    grad_dt = jnp.dot(normed_bf.T, d_dt_bf, preferred_element_type=jnp.float32)
    back_normed = jnp.dot(d_zx_bf, w_zx.T, preferred_element_type=jnp.float32)
    back_normed = back_normed + jnp.dot(d_bc_bf, w_bc.T, preferred_element_type=jnp.float32)
    back_normed = back_normed + jnp.dot(d_dt_bf, w_dt.T, preferred_element_type=jnp.float32)
    d_rows, d_norm = norm_back(back_normed)
    grad_in = (cotangent.astype(jnp.float32) + d_rows).astype(jnp.bfloat16)
    return (grad_in, (grad_zx, grad_bc, grad_dt, grad_out_w, d_conv, d_norm, d_gate), d_heads)

def reference(hidden, grad_out, segment_ids, w_zx, w_bc, w_dt, w_out, conv_params, norm_gain, gate_gain, head_params):
    weights = (w_zx, w_bc, w_dt, w_out, conv_params, norm_gain, gate_gain)
    count = hidden.shape[0] // SLOT
    rows_all = hidden.reshape(count, SLOT, hidden.shape[1])
    cot_all = grad_out.reshape(count, SLOT, hidden.shape[1])
    seg_all = segment_ids.reshape(count, SLOT)
    starting = tuple((jnp.zeros(weight.shape, jnp.float32) for weight in weights))

    def one_block(carried, sliced):
        sums, head_sum = carried
        output, saved = layer_forward(sliced[0], sliced[2], weights, head_params)
        grad_in, grads, head_grad = layer_backward(sliced[1], saved, weights)
        return ((jax.tree.map(jnp.add, sums, grads), head_sum + head_grad), (output, grad_in))
    (sums, head_sum), (outputs, grad_ins) = lax.scan(one_block, (starting, jnp.zeros(head_params.shape, jnp.float32)), (rows_all, cot_all, seg_all))
    return (outputs.reshape(hidden.shape), grad_ins.reshape(hidden.shape), sums[0], sums[1], sums[2], sums[3], sums[4], sums[5], sums[6], head_sum)
```

```python
import functools
import jax
import jax.numpy as jnp
from jax import lax
from jax.experimental import pallas as pl
from jax.experimental.pallas import tpu as pltpu
from jax.sharding import PartitionSpec as P

EPS = 1e-05
L = 128
HG = 4
LOG2E = 1.4426950408889634
bf16, f32 = jnp.bfloat16, jnp.float32
HIGHEST = lax.Precision.HIGHEST


def dot(a, b, dims=((1,), (0,)), precision=None):
    return lax.dot_general(a, b, (dims, ((), ())), preferred_element_type=f32, precision=precision)


def sigmoid(x):
    return 1.0 / (1.0 + jnp.exp(-x))


def conv_rows(ext, taps, masks, halo):
    rows = ext.shape[0] - halo
    width = 4
    v = ext[halo:]
    out = taps[4:5] + taps[3:4] * v
    for k in range(1, width):
        moved = pltpu.roll(ext, k, 0)[halo:]
        out = out + (taps[3 - k : 4 - k] * masks[:, k : k + 1]) * moved
    return out


def prep_kernel(bcdt_ref, taps_ref, heads_ref, m_ref, segc_ref, segr_ref,
                b_ref, c_ref, bt_ref, ct_ref, pre_ref, gm_ref, cum4_ref, cumr_ref, sc_ref, dt_ref):
    T = bcdt_ref.shape[0]
    nc = T // L
    N = b_ref.shape[1]
    H = dt_ref.shape[1]
    groups = cum4_ref.shape[0]
    taps = taps_ref[...]
    tri = (lax.broadcasted_iota(jnp.int32, (L, L), 0) >= lax.broadcasted_iota(jnp.int32, (L, L), 1))
    trif = tri.astype(f32)
    neg_rate = -jnp.exp(heads_ref[0:1, :H]) * LOG2E
    bias = heads_ref[1:2, :H]

    def chunk(c, carry):
        t0 = pl.multiple_of(c * L, L)
        here = pl.ds(t0, L)
        h0 = pl.multiple_of(jnp.maximum(t0 - 16, 0), 16)
        before = bcdt_ref[pl.ds(h0, 16), : 2 * N].astype(f32)
        v = bcdt_ref[here, : 2 * N].astype(f32)
        pre = conv_rows(jnp.concatenate([before, v], axis=0), taps, m_ref[here, :], 16)
        pre_ref[here, :] = pre
        act = pre * sigmoid(pre)
        b = act[:, :N]
        cc = act[:, N:]
        bb = b.astype(bf16)
        cb = cc.astype(bf16)
        b_ref[here, :] = bb
        c_ref[here, :] = cb
        bt_ref[:, here] = b.T.astype(bf16)
        ct_ref[:, here] = cc.T.astype(bf16)
        segc = segc_ref[here, 0:1]
        prev = segc_ref[here, 1:2]
        last = segc_ref[here, 2:3]
        same = segc == segr_ref[:, here]
        g = dot(cb, bb, ((1,), (1,)))
        gm_ref[pl.ds(c, 1)] = jnp.where(tri & same, g, 0.0)[None]
        raw = bcdt_ref[here, 2 * N : 2 * N + 128].astype(f32)[:, :H] + bias
        dt = jnp.maximum(raw, 0.0) + jnp.log1p(jnp.exp(-jnp.abs(raw)))
        a2 = neg_rate * dt
        cum = dot(trif, a2, precision=HIGHEST)
        end = cum[L - 1 : L]
        ein = jnp.where(segc == prev, jnp.exp2(cum), 0.0)
        lv = jnp.where(segc == last, jnp.exp2(end - cum), 0.0)
        dt_ref[here, :] = dt
        cumt = cum.T
        s0 = pl.multiple_of(c * (3 * L), L)
        for k in range(groups):
            cols = slice(HG * k, HG * (k + 1))
            cum4_ref[k, here, :] = cum[:, cols]
            cumr_ref[k, :, here] = cumt[cols]
            sc_ref[k, pl.ds(s0, L), :] = dt[:, cols].astype(bf16)
            sc_ref[k, pl.ds(s0 + L, L), :] = ein[:, cols].astype(bf16)
            sc_ref[k, pl.ds(s0 + 2 * L, L), :] = lv[:, cols].astype(bf16)
        return carry

    lax.fori_loop(0, nc, chunk, 0)


def prep(bcdt, taps, heads, masks, segc, segr, N, H):
    T = bcdt.shape[0]
    nc = T // L
    G = H // HG
    S = jax.ShapeDtypeStruct
    return pl.pallas_call(
        prep_kernel,
        out_shape=(S((T, N), bf16), S((T, N), bf16), S((N, T), bf16), S((N, T), bf16), S((T, 2 * N), f32),
                   S((nc, L, L), f32), S((G, T, HG), f32), S((G, HG, T), f32), S((G, 3 * T, HG), bf16), S((T, H), f32)),
        compiler_params=pltpu.CompilerParams(vmem_limit_bytes=60 << 20),
    )(bcdt, taps, heads, masks, segc, segr)


def lane_onehot(width, per):
    return (lax.broadcasted_iota(jnp.int32, (HG, width), 1) // per == lax.broadcasted_iota(jnp.int32, (HG, width), 0)).astype(bf16)


def half_masks(P):
    lane = lax.broadcasted_iota(jnp.int32, (1, 2 * P), 1)
    first = (lane < P).astype(f32)
    return first.astype(bf16), (1.0 - first).astype(bf16)


def decay(cum4, cumr, k):
    return jnp.exp2(jnp.minimum(cum4[:, k : k + 1] - cumr[k : k + 1, :], 0.0))


def fwd_kernel(u_ref, gate_ref, taps_ref, m_ref, b_ref, c_ref, bt_ref, gm_ref, cum4_ref, cumr_ref, sc_ref,
               gg_ref, ssq_ref, pre_ref, st_ref, state):
    T, W = u_ref.shape
    P = W // HG
    nc = T // L
    step = pl.program_id(0)
    taps = taps_ref[...]
    gain = taps[5:6]
    skip = taps[6:7]
    onehot = lane_onehot(W, P)
    ma, mb = half_masks(P)
    state[...] = jnp.zeros_like(state)

    @pl.when(step == 0)
    def _():
        ssq_ref[...] = jnp.zeros_like(ssq_ref)

    def chunk(c, carry):
        t0 = pl.multiple_of(c * L, L)
        here = pl.ds(t0, L)
        h0 = pl.multiple_of(jnp.maximum(t0 - 16, 0), 16)
        ext = jnp.concatenate([u_ref[pl.ds(h0, 16), :], u_ref[here, :]], axis=0).astype(f32)
        pre = conv_rows(ext, taps, m_ref[here, :], 16)
        pre_ref[here, :] = pre.astype(bf16)
        x = pre * sigmoid(pre)
        s0 = pl.multiple_of(c * (3 * L), L)
        exp = dot(sc_ref[0, pl.ds(s0, 3 * L), :], onehot)
        dtx, einx, lvx = exp[:L], exp[L : 2 * L], exp[2 * L :]
        xd = x * dtx
        xdb = xd.astype(bf16)
        gm = gm_ref[c]
        cum4 = cum4_ref[0, here, :]
        cumr = cumr_ref[0, :, here]
        sb = state[...].astype(bf16)
        st_ref[c] = sb
        inner = []
        for p in range(HG // 2):
            m0 = (decay(cum4, cumr, 2 * p) * gm).astype(bf16)
            m1 = (decay(cum4, cumr, 2 * p + 1) * gm).astype(bf16)
            xp = xdb[:, 2 * P * p : 2 * P * (p + 1)]
            inner.append(dot(jnp.concatenate([m0, m1], axis=1), jnp.concatenate([xp * ma, xp * mb], axis=0)))
        y = jnp.concatenate(inner, axis=1) + dot(c_ref[here, :], sb) * einx + skip * x
        state[...] = state[...] * einx[L - 1 : L] + dot(bt_ref[:, here], (xd * lvx).astype(bf16))
        gate = gate_ref[here, :].astype(f32)
        g = y * (gate * sigmoid(gate))
        gg_ref[here, :] = (g * gain).astype(bf16)
        g2 = g * g
        tot = g2[:, :128]
        for j in range(1, W // 128):
            tot = tot + g2[:, 128 * j : 128 * (j + 1)]
        ssq_ref[here, :] += tot
        return carry

    lax.fori_loop(0, nc, chunk, 0)


def fwd(zx, taps, masks, b, c, bt, gm, cum4, cumr, sc):
    T = zx.shape[0]
    E = zx.shape[1] // 2
    N = b.shape[1]
    G = cum4.shape[0]
    W = E // G
    nc = T // L
    S = jax.ShapeDtypeStruct
    col = lambda off: pl.BlockSpec((T, W), lambda g: (0, g + off))
    full = lambda a: pl.BlockSpec(a.shape, lambda g: (0,) * a.ndim)
    grp = lambda a: pl.BlockSpec((1,) + a.shape[1:], lambda g: (g, 0, 0))
    return pl.pallas_call(
        fwd_kernel,
        grid=(G,),
        in_specs=[col(G), col(0), pl.BlockSpec((8, W), lambda g: (0, g)), full(masks), full(b), full(c), full(bt), full(gm),
                  grp(cum4), grp(cumr), grp(sc)],
        out_specs=[col(0), pl.BlockSpec((T, 128), lambda g: (0, 0)), col(0), pl.BlockSpec((nc, N, W), lambda g: (0, 0, g))],
        out_shape=(S((T, E), bf16), S((T, 128), f32), S((T, E), bf16), S((nc, N, E), bf16)),
        scratch_shapes=[pltpu.VMEM((N, W), f32)],
        compiler_params=pltpu.CompilerParams(vmem_limit_bytes=60 << 20),
        cost_estimate=pl.CostEstimate(flops=T * E * (2 * L + 4 * N) * 2, bytes_accessed=T * E * 12, transcendentals=T * E * 4),
    )(zx, zx, taps, masks, b, c, bt, gm, cum4, cumr, sc)


def bwd_kernel(u_ref, gate_ref, pre_ref, dm_ref, rq_ref, taps_ref, m_ref, b_ref, c_ref, ct_ref, gm_ref, cum4_ref, cumr_ref, sc_ref, st_ref,
               du_ref, dgate_ref, dg_ref, db_ref, dc_ref, rs_ref, small_ref, kk_ref, ds, nxt, acc):
    T, W = u_ref.shape
    P = W // HG
    nc = T // L
    step = pl.program_id(0)
    taps = taps_ref[...]
    gain = taps[5:6]
    skip = taps[6:7]
    onehot = lane_onehot(W, P)
    ma, mb = half_masks(P)
    ds[...] = jnp.zeros_like(ds)
    nxt[...] = jnp.zeros_like(nxt)
    acc[...] = jnp.zeros_like(acc)

    @pl.when(step == 0)
    def _():
        dg_ref[...] = jnp.zeros_like(dg_ref)
        db_ref[...] = jnp.zeros_like(db_ref)
        dc_ref[...] = jnp.zeros_like(dc_ref)

    ri = lax.broadcasted_iota(jnp.int32, (4 * W, 16), 0)
    ci = lax.broadcasted_iota(jnp.int32, (4 * W, 16), 1)
    part = ri // W
    want = jnp.maximum(part - 1, 0) * HG + (ri % W) // P
    fold = (want == ci).astype(bf16)

    def eight(z):
        return jnp.sum(z.reshape(L // 8, 8, W), axis=0)

    def chunk(i, carry):
        c = nc - 1 - i
        t0 = pl.multiple_of(c * L, L)
        here = pl.ds(t0, L)
        u = u_ref[here, :].astype(f32)
        pre = pre_ref[here, :].astype(f32)
        sig = sigmoid(pre)
        x = pre * sig
        dsilu = sig + x * (1.0 - sig)
        s0 = pl.multiple_of(c * (3 * L), L)
        exp = dot(sc_ref[0, pl.ds(s0, 3 * L), :], onehot)
        dtx, einx, lvx = exp[:L], exp[L : 2 * L], exp[2 * L :]
        xdb = (x * dtx).astype(bf16)
        xd = xdb.astype(f32)
        gm = gm_ref[c]
        cum4 = cum4_ref[0, here, :]
        cumr = cumr_ref[0, :, here]
        sb = st_ref[c]
        es, ms, inner = [], [], []
        for p in range(HG // 2):
            e0 = decay(cum4, cumr, 2 * p)
            e1 = decay(cum4, cumr, 2 * p + 1)
            m0 = (e0 * gm).astype(bf16)
            m1 = (e1 * gm).astype(bf16)
            xp = xdb[:, 2 * P * p : 2 * P * (p + 1)]
            inner.append(dot(jnp.concatenate([m0, m1], axis=1), jnp.concatenate([xp * ma, xp * mb], axis=0)))
            es.append((e0, e1))
            ms.append((m0, m1))
        yn = jnp.concatenate(inner, axis=1) + dot(c_ref[here, :], sb) * einx
        y = yn + skip * x
        gate = gate_ref[here, :].astype(f32)
        sgate = sigmoid(gate)
        silu_g = gate * sgate
        g = y * silu_g
        r = rq_ref[here, 0:1]
        q = rq_ref[here, 1:2]
        dmr = dm_ref[here, :].astype(f32) * r
        dgg = gain * dmr - g * q
        dyb = (dgg * silu_g).astype(bf16)
        dy = dyb.astype(f32)
        dgate_ref[here, :] = (dgg * y * (sgate + silu_g * (1.0 - sgate))).astype(bf16)
        dxi = []
        dgc = dg_ref[c]
        for p in range(HG // 2):
            cols = slice(2 * P * p, 2 * P * (p + 1))
            dp = dyb[:, cols]
            dstack = jnp.concatenate([dp * ma, dp * mb], axis=0)
            dmm = dot(dstack, xdb[:, cols], ((1,), (1,)))
            dgc = dgc + dmm[:L] * es[p][0] + dmm[L:] * es[p][1]
            dxi.append(dot(jnp.concatenate(ms[p], axis=0), dstack, ((0,), (0,))))
        dg_ref[c] = dgc
        dxi = jnp.concatenate(dxi, axis=1)
        dsn = ds[...]
        dsb = dsn.astype(bf16)
        dye = (dy * einx).astype(bf16)
        dc_ref[here, :] += dot(dye, sb, ((1,), (1,)))
        kept = einx[L - 1 : L]
        kk_ref[pl.ds(c, 1), :] = kept * jnp.sum(sb.astype(f32) * dsn, axis=0, keepdims=True)
        db_ref[here, :] += dot((xd * lvx).astype(bf16), dsb, ((1,), (1,)))
        dxe = dot(b_ref[here, :], dsb) * lvx
        ds[...] = dsn * kept + dot(ct_ref[:, here], dye)
        dxd = dxi + dxe
        r1 = dy * yn - xd * dxi
        r1h = r1.astype(bf16)
        r1l = (r1 - r1h.astype(f32)).astype(bf16)
        rs_ref[0, here, :] = dot(jnp.concatenate([r1h, r1l, (xd * dxe).astype(bf16), (x * dxd).astype(bf16)], axis=1), fold)
        dpre = (dxd * dtx + skip * dy) * dsilu
        ext = jnp.concatenate([dpre, nxt[...]], axis=0)
        nxt[...] = dpre[:8]
        du = taps[3:4] * dpre
        acc[0:8, :] += eight(dmr * g)
        acc[8:16, :] += eight(dy * x)
        acc[16:24, :] += eight(dpre)
        acc[24:32, :] += eight(dpre * u)
        mrows = m_ref[pl.ds(t0, L + 8), :]
        for k in range(1, 4):
            sk = pltpu.roll(ext * mrows[:, k : k + 1], L + 8 - k, 0)[:L]
            du = du + taps[3 - k : 4 - k] * sk
            acc[24 + 8 * k : 32 + 8 * k, :] += eight(sk * u)
        du_ref[here, :] = du.astype(bf16)
        return carry

    lax.fori_loop(0, nc, chunk, 0)
    for j in range(7):
        small_ref[j : j + 1, :] = jnp.sum(acc[8 * j : 8 * j + 8, :], axis=0, keepdims=True)
    small_ref[7:8, :] = jnp.zeros((1, W), f32)


def bwd(zx, pre, dm, rq, taps, masks, b, c, ct, gm, cum4, cumr, sc, st):
    T = zx.shape[0]
    E = zx.shape[1] // 2
    N = b.shape[1]
    G = cum4.shape[0]
    W = E // G
    nc = T // L
    S = jax.ShapeDtypeStruct
    col = lambda off: pl.BlockSpec((T, W), lambda g: (0, g + off))
    full = lambda a: pl.BlockSpec(a.shape, lambda g: (0,) * a.ndim)
    whole = lambda s: pl.BlockSpec(s, lambda g: (0,) * len(s))
    grp = lambda a: pl.BlockSpec((1,) + a.shape[1:], lambda g: (g, 0, 0))
    masks = jnp.pad(masks, ((0, 8), (0, 0)))
    return pl.pallas_call(
        bwd_kernel,
        grid=(G,),
        in_specs=[col(G), col(0), col(0), col(0), full(rq), pl.BlockSpec((8, W), lambda g: (0, g)), full(masks), full(b), full(c),
                  full(ct), full(gm), grp(cum4), grp(cumr), grp(sc), pl.BlockSpec((nc, N, W), lambda g: (0, 0, g))],
        out_specs=[col(0), col(0), whole((nc, L, L)), whole((T, N)), whole((T, N)), pl.BlockSpec((1, T, 16), lambda g: (g, 0, 0)),
                   pl.BlockSpec((8, W), lambda g: (0, g)), pl.BlockSpec((nc, W), lambda g: (0, g))],
        out_shape=(S((T, E), bf16), S((T, E), bf16), S((nc, L, L), f32), S((T, N), f32), S((T, N), f32), S((G, T, 16), f32),
                   S((8, E), f32), S((nc, E), f32)),
        scratch_shapes=[pltpu.VMEM((N, W), f32), pltpu.VMEM((8, W), f32), pltpu.VMEM((56, W), f32)],
        compiler_params=pltpu.CompilerParams(vmem_limit_bytes=60 << 20),
        cost_estimate=pl.CostEstimate(flops=T * E * (8 * L + 12 * N), bytes_accessed=T * E * 16, transcendentals=T * E * 4),
    )(zx, zx, pre, dm, rq, taps, masks, b, c, ct, gm, cum4, cumr, sc, st)


def post_kernel(bcdt_ref, pre_ref, taps_ref, heads_ref, m_ref, segc_ref, segr_ref, b_ref, c_ref, dg_ref, db_ref, dc_ref, rs_ref, kk_ref, dt_ref,
                out_ref, small_ref, hs_ref, nxt, acc, hacc):
    T = bcdt_ref.shape[0]
    nc = T // L
    N = b_ref.shape[1]
    H = dt_ref.shape[1]
    G = H // HG
    taps = taps_ref[...]
    tri = (lax.broadcasted_iota(jnp.int32, (L, L), 0) >= lax.broadcasted_iota(jnp.int32, (L, L), 1))
    upper = (lax.broadcasted_iota(jnp.int32, (L, L), 0) <= lax.broadcasted_iota(jnp.int32, (L, L), 1)).astype(f32)
    strict = 1.0 - upper
    rate = -jnp.exp(heads_ref[0:1, :H])
    bias = heads_ref[1:2, :H]
    nxt[...] = jnp.zeros_like(nxt)
    acc[...] = jnp.zeros_like(acc)
    hacc[...] = jnp.zeros_like(hacc)

    def eight(z):
        return jnp.sum(z.reshape(L // 8, 8, z.shape[1]), axis=0)

    def chunk(i, carry):
        c = nc - 1 - i
        t0 = pl.multiple_of(c * L, L)
        here = pl.ds(t0, L)
        same = segc_ref[here, 0:1] == segr_ref[:, here]
        dg = jnp.where(tri & same, dg_ref[c], 0.0)
        dgb = dg.astype(bf16)
        dcv = dc_ref[here, :] + dot(dgb, b_ref[here, :])
        dbv = db_ref[here, :] + dot(dg.T.astype(bf16), c_ref[here, :])
        pre = pre_ref[here, :]
        sig = sigmoid(pre)
        dpre = jnp.concatenate([dbv, dcv], axis=1) * (sig + pre * sig * (1.0 - sig))
        v = bcdt_ref[here, : 2 * N].astype(f32)
        ext = jnp.concatenate([dpre, nxt[...]], axis=0)
        nxt[...] = dpre[:8]
        dv = taps[3:4] * dpre
        acc[0:8, :] += eight(dpre)
        acc[8:16, :] += eight(dpre * v)
        mrows = m_ref[pl.ds(t0, L + 8), :]
        for k in range(1, 4):
            sk = pltpu.roll(ext * mrows[:, k : k + 1], L + 8 - k, 0)[:L]
            dv = dv + taps[3 - k : 4 - k] * sk
            acc[8 + 8 * k : 16 + 8 * k, :] += eight(sk * v)
        out_ref[here, : 2 * N] = dv.astype(bf16)
        r1 = jnp.concatenate([rs_ref[k, here, 0:HG] for k in range(G)], axis=1)
        r2 = jnp.concatenate([rs_ref[k, here, HG : 2 * HG] for k in range(G)], axis=1)
        r3 = jnp.concatenate([rs_ref[k, here, 2 * HG : 3 * HG] for k in range(G)], axis=1)
        da = dot(upper, r1, precision=HIGHEST) + dot(strict, r2, precision=HIGHEST) + kk_ref[pl.ds(c, 1), :]
        dt = dt_ref[here, :]
        raw = bcdt_ref[here, 2 * N : 2 * N + 128].astype(f32)[:, :H] + bias
        ddt = (r3 + da * rate) * sigmoid(raw)
        hacc[0:8, :] += eight(da * rate * dt)
        hacc[8:16, :] += eight(ddt)
        out_ref[here, 2 * N :] = jnp.concatenate([ddt, jnp.zeros((L, out_ref.shape[1] - 2 * N - H), f32)], axis=1).astype(bf16)
        return carry

    lax.fori_loop(0, nc, chunk, 0)
    for j in range(5):
        small_ref[j : j + 1, :] = jnp.sum(acc[8 * j : 8 * j + 8, :], axis=0, keepdims=True)
    small_ref[5:8, :] = jnp.zeros((3, 2 * N), f32)
    for j in range(2):
        hs_ref[j : j + 1, :] = jnp.sum(hacc[8 * j : 8 * j + 8, :], axis=0, keepdims=True)


def post(bcdt, pre, taps, heads, masks, segc, segr, b, c, dg, db, dc, rs, kk, dt):
    T = bcdt.shape[0]
    N = b.shape[1]
    H = dt.shape[1]
    S = jax.ShapeDtypeStruct
    masks = jnp.pad(masks, ((0, 8), (0, 0)))
    return pl.pallas_call(
        post_kernel,
        out_shape=(S(bcdt.shape, bf16), S((8, 2 * N), f32), S((2, H), f32)),
        scratch_shapes=[pltpu.VMEM((8, 2 * N), f32), pltpu.VMEM((40, 2 * N), f32), pltpu.VMEM((16, H), f32)],
        compiler_params=pltpu.CompilerParams(vmem_limit_bytes=60 << 20),
    )(bcdt, pre, taps, heads, masks, segc, segr, b, c, dg, db, dc, rs, kk, dt)


def layer(hidden, grad_out, seg, w_zx, w_bcdt, w_out, conv, norm_gain, gate_gain, heads):
    T, D = hidden.shape
    E = w_out.shape[0]
    H = heads.shape[1]
    N = (conv.shape[1] - E) // 2
    rows = hidden.astype(f32)
    rinv = lax.rsqrt(jnp.mean(rows * rows, axis=-1, keepdims=True) + EPS)
    xhat = rows * rinv
    normed = (xhat * norm_gain).astype(bf16)
    zx = dot(normed, w_zx).astype(bf16)
    bcdt = dot(normed, w_bcdt).astype(bf16)
    pos = jnp.arange(T, dtype=jnp.int32)
    masks = jnp.stack([jnp.ones((T,), f32)] + [((jnp.roll(seg, k) == seg) & (pos >= k)).astype(f32) for k in range(1, 4)], axis=1)
    lastid = seg[L - 1 :: L]
    previd = jnp.concatenate([jnp.full((1,), -1, jnp.int32), lastid[:-1]])
    segc = jnp.stack([seg, jnp.repeat(previd, L), jnp.repeat(lastid, L)], axis=1)
    segr = seg[None, :]
    taps_u = jnp.concatenate([conv[:, :E], gate_gain[None], jnp.repeat(heads[2], E // H)[None], jnp.zeros((1, E), f32)], axis=0)
    taps_bc = jnp.concatenate([conv[:, E:], jnp.zeros((3, 2 * N), f32)], axis=0)
    heads_p = jnp.pad(heads, ((0, 5), (0, 128 - H)))
    b, c, bt, ct, pre_bc, gm, cum4, cumr, sc, dt = prep(bcdt, taps_bc, heads_p, masks, segc, segr, N, H)
    gg, ssq, pre, st = fwd(zx, taps_u, masks, b, c, bt, gm, cum4, cumr, sc)
    r = lax.rsqrt(jnp.sum(ssq, axis=1, keepdims=True) / E + EPS)
    output = (rows + r * dot(gg, w_out)).astype(bf16)
    dm = dot(grad_out, w_out, ((1,), (1,))).astype(bf16)
    gos = (grad_out.astype(f32) * r).astype(bf16)
    g_out = dot(gg, gos, ((0,), (0,))).astype(bf16)
    s = jnp.sum(gg.astype(f32) * dm.astype(f32), axis=1, keepdims=True)
    rq = jnp.concatenate([r, r * r * r * s / E], axis=1)
    du, dgate, dg, db, dc, rs, small, kk = bwd(zx, pre, dm, rq, taps_u, masks, b, c, ct, gm, cum4, cumr, sc, st)
    kkh = jnp.sum(kk.reshape(kk.shape[0], H, E // H), axis=2)
    dbcdt, small_bc, hs = post(bcdt, pre_bc, taps_bc, heads_p, masks, segc, segr, b, c, dg, db, dc, rs, kkh, dt)
    g_gate = dot(normed, dgate, ((0,), (0,))).astype(bf16)
    g_u = dot(normed, du, ((0,), (0,))).astype(bf16)
    g_bcdt = dot(normed, dbcdt, ((0,), (0,))).astype(bf16)
    bn = dot(dgate, w_zx[:, :E], ((1,), (1,))) + dot(du, w_zx[:, E:], ((1,), (1,))) + dot(dbcdt, w_bcdt, ((1,), (1,)))
    gb = bn * norm_gain
    d_rows = rinv * (gb - xhat * jnp.mean(gb * xhat, axis=-1, keepdims=True))
    grad_in = (grad_out.astype(f32) + d_rows).astype(bf16)
    d_norm = jnp.sum(bn * xhat, axis=0)
    d_conv_u = jnp.stack([small[6], small[5], small[4], small[3], small[2]])
    d_conv_bc = jnp.stack([small_bc[4], small_bc[3], small_bc[2], small_bc[1], small_bc[0]])
    d_conv = jnp.concatenate([d_conv_u, d_conv_bc], axis=1)
    d_heads = jnp.concatenate([hs, jnp.sum(small[1].reshape(1, H, E // H), axis=2)], axis=0)
    return output, grad_in, g_gate, g_u, g_bcdt, g_out, d_conv, d_norm, small[0], d_heads


AXES = ("dp", "fsdp")


def per_device(hidden, grad_out, segment_ids, w_zx, w_bc, w_dt, w_out, conv_params, norm_gain, gate_gain, head_params):
    n = lax.axis_size(AXES)
    E = w_out.shape[0] * n
    H = w_dt.shape[1]
    gather = lambda w, axis=0: lax.all_gather(w, AXES, axis=axis, tiled=True)
    scatter = lambda w, axis=0: lax.psum_scatter(w, AXES, scatter_dimension=axis, tiled=True)
    pad = 128 - H
    full_zx = gather(w_zx)
    full_bcdt = gather(jnp.concatenate([w_bc, w_dt, jnp.zeros((w_dt.shape[0], pad), bf16)], axis=1))
    full_out = gather(w_out)
    small = jnp.concatenate([conv_params.reshape(-1), norm_gain, gate_gain])
    smalls = gather(small[None])
    nc_, k1 = conv_params.shape[1], conv_params.shape[0]
    conv = smalls[:, : k1 * nc_].reshape(n, k1, nc_).transpose(1, 0, 2).reshape(k1, n * nc_).astype(f32)
    ng = smalls[:, k1 * nc_ : k1 * nc_ + norm_gain.shape[0]].reshape(-1).astype(f32)
    gg = smalls[:, k1 * nc_ + norm_gain.shape[0] :].reshape(-1).astype(f32)
    output, grad_in, g_gate, g_u, g_bcdt, g_out, d_conv, d_norm, d_gg, d_heads = layer(
        hidden, grad_out, segment_ids, full_zx, full_bcdt, full_out, conv, ng, gg, head_params)
    s_out = scatter(g_out).astype(f32)
    s_zx = scatter(jnp.concatenate([g_gate, g_u], axis=1)).astype(f32)
    s_bcdt = scatter(g_bcdt).astype(f32)
    rows = jnp.concatenate([d_conv.reshape(k1, n, nc_).transpose(1, 0, 2).reshape(n, -1), d_norm.reshape(n, -1), d_gg.reshape(n, -1)], axis=1)
    s_small = scatter(rows)[0]
    N2 = w_bc.shape[1]
    return (output, grad_in, s_zx, s_bcdt[:, :N2], s_bcdt[:, N2 : N2 + H], s_out, s_small[: k1 * nc_].reshape(k1, nc_),
            s_small[k1 * nc_ : k1 * nc_ + norm_gain.shape[0]], s_small[k1 * nc_ + norm_gain.shape[0] :], lax.psum(d_heads, AXES))


def solution(mesh):
    row, col, vec, rep = P(AXES, None), P(None, AXES), P(AXES), P()
    return jax.shard_map(
        per_device,
        mesh=mesh,
        in_specs=(row, row, vec, row, row, row, row, col, vec, vec, rep),
        out_specs=(row, row, row, row, row, row, col, vec, vec, rep),
        check_vma=False,
    )
```

```python
import functools
import jax
import jax.numpy as jnp
from jax import lax
from jax.experimental import pallas as pl
from jax.experimental.pallas import tpu as pltpu
from jax.sharding import PartitionSpec as P

EPS = 1e-05
L = 128
HG = 4
LOG2E = 1.4426950408889634
bf16, f32 = jnp.bfloat16, jnp.float32
HIGHEST = lax.Precision.HIGHEST


def dot(a, b, dims=((1,), (0,)), precision=None):
    return lax.dot_general(a, b, (dims, ((), ())), preferred_element_type=f32, precision=precision)


def sigmoid(x):
    return 1.0 / (1.0 + jnp.exp(-x))


def conv_rows(ext, taps, masks, halo):
    rows = ext.shape[0] - halo
    width = 4
    v = ext[halo:]
    out = taps[4:5] + taps[3:4] * v
    for k in range(1, width):
        moved = pltpu.roll(ext, k, 0)[halo:]
        out = out + (taps[3 - k : 4 - k] * masks[:, k : k + 1]) * moved
    return out


def prep_kernel(bcdt_ref, taps_ref, heads_ref, m_ref, segc_ref, segr_ref,
                b_ref, c_ref, bt_ref, ct_ref, pre_ref, gm_ref, cum4_ref, cumr_ref, sc_ref, dt_ref):
    T = bcdt_ref.shape[0]
    nc = T // L
    N = b_ref.shape[1]
    H = dt_ref.shape[1]
    groups = cum4_ref.shape[0]
    taps = taps_ref[...]
    tri = (lax.broadcasted_iota(jnp.int32, (L, L), 0) >= lax.broadcasted_iota(jnp.int32, (L, L), 1))
    trif = tri.astype(f32)
    neg_rate = -jnp.exp(heads_ref[0:1, :H]) * LOG2E
    bias = heads_ref[1:2, :H]

    def chunk(c, carry):
        t0 = pl.multiple_of(c * L, L)
        here = pl.ds(t0, L)
        h0 = pl.multiple_of(jnp.maximum(t0 - 16, 0), 16)
        before = bcdt_ref[pl.ds(h0, 16), : 2 * N].astype(f32)
        v = bcdt_ref[here, : 2 * N].astype(f32)
        pre = conv_rows(jnp.concatenate([before, v], axis=0), taps, m_ref[here, :], 16)
        pre_ref[here, :] = pre
        act = pre * sigmoid(pre)
        b = act[:, :N]
        cc = act[:, N:]
        bb = b.astype(bf16)
        cb = cc.astype(bf16)
        b_ref[here, :] = bb
        c_ref[here, :] = cb
        bt_ref[:, here] = b.T.astype(bf16)
        ct_ref[:, here] = cc.T.astype(bf16)
        segc = segc_ref[here, 0:1]
        prev = segc_ref[here, 1:2]
        last = segc_ref[here, 2:3]
        same = segc == segr_ref[:, here]
        g = dot(cb, bb, ((1,), (1,)))
        gm_ref[pl.ds(c, 1)] = jnp.where(tri & same, g, 0.0)[None]
        raw = bcdt_ref[here, 2 * N : 2 * N + 128].astype(f32)[:, :H] + bias
        dt = jnp.maximum(raw, 0.0) + jnp.log1p(jnp.exp(-jnp.abs(raw)))
        a2 = neg_rate * dt
        cum = dot(trif, a2, precision=HIGHEST)
        end = cum[L - 1 : L]
        ein = jnp.where(segc == prev, jnp.exp2(cum), 0.0)
        lv = jnp.where(segc == last, jnp.exp2(end - cum), 0.0)
        dt_ref[here, :] = dt
        cumt = cum.T
        s0 = pl.multiple_of(c * (3 * L), L)
        for k in range(groups):
            cols = slice(HG * k, HG * (k + 1))
            cum4_ref[k, here, :] = cum[:, cols]
            cumr_ref[k, :, here] = cumt[cols]
            sc_ref[k, pl.ds(s0, L), :] = dt[:, cols].astype(bf16)
            sc_ref[k, pl.ds(s0 + L, L), :] = ein[:, cols].astype(bf16)
            sc_ref[k, pl.ds(s0 + 2 * L, L), :] = lv[:, cols].astype(bf16)
        return carry

    lax.fori_loop(0, nc, chunk, 0)


def prep(bcdt, taps, heads, masks, segc, segr, N, H):
    T = bcdt.shape[0]
    nc = T // L
    G = H // HG
    S = jax.ShapeDtypeStruct
    return pl.pallas_call(
        prep_kernel,
        out_shape=(S((T, N), bf16), S((T, N), bf16), S((N, T), bf16), S((N, T), bf16), S((T, 2 * N), f32),
                   S((nc, L, L), f32), S((G, T, HG), f32), S((G, HG, T), f32), S((G, 3 * T, HG), bf16), S((T, H), f32)),
        compiler_params=pltpu.CompilerParams(vmem_limit_bytes=60 << 20),
    )(bcdt, taps, heads, masks, segc, segr)


def lane_onehot(width, per):
    return (lax.broadcasted_iota(jnp.int32, (HG, width), 1) // per == lax.broadcasted_iota(jnp.int32, (HG, width), 0)).astype(bf16)


def half_masks(P):
    lane = lax.broadcasted_iota(jnp.int32, (1, 2 * P), 1)
    first = (lane < P).astype(f32)
    return first.astype(bf16), (1.0 - first).astype(bf16)


def decay(cum4, cumr, k):
    return jnp.exp2(jnp.minimum(cum4[:, k : k + 1] - cumr[k : k + 1, :], 0.0))


def fwd_kernel(u_ref, gate_ref, taps_ref, m_ref, b_ref, c_ref, bt_ref, gm_ref, cum4_ref, cumr_ref, sc_ref,
               gg_ref, ssq_ref, pre_ref, st_ref, state):
    T, W = u_ref.shape
    P = W // HG
    nc = T // L
    step = pl.program_id(0)
    taps = taps_ref[...]
    gain = taps[5:6]
    skip = taps[6:7]
    onehot = lane_onehot(W, P)
    ma, mb = half_masks(P)
    state[...] = jnp.zeros_like(state)

    @pl.when(step == 0)
    def _():
        ssq_ref[...] = jnp.zeros_like(ssq_ref)

    def chunk(c, carry):
        t0 = pl.multiple_of(c * L, L)
        here = pl.ds(t0, L)
        h0 = pl.multiple_of(jnp.maximum(t0 - 16, 0), 16)
        ext = jnp.concatenate([u_ref[pl.ds(h0, 16), :], u_ref[here, :]], axis=0).astype(f32)
        pre = conv_rows(ext, taps, m_ref[here, :], 16)
        pre_ref[here, :] = pre.astype(bf16)
        x = pre * sigmoid(pre)
        s0 = pl.multiple_of(c * (3 * L), L)
        exp = dot(sc_ref[0, pl.ds(s0, 3 * L), :], onehot)
        dtx, einx, lvx = exp[:L], exp[L : 2 * L], exp[2 * L :]
        xd = x * dtx
        xdb = xd.astype(bf16)
        gm = gm_ref[c]
        cum4 = cum4_ref[0, here, :]
        cumr = cumr_ref[0, :, here]
        sb = state[...].astype(bf16)
        st_ref[c] = sb
        inner = []
        for p in range(HG // 2):
            m0 = (decay(cum4, cumr, 2 * p) * gm).astype(bf16)
            m1 = (decay(cum4, cumr, 2 * p + 1) * gm).astype(bf16)
            xp = xdb[:, 2 * P * p : 2 * P * (p + 1)]
            inner.append(dot(jnp.concatenate([m0, m1], axis=1), jnp.concatenate([xp * ma, xp * mb], axis=0)))
        y = jnp.concatenate(inner, axis=1) + dot(c_ref[here, :], sb) * einx + skip * x
        state[...] = state[...] * einx[L - 1 : L] + dot(bt_ref[:, here], (xd * lvx).astype(bf16))
        gate = gate_ref[here, :].astype(f32)
        g = y * (gate * sigmoid(gate))
        gg_ref[here, :] = (g * gain).astype(bf16)
        g2 = g * g
        tot = g2[:, :128]
        for j in range(1, W // 128):
            tot = tot + g2[:, 128 * j : 128 * (j + 1)]
        ssq_ref[here, :] += tot
        return carry

    lax.fori_loop(0, nc, chunk, 0)


def fwd(u, gate, taps, masks, b, c, bt, gm, cum4, cumr, sc):
    T, E = gate.shape
    N = b.shape[1]
    G = cum4.shape[0]
    W = E // G
    nc = T // L
    S = jax.ShapeDtypeStruct
    col = lambda off: pl.BlockSpec((T, W), lambda g: (0, g + off))
    full = lambda a: pl.BlockSpec(a.shape, lambda g: (0,) * a.ndim)
    grp = lambda a: pl.BlockSpec((1,) + a.shape[1:], lambda g: (g, 0, 0))
    return pl.pallas_call(
        fwd_kernel,
        grid=(G,),
        in_specs=[col(0), col(0), pl.BlockSpec((8, W), lambda g: (0, g)), full(masks), full(b), full(c), full(bt), full(gm),
                  grp(cum4), grp(cumr), grp(sc)],
        out_specs=[col(0), pl.BlockSpec((T, 128), lambda g: (0, 0)), col(0), pl.BlockSpec((nc, N, W), lambda g: (0, 0, g))],
        out_shape=(S((T, E), bf16), S((T, 128), f32), S((T, E), bf16), S((nc, N, E), bf16)),
        scratch_shapes=[pltpu.VMEM((N, W), f32)],
        compiler_params=pltpu.CompilerParams(vmem_limit_bytes=60 << 20),
        cost_estimate=pl.CostEstimate(flops=T * E * (2 * L + 4 * N) * 2, bytes_accessed=T * E * 12, transcendentals=T * E * 4),
    )(u, gate, taps, masks, b, c, bt, gm, cum4, cumr, sc)


def bwd_kernel(u_ref, gate_ref, pre_ref, dm_ref, rq_ref, taps_ref, m_ref, b_ref, c_ref, ct_ref, gm_ref, cum4_ref, cumr_ref, sc_ref, st_ref,
               du_ref, dgate_ref, dg_ref, db_ref, dc_ref, rs_ref, small_ref, kk_ref, ds, nxt, acc):
    T, W = u_ref.shape
    P = W // HG
    nc = T // L
    step = pl.program_id(0)
    taps = taps_ref[...]
    gain = taps[5:6]
    skip = taps[6:7]
    onehot = lane_onehot(W, P)
    ma, mb = half_masks(P)
    ds[...] = jnp.zeros_like(ds)
    nxt[...] = jnp.zeros_like(nxt)
    acc[...] = jnp.zeros_like(acc)

    @pl.when(step == 0)
    def _():
        dg_ref[...] = jnp.zeros_like(dg_ref)
        db_ref[...] = jnp.zeros_like(db_ref)
        dc_ref[...] = jnp.zeros_like(dc_ref)

    ri = lax.broadcasted_iota(jnp.int32, (4 * W, 16), 0)
    ci = lax.broadcasted_iota(jnp.int32, (4 * W, 16), 1)
    part = ri // W
    want = jnp.maximum(part - 1, 0) * HG + (ri % W) // P
    fold = (want == ci).astype(bf16)

    def eight(z):
        return jnp.sum(z.reshape(L // 8, 8, W), axis=0)

    def chunk(i, carry):
        c = nc - 1 - i
        t0 = pl.multiple_of(c * L, L)
        here = pl.ds(t0, L)
        u = u_ref[here, :].astype(f32)
        pre = pre_ref[here, :].astype(f32)
        sig = sigmoid(pre)
        x = pre * sig
        dsilu = sig + x * (1.0 - sig)
        s0 = pl.multiple_of(c * (3 * L), L)
        exp = dot(sc_ref[0, pl.ds(s0, 3 * L), :], onehot)
        dtx, einx, lvx = exp[:L], exp[L : 2 * L], exp[2 * L :]
        xdb = (x * dtx).astype(bf16)
        xd = xdb.astype(f32)
        gm = gm_ref[c]
        cum4 = cum4_ref[0, here, :]
        cumr = cumr_ref[0, :, here]
        sb = st_ref[c]
        es, ms, inner = [], [], []
        for p in range(HG // 2):
            e0 = decay(cum4, cumr, 2 * p)
            e1 = decay(cum4, cumr, 2 * p + 1)
            m0 = (e0 * gm).astype(bf16)
            m1 = (e1 * gm).astype(bf16)
            xp = xdb[:, 2 * P * p : 2 * P * (p + 1)]
            inner.append(dot(jnp.concatenate([m0, m1], axis=1), jnp.concatenate([xp * ma, xp * mb], axis=0)))
            es.append((e0, e1))
            ms.append((m0, m1))
        yn = jnp.concatenate(inner, axis=1) + dot(c_ref[here, :], sb) * einx
        y = yn + skip * x
        gate = gate_ref[here, :].astype(f32)
        sgate = sigmoid(gate)
        silu_g = gate * sgate
        g = y * silu_g
        r = rq_ref[here, 0:1]
        q = rq_ref[here, 1:2]
        dmr = dm_ref[here, :].astype(f32) * r
        dgg = gain * dmr - g * q
        dyb = (dgg * silu_g).astype(bf16)
        dy = dyb.astype(f32)
        dgate_ref[here, :] = (dgg * y * (sgate + silu_g * (1.0 - sgate))).astype(bf16)
        dxi = []
        dgc = dg_ref[c]
        for p in range(HG // 2):
            cols = slice(2 * P * p, 2 * P * (p + 1))
            dp = dyb[:, cols]
            dstack = jnp.concatenate([dp * ma, dp * mb], axis=0)
            dmm = dot(dstack, xdb[:, cols], ((1,), (1,)))
            dgc = dgc + dmm[:L] * es[p][0] + dmm[L:] * es[p][1]
            dxi.append(dot(jnp.concatenate(ms[p], axis=0), dstack, ((0,), (0,))))
        dg_ref[c] = dgc
        dxi = jnp.concatenate(dxi, axis=1)
        dsn = ds[...]
        dsb = dsn.astype(bf16)
        dye = (dy * einx).astype(bf16)
        dc_ref[here, :] += dot(dye, sb, ((1,), (1,)))
        kept = einx[L - 1 : L]
        kk_ref[pl.ds(c, 1), :] = kept * jnp.sum(sb.astype(f32) * dsn, axis=0, keepdims=True)
        db_ref[here, :] += dot((xd * lvx).astype(bf16), dsb, ((1,), (1,)))
        dxe = dot(b_ref[here, :], dsb) * lvx
        ds[...] = dsn * kept + dot(ct_ref[:, here], dye)
        dxd = dxi + dxe
        r1 = dy * yn - xd * dxi
        r1h = r1.astype(bf16)
        r1l = (r1 - r1h.astype(f32)).astype(bf16)
        rs_ref[0, here, :] = dot(jnp.concatenate([r1h, r1l, (xd * dxe).astype(bf16), (x * dxd).astype(bf16)], axis=1), fold)
        dpre = (dxd * dtx + skip * dy) * dsilu
        ext = jnp.concatenate([dpre, nxt[...]], axis=0)
        nxt[...] = dpre[:8]
        du = taps[3:4] * dpre
        acc[0:8, :] += eight(dmr * g)
        acc[8:16, :] += eight(dy * x)
        acc[16:24, :] += eight(dpre)
        acc[24:32, :] += eight(dpre * u)
        mrows = m_ref[pl.ds(t0, L + 8), :]
        for k in range(1, 4):
            sk = pltpu.roll(ext * mrows[:, k : k + 1], L + 8 - k, 0)[:L]
            du = du + taps[3 - k : 4 - k] * sk
            acc[24 + 8 * k : 32 + 8 * k, :] += eight(sk * u)
        du_ref[here, :] = du.astype(bf16)
        return carry

    lax.fori_loop(0, nc, chunk, 0)
    for j in range(7):
        small_ref[j : j + 1, :] = jnp.sum(acc[8 * j : 8 * j + 8, :], axis=0, keepdims=True)
    small_ref[7:8, :] = jnp.zeros((1, W), f32)


def bwd(u, gate, pre, dm, rq, taps, masks, b, c, ct, gm, cum4, cumr, sc, st):
    T, E = gate.shape
    N = b.shape[1]
    G = cum4.shape[0]
    W = E // G
    nc = T // L
    S = jax.ShapeDtypeStruct
    col = lambda off: pl.BlockSpec((T, W), lambda g: (0, g + off))
    full = lambda a: pl.BlockSpec(a.shape, lambda g: (0,) * a.ndim)
    whole = lambda s: pl.BlockSpec(s, lambda g: (0,) * len(s))
    grp = lambda a: pl.BlockSpec((1,) + a.shape[1:], lambda g: (g, 0, 0))
    masks = jnp.pad(masks, ((0, 8), (0, 0)))
    return pl.pallas_call(
        bwd_kernel,
        grid=(G,),
        in_specs=[col(0), col(0), col(0), col(0), full(rq), pl.BlockSpec((8, W), lambda g: (0, g)), full(masks), full(b), full(c),
                  full(ct), full(gm), grp(cum4), grp(cumr), grp(sc), pl.BlockSpec((nc, N, W), lambda g: (0, 0, g))],
        out_specs=[col(0), col(0), whole((nc, L, L)), whole((T, N)), whole((T, N)), pl.BlockSpec((1, T, 16), lambda g: (g, 0, 0)),
                   pl.BlockSpec((8, W), lambda g: (0, g)), pl.BlockSpec((nc, W), lambda g: (0, g))],
        out_shape=(S((T, E), bf16), S((T, E), bf16), S((nc, L, L), f32), S((T, N), f32), S((T, N), f32), S((G, T, 16), f32),
                   S((8, E), f32), S((nc, E), f32)),
        scratch_shapes=[pltpu.VMEM((N, W), f32), pltpu.VMEM((8, W), f32), pltpu.VMEM((56, W), f32)],
        compiler_params=pltpu.CompilerParams(vmem_limit_bytes=60 << 20),
        cost_estimate=pl.CostEstimate(flops=T * E * (8 * L + 12 * N), bytes_accessed=T * E * 16, transcendentals=T * E * 4),
    )(u, gate, pre, dm, rq, taps, masks, b, c, ct, gm, cum4, cumr, sc, st)


def post_kernel(bcdt_ref, pre_ref, taps_ref, heads_ref, m_ref, segc_ref, segr_ref, b_ref, c_ref, dg_ref, db_ref, dc_ref, rs_ref, kk_ref, dt_ref,
                out_ref, small_ref, hs_ref, nxt, acc, hacc):
    T = bcdt_ref.shape[0]
    nc = T // L
    N = b_ref.shape[1]
    H = dt_ref.shape[1]
    G = H // HG
    taps = taps_ref[...]
    tri = (lax.broadcasted_iota(jnp.int32, (L, L), 0) >= lax.broadcasted_iota(jnp.int32, (L, L), 1))
    upper = (lax.broadcasted_iota(jnp.int32, (L, L), 0) <= lax.broadcasted_iota(jnp.int32, (L, L), 1)).astype(f32)
    strict = 1.0 - upper
    rate = -jnp.exp(heads_ref[0:1, :H])
    bias = heads_ref[1:2, :H]
    nxt[...] = jnp.zeros_like(nxt)
    acc[...] = jnp.zeros_like(acc)
    hacc[...] = jnp.zeros_like(hacc)

    def eight(z):
        return jnp.sum(z.reshape(L // 8, 8, z.shape[1]), axis=0)

    def chunk(i, carry):
        c = nc - 1 - i
        t0 = pl.multiple_of(c * L, L)
        here = pl.ds(t0, L)
        same = segc_ref[here, 0:1] == segr_ref[:, here]
        dg = jnp.where(tri & same, dg_ref[c], 0.0)
        dgb = dg.astype(bf16)
        dcv = dc_ref[here, :] + dot(dgb, b_ref[here, :])
        dbv = db_ref[here, :] + dot(dg.T.astype(bf16), c_ref[here, :])
        pre = pre_ref[here, :]
        sig = sigmoid(pre)
        dpre = jnp.concatenate([dbv, dcv], axis=1) * (sig + pre * sig * (1.0 - sig))
        v = bcdt_ref[here, : 2 * N].astype(f32)
        ext = jnp.concatenate([dpre, nxt[...]], axis=0)
        nxt[...] = dpre[:8]
        dv = taps[3:4] * dpre
        acc[0:8, :] += eight(dpre)
        acc[8:16, :] += eight(dpre * v)
        mrows = m_ref[pl.ds(t0, L + 8), :]
        for k in range(1, 4):
            sk = pltpu.roll(ext * mrows[:, k : k + 1], L + 8 - k, 0)[:L]
            dv = dv + taps[3 - k : 4 - k] * sk
            acc[8 + 8 * k : 16 + 8 * k, :] += eight(sk * v)
        out_ref[here, : 2 * N] = dv.astype(bf16)
        r1 = jnp.concatenate([rs_ref[k, here, 0:HG] for k in range(G)], axis=1)
        r2 = jnp.concatenate([rs_ref[k, here, HG : 2 * HG] for k in range(G)], axis=1)
        r3 = jnp.concatenate([rs_ref[k, here, 2 * HG : 3 * HG] for k in range(G)], axis=1)
        da = dot(upper, r1, precision=HIGHEST) + dot(strict, r2, precision=HIGHEST) + kk_ref[pl.ds(c, 1), :]
        dt = dt_ref[here, :]
        raw = bcdt_ref[here, 2 * N : 2 * N + 128].astype(f32)[:, :H] + bias
        ddt = (r3 + da * rate) * sigmoid(raw)
        hacc[0:8, :] += eight(da * rate * dt)
        hacc[8:16, :] += eight(ddt)
        out_ref[here, 2 * N :] = jnp.concatenate([ddt, jnp.zeros((L, out_ref.shape[1] - 2 * N - H), f32)], axis=1).astype(bf16)
        return carry

    lax.fori_loop(0, nc, chunk, 0)
    for j in range(5):
        small_ref[j : j + 1, :] = jnp.sum(acc[8 * j : 8 * j + 8, :], axis=0, keepdims=True)
    small_ref[5:8, :] = jnp.zeros((3, 2 * N), f32)
    for j in range(2):
        hs_ref[j : j + 1, :] = jnp.sum(hacc[8 * j : 8 * j + 8, :], axis=0, keepdims=True)


def post(bcdt, pre, taps, heads, masks, segc, segr, b, c, dg, db, dc, rs, kk, dt):
    T = bcdt.shape[0]
    N = b.shape[1]
    H = dt.shape[1]
    S = jax.ShapeDtypeStruct
    masks = jnp.pad(masks, ((0, 8), (0, 0)))
    return pl.pallas_call(
        post_kernel,
        out_shape=(S(bcdt.shape, bf16), S((8, 2 * N), f32), S((2, H), f32)),
        scratch_shapes=[pltpu.VMEM((8, 2 * N), f32), pltpu.VMEM((40, 2 * N), f32), pltpu.VMEM((16, H), f32)],
        compiler_params=pltpu.CompilerParams(vmem_limit_bytes=60 << 20),
    )(bcdt, pre, taps, heads, masks, segc, segr, b, c, dg, db, dc, rs, kk, dt)


AXES = ("dp", "fsdp")
MESH = pl.DeviceIdType.MESH


class Place:
    def __init__(self, nd, nf):
        self.zn, self.nf = nd // 2, nf
        d, f = lax.axis_index("dp"), lax.axis_index("fsdp")
        self.z, self.y = d // 2, d % 2
        self.x, self.c = f // 2, f % 2

    def dev(self, z, y, x, c):
        return (z * 2 + y, x * 2 + c)

    def idx(self, z, y, x, c):
        return (z * 2 + y) * self.nf + x * 2 + c

    def barrier(self):
        z, y, x, c, zn = self.z, self.y, self.x, self.c, self.zn
        sem = pltpu.get_barrier_semaphore()
        for there in ((z, y, 1 - x, c), (z, 1 - y, x, c), (z, y, x, 1 - c)):
            pl.semaphore_signal(sem, inc=1, device_id=self.dev(*there), device_id_type=MESH)

        @pl.when(z > 0)
        def _():
            pl.semaphore_signal(sem, inc=1, device_id=self.dev(z - 1, y, x, c), device_id_type=MESH)

        @pl.when(z < zn - 1)
        def _():
            pl.semaphore_signal(sem, inc=1, device_id=self.dev(z + 1, y, x, c), device_id_type=MESH)

        pl.semaphore_wait(sem, 3 + (z + zn - 1) // zn + (2 * zn - 2 - z) // zn)


def gather_kernel(nd, nf, src_ref, out_ref, own_sem, z_send, z_recv, x_send, x_recv, y_send, y_recv, dx_send, dx_recv, dy_send, dy_recv, c_send, c_recv):
    at = Place(nd, nf)
    z, y, x, c, zn = at.z, at.y, at.x, at.c, at.zn
    half = out_ref.shape[2] // 256 * 128
    lo, hi = pl.ds(0, half), pl.ds(half, out_ref.shape[2] - half)
    at.barrier()

    def copy(block, to, send, recv, cols=None, src=None):
        ref = out_ref.at[block] if cols is None else out_ref.at[block, :, cols]
        return pltpu.make_async_remote_copy(src_ref=ref if src is None else src, dst_ref=ref, send_sem=send, recv_sem=recv,
                                            device_id=at.dev(*to), device_id_type=MESH)

    def block(zs, col):
        return at.idx(zs, 1 - y if col & 2 else y, 1 - x if col & 1 else x, c)

    def up(zs, src=None):
        return copy(block(zs, 0), (z + 1, y, x, c), z_send.at[0, zs], z_recv.at[zs], src=src)

    def down(zs, src=None):
        return copy(block(zs, 0), (z - 1, y, x, c), z_send.at[1, zs], z_recv.at[zs], src=src)

    def to_x(zs, src=None):
        return copy(block(zs, 0), (z, y, 1 - x, c), x_send.at[zs], x_recv.at[zs], src=src)

    def to_y(zs, src=None):
        return copy(block(zs, 0), (z, 1 - y, x, c), y_send.at[zs], y_recv.at[zs], src=src)

    def diag_y(zs):
        return copy(block(zs, 1), (z, 1 - y, x, c), dy_send.at[zs], dy_recv.at[zs], lo)

    def diag_x(zs):
        return copy(block(zs, 2), (z, y, 1 - x, c), dx_send.at[zs], dx_recv.at[zs], hi)

    def to_core(zs, col, src=None):
        return copy(block(zs, col), (z, y, x, 1 - c), c_send.at[zs, col], c_recv.at[zs, col], src=src)

    own = pltpu.make_async_copy(src_ref, out_ref.at[block(z, 0)], own_sem)
    own.start()

    @pl.when(z < zn - 1)
    def _():
        up(z, src_ref).start()

    @pl.when(z > 0)
    def _():
        down(z, src_ref).start()

    to_x(z, src_ref).start()
    to_y(z, src_ref).start()
    to_core(z, 0, src_ref).start()

    def each(dist, fn):
        if dist == 0:
            fn(z, 0)
            return

        @pl.when(z - dist >= 0)
        def _():
            fn(z - dist, 1)

        @pl.when(z + dist < zn)
        def _():
            fn(z + dist, -1)

    def from_z(zs, way):
        copy(block(zs, 0), (z, y, x, c), z_send.at[0, zs], z_recv.at[zs]).wait_recv()
        if way > 0:
            @pl.when(z < zn - 1)
            def _():
                up(zs).start()
        else:
            @pl.when(z > 0)
            def _():
                down(zs).start()
        to_x(zs).start()
        to_y(zs).start()
        to_core(zs, 0).start()

    def from_xy(zs, way):
        to_x(zs).wait_recv()
        diag_y(zs).start()
        to_core(zs, 1).start()
        to_y(zs).wait_recv()
        diag_x(zs).start()
        to_core(zs, 2).start()

    def from_diag(zs, way):
        diag_y(zs).wait_recv()
        diag_x(zs).wait_recv()
        to_core(zs, 3).start()

    for dist in range(zn):
        if dist:
            each(dist, from_z)
        each(dist, from_xy)
    for dist in range(zn):
        each(dist, from_diag)
    own.wait()

    def sent(zs, way):
        for col in range(4):
            to_core(zs, col).wait_recv()
            to_core(zs, col).wait_send()
        to_x(zs).wait_send()
        to_y(zs).wait_send()
        diag_x(zs).wait_send()
        diag_y(zs).wait_send()
        if way >= 0:
            @pl.when(z < zn - 1)
            def _():
                up(zs).wait_send()
        if way <= 0:
            @pl.when(z > 0)
            def _():
                down(zs).wait_send()

    for dist in range(zn):
        each(dist, sent)


def gather_rows(shard, nd, nf, cid):
    zn = nd // 2
    D = pltpu.SemaphoreType.DMA
    return pl.pallas_call(
        functools.partial(gather_kernel, nd, nf),
        out_shape=jax.ShapeDtypeStruct((nd * nf,) + shard.shape, shard.dtype),
        in_specs=[pl.BlockSpec(memory_space=pl.ANY)],
        out_specs=pl.BlockSpec(memory_space=pl.ANY),
        scratch_shapes=[D(()), D((2, zn)), D((zn,)), D((zn,)), D((zn,)), D((zn,)), D((zn,)), D((zn,)), D((zn,)), D((zn,)), D((zn,)),
                        D((zn, 4)), D((zn, 4))],
        compiler_params=pltpu.CompilerParams(collective_id=cid, has_side_effects=True),
    )(shard)


def scatter_kernel(nd, nf, parts, *refs):
    scatter_body(nd, nf, refs[:parts], *refs[parts:])


def scatter_body(nd, nf, g_refs, out_ref, acc, c_in, d_in, xy_in, z_in,
                   load_sem, c_send, c_recv, dx_send, dx_recv, dy_send, dy_recv, x_send, x_recv, y_send, y_recv, z_send, z_recv):
    at = Place(nd, nf)
    z, y, x, c, zn = at.z, at.y, at.x, at.c, at.zn
    cols = out_ref.shape[1]
    offs = [sum(r.shape[2] for r in g_refs[:k]) for k in range(len(g_refs))]
    half = cols // 256 * 128
    lo, hi = pl.ds(0, half), pl.ds(half, cols - half)
    at.barrier()

    def idx(zs, col, core):
        return at.idx(zs, 1 - y if col & 2 else y, 1 - x if col & 1 else x, core)

    def remote(src, dst, to, send, recv):
        return pltpu.make_async_remote_copy(src_ref=src, dst_ref=dst, send_sem=send, recv_sem=recv, device_id=at.dev(*to), device_id_type=MESH)

    def load(zs, col):
        return [pltpu.make_async_copy(r.at[idx(zs, col, c)], acc.at[zs, col, :, pl.ds(o, r.shape[2])], load_sem.at[zs, col, k])
                for k, (r, o) in enumerate(zip(g_refs, offs))]

    def core(zs, col):
        return [remote(r.at[idx(zs, col, 1 - c)], c_in.at[zs, col, :, pl.ds(o, r.shape[2])], (z, y, x, 1 - c),
                       c_send.at[zs, col, k], c_recv.at[zs, col, k])
                for k, (r, o) in enumerate(zip(g_refs, offs))]

    def diag_x(zs):
        return remote(acc.at[zs, 3, :, lo], d_in.at[0, zs, :, lo], (z, y, 1 - x, c), dx_send.at[zs], dx_recv.at[zs])

    def diag_y(zs):
        return remote(acc.at[zs, 3, :, hi], d_in.at[1, zs, :, hi], (z, 1 - y, x, c), dy_send.at[zs], dy_recv.at[zs])

    def to_x(zs):
        return remote(acc.at[zs, 1], xy_in.at[0, zs], (z, y, 1 - x, c), x_send.at[zs], x_recv.at[zs])

    def to_y(zs):
        return remote(acc.at[zs, 2], xy_in.at[1, zs], (z, 1 - y, x, c), y_send.at[zs], y_recv.at[zs])

    def up(zs):
        return remote(acc.at[zs, 0], z_in.at[0, zs], (z + 1, y, x, c), z_send.at[zs], z_recv.at[0, zs])

    def down(zs):
        return remote(acc.at[zs, 0], z_in.at[1, zs], (z - 1, y, x, c), z_send.at[zs], z_recv.at[1, zs])

    def each(dist, fn):
        if dist == 0:
            fn(z)
            return

        @pl.when(z - dist >= 0)
        def _():
            fn(z - dist)

        @pl.when(z + dist < zn)
        def _():
            fn(z + dist)

    order = list(range(zn - 1, -1, -1))
    for col in (3, 1, 2, 0):
        for dist in order:
            def begin(zs):
                for cp in core(zs, col) + load(zs, col):
                    cp.start()
            each(dist, begin)

    def ready(zs, col):
        for cp in load(zs, col):
            cp.wait()
        for cp in core(zs, col):
            cp.wait_recv()

    def diag(zs):
        ready(zs, 3)
        acc[zs, 3] = acc[zs, 3] + c_in[zs, 3]
        diag_x(zs).start()
        diag_y(zs).start()

    def sides(zs):
        ready(zs, 1)
        diag_y(zs).wait_recv()
        acc[zs, 1, :, lo] = acc[zs, 1, :, lo] + c_in[zs, 1, :, lo]
        acc[zs, 1, :, hi] = (acc[zs, 1, :, hi].astype(f32) + c_in[zs, 1, :, hi].astype(f32) + d_in[1, zs, :, hi].astype(f32)).astype(bf16)
        to_x(zs).start()
        ready(zs, 2)
        diag_x(zs).wait_recv()
        acc[zs, 2, :, lo] = (acc[zs, 2, :, lo].astype(f32) + c_in[zs, 2, :, lo].astype(f32) + d_in[0, zs, :, lo].astype(f32)).astype(bf16)
        acc[zs, 2, :, hi] = acc[zs, 2, :, hi] + c_in[zs, 2, :, hi]
        to_y(zs).start()

    def column(zs):
        ready(zs, 0)
        to_x(zs).wait_recv()
        to_y(zs).wait_recv()
        return (acc[zs, 0].astype(f32) + c_in[zs, 0].astype(f32)) + (xy_in[0, zs].astype(f32) + xy_in[1, zs].astype(f32))

    def pass_on(zs):
        total = column(zs)

        @pl.when(zs > z)
        def _():
            @pl.when(z > 0)
            def _():
                up(zs).wait_recv()
                acc[zs, 0] = (total + z_in[0, zs].astype(f32)).astype(bf16)

            @pl.when(z == 0)
            def _():
                acc[zs, 0] = total.astype(bf16)
            up(zs).start()

        @pl.when(zs < z)
        def _():
            @pl.when(z < zn - 1)
            def _():
                down(zs).wait_recv()
                acc[zs, 0] = (total + z_in[1, zs].astype(f32)).astype(bf16)

            @pl.when(z == zn - 1)
            def _():
                acc[zs, 0] = total.astype(bf16)
            down(zs).start()

    for dist in order:
        each(dist, diag)
    for dist in order:
        each(dist, sides)
    for dist in order[:-1]:
        each(dist, pass_on)
    out_ref[...] = column(z)

    @pl.when(z > 0)
    def _():
        up(z).wait_recv()
        out_ref[...] += z_in[0, z].astype(f32)

    @pl.when(z < zn - 1)
    def _():
        down(z).wait_recv()
        out_ref[...] += z_in[1, z].astype(f32)

    def sent(zs):
        for col in range(4):
            for cp in core(zs, col):
                cp.wait_send()
        diag_x(zs).wait_send()
        diag_y(zs).wait_send()
        to_x(zs).wait_send()
        to_y(zs).wait_send()

    for dist in order:
        each(dist, sent)
        if dist:
            each(dist, lambda zs: up(zs).wait_send())


def scatter_rows(gs, nd, nf, cid):
    zn, parts = nd // 2, len(gs)
    rows, cols = gs[0].shape[1], sum(g.shape[2] for g in gs)
    D = pltpu.SemaphoreType.DMA
    V = pltpu.VMEM
    return pl.pallas_call(
        functools.partial(scatter_kernel, nd, nf, parts),
        out_shape=jax.ShapeDtypeStruct((rows, cols), f32),
        in_specs=[pl.BlockSpec(memory_space=pl.ANY)] * parts,
        out_specs=pl.BlockSpec(memory_space=pltpu.VMEM),
        scratch_shapes=[V((zn, 4, rows, cols), bf16), V((zn, 4, rows, cols), bf16), V((2, zn, rows, cols), bf16), V((2, zn, rows, cols), bf16),
                        V((2, zn, rows, cols), bf16), D((zn, 4, parts)), D((zn, 4, parts)), D((zn, 4, parts)), D((zn,)), D((zn,)), D((zn,)), D((zn,)), D((zn,)), D((zn,)),
                        D((zn,)), D((zn,)), D((zn,)), D((2, zn))],
        compiler_params=pltpu.CompilerParams(collective_id=cid, has_side_effects=True, vmem_limit_bytes=62 << 20),
    )(*gs)


def exchange_kernel(nd, nf, g_ref, out_ref, got, send, recv):
    n = nd * nf
    me = lax.axis_index("dp") * nf + lax.axis_index("fsdp")
    sem = pltpu.get_barrier_semaphore()

    def peer(k):
        return lax.rem(me + k, n)

    def greet(k, carry):
        pl.semaphore_signal(sem, inc=1, device_id=(peer(k) // nf, peer(k) % nf), device_id_type=MESH)
        return carry

    lax.fori_loop(1, n, greet, 0)
    pl.semaphore_wait(sem, n - 1)

    def copy(k):
        p = peer(k)
        return pltpu.make_async_remote_copy(src_ref=g_ref.at[p], dst_ref=got.at[k], send_sem=send.at[k], recv_sem=recv.at[k],
                                            device_id=(p // nf, p % nf), device_id_type=MESH)

    def begin(k, carry):
        copy(k).start()
        return carry

    lax.fori_loop(1, n, begin, 0)

    def add(k, total):
        copy(k).wait_recv()
        return total + got[k]

    out_ref[...] = lax.fori_loop(1, n, add, g_ref[me])

    def end(k, carry):
        copy(k).wait_send()
        return carry

    lax.fori_loop(1, n, end, 0)


def exchange(g, nd, nf, cid):
    n = nd * nf
    D = pltpu.SemaphoreType.DMA
    vm = pl.BlockSpec(memory_space=pltpu.VMEM)
    return pl.pallas_call(
        functools.partial(exchange_kernel, nd, nf),
        out_shape=jax.ShapeDtypeStruct(g.shape[1:], g.dtype),
        in_specs=[vm],
        out_specs=vm,
        scratch_shapes=[pltpu.VMEM(g.shape, g.dtype), D((n,)), D((n,))],
        compiler_params=pltpu.CompilerParams(collective_id=cid, has_side_effects=True),
    )(g)


def layer(nd, nf, hidden, grad_out, seg, shard_a, shard_gate, shard_out, head_params, sizes):
    n = nd * nf
    E, N, H, K1, S = sizes
    T, D = hidden.shape
    wide = 2 * N + 128
    full_gate = lax.all_gather(shard_gate, AXES, axis=0, tiled=True)
    full_out = lax.all_gather(shard_out, AXES, axis=0, tiled=True)
    full_a = gather_rows(shard_a, nd, nf, 0)
    off = E + 2 * N + H
    flat = full_a[:, :, off : off + S].reshape(n, -1)
    ncol, nrow, ngate = (E + 2 * N) // n, D // n, E // n
    conv = flat[:, : K1 * ncol].reshape(n, K1, ncol).transpose(1, 0, 2).reshape(K1, n * ncol).astype(f32)
    norm_gain = flat[:, K1 * ncol : K1 * ncol + nrow].reshape(-1).astype(f32)
    gate_gain = flat[:, K1 * ncol + nrow : K1 * ncol + nrow + ngate].reshape(-1).astype(f32)
    full_a = full_a.reshape(D, E + wide)
    rows = hidden.astype(f32)
    rinv = lax.rsqrt(jnp.mean(rows * rows, axis=-1, keepdims=True) + EPS)
    xhat = rows * rinv
    normed = (xhat * norm_gain).astype(bf16)
    ubc = dot(normed, full_a).astype(bf16)
    gate = dot(normed, full_gate).astype(bf16)
    bcdt = ubc[:, E:]
    pos = jnp.arange(T, dtype=jnp.int32)
    masks = jnp.stack([jnp.ones((T,), f32)] + [((jnp.roll(seg, k) == seg) & (pos >= k)).astype(f32) for k in range(1, 4)], axis=1)
    lastid = seg[L - 1 :: L]
    previd = jnp.concatenate([jnp.full((1,), -1, jnp.int32), lastid[:-1]])
    segc = jnp.stack([seg, jnp.repeat(previd, L), jnp.repeat(lastid, L)], axis=1)
    segr = seg[None, :]
    taps_u = jnp.concatenate([conv[:, :E], gate_gain[None], jnp.repeat(head_params[2], E // H)[None], jnp.zeros((1, E), f32)], axis=0)
    taps_bc = jnp.concatenate([conv[:, E:], jnp.zeros((3, 2 * N), f32)], axis=0)
    heads_p = jnp.pad(head_params, ((0, 5), (0, 128 - H)))
    b, c, bt, ct, pre_bc, gm, cum4, cumr, sc, dt = prep(bcdt, taps_bc, heads_p, masks, segc, segr, N, H)
    gg, ssq, pre, st = fwd(ubc, gate, taps_u, masks, b, c, bt, gm, cum4, cumr, sc)
    r = lax.rsqrt(jnp.sum(ssq, axis=1, keepdims=True) / E + EPS)
    gos = (grad_out.astype(f32) * r).astype(bf16)
    g_out = dot(gg, gos, ((0,), (0,))).astype(bf16)
    s_out = lax.psum_scatter(g_out, AXES, scatter_dimension=0, tiled=True).astype(f32)
    output = (rows + r * dot(gg, full_out)).astype(bf16)
    dm = dot(grad_out, full_out, ((1,), (1,))).astype(bf16)
    s = jnp.sum(gg.astype(f32) * dm.astype(f32), axis=1, keepdims=True)
    rq = jnp.concatenate([r, r * r * r * s / E], axis=1)
    du, dgate, dg, db, dc, rs, small, kk = bwd(ubc, gate, pre, dm, rq, taps_u, masks, b, c, ct, gm, cum4, cumr, sc, st)
    kkh = jnp.sum(kk.reshape(kk.shape[0], H, E // H), axis=2)
    dbcdt, small_bc, hs = post(bcdt, pre_bc, taps_bc, heads_p, masks, segc, segr, b, c, dg, db, dc, rs, kkh, dt)
    g_gate = dot(normed, dgate, ((0,), (0,))).astype(bf16)
    g_u = dot(normed, du, ((0,), (0,))).astype(bf16)
    g_bcdt = dot(normed, dbcdt, ((0,), (0,))).astype(bf16)
    s_in = scatter_rows([g.reshape(n, D // n, -1) for g in (g_gate, g_u, g_bcdt)], nd, nf, 1)
    bn = dot(dgate, full_gate, ((1,), (1,))) + dot(du, full_a[:, :E], ((1,), (1,))) + dot(dbcdt, full_a[:, E:], ((1,), (1,)))
    gb = bn * norm_gain
    d_rows = rinv * (gb - xhat * jnp.mean(gb * xhat, axis=-1, keepdims=True))
    grad_in = (grad_out.astype(f32) + d_rows).astype(bf16)
    d_norm = jnp.sum(bn * xhat, axis=0)
    d_conv = jnp.concatenate([jnp.stack([small[6], small[5], small[4], small[3], small[2]]),
                              jnp.stack([small_bc[4], small_bc[3], small_bc[2], small_bc[1], small_bc[0]])], axis=1)
    d_heads = jnp.concatenate([hs, jnp.sum(small[1].reshape(1, H, E // H), axis=2)], axis=0)
    mine = jnp.concatenate([d_conv.reshape(K1, n, ncol).transpose(1, 0, 2).reshape(n, -1), d_norm.reshape(n, -1), small[0].reshape(n, -1),
                            jnp.broadcast_to(d_heads.reshape(1, -1), (n, d_heads.size))], axis=1)
    tiles = -(-mine.shape[1] // 1024)
    mine = jnp.pad(mine, ((0, 0), (0, tiles * 1024 - mine.shape[1]))).reshape(n, tiles * 8, 128)
    tot = exchange(mine, nd, nf, 2).reshape(-1)
    cut = [0, K1 * ncol, nrow, ngate, d_heads.size]
    ends = [sum(cut[: k + 1]) for k in range(5)]
    t_conv, t_norm, t_gate, t_heads = (tot[ends[k] : ends[k + 1]] for k in range(4))
    return (output, grad_in, s_in[:, : 2 * E], s_in[:, 2 * E : 2 * E + 2 * N], s_in[:, 2 * E + 2 * N : 2 * E + 2 * N + H], s_out,
            t_conv.reshape(K1, ncol), t_norm, t_gate, t_heads.reshape(d_heads.shape))


def per_device(nd, nf, hidden, grad_out, segment_ids, w_zx, w_bc, w_dt, w_out, conv_params, norm_gain, gate_gain, head_params):
    n = nd * nf
    E, N2, H = w_out.shape[0] * n, w_bc.shape[1], w_dt.shape[1]
    rows = w_zx.shape[0]
    small = jnp.concatenate([conv_params.reshape(-1), norm_gain, gate_gain])
    S = -(-small.shape[0] // rows)
    assert S + H <= 128
    small = jnp.pad(small, (0, S * rows - small.shape[0])).reshape(rows, S)
    shard_a = jnp.concatenate([w_zx[:, E:], w_bc, w_dt, small, jnp.zeros((rows, 128 - H - S), bf16)], axis=1)
    return layer(nd, nf, hidden, grad_out, segment_ids, shard_a, w_zx[:, :E], w_out, head_params, (E, N2 // 2, H, conv_params.shape[0], S))


def solution(mesh):
    row, col, vec, rep = P(AXES, None), P(None, AXES), P(AXES), P()
    return jax.shard_map(
        functools.partial(per_device, mesh.shape["dp"], mesh.shape["fsdp"]),
        mesh=mesh,
        in_specs=(row, row, vec, row, row, row, row, col, vec, vec, rep),
        out_specs=(row, row, row, row, row, row, col, vec, vec, rep),
        check_vma=False,
    )
```

```python
import functools
import jax
import jax.numpy as jnp
from jax import lax
from jax.experimental import pallas as pl
from jax.experimental.pallas import tpu as pltpu
from jax.sharding import PartitionSpec as P

EPS = 1e-05
L = 128
HG = 4
LOG2E = 1.4426950408889634
BWD_TICKS = 44
TAIL_TICKS = 22
bf16, f32 = jnp.bfloat16, jnp.float32
HIGHEST = lax.Precision.HIGHEST


AXES = ("dp", "fsdp")
MESH = pl.DeviceIdType.MESH


class Place:
    def __init__(self, nd, nf):
        self.zn, self.nf = nd // 2, nf
        d, f = lax.axis_index("dp"), lax.axis_index("fsdp")
        self.z, self.y = d // 2, d % 2
        self.x, self.c = f // 2, f % 2

    def dev(self, z, y, x, c):
        return (z * 2 + y, x * 2 + c)

    def idx(self, z, y, x, c):
        return (z * 2 + y) * self.nf + x * 2 + c

    def barrier(self):
        z, y, x, c, zn = self.z, self.y, self.x, self.c, self.zn
        sem = pltpu.get_barrier_semaphore()
        for there in ((z, y, 1 - x, c), (z, 1 - y, x, c), (z, y, x, 1 - c)):
            pl.semaphore_signal(sem, inc=1, device_id=self.dev(*there), device_id_type=MESH)

        @pl.when(z > 0)
        def _():
            pl.semaphore_signal(sem, inc=1, device_id=self.dev(z - 1, y, x, c), device_id_type=MESH)

        @pl.when(z < zn - 1)
        def _():
            pl.semaphore_signal(sem, inc=1, device_id=self.dev(z + 1, y, x, c), device_id_type=MESH)

        pl.semaphore_wait(sem, 3 + (z + zn - 1) // zn + (2 * zn - 2 - z) // zn)


def gather_kernel(nd, nf, src_ref, out_ref, own_sem, z_send, z_recv, x_send, x_recv, y_send, y_recv, dx_send, dx_recv, dy_send, dy_recv, c_send, c_recv):
    at = Place(nd, nf)
    z, y, x, c, zn = at.z, at.y, at.x, at.c, at.zn
    half = out_ref.shape[2] // 256 * 128
    lo, hi = pl.ds(0, half), pl.ds(half, out_ref.shape[2] - half)
    at.barrier()

    def copy(block, to, send, recv, cols=None, src=None):
        ref = out_ref.at[block] if cols is None else out_ref.at[block, :, cols]
        return pltpu.make_async_remote_copy(src_ref=ref if src is None else src, dst_ref=ref, send_sem=send, recv_sem=recv,
                                            device_id=at.dev(*to), device_id_type=MESH)

    def block(zs, col):
        return at.idx(zs, 1 - y if col & 2 else y, 1 - x if col & 1 else x, c)

    def up(zs, src=None):
        return copy(block(zs, 0), (z + 1, y, x, c), z_send.at[0, zs], z_recv.at[zs], src=src)

    def down(zs, src=None):
        return copy(block(zs, 0), (z - 1, y, x, c), z_send.at[1, zs], z_recv.at[zs], src=src)

    def to_x(zs, src=None):
        return copy(block(zs, 0), (z, y, 1 - x, c), x_send.at[zs], x_recv.at[zs], src=src)

    def to_y(zs, src=None):
        return copy(block(zs, 0), (z, 1 - y, x, c), y_send.at[zs], y_recv.at[zs], src=src)

    def diag_y(zs):
        return copy(block(zs, 1), (z, 1 - y, x, c), dy_send.at[zs], dy_recv.at[zs], lo)

    def diag_x(zs):
        return copy(block(zs, 2), (z, y, 1 - x, c), dx_send.at[zs], dx_recv.at[zs], hi)

    def to_core(zs, col, src=None):
        return copy(block(zs, col), (z, y, x, 1 - c), c_send.at[zs, col], c_recv.at[zs, col], src=src)

    own = pltpu.make_async_copy(src_ref, out_ref.at[block(z, 0)], own_sem)
    own.start()

    @pl.when(z < zn - 1)
    def _():
        up(z, src_ref).start()

    @pl.when(z > 0)
    def _():
        down(z, src_ref).start()

    to_x(z, src_ref).start()
    to_y(z, src_ref).start()
    to_core(z, 0, src_ref).start()

    def each(dist, fn):
        if dist == 0:
            fn(z, 0)
            return

        @pl.when(z - dist >= 0)
        def _():
            fn(z - dist, 1)

        @pl.when(z + dist < zn)
        def _():
            fn(z + dist, -1)

    def from_z(zs, way):
        copy(block(zs, 0), (z, y, x, c), z_send.at[0, zs], z_recv.at[zs]).wait_recv()
        if way > 0:
            @pl.when(z < zn - 1)
            def _():
                up(zs).start()
        else:
            @pl.when(z > 0)
            def _():
                down(zs).start()
        to_x(zs).start()
        to_y(zs).start()
        to_core(zs, 0).start()

    def from_xy(zs, way):
        to_x(zs).wait_recv()
        diag_y(zs).start()
        to_core(zs, 1).start()
        to_y(zs).wait_recv()
        diag_x(zs).start()
        to_core(zs, 2).start()

    def from_diag(zs, way):
        diag_y(zs).wait_recv()
        diag_x(zs).wait_recv()
        to_core(zs, 3).start()

    for dist in range(zn):
        if dist:
            each(dist, from_z)
        each(dist, from_xy)
    for dist in range(zn):
        each(dist, from_diag)
    own.wait()

    def sent(zs, way):
        for col in range(4):
            to_core(zs, col).wait_recv()
            to_core(zs, col).wait_send()
        to_x(zs).wait_send()
        to_y(zs).wait_send()
        diag_x(zs).wait_send()
        diag_y(zs).wait_send()
        if way >= 0:
            @pl.when(z < zn - 1)
            def _():
                up(zs).wait_send()
        if way <= 0:
            @pl.when(z > 0)
            def _():
                down(zs).wait_send()

    for dist in range(zn):
        each(dist, sent)


def gather_rows(shard, nd, nf, cid):
    zn = nd // 2
    D = pltpu.SemaphoreType.DMA
    return pl.pallas_call(
        functools.partial(gather_kernel, nd, nf),
        out_shape=jax.ShapeDtypeStruct((nd * nf,) + shard.shape, shard.dtype),
        in_specs=[pl.BlockSpec(memory_space=pl.ANY)],
        out_specs=pl.BlockSpec(memory_space=pl.ANY),
        scratch_shapes=[D(()), D((2, zn)), D((zn,)), D((zn,)), D((zn,)), D((zn,)), D((zn,)), D((zn,)), D((zn,)), D((zn,)), D((zn,)),
                        D((zn, 4)), D((zn, 4))],
        compiler_params=pltpu.CompilerParams(collective_id=cid, has_side_effects=True),
    )(shard)


class Scatter:
    def __init__(self, nd, nf, g_refs, out_ref, acc, c_in, d_in, xy_in, z_in,
                 load_sem, c_send, c_recv, dx_send, dx_recv, dy_send, dy_recv, x_send, x_recv, y_send, y_recv, z_send, z_recv):
        at = Place(nd, nf)
        z, y, x, c, zn = at.z, at.y, at.x, at.c, at.zn
        cols = out_ref.shape[1]
        offs = [sum(r.shape[2] for r in g_refs[:k]) for k in range(len(g_refs))]
        half = cols // 256 * 128
        lo, hi = pl.ds(0, half), pl.ds(half, cols - half)

        def idx(zs, col, core):
            return at.idx(zs, 1 - y if col & 2 else y, 1 - x if col & 1 else x, core)

        def remote(src, dst, to, send, recv):
            return pltpu.make_async_remote_copy(src_ref=src, dst_ref=dst, send_sem=send, recv_sem=recv, device_id=at.dev(*to), device_id_type=MESH)

        def load(zs, col):
            return [pltpu.make_async_copy(r.at[idx(zs, col, c)], acc.at[zs, col, :, pl.ds(o, r.shape[2])], load_sem.at[zs, col, k])
                    for k, (r, o) in enumerate(zip(g_refs, offs))]

        def core(zs, col):
            return [remote(r.at[idx(zs, col, 1 - c)], c_in.at[zs, col, :, pl.ds(o, r.shape[2])], (z, y, x, 1 - c),
                           c_send.at[zs, col, k], c_recv.at[zs, col, k])
                    for k, (r, o) in enumerate(zip(g_refs, offs))]

        def diag_x(zs):
            return remote(acc.at[zs, 3, :, lo], d_in.at[zs, :, lo], (z, y, 1 - x, c), dx_send.at[zs], dx_recv.at[zs])

        def diag_y(zs):
            return remote(acc.at[zs, 3, :, hi], d_in.at[zs, :, hi], (z, 1 - y, x, c), dy_send.at[zs], dy_recv.at[zs])

        def to_x(zs):
            return remote(acc.at[zs, 1], xy_in.at[0, zs], (z, y, 1 - x, c), x_send.at[zs], x_recv.at[zs])

        def to_y(zs):
            return remote(acc.at[zs, 2], xy_in.at[1, zs], (z, 1 - y, x, c), y_send.at[zs], y_recv.at[zs])

        def up(zs):
            return remote(acc.at[zs, 0], z_in.at[0, zs], (z + 1, y, x, c), z_send.at[zs], z_recv.at[0, zs])

        def down(zs):
            return remote(acc.at[zs, 0], z_in.at[1, zs], (z - 1, y, x, c), z_send.at[zs], z_recv.at[1, zs])

        def each(dist, fn):
            if dist == 0:
                fn(z)
                return

            @pl.when(z - dist >= 0)
            def _():
                fn(z - dist)

            @pl.when(z + dist < zn)
            def _():
                fn(z + dist)

        order = list(range(zn - 1, -1, -1))

        def begin():
            at.barrier()
            for col in (3, 1, 2, 0):
                for dist in order:
                    def one(zs):
                        for cp in core(zs, col) + load(zs, col):
                            cp.start()
                    each(dist, one)

        def ready(zs, col):
            for cp in load(zs, col):
                cp.wait()
            for cp in core(zs, col):
                cp.wait_recv()

        def wide(*terms):
            total = terms[0].astype(f32)
            for t in terms[1:]:
                total = total + t.astype(f32)
            return total

        def diag(zs):
            ready(zs, 3)
            acc[zs, 3] = wide(acc[zs, 3], c_in[zs, 3]).astype(bf16)
            diag_x(zs).start()
            diag_y(zs).start()

        def sides(zs):
            ready(zs, 1)
            diag_y(zs).wait_recv()
            acc[zs, 1, :, lo] = wide(acc[zs, 1, :, lo], c_in[zs, 1, :, lo]).astype(bf16)
            acc[zs, 1, :, hi] = wide(acc[zs, 1, :, hi], c_in[zs, 1, :, hi], d_in[zs, :, hi]).astype(bf16)
            to_x(zs).start()
            ready(zs, 2)
            diag_x(zs).wait_recv()
            acc[zs, 2, :, lo] = wide(acc[zs, 2, :, lo], c_in[zs, 2, :, lo], d_in[zs, :, lo]).astype(bf16)
            acc[zs, 2, :, hi] = wide(acc[zs, 2, :, hi], c_in[zs, 2, :, hi]).astype(bf16)
            to_y(zs).start()

        def column(zs):
            ready(zs, 0)
            to_x(zs).wait_recv()
            to_y(zs).wait_recv()
            return wide(acc[zs, 0], c_in[zs, 0]) + wide(xy_in[0, zs], xy_in[1, zs])

        def pass_on(zs):
            total = column(zs)

            @pl.when(zs > z)
            def _():
                @pl.when(z > 0)
                def _():
                    up(zs).wait_recv()
                    acc[zs, 0] = (total + z_in[0, zs].astype(f32)).astype(bf16)

                @pl.when(z == 0)
                def _():
                    acc[zs, 0] = total.astype(bf16)
                up(zs).start()

            @pl.when(zs < z)
            def _():
                @pl.when(z < zn - 1)
                def _():
                    down(zs).wait_recv()
                    acc[zs, 0] = (total + z_in[1, zs].astype(f32)).astype(bf16)

                @pl.when(z == zn - 1)
                def _():
                    acc[zs, 0] = total.astype(bf16)
                down(zs).start()

        def finish():
            out_ref[...] = column(z)

            @pl.when(z > 0)
            def _():
                up(z).wait_recv()
                out_ref[...] += z_in[0, z].astype(f32)

            @pl.when(z < zn - 1)
            def _():
                down(z).wait_recv()
                out_ref[...] += z_in[1, z].astype(f32)

            def sent(zs):
                for col in range(4):
                    for cp in core(zs, col):
                        cp.wait_send()
                diag_x(zs).wait_send()
                diag_y(zs).wait_send()
                to_x(zs).wait_send()
                to_y(zs).wait_send()

            for dist in order:
                each(dist, sent)
                if dist:
                    each(dist, lambda zs: up(zs).wait_send())

        self.begin, self.finish = begin, finish
        self.diag = [functools.partial(each, dist, diag) for dist in order]
        self.sides = [functools.partial(each, dist, sides) for dist in order]
        self.pass_on = [functools.partial(each, dist, pass_on) for dist in order[:-1]]

    def plan(self, diag, sides, side_gap, pass_on, pass_gap):
        ticks = {0: [self.begin], diag: list(self.diag)}
        for k, fn in enumerate(self.sides):
            ticks.setdefault(sides + k * side_gap, []).append(fn)
        for k, fn in enumerate(self.pass_on):
            ticks.setdefault(pass_on + k * pass_gap, []).append(fn)
        return ticks

    @staticmethod
    def scratch(nd, rows, cols, parts):
        zn = nd // 2
        D, V = pltpu.SemaphoreType.DMA, pltpu.VMEM
        return [V((zn, 4, rows, cols), bf16), V((zn, 4, rows, cols), bf16), V((zn, rows, cols), bf16), V((2, zn, rows, cols), bf16),
                V((2, zn, rows, cols), bf16), D((zn, 4, parts)), D((zn, 4, parts)), D((zn, 4, parts))] + [D((zn,))] * 9 + [D((2, zn))]


def run_ticks(ticks, now, last):
    for tick, fns in ticks.items():
        if tick <= last:
            @pl.when(now == tick)
            def _(fns=fns):
                for fn in fns:
                    fn()


def run_rest(ticks, last):
    for tick, fns in sorted(ticks.items()):
        if tick > last:
            for fn in fns:
                fn()


def exchange_kernel(nd, nf, g_ref, out_ref, got, send, recv):
    n = nd * nf
    me = lax.axis_index("dp") * nf + lax.axis_index("fsdp")
    sem = pltpu.get_barrier_semaphore()

    def peer(k):
        return lax.rem(me + k, n)

    def greet(k, carry):
        pl.semaphore_signal(sem, inc=1, device_id=(peer(k) // nf, peer(k) % nf), device_id_type=MESH)
        return carry

    lax.fori_loop(1, n, greet, 0)
    pl.semaphore_wait(sem, n - 1)

    def copy(k):
        p = peer(k)
        return pltpu.make_async_remote_copy(src_ref=g_ref.at[p], dst_ref=got.at[k], send_sem=send.at[k], recv_sem=recv.at[k],
                                            device_id=(p // nf, p % nf), device_id_type=MESH)

    def begin(k, carry):
        copy(k).start()
        return carry

    lax.fori_loop(1, n, begin, 0)

    def add(k, total):
        copy(k).wait_recv()
        return total + got[k]

    out_ref[...] = lax.fori_loop(1, n, add, g_ref[me])

    def end(k, carry):
        copy(k).wait_send()
        return carry

    lax.fori_loop(1, n, end, 0)


def exchange(g, nd, nf, cid):
    n = nd * nf
    D = pltpu.SemaphoreType.DMA
    vm = pl.BlockSpec(memory_space=pltpu.VMEM)
    return pl.pallas_call(
        functools.partial(exchange_kernel, nd, nf),
        out_shape=jax.ShapeDtypeStruct(g.shape[1:], g.dtype),
        in_specs=[vm],
        out_specs=vm,
        scratch_shapes=[pltpu.VMEM(g.shape, g.dtype), D((n,)), D((n,))],
        compiler_params=pltpu.CompilerParams(collective_id=cid, has_side_effects=True),
    )(g)


def dot(a, b, dims=((1,), (0,)), precision=None):
    return lax.dot_general(a, b, (dims, ((), ())), preferred_element_type=f32, precision=precision)


def sigmoid(x):
    return 1.0 / (1.0 + jnp.exp(-x))


def conv_rows(ext, taps, masks, halo):
    rows = ext.shape[0] - halo
    width = 4
    v = ext[halo:]
    out = taps[4:5] + taps[3:4] * v
    for k in range(1, width):
        moved = pltpu.roll(ext, k, 0)[halo:]
        out = out + (taps[3 - k : 4 - k] * masks[:, k : k + 1]) * moved
    return out


def prep_kernel(bcdt_ref, taps_ref, heads_ref, m_ref, segc_ref, segr_ref,
                b_ref, c_ref, bt_ref, ct_ref, pre_ref, gm_ref, cum4_ref, cumr_ref, sc_ref, dt_ref):
    T = bcdt_ref.shape[0]
    nc = T // L
    N = b_ref.shape[1]
    H = dt_ref.shape[1]
    groups = cum4_ref.shape[0]
    taps = taps_ref[...]
    tri = (lax.broadcasted_iota(jnp.int32, (L, L), 0) >= lax.broadcasted_iota(jnp.int32, (L, L), 1))
    trif = tri.astype(f32)
    neg_rate = -jnp.exp(heads_ref[0:1, :H]) * LOG2E
    bias = heads_ref[1:2, :H]

    def chunk(c, carry):
        t0 = pl.multiple_of(c * L, L)
        here = pl.ds(t0, L)
        h0 = pl.multiple_of(jnp.maximum(t0 - 16, 0), 16)
        before = bcdt_ref[pl.ds(h0, 16), : 2 * N].astype(f32)
        v = bcdt_ref[here, : 2 * N].astype(f32)
        pre = conv_rows(jnp.concatenate([before, v], axis=0), taps, m_ref[here, :], 16)
        pre_ref[here, :] = pre
        act = pre * sigmoid(pre)
        b = act[:, :N]
        cc = act[:, N:]
        bb = b.astype(bf16)
        cb = cc.astype(bf16)
        b_ref[here, :] = bb
        c_ref[here, :] = cb
        bt_ref[:, here] = b.T.astype(bf16)
        ct_ref[:, here] = cc.T.astype(bf16)
        segc = segc_ref[here, 0:1]
        prev = segc_ref[here, 1:2]
        last = segc_ref[here, 2:3]
        same = segc == segr_ref[:, here]
        g = dot(cb, bb, ((1,), (1,)))
        gm_ref[pl.ds(c, 1)] = jnp.where(tri & same, g, 0.0)[None]
        raw = bcdt_ref[here, 2 * N : 2 * N + 128].astype(f32)[:, :H] + bias
        dt = jnp.maximum(raw, 0.0) + jnp.log1p(jnp.exp(-jnp.abs(raw)))
        a2 = neg_rate * dt
        cum = dot(trif, a2, precision=HIGHEST)
        end = cum[L - 1 : L]
        ein = jnp.where(segc == prev, jnp.exp2(cum), 0.0)
        lv = jnp.where(segc == last, jnp.exp2(end - cum), 0.0)
        dt_ref[here, :] = dt
        cumt = cum.T
        s0 = pl.multiple_of(c * (3 * L), L)
        for k in range(groups):
            cols = slice(HG * k, HG * (k + 1))
            cum4_ref[k, here, :] = cum[:, cols]
            cumr_ref[k, :, here] = cumt[cols]
            sc_ref[k, pl.ds(s0, L), :] = dt[:, cols].astype(bf16)
            sc_ref[k, pl.ds(s0 + L, L), :] = ein[:, cols].astype(bf16)
            sc_ref[k, pl.ds(s0 + 2 * L, L), :] = lv[:, cols].astype(bf16)
        return carry

    lax.fori_loop(0, nc, chunk, 0)


def prep(bcdt, taps, heads, masks, segc, segr, N, H):
    T = bcdt.shape[0]
    nc = T // L
    G = H // HG
    S = jax.ShapeDtypeStruct
    return pl.pallas_call(
        prep_kernel,
        out_shape=(S((T, N), bf16), S((T, N), bf16), S((N, T), bf16), S((N, T), bf16), S((T, 2 * N), f32),
                   S((nc, L, L), f32), S((G, T, HG), f32), S((G, HG, T), f32), S((G, 3 * T, HG), bf16), S((T, H), f32)),
        compiler_params=pltpu.CompilerParams(vmem_limit_bytes=60 << 20),
    )(bcdt, taps, heads, masks, segc, segr)


def lane_onehot(width, per):
    return (lax.broadcasted_iota(jnp.int32, (HG, width), 1) // per == lax.broadcasted_iota(jnp.int32, (HG, width), 0)).astype(bf16)


def half_masks(P):
    lane = lax.broadcasted_iota(jnp.int32, (1, 2 * P), 1)
    first = (lane < P).astype(f32)
    return first.astype(bf16), (1.0 - first).astype(bf16)


def decay(cum4, cumr, k):
    return jnp.exp2(jnp.minimum(cum4[:, k : k + 1] - cumr[k : k + 1, :], 0.0))


def fwd_kernel(u_ref, gate_ref, taps_ref, m_ref, b_ref, c_ref, bt_ref, gm_ref, cum4_ref, cumr_ref, sc_ref,
               gg_ref, ssq_ref, pre_ref, st_ref, state):
    T, W = u_ref.shape
    P = W // HG
    nc = T // L
    step = pl.program_id(0)
    taps = taps_ref[...]
    gain = taps[5:6]
    skip = taps[6:7]
    onehot = lane_onehot(W, P)
    ma, mb = half_masks(P)
    state[...] = jnp.zeros_like(state)

    @pl.when(step == 0)
    def _():
        ssq_ref[...] = jnp.zeros_like(ssq_ref)

    def chunk(c, carry):
        t0 = pl.multiple_of(c * L, L)
        here = pl.ds(t0, L)
        h0 = pl.multiple_of(jnp.maximum(t0 - 16, 0), 16)
        ext = jnp.concatenate([u_ref[pl.ds(h0, 16), :], u_ref[here, :]], axis=0).astype(f32)
        pre = conv_rows(ext, taps, m_ref[here, :], 16)
        pre_ref[here, :] = pre.astype(bf16)
        x = pre * sigmoid(pre)
        s0 = pl.multiple_of(c * (3 * L), L)
        exp = dot(sc_ref[0, pl.ds(s0, 3 * L), :], onehot)
        dtx, einx, lvx = exp[:L], exp[L : 2 * L], exp[2 * L :]
        xd = x * dtx
        xdb = xd.astype(bf16)
        gm = gm_ref[c]
        cum4 = cum4_ref[0, here, :]
        cumr = cumr_ref[0, :, here]
        sb = state[...].astype(bf16)
        st_ref[c] = sb
        inner = []
        for p in range(HG // 2):
            m0 = (decay(cum4, cumr, 2 * p) * gm).astype(bf16)
            m1 = (decay(cum4, cumr, 2 * p + 1) * gm).astype(bf16)
            xp = xdb[:, 2 * P * p : 2 * P * (p + 1)]
            inner.append(dot(jnp.concatenate([m0, m1], axis=1), jnp.concatenate([xp * ma, xp * mb], axis=0)))
        y = jnp.concatenate(inner, axis=1) + dot(c_ref[here, :], sb) * einx + skip * x
        state[...] = state[...] * einx[L - 1 : L] + dot(bt_ref[:, here], (xd * lvx).astype(bf16))
        gate = gate_ref[here, :].astype(f32)
        g = y * (gate * sigmoid(gate))
        gg_ref[here, :] = (g * gain).astype(bf16)
        g2 = g * g
        tot = g2[:, :128]
        for j in range(1, W // 128):
            tot = tot + g2[:, 128 * j : 128 * (j + 1)]
        ssq_ref[here, :] += tot
        return carry

    lax.fori_loop(0, nc, chunk, 0)


def fwd(u, gate, taps, masks, b, c, bt, gm, cum4, cumr, sc):
    T, E = gate.shape
    N = b.shape[1]
    G = cum4.shape[0]
    W = E // G
    nc = T // L
    S = jax.ShapeDtypeStruct
    col = lambda off: pl.BlockSpec((T, W), lambda g: (0, g + off))
    full = lambda a: pl.BlockSpec(a.shape, lambda g: (0,) * a.ndim)
    grp = lambda a: pl.BlockSpec((1,) + a.shape[1:], lambda g: (g, 0, 0))
    return pl.pallas_call(
        fwd_kernel,
        grid=(G,),
        in_specs=[col(0), col(0), pl.BlockSpec((8, W), lambda g: (0, g)), full(masks), full(b), full(c), full(bt), full(gm),
                  grp(cum4), grp(cumr), grp(sc)],
        out_specs=[col(0), pl.BlockSpec((T, 128), lambda g: (0, 0)), col(0), pl.BlockSpec((nc, N, W), lambda g: (0, 0, g))],
        out_shape=(S((T, E), bf16), S((T, 128), f32), S((T, E), bf16), S((nc, N, E), bf16)),
        scratch_shapes=[pltpu.VMEM((N, W), f32)],
        compiler_params=pltpu.CompilerParams(vmem_limit_bytes=60 << 20),
        cost_estimate=pl.CostEstimate(flops=T * E * (2 * L + 4 * N) * 2, bytes_accessed=T * E * 12, transcendentals=T * E * 4),
    )(u, gate, taps, masks, b, c, bt, gm, cum4, cumr, sc)


def bwd_kernel(*refs):
    bwd_body(lambda now: None, *refs)


def bwd_scatter_kernel(nd, nf, parts, *refs):
    g_refs, ins, outs = refs[:parts], refs[parts : parts + 15], refs[parts + 15 : parts + 23]
    own, comm = refs[parts + 23 : parts + 26], refs[parts + 26 :]
    sc = Scatter(nd, nf, g_refs, outs[7], *comm)
    nc = ins[0].shape[0] // L
    last = pl.num_programs(0) * nc - 1
    ticks = sc.plan(7, 12, 3, 28, 6)
    bwd_body(lambda now: run_ticks(ticks, now, BWD_TICKS), *ins, *outs[:7], *own)

    @pl.when(pl.program_id(0) == pl.num_programs(0) - 1)
    def _():
        run_rest(ticks, BWD_TICKS)
        sc.finish()


def bwd_body(tick, u_ref, gate_ref, pre_ref, dm_ref, rq_ref, taps_ref, m_ref, b_ref, c_ref, ct_ref, gm_ref, cum4_ref, cumr_ref, sc_ref, st_ref,
               dz_ref, dg_ref, db_ref, dc_ref, rs_ref, small_ref, kk_ref, ds, nxt, acc):
    T, W = u_ref.shape
    P = W // HG
    nc = T // L
    step = pl.program_id(0)
    taps = taps_ref[...]
    gain = taps[5:6]
    skip = taps[6:7]
    onehot = lane_onehot(W, P)
    ma, mb = half_masks(P)
    ds[...] = jnp.zeros_like(ds)
    nxt[...] = jnp.zeros_like(nxt)
    acc[...] = jnp.zeros_like(acc)

    @pl.when(step == 0)
    def _():
        dg_ref[...] = jnp.zeros_like(dg_ref)
        db_ref[...] = jnp.zeros_like(db_ref)
        dc_ref[...] = jnp.zeros_like(dc_ref)

    ri = lax.broadcasted_iota(jnp.int32, (4 * W, 16), 0)
    ci = lax.broadcasted_iota(jnp.int32, (4 * W, 16), 1)
    part = ri // W
    want = jnp.maximum(part - 1, 0) * HG + (ri % W) // P
    fold = (want == ci).astype(bf16)

    def eight(z):
        return jnp.sum(z.reshape(L // 8, 8, W), axis=0)

    def chunk(i, carry):
        tick(step * nc + i)
        c = nc - 1 - i
        t0 = pl.multiple_of(c * L, L)
        here = pl.ds(t0, L)
        u = u_ref[here, :].astype(f32)
        pre = pre_ref[here, :].astype(f32)
        sig = sigmoid(pre)
        x = pre * sig
        dsilu = sig + x * (1.0 - sig)
        s0 = pl.multiple_of(c * (3 * L), L)
        exp = dot(sc_ref[0, pl.ds(s0, 3 * L), :], onehot)
        dtx, einx, lvx = exp[:L], exp[L : 2 * L], exp[2 * L :]
        xdb = (x * dtx).astype(bf16)
        xd = xdb.astype(f32)
        gm = gm_ref[c]
        cum4 = cum4_ref[0, here, :]
        cumr = cumr_ref[0, :, here]
        sb = st_ref[c]
        es, ms, inner = [], [], []
        for p in range(HG // 2):
            e0 = decay(cum4, cumr, 2 * p)
            e1 = decay(cum4, cumr, 2 * p + 1)
            m0 = (e0 * gm).astype(bf16)
            m1 = (e1 * gm).astype(bf16)
            xp = xdb[:, 2 * P * p : 2 * P * (p + 1)]
            inner.append(dot(jnp.concatenate([m0, m1], axis=1), jnp.concatenate([xp * ma, xp * mb], axis=0)))
            es.append((e0, e1))
            ms.append((m0, m1))
        yn = jnp.concatenate(inner, axis=1) + dot(c_ref[here, :], sb) * einx
        y = yn + skip * x
        gate = gate_ref[here, :].astype(f32)
        sgate = sigmoid(gate)
        silu_g = gate * sgate
        g = y * silu_g
        r = rq_ref[here, 0:1]
        q = rq_ref[here, 1:2]
        dmr = dm_ref[here, :].astype(f32) * r
        dgg = gain * dmr - g * q
        dyb = (dgg * silu_g).astype(bf16)
        dy = dyb.astype(f32)
        dz_ref[0, here, :] = (dgg * y * (sgate + silu_g * (1.0 - sgate))).astype(bf16)
        dxi = []
        dgc = dg_ref[c]
        for p in range(HG // 2):
            cols = slice(2 * P * p, 2 * P * (p + 1))
            dp = dyb[:, cols]
            dstack = jnp.concatenate([dp * ma, dp * mb], axis=0)
            dmm = dot(dstack, xdb[:, cols], ((1,), (1,)))
            dgc = dgc + dmm[:L] * es[p][0] + dmm[L:] * es[p][1]
            dxi.append(dot(jnp.concatenate(ms[p], axis=0), dstack, ((0,), (0,))))
        dg_ref[c] = dgc
        dxi = jnp.concatenate(dxi, axis=1)
        dsn = ds[...]
        dsb = dsn.astype(bf16)
        dye = (dy * einx).astype(bf16)
        dc_ref[here, :] += dot(dye, sb, ((1,), (1,)))
        kept = einx[L - 1 : L]
        kk_ref[pl.ds(c, 1), :] = kept * jnp.sum(sb.astype(f32) * dsn, axis=0, keepdims=True)
        db_ref[here, :] += dot((xd * lvx).astype(bf16), dsb, ((1,), (1,)))
        dxe = dot(b_ref[here, :], dsb) * lvx
        ds[...] = dsn * kept + dot(ct_ref[:, here], dye)
        dxd = dxi + dxe
        r1 = dy * yn - xd * dxi
        r1h = r1.astype(bf16)
        r1l = (r1 - r1h.astype(f32)).astype(bf16)
        rs_ref[0, here, :] = dot(jnp.concatenate([r1h, r1l, (xd * dxe).astype(bf16), (x * dxd).astype(bf16)], axis=1), fold)
        dpre = (dxd * dtx + skip * dy) * dsilu
        ext = jnp.concatenate([dpre, nxt[...]], axis=0)
        nxt[...] = dpre[:8]
        du = taps[3:4] * dpre
        acc[0:8, :] += eight(dmr * g)
        acc[8:16, :] += eight(dy * x)
        acc[16:24, :] += eight(dpre)
        acc[24:32, :] += eight(dpre * u)
        mrows = m_ref[pl.ds(t0, L + 8), :]
        for k in range(1, 4):
            sk = pltpu.roll(ext * mrows[:, k : k + 1], L + 8 - k, 0)[:L]
            du = du + taps[3 - k : 4 - k] * sk
            acc[24 + 8 * k : 32 + 8 * k, :] += eight(sk * u)
        dz_ref[1, here, :] = du.astype(bf16)
        return carry

    lax.fori_loop(0, nc, chunk, 0)
    for j in range(7):
        small_ref[j : j + 1, :] = jnp.sum(acc[8 * j : 8 * j + 8, :], axis=0, keepdims=True)
    small_ref[7:8, :] = jnp.zeros((1, W), f32)


def bwd(half, halves, u, gate, pre, dm, rq, taps, masks, b, c, ct, gm, cum4, cumr, sc, st, comm=None):
    T, E = gate.shape
    N = b.shape[1]
    G = cum4.shape[0]
    W = E // G
    nc = T // L
    Gh = G // halves
    Eh = E // halves
    g0 = half * Gh
    S = jax.ShapeDtypeStruct
    col = pl.BlockSpec((T, W), lambda g: (0, g + g0))
    full = lambda a: pl.BlockSpec(a.shape, lambda g: (0,) * a.ndim)
    whole = lambda s: pl.BlockSpec(s, lambda g: (0,) * len(s))
    grp = lambda a: pl.BlockSpec((1,) + a.shape[1:], lambda g: (g + g0, 0, 0))
    in_specs = [col, col, col, col, full(rq), pl.BlockSpec((8, W), lambda g: (0, g + g0)), full(masks), full(b), full(c),
                full(ct), full(gm), grp(cum4), grp(cumr), grp(sc), pl.BlockSpec((nc, N, W), lambda g: (0, 0, g + g0))]
    out_specs = [pl.BlockSpec((2, T, W), lambda g: (0, 0, g)), whole((nc, L, L)), whole((T, N)), whole((T, N)),
                 pl.BlockSpec((1, T, 16), lambda g: (g, 0, 0)), pl.BlockSpec((8, W), lambda g: (0, g)), pl.BlockSpec((nc, W), lambda g: (0, g))]
    out_shape = [S((2, T, Eh), bf16), S((nc, L, L), f32), S((T, N), f32), S((T, N), f32), S((Gh, T, 16), f32), S((8, Eh), f32), S((nc, Eh), f32)]
    scratch = [pltpu.VMEM((N, W), f32), pltpu.VMEM((8, W), f32), pltpu.VMEM((56, W), f32)]
    kernel, first, params = bwd_kernel, (), {}
    if comm:
        nd, nf, cid, first = comm
        rows, cols = first[0].shape[1], sum(g.shape[2] for g in first)
        kernel = functools.partial(bwd_scatter_kernel, nd, nf, len(first))
        in_specs = [pl.BlockSpec(memory_space=pl.ANY)] * len(first) + in_specs
        out_specs.append(whole((rows, cols)))
        out_shape.append(S((rows, cols), f32))
        scratch += Scatter.scratch(nd, rows, cols, len(first))
        params = dict(collective_id=cid, has_side_effects=True)
    return pl.pallas_call(
        kernel,
        grid=(Gh,),
        in_specs=in_specs,
        out_specs=out_specs,
        out_shape=out_shape,
        scratch_shapes=scratch,
        compiler_params=pltpu.CompilerParams(vmem_limit_bytes=60 << 20, **params),
        cost_estimate=pl.CostEstimate(flops=T * Eh * (8 * L + 12 * N), bytes_accessed=T * Eh * 16, transcendentals=T * Eh * 4),
    )(*first, u, gate, pre, dm, rq, taps, masks, b, c, ct, gm, cum4, cumr, sc, st)


def post_kernel(bcdt_ref, pre_ref, taps_ref, heads_ref, m_ref, segc_ref, segr_ref, b_ref, c_ref, dg0_ref, db0_ref, dc0_ref, rs0_ref, dg1_ref, db1_ref, dc1_ref, rs1_ref, kk_ref, dt_ref,
                out_ref, small_ref, hs_ref, nxt, acc, hacc):
    T = bcdt_ref.shape[0]
    nc = T // L
    N = b_ref.shape[1]
    H = dt_ref.shape[1]
    G = H // HG
    taps = taps_ref[...]
    tri = (lax.broadcasted_iota(jnp.int32, (L, L), 0) >= lax.broadcasted_iota(jnp.int32, (L, L), 1))
    upper = (lax.broadcasted_iota(jnp.int32, (L, L), 0) <= lax.broadcasted_iota(jnp.int32, (L, L), 1)).astype(f32)
    strict = 1.0 - upper
    rate = -jnp.exp(heads_ref[0:1, :H])
    bias = heads_ref[1:2, :H]
    nxt[...] = jnp.zeros_like(nxt)
    acc[...] = jnp.zeros_like(acc)
    hacc[...] = jnp.zeros_like(hacc)

    def eight(z):
        return jnp.sum(z.reshape(L // 8, 8, z.shape[1]), axis=0)

    def chunk(i, carry):
        c = nc - 1 - i
        t0 = pl.multiple_of(c * L, L)
        here = pl.ds(t0, L)
        same = segc_ref[here, 0:1] == segr_ref[:, here]
        dg = jnp.where(tri & same, dg0_ref[c] + dg1_ref[c], 0.0)
        dgb = dg.astype(bf16)
        dcv = dc0_ref[here, :] + dc1_ref[here, :] + dot(dgb, b_ref[here, :])
        dbv = db0_ref[here, :] + db1_ref[here, :] + dot(dg.T.astype(bf16), c_ref[here, :])
        pre = pre_ref[here, :]
        sig = sigmoid(pre)
        dpre = jnp.concatenate([dbv, dcv], axis=1) * (sig + pre * sig * (1.0 - sig))
        v = bcdt_ref[here, : 2 * N].astype(f32)
        ext = jnp.concatenate([dpre, nxt[...]], axis=0)
        nxt[...] = dpre[:8]
        dv = taps[3:4] * dpre
        acc[0:8, :] += eight(dpre)
        acc[8:16, :] += eight(dpre * v)
        mrows = m_ref[pl.ds(t0, L + 8), :]
        for k in range(1, 4):
            sk = pltpu.roll(ext * mrows[:, k : k + 1], L + 8 - k, 0)[:L]
            dv = dv + taps[3 - k : 4 - k] * sk
            acc[8 + 8 * k : 16 + 8 * k, :] += eight(sk * v)
        out_ref[here, : 2 * N] = dv.astype(bf16)
        r1 = jnp.concatenate([r[k, here, 0:HG] for r in (rs0_ref, rs1_ref) for k in range(G // 2)], axis=1)
        r2 = jnp.concatenate([r[k, here, HG : 2 * HG] for r in (rs0_ref, rs1_ref) for k in range(G // 2)], axis=1)
        r3 = jnp.concatenate([r[k, here, 2 * HG : 3 * HG] for r in (rs0_ref, rs1_ref) for k in range(G // 2)], axis=1)
        da = dot(upper, r1, precision=HIGHEST) + dot(strict, r2, precision=HIGHEST) + kk_ref[pl.ds(c, 1), :]
        dt = dt_ref[here, :]
        raw = bcdt_ref[here, 2 * N : 2 * N + 128].astype(f32)[:, :H] + bias
        ddt = (r3 + da * rate) * sigmoid(raw)
        hacc[0:8, :] += eight(da * rate * dt)
        hacc[8:16, :] += eight(ddt)
        out_ref[here, 2 * N :] = jnp.concatenate([ddt, jnp.zeros((L, out_ref.shape[1] - 2 * N - H), f32)], axis=1).astype(bf16)
        return carry

    lax.fori_loop(0, nc, chunk, 0)
    for j in range(5):
        small_ref[j : j + 1, :] = jnp.sum(acc[8 * j : 8 * j + 8, :], axis=0, keepdims=True)
    small_ref[5:8, :] = jnp.zeros((3, 2 * N), f32)
    for j in range(2):
        hs_ref[j : j + 1, :] = jnp.sum(hacc[8 * j : 8 * j + 8, :], axis=0, keepdims=True)


def post(bcdt, pre, taps, heads, masks, segc, segr, b, c, first, second, kk, dt):
    T = bcdt.shape[0]
    N = b.shape[1]
    H = dt.shape[1]
    S = jax.ShapeDtypeStruct
    return pl.pallas_call(
        post_kernel,
        out_shape=(S(bcdt.shape, bf16), S((8, 2 * N), f32), S((2, H), f32)),
        scratch_shapes=[pltpu.VMEM((8, 2 * N), f32), pltpu.VMEM((40, 2 * N), f32), pltpu.VMEM((16, H), f32)],
        compiler_params=pltpu.CompilerParams(vmem_limit_bytes=60 << 20),
    )(bcdt, pre, taps, heads, masks, segc, segr, b, c, *first, *second, kk, dt)


KT = 384


def tail_kernel(nd, nf, parts, *refs):
    g_refs, refs = refs[:parts], refs[parts:]
    dz0_ref, dz1_ref, dbc_ref, wg_ref, wa_ref, gg_ref, wo_ref, hid_ref, go_ref, r_ref, gain_ref, sum_ref, gin_ref, out_ref, dn_ref = refs[:15]
    lhs, rhs, acc, dn = refs[15:19]
    sc = Scatter(nd, nf, g_refs, sum_ref, *refs[19:])
    T, D = hid_ref.shape
    step = pl.program_id(0)
    steps = pl.num_programs(0)
    nk = (steps - 1) // 3
    q = nk // 2
    ticks = sc.plan(3, 5, 2, 14, 3)
    run_ticks(ticks, step, TAIL_TICKS)

    def load(cond, ref, src):
        @pl.when(cond)
        def _():
            ref[...] = src[0] if len(src.shape) == 3 else src[...]

    gate_part = step < nk
    u_part = (step >= nk) & (step < 2 * nk)
    bc_part = step == 2 * nk
    out_part = step > 2 * nk
    load((step < 2 * nk) & (step % nk < q), lhs, dz0_ref)
    load((step < 2 * nk) & (step % nk >= q), lhs, dz1_ref)
    load(bc_part, lhs, dbc_ref)
    load(out_part, lhs, gg_ref)
    load(gate_part, rhs, wg_ref)
    load(u_part | bc_part, rhs, wa_ref)

    @pl.when((step == 0) | (step == 2 * nk + 1))
    def _():
        acc[...] = jnp.zeros_like(acc)

    BN = 256

    @pl.when(step <= 2 * nk)
    def _():
        def block(j, carry):
            cols = pl.ds(pl.multiple_of(j * BN, BN), BN)
            acc[:, cols] += dot(lhs[...], rhs[cols, :], ((1,), (1,)))
            return carry
        lax.fori_loop(0, D // BN, block, 0)

    @pl.when(out_part)
    def _():
        def block(j, carry):
            cols = pl.ds(pl.multiple_of(j * BN, BN), BN)
            acc[:, cols] += dot(lhs[...], wo_ref[:, cols])
            return carry
        lax.fori_loop(0, D // BN, block, 0)

    @pl.when(step == 2 * nk)
    def _():
        gain = gain_ref[...]
        dn[...] = jnp.zeros_like(dn)

        def rows_of(i, carry):
            here = pl.ds(pl.multiple_of(i * 64, 64), 64)
            rows = hid_ref[here, :].astype(f32)
            rinv = lax.rsqrt(jnp.mean(rows * rows, axis=-1, keepdims=True) + EPS)
            xhat = rows * rinv
            bn = acc[here, :]
            prod = bn * xhat
            dn[...] += jnp.sum(prod.reshape(8, 8, D), axis=0)
            mean = jnp.mean(prod * gain, axis=-1, keepdims=True)
            gin_ref[here, :] = (go_ref[here, :].astype(f32) + rinv * (bn * gain - xhat * mean)).astype(bf16)
            return carry
        lax.fori_loop(0, T // 64, rows_of, 0)
        dn_ref[...] = jnp.sum(dn[...], axis=0, keepdims=True)

    @pl.when(step == steps - 1)
    def _():
        def rows_of(i, carry):
            here = pl.ds(pl.multiple_of(i * 64, 64), 64)
            out_ref[here, :] = (hid_ref[here, :].astype(f32) + r_ref[here, :] * acc[here, :]).astype(bf16)
            return carry
        lax.fori_loop(0, T // 64, rows_of, 0)
        run_rest(ticks, TAIL_TICKS)
        sc.finish()


def tail(nd, nf, cid, gs, dz0, dz1, dbcdt, full_gate, full_a, gg, full_out, hidden, grad_out, r, norm_gain):
    T, D = hidden.shape
    E = full_out.shape[0]
    nk, q = E // KT, E // KT // 2
    rows, cols = gs[0].shape[1], sum(g.shape[2] for g in gs)
    S = jax.ShapeDtypeStruct
    any_ = pl.BlockSpec(memory_space=pl.ANY)
    whole = lambda s: pl.BlockSpec(s, lambda k: (0,) * len(s), pipeline_mode=pl.Buffered(1))
    clip = jnp.clip
    first = pl.BlockSpec((1, T, KT), lambda k: (jnp.minimum(k // nk, 1), 0, clip(jnp.minimum(k, 2 * nk - 1) % nk, 0, q - 1)))
    second = pl.BlockSpec((1, T, KT), lambda k: (jnp.minimum(k // nk, 1), 0, clip(jnp.minimum(k, 2 * nk - 1) % nk - q, 0, q - 1)))
    return pl.pallas_call(
        functools.partial(tail_kernel, nd, nf, len(gs)),
        grid=(3 * nk + 1,),
        in_specs=[any_] * len(gs) + [
            first, second, whole((T, KT)),
            pl.BlockSpec((D, KT), lambda k: (0, clip(k, 0, nk - 1))), pl.BlockSpec((D, KT), lambda k: (0, clip(k - nk, 0, nk))),
            pl.BlockSpec((T, KT), lambda k: (0, clip(k - 2 * nk - 1, 0, nk - 1))), pl.BlockSpec((KT, D), lambda k: (clip(k - 2 * nk - 1, 0, nk - 1), 0)),
            whole((T, D)), whole((T, D)), whole((T, 1)), whole((1, D))],
        out_specs=[whole((rows, cols)), whole((T, D)), whole((T, D)), whole((1, D))],
        out_shape=(S((rows, cols), f32), S((T, D), bf16), S((T, D), bf16), S((1, D), f32)),
        scratch_shapes=[pltpu.VMEM((T, KT), bf16), pltpu.VMEM((D, KT), bf16), pltpu.VMEM((T, D), f32), pltpu.VMEM((8, D), f32)]
        + Scatter.scratch(nd, rows, cols, len(gs)),
        compiler_params=pltpu.CompilerParams(collective_id=cid, has_side_effects=True, vmem_limit_bytes=63 << 20),
        cost_estimate=pl.CostEstimate(flops=2 * T * D * 3 * E, bytes_accessed=8 * D * E, transcendentals=0),
    )(*gs, dz0, dz1, dbcdt, full_gate, full_a, gg, full_out, hidden, grad_out, r, norm_gain)


def layer(nd, nf, hidden, grad_out, seg, shard_a, shard_gate, shard_out, head_params, sizes):
    n = nd * nf
    E, N, H, K1, S = sizes
    T, D = hidden.shape
    wide = 2 * N + 128
    full_gate = lax.all_gather(shard_gate, AXES, axis=0, tiled=True)
    full_out = lax.all_gather(shard_out, AXES, axis=0, tiled=True)
    full_a = gather_rows(shard_a, nd, nf, 0)
    off = E + 2 * N + H
    flat = full_a[:, :, off : off + S].reshape(n, -1)
    ncol, nrow, ngate = (E + 2 * N) // n, D // n, E // n
    conv = flat[:, : K1 * ncol].reshape(n, K1, ncol).transpose(1, 0, 2).reshape(K1, n * ncol).astype(f32)
    norm_gain = flat[:, K1 * ncol : K1 * ncol + nrow].reshape(-1).astype(f32)
    gate_gain = flat[:, K1 * ncol + nrow : K1 * ncol + nrow + ngate].reshape(-1).astype(f32)
    full_a = full_a.reshape(D, E + wide)
    rows = hidden.astype(f32)
    rinv = lax.rsqrt(jnp.mean(rows * rows, axis=-1, keepdims=True) + EPS)
    xhat = rows * rinv
    normed = (xhat * norm_gain).astype(bf16)
    ubc = dot(normed, full_a).astype(bf16)
    gate = dot(normed, full_gate).astype(bf16)
    bcdt = ubc[:, E:]
    pos = jnp.arange(T, dtype=jnp.int32)
    masks = jnp.stack([jnp.ones((T,), f32)] + [((jnp.roll(seg, k) == seg) & (pos >= k)).astype(f32) for k in range(1, 4)], axis=1)
    lastid = seg[L - 1 :: L]
    previd = jnp.concatenate([jnp.full((1,), -1, jnp.int32), lastid[:-1]])
    segc = jnp.stack([seg, jnp.repeat(previd, L), jnp.repeat(lastid, L)], axis=1)
    segr = seg[None, :]
    taps_u = jnp.concatenate([conv[:, :E], gate_gain[None], jnp.repeat(head_params[2], E // H)[None], jnp.zeros((1, E), f32)], axis=0)
    taps_bc = jnp.concatenate([conv[:, E:], jnp.zeros((3, 2 * N), f32)], axis=0)
    heads_p = jnp.pad(head_params, ((0, 5), (0, 128 - H)))
    b, c, bt, ct, pre_bc, gm, cum4, cumr, sc, dt = prep(bcdt, taps_bc, heads_p, masks, segc, segr, N, H)
    gg, ssq, pre, st = fwd(ubc, gate, taps_u, masks, b, c, bt, gm, cum4, cumr, sc)
    r = lax.rsqrt(jnp.sum(ssq, axis=1, keepdims=True) / E + EPS)
    gos = (grad_out.astype(f32) * r).astype(bf16)
    g_out = dot(gg, gos, ((0,), (0,))).astype(bf16)
    s_out = lax.psum_scatter(g_out, AXES, scatter_dimension=0, tiled=True).astype(f32)
    dm = dot(grad_out, full_out, ((1,), (1,))).astype(bf16)
    s = jnp.sum(gg.astype(f32) * dm.astype(f32), axis=1, keepdims=True)
    rq = jnp.concatenate([r, r * r * r * s / E], axis=1)
    masks8 = jnp.pad(masks, ((0, 8), (0, 0)))
    shape = lambda g: g.reshape(n, D // n, -1)
    grad = lambda dz: shape(dot(normed, dz, ((0,), (0,))).astype(bf16))
    back = functools.partial(bwd, u=ubc, gate=gate, pre=pre, dm=dm, rq=rq, taps=taps_u, masks=masks8, b=b, c=c, ct=ct, gm=gm, cum4=cum4,
                             cumr=cumr, sc=sc, st=st)
    dz0, dg0, db0, dc0, rs0, small0, kk0 = back(0, 2)
    dz1, dg1, db1, dc1, rs1, small1, kk1, sum0 = back(1, 2, comm=(nd, nf, 3, (grad(dz0[0]), grad(dz0[1]))))
    small = jnp.concatenate([small0, small1], axis=1)
    kk = jnp.concatenate([kk0, kk1], axis=1)
    kkh = jnp.sum(kk.reshape(kk.shape[0], H, E // H), axis=2)
    dbcdt, small_bc, hs = post(bcdt, pre_bc, taps_bc, heads_p, masks8, segc, segr, b, c, (dg0, db0, dc0, rs0), (dg1, db1, dc1, rs1), kkh, dt)
    sum1, grad_in, output, d_norm = tail(nd, nf, 1, (grad(dz1[0]), grad(dz1[1]), grad(dbcdt)), dz0, dz1, dbcdt, full_gate, full_a, gg, full_out,
                                         hidden, grad_out, r, norm_gain[None])
    d_conv = jnp.concatenate([jnp.stack([small[6], small[5], small[4], small[3], small[2]]),
                              jnp.stack([small_bc[4], small_bc[3], small_bc[2], small_bc[1], small_bc[0]])], axis=1)
    d_heads = jnp.concatenate([hs, jnp.sum(small[1].reshape(1, H, E // H), axis=2)], axis=0)
    mine = jnp.concatenate([d_conv.reshape(K1, n, ncol).transpose(1, 0, 2).reshape(n, -1), d_norm.reshape(n, -1), small[0].reshape(n, -1),
                            jnp.broadcast_to(d_heads.reshape(1, -1), (n, d_heads.size))], axis=1)
    tiles = -(-mine.shape[1] // 1024)
    mine = jnp.pad(mine, ((0, 0), (0, tiles * 1024 - mine.shape[1]))).reshape(n, tiles * 8, 128)
    tot = exchange(mine, nd, nf, 2).reshape(-1)
    cut = [0, K1 * ncol, nrow, ngate, d_heads.size]
    ends = [sum(cut[: k + 1]) for k in range(5)]
    t_conv, t_norm, t_gate, t_heads = (tot[ends[k] : ends[k + 1]] for k in range(4))
    Eh = E // 2
    s_zx = jnp.concatenate([sum0[:, :Eh], sum1[:, :Eh], sum0[:, Eh:], sum1[:, Eh : 2 * Eh]], axis=1)
    return (output, grad_in, s_zx, sum1[:, 2 * Eh : 2 * Eh + 2 * N], sum1[:, 2 * Eh + 2 * N : 2 * Eh + 2 * N + H], s_out,
            t_conv.reshape(K1, ncol), t_norm, t_gate, t_heads.reshape(d_heads.shape))


def per_device(nd, nf, hidden, grad_out, segment_ids, w_zx, w_bc, w_dt, w_out, conv_params, norm_gain, gate_gain, head_params):
    n = nd * nf
    E, N2, H = w_out.shape[0] * n, w_bc.shape[1], w_dt.shape[1]
    rows = w_zx.shape[0]
    small = jnp.concatenate([conv_params.reshape(-1), norm_gain, gate_gain])
    S = -(-small.shape[0] // rows)
    assert S + H <= 128
    small = jnp.pad(small, (0, S * rows - small.shape[0])).reshape(rows, S)
    shard_a = jnp.concatenate([w_zx[:, E:], w_bc, w_dt, small, jnp.zeros((rows, 128 - H - S), bf16)], axis=1)
    return layer(nd, nf, hidden, grad_out, segment_ids, shard_a, w_zx[:, :E], w_out, head_params, (E, N2 // 2, H, conv_params.shape[0], S))


def solution(mesh):
    row, col, vec, rep = P(AXES, None), P(None, AXES), P(AXES), P()
    return jax.shard_map(
        functools.partial(per_device, mesh.shape["dp"], mesh.shape["fsdp"]),
        mesh=mesh,
        in_specs=(row, row, vec, row, row, row, row, col, vec, vec, rep),
        out_specs=(row, row, row, row, row, row, col, vec, vec, rep),
        check_vma=False,
    )
```

```python
import functools
import jax
import jax.numpy as jnp
from jax import lax
from jax.experimental import pallas as pl
from jax.experimental.pallas import tpu as pltpu
from jax.sharding import PartitionSpec as P

EPS = 1e-05
L = 128
HG = 4
LOG2E = 1.4426950408889634
BWD_TICKS = 44
TAIL_TICKS = 44
TAIL_PLAN = (8, 14, 4, 28, 4)
bf16, f32 = jnp.bfloat16, jnp.float32
HIGHEST = lax.Precision.HIGHEST


AXES = ("dp", "fsdp")
MESH = pl.DeviceIdType.MESH


class Place:
    def __init__(self, nd, nf):
        self.zn, self.nf = nd // 2, nf
        d, f = lax.axis_index("dp"), lax.axis_index("fsdp")
        self.z, self.y = d // 2, d % 2
        self.x, self.c = f // 2, f % 2

    def dev(self, z, y, x, c):
        return (z * 2 + y, x * 2 + c)

    def idx(self, z, y, x, c):
        return (z * 2 + y) * self.nf + x * 2 + c

    def barrier(self):
        z, y, x, c, zn = self.z, self.y, self.x, self.c, self.zn
        sem = pltpu.get_barrier_semaphore()
        for there in ((z, y, 1 - x, c), (z, 1 - y, x, c), (z, y, x, 1 - c)):
            pl.semaphore_signal(sem, inc=1, device_id=self.dev(*there), device_id_type=MESH)

        @pl.when(z > 0)
        def _():
            pl.semaphore_signal(sem, inc=1, device_id=self.dev(z - 1, y, x, c), device_id_type=MESH)

        @pl.when(z < zn - 1)
        def _():
            pl.semaphore_signal(sem, inc=1, device_id=self.dev(z + 1, y, x, c), device_id_type=MESH)

        pl.semaphore_wait(sem, 3 + (z + zn - 1) // zn + (2 * zn - 2 - z) // zn)


def gather_kernel(nd, nf, src_ref, out_ref, own_sem, z_send, z_recv, x_send, x_recv, y_send, y_recv, dx_send, dx_recv, dy_send, dy_recv, c_send, c_recv):
    at = Place(nd, nf)
    z, y, x, c, zn = at.z, at.y, at.x, at.c, at.zn
    half = out_ref.shape[2] // 256 * 128
    lo, hi = pl.ds(0, half), pl.ds(half, out_ref.shape[2] - half)
    at.barrier()

    def copy(block, to, send, recv, cols=None, src=None):
        ref = out_ref.at[block] if cols is None else out_ref.at[block, :, cols]
        return pltpu.make_async_remote_copy(src_ref=ref if src is None else src, dst_ref=ref, send_sem=send, recv_sem=recv,
                                            device_id=at.dev(*to), device_id_type=MESH)

    def block(zs, col):
        return at.idx(zs, 1 - y if col & 2 else y, 1 - x if col & 1 else x, c)

    def up(zs, src=None):
        return copy(block(zs, 0), (z + 1, y, x, c), z_send.at[0, zs], z_recv.at[zs], src=src)

    def down(zs, src=None):
        return copy(block(zs, 0), (z - 1, y, x, c), z_send.at[1, zs], z_recv.at[zs], src=src)

    def to_x(zs, src=None):
        return copy(block(zs, 0), (z, y, 1 - x, c), x_send.at[zs], x_recv.at[zs], src=src)

    def to_y(zs, src=None):
        return copy(block(zs, 0), (z, 1 - y, x, c), y_send.at[zs], y_recv.at[zs], src=src)

    def diag_y(zs):
        return copy(block(zs, 1), (z, 1 - y, x, c), dy_send.at[zs], dy_recv.at[zs], lo)

    def diag_x(zs):
        return copy(block(zs, 2), (z, y, 1 - x, c), dx_send.at[zs], dx_recv.at[zs], hi)

    def to_core(zs, col, src=None):
        return copy(block(zs, col), (z, y, x, 1 - c), c_send.at[zs, col], c_recv.at[zs, col], src=src)

    own = pltpu.make_async_copy(src_ref, out_ref.at[block(z, 0)], own_sem)
    own.start()

    @pl.when(z < zn - 1)
    def _():
        up(z, src_ref).start()

    @pl.when(z > 0)
    def _():
        down(z, src_ref).start()

    to_x(z, src_ref).start()
    to_y(z, src_ref).start()
    to_core(z, 0, src_ref).start()

    def each(dist, fn):
        if dist == 0:
            fn(z, 0)
            return

        @pl.when(z - dist >= 0)
        def _():
            fn(z - dist, 1)

        @pl.when(z + dist < zn)
        def _():
            fn(z + dist, -1)

    def from_z(zs, way):
        copy(block(zs, 0), (z, y, x, c), z_send.at[0, zs], z_recv.at[zs]).wait_recv()
        if way > 0:
            @pl.when(z < zn - 1)
            def _():
                up(zs).start()
        else:
            @pl.when(z > 0)
            def _():
                down(zs).start()
        to_x(zs).start()
        to_y(zs).start()
        to_core(zs, 0).start()

    def from_xy(zs, way):
        to_x(zs).wait_recv()
        diag_y(zs).start()
        to_core(zs, 1).start()
        to_y(zs).wait_recv()
        diag_x(zs).start()
        to_core(zs, 2).start()

    def from_diag(zs, way):
        diag_y(zs).wait_recv()
        diag_x(zs).wait_recv()
        to_core(zs, 3).start()

    for dist in range(zn):
        if dist:
            each(dist, from_z)
        each(dist, from_xy)
    for dist in range(zn):
        each(dist, from_diag)
    own.wait()

    def sent(zs, way):
        for col in range(4):
            to_core(zs, col).wait_recv()
            to_core(zs, col).wait_send()
        to_x(zs).wait_send()
        to_y(zs).wait_send()
        diag_x(zs).wait_send()
        diag_y(zs).wait_send()
        if way >= 0:
            @pl.when(z < zn - 1)
            def _():
                up(zs).wait_send()
        if way <= 0:
            @pl.when(z > 0)
            def _():
                down(zs).wait_send()

    for dist in range(zn):
        each(dist, sent)


def gather_rows(shard, nd, nf, cid):
    zn = nd // 2
    D = pltpu.SemaphoreType.DMA
    return pl.pallas_call(
        functools.partial(gather_kernel, nd, nf),
        out_shape=jax.ShapeDtypeStruct((nd * nf,) + shard.shape, shard.dtype),
        in_specs=[pl.BlockSpec(memory_space=pl.ANY)],
        out_specs=pl.BlockSpec(memory_space=pl.ANY),
        scratch_shapes=[D(()), D((2, zn)), D((zn,)), D((zn,)), D((zn,)), D((zn,)), D((zn,)), D((zn,)), D((zn,)), D((zn,)), D((zn,)),
                        D((zn, 4)), D((zn, 4))],
        compiler_params=pltpu.CompilerParams(collective_id=cid, has_side_effects=True),
    )(shard)


class Scatter:
    def __init__(self, nd, nf, g_refs, out_ref, acc, c_in, d_in, xy_in, z_in,
                 load_sem, c_send, c_recv, dx_send, dx_recv, dy_send, dy_recv, x_send, x_recv, y_send, y_recv, z_send, z_recv):
        at = Place(nd, nf)
        z, y, x, c, zn = at.z, at.y, at.x, at.c, at.zn
        cols = out_ref.shape[1]
        offs = [sum(r.shape[2] for r in g_refs[:k]) for k in range(len(g_refs))]
        half = cols // 256 * 128
        lo, hi = pl.ds(0, half), pl.ds(half, cols - half)

        def idx(zs, col, core):
            return at.idx(zs, 1 - y if col & 2 else y, 1 - x if col & 1 else x, core)

        def remote(src, dst, to, send, recv):
            return pltpu.make_async_remote_copy(src_ref=src, dst_ref=dst, send_sem=send, recv_sem=recv, device_id=at.dev(*to), device_id_type=MESH)

        def load(zs, col):
            return [pltpu.make_async_copy(r.at[idx(zs, col, c)], acc.at[zs, col, :, pl.ds(o, r.shape[2])], load_sem.at[zs, col, k])
                    for k, (r, o) in enumerate(zip(g_refs, offs))]

        def core(zs, col):
            return [remote(r.at[idx(zs, col, 1 - c)], c_in.at[zs, col, :, pl.ds(o, r.shape[2])], (z, y, x, 1 - c),
                           c_send.at[zs, col, k], c_recv.at[zs, col, k])
                    for k, (r, o) in enumerate(zip(g_refs, offs))]

        def diag_x(zs):
            return remote(acc.at[zs, 3, :, lo], d_in.at[zs, :, lo], (z, y, 1 - x, c), dx_send.at[zs], dx_recv.at[zs])

        def diag_y(zs):
            return remote(acc.at[zs, 3, :, hi], d_in.at[zs, :, hi], (z, 1 - y, x, c), dy_send.at[zs], dy_recv.at[zs])

        def to_x(zs):
            return remote(acc.at[zs, 1], xy_in.at[0, zs], (z, y, 1 - x, c), x_send.at[zs], x_recv.at[zs])

        def to_y(zs):
            return remote(acc.at[zs, 2], xy_in.at[1, zs], (z, 1 - y, x, c), y_send.at[zs], y_recv.at[zs])

        def up(zs):
            return remote(acc.at[zs, 0], z_in.at[zs + 1], (z + 1, y, x, c), z_send.at[zs], z_recv.at[0, zs])

        def down(zs):
            return remote(acc.at[zs, 0], z_in.at[zs], (z - 1, y, x, c), z_send.at[zs], z_recv.at[1, zs])

        def each(dist, fn):
            if dist == 0:
                fn(z)
                return

            @pl.when(z - dist >= 0)
            def _():
                fn(z - dist)

            @pl.when(z + dist < zn)
            def _():
                fn(z + dist)

        order = list(range(zn - 1, -1, -1))

        def begin():
            at.barrier()
            for col in (3, 1, 2, 0):
                for dist in order:
                    def one(zs):
                        for cp in core(zs, col) + load(zs, col):
                            cp.start()
                    each(dist, one)

        def ready(zs, col):
            for cp in load(zs, col):
                cp.wait()
            for cp in core(zs, col):
                cp.wait_recv()

        def wide(*terms):
            total = terms[0].astype(f32)
            for t in terms[1:]:
                total = total + t.astype(f32)
            return total

        def diag(zs):
            ready(zs, 3)
            acc[zs, 3] = wide(acc[zs, 3], c_in[zs, 3]).astype(bf16)
            diag_x(zs).start()
            diag_y(zs).start()

        def sides(zs):
            ready(zs, 1)
            diag_y(zs).wait_recv()
            acc[zs, 1, :, lo] = wide(acc[zs, 1, :, lo], c_in[zs, 1, :, lo]).astype(bf16)
            acc[zs, 1, :, hi] = wide(acc[zs, 1, :, hi], c_in[zs, 1, :, hi], d_in[zs, :, hi]).astype(bf16)
            to_x(zs).start()
            ready(zs, 2)
            diag_x(zs).wait_recv()
            acc[zs, 2, :, lo] = wide(acc[zs, 2, :, lo], c_in[zs, 2, :, lo], d_in[zs, :, lo]).astype(bf16)
            acc[zs, 2, :, hi] = wide(acc[zs, 2, :, hi], c_in[zs, 2, :, hi]).astype(bf16)
            to_y(zs).start()

        def column(zs):
            ready(zs, 0)
            to_x(zs).wait_recv()
            to_y(zs).wait_recv()
            return wide(acc[zs, 0], c_in[zs, 0]) + wide(xy_in[0, zs], xy_in[1, zs])

        def pass_on(zs):
            total = column(zs)

            @pl.when(zs > z)
            def _():
                @pl.when(z > 0)
                def _():
                    up(zs).wait_recv()
                    acc[zs, 0] = (total + z_in[zs + 1].astype(f32)).astype(bf16)

                @pl.when(z == 0)
                def _():
                    acc[zs, 0] = total.astype(bf16)
                up(zs).start()

            @pl.when(zs < z)
            def _():
                @pl.when(z < zn - 1)
                def _():
                    down(zs).wait_recv()
                    acc[zs, 0] = (total + z_in[zs].astype(f32)).astype(bf16)

                @pl.when(z == zn - 1)
                def _():
                    acc[zs, 0] = total.astype(bf16)
                down(zs).start()

        def finish():
            out_ref[...] = column(z)

            @pl.when(z > 0)
            def _():
                up(z).wait_recv()
                out_ref[...] += z_in[z + 1].astype(f32)

            @pl.when(z < zn - 1)
            def _():
                down(z).wait_recv()
                out_ref[...] += z_in[z].astype(f32)

            def sent(zs):
                for col in range(4):
                    for cp in core(zs, col):
                        cp.wait_send()
                diag_x(zs).wait_send()
                diag_y(zs).wait_send()
                to_x(zs).wait_send()
                to_y(zs).wait_send()

            for dist in order:
                each(dist, sent)
                if dist:
                    each(dist, lambda zs: up(zs).wait_send())

        self.begin, self.finish = begin, finish
        self.diag = [functools.partial(each, dist, diag) for dist in order]
        self.sides = [functools.partial(each, dist, sides) for dist in order]
        self.pass_on = [functools.partial(each, dist, pass_on) for dist in order[:-1]]

    def plan(self, diag, sides, side_gap, pass_on, pass_gap):
        ticks = {0: [self.begin], diag: list(self.diag)}
        for k, fn in enumerate(self.sides):
            ticks.setdefault(sides + k * side_gap, []).append(fn)
        for k, fn in enumerate(self.pass_on):
            ticks.setdefault(pass_on + k * pass_gap, []).append(fn)
        return ticks

    @staticmethod
    def scratch(nd, rows, cols, parts):
        zn = nd // 2
        D, V = pltpu.SemaphoreType.DMA, pltpu.VMEM
        return [V((zn, 4, rows, cols), bf16), V((zn, 4, rows, cols), bf16), V((zn, rows, cols), bf16), V((2, zn, rows, cols), bf16),
                V((zn + 1, rows, cols), bf16), D((zn, 4, parts)), D((zn, 4, parts)), D((zn, 4, parts))] + [D((zn,))] * 9 + [D((2, zn))]


def run_ticks(ticks, now, last):
    for tick, fns in ticks.items():
        if tick <= last:
            @pl.when(now == tick)
            def _(fns=fns):
                for fn in fns:
                    fn()


def run_rest(ticks, last):
    for tick, fns in sorted(ticks.items()):
        if tick > last:
            for fn in fns:
                fn()


def exchange_kernel(nd, nf, g_ref, out_ref, got, send, recv):
    n = nd * nf
    me = lax.axis_index("dp") * nf + lax.axis_index("fsdp")
    sem = pltpu.get_barrier_semaphore()

    def peer(k):
        return lax.rem(me + k, n)

    def greet(k, carry):
        pl.semaphore_signal(sem, inc=1, device_id=(peer(k) // nf, peer(k) % nf), device_id_type=MESH)
        return carry

    lax.fori_loop(1, n, greet, 0)
    pl.semaphore_wait(sem, n - 1)

    def copy(k):
        p = peer(k)
        return pltpu.make_async_remote_copy(src_ref=g_ref.at[p], dst_ref=got.at[k], send_sem=send.at[k], recv_sem=recv.at[k],
                                            device_id=(p // nf, p % nf), device_id_type=MESH)

    def begin(k, carry):
        copy(k).start()
        return carry

    lax.fori_loop(1, n, begin, 0)

    def add(k, total):
        copy(k).wait_recv()
        return total + got[k]

    out_ref[...] = lax.fori_loop(1, n, add, g_ref[me])

    def end(k, carry):
        copy(k).wait_send()
        return carry

    lax.fori_loop(1, n, end, 0)


def exchange(g, nd, nf, cid):
    n = nd * nf
    D = pltpu.SemaphoreType.DMA
    vm = pl.BlockSpec(memory_space=pltpu.VMEM)
    return pl.pallas_call(
        functools.partial(exchange_kernel, nd, nf),
        out_shape=jax.ShapeDtypeStruct(g.shape[1:], g.dtype),
        in_specs=[vm],
        out_specs=vm,
        scratch_shapes=[pltpu.VMEM(g.shape, g.dtype), D((n,)), D((n,))],
        compiler_params=pltpu.CompilerParams(collective_id=cid, has_side_effects=True),
    )(g)


def dot(a, b, dims=((1,), (0,)), precision=None):
    return lax.dot_general(a, b, (dims, ((), ())), preferred_element_type=f32, precision=precision)


def sigmoid(x):
    return 1.0 / (1.0 + jnp.exp(-x))


def conv_rows(ext, taps, masks, halo):
    rows = ext.shape[0] - halo
    width = 4
    v = ext[halo:]
    out = taps[4:5] + taps[3:4] * v
    for k in range(1, width):
        moved = pltpu.roll(ext, k, 0)[halo:]
        out = out + (taps[3 - k : 4 - k] * masks[:, k : k + 1]) * moved
    return out


def prep_kernel(bcdt_ref, taps_ref, heads_ref, m_ref, segc_ref, segr_ref,
                b_ref, c_ref, bt_ref, ct_ref, pre_ref, gm_ref, cum4_ref, cumr_ref, sc_ref, dt_ref):
    T = bcdt_ref.shape[0]
    nc = T // L
    N = b_ref.shape[1]
    H = dt_ref.shape[1]
    groups = cum4_ref.shape[0]
    taps = taps_ref[...]
    tri = (lax.broadcasted_iota(jnp.int32, (L, L), 0) >= lax.broadcasted_iota(jnp.int32, (L, L), 1))
    trif = tri.astype(f32)
    neg_rate = -jnp.exp(heads_ref[0:1, :H]) * LOG2E
    bias = heads_ref[1:2, :H]

    def chunk(c, carry):
        t0 = pl.multiple_of(c * L, L)
        here = pl.ds(t0, L)
        h0 = pl.multiple_of(jnp.maximum(t0 - 16, 0), 16)
        before = bcdt_ref[pl.ds(h0, 16), : 2 * N].astype(f32)
        v = bcdt_ref[here, : 2 * N].astype(f32)
        pre = conv_rows(jnp.concatenate([before, v], axis=0), taps, m_ref[here, :], 16)
        pre_ref[here, :] = pre
        act = pre * sigmoid(pre)
        b = act[:, :N]
        cc = act[:, N:]
        bb = b.astype(bf16)
        cb = cc.astype(bf16)
        b_ref[here, :] = bb
        c_ref[here, :] = cb
        bt_ref[:, here] = b.T.astype(bf16)
        ct_ref[:, here] = cc.T.astype(bf16)
        segc = segc_ref[here, 0:1]
        prev = segc_ref[here, 1:2]
        last = segc_ref[here, 2:3]
        same = segc == segr_ref[:, here]
        g = dot(cb, bb, ((1,), (1,)))
        gm_ref[pl.ds(c, 1)] = jnp.where(tri & same, g, 0.0)[None]
        raw = bcdt_ref[here, 2 * N : 2 * N + 128].astype(f32)[:, :H] + bias
        dt = jnp.maximum(raw, 0.0) + jnp.log1p(jnp.exp(-jnp.abs(raw)))
        a2 = neg_rate * dt
        cum = dot(trif, a2, precision=HIGHEST)
        end = cum[L - 1 : L]
        ein = jnp.where(segc == prev, jnp.exp2(cum), 0.0)
        lv = jnp.where(segc == last, jnp.exp2(end - cum), 0.0)
        dt_ref[here, :] = dt
        cumt = cum.T
        s0 = pl.multiple_of(c * (3 * L), L)
        for k in range(groups):
            cols = slice(HG * k, HG * (k + 1))
            cum4_ref[k, here, :] = cum[:, cols]
            cumr_ref[k, :, here] = cumt[cols]
            sc_ref[k, pl.ds(s0, L), :] = dt[:, cols].astype(bf16)
            sc_ref[k, pl.ds(s0 + L, L), :] = ein[:, cols].astype(bf16)
            sc_ref[k, pl.ds(s0 + 2 * L, L), :] = lv[:, cols].astype(bf16)
        return carry

    lax.fori_loop(0, nc, chunk, 0)


def prep(bcdt, taps, heads, masks, segc, segr, N, H):
    T = bcdt.shape[0]
    nc = T // L
    G = H // HG
    S = jax.ShapeDtypeStruct
    return pl.pallas_call(
        prep_kernel,
        out_shape=(S((T, N), bf16), S((T, N), bf16), S((N, T), bf16), S((N, T), bf16), S((T, 2 * N), f32),
                   S((nc, L, L), f32), S((G, T, HG), f32), S((G, HG, T), f32), S((G, 3 * T, HG), bf16), S((T, H), f32)),
        compiler_params=pltpu.CompilerParams(vmem_limit_bytes=60 << 20),
    )(bcdt, taps, heads, masks, segc, segr)


def lane_onehot(width, per):
    return (lax.broadcasted_iota(jnp.int32, (HG, width), 1) // per == lax.broadcasted_iota(jnp.int32, (HG, width), 0)).astype(bf16)


def half_masks(P):
    lane = lax.broadcasted_iota(jnp.int32, (1, 2 * P), 1)
    first = (lane < P).astype(f32)
    return first.astype(bf16), (1.0 - first).astype(bf16)


def decay(cum4, cumr, k):
    return jnp.exp2(jnp.minimum(cum4[:, k : k + 1] - cumr[k : k + 1, :], 0.0))


def fwd_kernel(u_ref, gate_ref, taps_ref, m_ref, b_ref, c_ref, bt_ref, gm_ref, cum4_ref, cumr_ref, sc_ref,
               gg_ref, ssq_ref, pre_ref, st_ref, state):
    T, W = u_ref.shape
    P = W // HG
    nc = T // L
    step = pl.program_id(0)
    taps = taps_ref[...]
    gain = taps[5:6]
    skip = taps[6:7]
    onehot = lane_onehot(W, P)
    ma, mb = half_masks(P)
    state[...] = jnp.zeros_like(state)

    @pl.when(step == 0)
    def _():
        ssq_ref[...] = jnp.zeros_like(ssq_ref)

    def chunk(c, carry):
        t0 = pl.multiple_of(c * L, L)
        here = pl.ds(t0, L)
        h0 = pl.multiple_of(jnp.maximum(t0 - 16, 0), 16)
        ext = jnp.concatenate([u_ref[pl.ds(h0, 16), :], u_ref[here, :]], axis=0).astype(f32)
        pre = conv_rows(ext, taps, m_ref[here, :], 16)
        pre_ref[here, :] = pre.astype(bf16)
        x = pre * sigmoid(pre)
        s0 = pl.multiple_of(c * (3 * L), L)
        exp = dot(sc_ref[0, pl.ds(s0, 3 * L), :], onehot)
        dtx, einx, lvx = exp[:L], exp[L : 2 * L], exp[2 * L :]
        xd = x * dtx
        xdb = xd.astype(bf16)
        gm = gm_ref[c]
        cum4 = cum4_ref[0, here, :]
        cumr = cumr_ref[0, :, here]
        sb = state[...].astype(bf16)
        st_ref[c] = sb
        inner = []
        for p in range(HG // 2):
            m0 = (decay(cum4, cumr, 2 * p) * gm).astype(bf16)
            m1 = (decay(cum4, cumr, 2 * p + 1) * gm).astype(bf16)
            xp = xdb[:, 2 * P * p : 2 * P * (p + 1)]
            inner.append(dot(jnp.concatenate([m0, m1], axis=1), jnp.concatenate([xp * ma, xp * mb], axis=0)))
        y = jnp.concatenate(inner, axis=1) + dot(c_ref[here, :], sb) * einx + skip * x
        state[...] = state[...] * einx[L - 1 : L] + dot(bt_ref[:, here], (xd * lvx).astype(bf16))
        gate = gate_ref[here, :].astype(f32)
        g = y * (gate * sigmoid(gate))
        gg_ref[here, :] = (g * gain).astype(bf16)
        g2 = g * g
        tot = g2[:, :128]
        for j in range(1, W // 128):
            tot = tot + g2[:, 128 * j : 128 * (j + 1)]
        ssq_ref[here, :] += tot
        return carry

    lax.fori_loop(0, nc, chunk, 0)


def fwd(u, gate, taps, masks, b, c, bt, gm, cum4, cumr, sc):
    T, E = gate.shape
    N = b.shape[1]
    G = cum4.shape[0]
    W = E // G
    nc = T // L
    S = jax.ShapeDtypeStruct
    col = lambda off: pl.BlockSpec((T, W), lambda g: (0, g + off))
    full = lambda a: pl.BlockSpec(a.shape, lambda g: (0,) * a.ndim)
    grp = lambda a: pl.BlockSpec((1,) + a.shape[1:], lambda g: (g, 0, 0))
    return pl.pallas_call(
        fwd_kernel,
        grid=(G,),
        in_specs=[col(0), col(0), pl.BlockSpec((8, W), lambda g: (0, g)), full(masks), full(b), full(c), full(bt), full(gm),
                  grp(cum4), grp(cumr), grp(sc)],
        out_specs=[col(0), pl.BlockSpec((T, 128), lambda g: (0, 0)), col(0), pl.BlockSpec((nc, N, W), lambda g: (0, 0, g))],
        out_shape=(S((T, E), bf16), S((T, 128), f32), S((T, E), bf16), S((nc, N, E), bf16)),
        scratch_shapes=[pltpu.VMEM((N, W), f32)],
        compiler_params=pltpu.CompilerParams(vmem_limit_bytes=60 << 20),
        cost_estimate=pl.CostEstimate(flops=T * E * (2 * L + 4 * N) * 2, bytes_accessed=T * E * 12, transcendentals=T * E * 4),
    )(u, gate, taps, masks, b, c, bt, gm, cum4, cumr, sc)


def bwd_kernel(*refs):
    bwd_body(lambda now: None, *refs)


def bwd_scatter_kernel(nd, nf, parts, *refs):
    g_refs, ins, outs = refs[:parts], refs[parts : parts + 15], refs[parts + 15 : parts + 23]
    own, comm = refs[parts + 23 : parts + 26], refs[parts + 26 :]
    sc = Scatter(nd, nf, g_refs, outs[7], *comm)
    nc = ins[0].shape[0] // L
    ticks = sc.plan(7, 12, 3, 28, 6)
    bwd_body(lambda now: run_ticks(ticks, now, BWD_TICKS), *ins, *outs[:7], *own)

    @pl.when(pl.program_id(0) == pl.num_programs(0) - 1)
    def _():
        run_rest(ticks, BWD_TICKS)
        sc.finish()


def bwd_body(tick, u_ref, gate_ref, pre_ref, dm_ref, rq_ref, taps_ref, m_ref, b_ref, c_ref, ct_ref, gm_ref, cum4_ref, cumr_ref, sc_ref, st_ref,
               dz_ref, dg_ref, db_ref, dc_ref, rs_ref, small_ref, kk_ref, ds, nxt, acc):
    T, W = u_ref.shape
    P = W // HG
    nc = T // L
    step = pl.program_id(0)
    taps = taps_ref[...]
    gain = taps[5:6]
    skip = taps[6:7]
    onehot = lane_onehot(W, P)
    ma, mb = half_masks(P)
    ds[...] = jnp.zeros_like(ds)
    nxt[...] = jnp.zeros_like(nxt)
    acc[...] = jnp.zeros_like(acc)

    @pl.when(step == 0)
    def _():
        dg_ref[...] = jnp.zeros_like(dg_ref)
        db_ref[...] = jnp.zeros_like(db_ref)
        dc_ref[...] = jnp.zeros_like(dc_ref)

    ri = lax.broadcasted_iota(jnp.int32, (4 * W, 16), 0)
    ci = lax.broadcasted_iota(jnp.int32, (4 * W, 16), 1)
    part = ri // W
    want = jnp.maximum(part - 1, 0) * HG + (ri % W) // P
    fold = (want == ci).astype(bf16)

    def eight(z):
        return jnp.sum(z.reshape(L // 8, 8, W), axis=0)

    def chunk(i, carry):
        tick(step * nc + i)
        c = nc - 1 - i
        t0 = pl.multiple_of(c * L, L)
        here = pl.ds(t0, L)
        u = u_ref[here, :].astype(f32)
        pre = pre_ref[here, :].astype(f32)
        sig = sigmoid(pre)
        x = pre * sig
        dsilu = sig + x * (1.0 - sig)
        s0 = pl.multiple_of(c * (3 * L), L)
        exp = dot(sc_ref[0, pl.ds(s0, 3 * L), :], onehot)
        dtx, einx, lvx = exp[:L], exp[L : 2 * L], exp[2 * L :]
        xdb = (x * dtx).astype(bf16)
        xd = xdb.astype(f32)
        gm = gm_ref[c]
        cum4 = cum4_ref[0, here, :]
        cumr = cumr_ref[0, :, here]
        sb = st_ref[c]
        es, ms, inner = [], [], []
        for p in range(HG // 2):
            e0 = decay(cum4, cumr, 2 * p)
            e1 = decay(cum4, cumr, 2 * p + 1)
            m0 = (e0 * gm).astype(bf16)
            m1 = (e1 * gm).astype(bf16)
            xp = xdb[:, 2 * P * p : 2 * P * (p + 1)]
            inner.append(dot(jnp.concatenate([m0, m1], axis=1), jnp.concatenate([xp * ma, xp * mb], axis=0)))
            es.append((e0, e1))
            ms.append((m0, m1))
        yn = jnp.concatenate(inner, axis=1) + dot(c_ref[here, :], sb) * einx
        y = yn + skip * x
        gate = gate_ref[here, :].astype(f32)
        sgate = sigmoid(gate)
        silu_g = gate * sgate
        g = y * silu_g
        r = rq_ref[here, 0:1]
        q = rq_ref[here, 1:2]
        dmr = dm_ref[here, :].astype(f32) * r
        dgg = gain * dmr - g * q
        dyb = (dgg * silu_g).astype(bf16)
        dy = dyb.astype(f32)
        dz_ref[0, here, :] = (dgg * y * (sgate + silu_g * (1.0 - sgate))).astype(bf16)
        dxi = []
        dgc = dg_ref[c]
        for p in range(HG // 2):
            cols = slice(2 * P * p, 2 * P * (p + 1))
            dp = dyb[:, cols]
            dstack = jnp.concatenate([dp * ma, dp * mb], axis=0)
            dmm = dot(dstack, xdb[:, cols], ((1,), (1,)))
            dgc = dgc + dmm[:L] * es[p][0] + dmm[L:] * es[p][1]
            dxi.append(dot(jnp.concatenate(ms[p], axis=0), dstack, ((0,), (0,))))
        dg_ref[c] = dgc
        dxi = jnp.concatenate(dxi, axis=1)
        dsn = ds[...]
        dsb = dsn.astype(bf16)
        dye = (dy * einx).astype(bf16)
        dc_ref[here, :] += dot(dye, sb, ((1,), (1,)))
        kept = einx[L - 1 : L]
        kk_ref[pl.ds(c, 1), :] = kept * jnp.sum(sb.astype(f32) * dsn, axis=0, keepdims=True)
        db_ref[here, :] += dot((xd * lvx).astype(bf16), dsb, ((1,), (1,)))
        dxe = dot(b_ref[here, :], dsb) * lvx
        ds[...] = dsn * kept + dot(ct_ref[:, here], dye)
        dxd = dxi + dxe
        r1 = dy * yn - xd * dxi
        r1h = r1.astype(bf16)
        r1l = (r1 - r1h.astype(f32)).astype(bf16)
        rs_ref[0, here, :] = dot(jnp.concatenate([r1h, r1l, (xd * dxe).astype(bf16), (x * dxd).astype(bf16)], axis=1), fold)
        dpre = (dxd * dtx + skip * dy) * dsilu
        ext = jnp.concatenate([dpre, nxt[...]], axis=0)
        nxt[...] = dpre[:8]
        du = taps[3:4] * dpre
        acc[0:8, :] += eight(dmr * g)
        acc[8:16, :] += eight(dy * x)
        acc[16:24, :] += eight(dpre)
        acc[24:32, :] += eight(dpre * u)
        mrows = m_ref[pl.ds(t0, L + 8), :]
        for k in range(1, 4):
            sk = pltpu.roll(ext * mrows[:, k : k + 1], L + 8 - k, 0)[:L]
            du = du + taps[3 - k : 4 - k] * sk
            acc[24 + 8 * k : 32 + 8 * k, :] += eight(sk * u)
        dz_ref[1, here, :] = du.astype(bf16)
        return carry

    lax.fori_loop(0, nc, chunk, 0)
    for j in range(7):
        small_ref[j : j + 1, :] = jnp.sum(acc[8 * j : 8 * j + 8, :], axis=0, keepdims=True)
    small_ref[7:8, :] = jnp.zeros((1, W), f32)


def bwd(half, halves, u, gate, pre, dm, rq, taps, masks, b, c, ct, gm, cum4, cumr, sc, st, comm=None):
    T, E = gate.shape
    N = b.shape[1]
    G = cum4.shape[0]
    W = E // G
    nc = T // L
    Gh = G // halves
    Eh = E // halves
    g0 = half * Gh
    S = jax.ShapeDtypeStruct
    col = pl.BlockSpec((T, W), lambda g: (0, g + g0))
    full = lambda a: pl.BlockSpec(a.shape, lambda g: (0,) * a.ndim)
    whole = lambda s: pl.BlockSpec(s, lambda g: (0,) * len(s))
    grp = lambda a: pl.BlockSpec((1,) + a.shape[1:], lambda g: (g + g0, 0, 0))
    in_specs = [col, col, col, col, full(rq), pl.BlockSpec((8, W), lambda g: (0, g + g0)), full(masks), full(b), full(c),
                full(ct), full(gm), grp(cum4), grp(cumr), grp(sc), pl.BlockSpec((nc, N, W), lambda g: (0, 0, g + g0))]
    out_specs = [pl.BlockSpec((2, T, W), lambda g: (0, 0, g)), whole((nc, L, L)), whole((T, N)), whole((T, N)),
                 pl.BlockSpec((1, T, 16), lambda g: (g, 0, 0)), pl.BlockSpec((8, W), lambda g: (0, g)), pl.BlockSpec((nc, W), lambda g: (0, g))]
    out_shape = [S((2, T, Eh), bf16), S((nc, L, L), f32), S((T, N), f32), S((T, N), f32), S((Gh, T, 16), f32), S((8, Eh), f32), S((nc, Eh), f32)]
    scratch = [pltpu.VMEM((N, W), f32), pltpu.VMEM((8, W), f32), pltpu.VMEM((56, W), f32)]
    kernel, first, params = bwd_kernel, (), {}
    if comm:
        nd, nf, cid, first = comm
        rows, cols = first[0].shape[1], sum(g.shape[2] for g in first)
        kernel = functools.partial(bwd_scatter_kernel, nd, nf, len(first))
        in_specs = [pl.BlockSpec(memory_space=pl.ANY)] * len(first) + in_specs
        out_specs.append(whole((rows, cols)))
        out_shape.append(S((rows, cols), f32))
        scratch += Scatter.scratch(nd, rows, cols, len(first))
        params = dict(collective_id=cid, has_side_effects=True)
    return pl.pallas_call(
        kernel,
        grid=(Gh,),
        in_specs=in_specs,
        out_specs=out_specs,
        out_shape=out_shape,
        scratch_shapes=scratch,
        compiler_params=pltpu.CompilerParams(vmem_limit_bytes=60 << 20, **params),
        cost_estimate=pl.CostEstimate(flops=T * Eh * (8 * L + 12 * N), bytes_accessed=T * Eh * 16, transcendentals=T * Eh * 4),
    )(*first, u, gate, pre, dm, rq, taps, masks, b, c, ct, gm, cum4, cumr, sc, st)


def post_kernel(bcdt_ref, pre_ref, taps_ref, heads_ref, m_ref, segc_ref, segr_ref, b_ref, c_ref, dg0_ref, db0_ref, dc0_ref, rs0_ref, dg1_ref, db1_ref, dc1_ref, rs1_ref, kk_ref, dt_ref,
                out_ref, small_ref, hs_ref, nxt, acc, hacc):
    T = bcdt_ref.shape[0]
    nc = T // L
    N = b_ref.shape[1]
    H = dt_ref.shape[1]
    G = H // HG
    taps = taps_ref[...]
    tri = (lax.broadcasted_iota(jnp.int32, (L, L), 0) >= lax.broadcasted_iota(jnp.int32, (L, L), 1))
    upper = (lax.broadcasted_iota(jnp.int32, (L, L), 0) <= lax.broadcasted_iota(jnp.int32, (L, L), 1)).astype(f32)
    strict = 1.0 - upper
    rate = -jnp.exp(heads_ref[0:1, :H])
    bias = heads_ref[1:2, :H]
    nxt[...] = jnp.zeros_like(nxt)
    acc[...] = jnp.zeros_like(acc)
    hacc[...] = jnp.zeros_like(hacc)

    def eight(z):
        return jnp.sum(z.reshape(L // 8, 8, z.shape[1]), axis=0)

    def chunk(i, carry):
        c = nc - 1 - i
        t0 = pl.multiple_of(c * L, L)
        here = pl.ds(t0, L)
        same = segc_ref[here, 0:1] == segr_ref[:, here]
        dg = jnp.where(tri & same, dg0_ref[c] + dg1_ref[c], 0.0)
        dgb = dg.astype(bf16)
        dcv = dc0_ref[here, :] + dc1_ref[here, :] + dot(dgb, b_ref[here, :])
        dbv = db0_ref[here, :] + db1_ref[here, :] + dot(dg.T.astype(bf16), c_ref[here, :])
        pre = pre_ref[here, :]
        sig = sigmoid(pre)
        dpre = jnp.concatenate([dbv, dcv], axis=1) * (sig + pre * sig * (1.0 - sig))
        v = bcdt_ref[here, : 2 * N].astype(f32)
        ext = jnp.concatenate([dpre, nxt[...]], axis=0)
        nxt[...] = dpre[:8]
        dv = taps[3:4] * dpre
        acc[0:8, :] += eight(dpre)
        acc[8:16, :] += eight(dpre * v)
        mrows = m_ref[pl.ds(t0, L + 8), :]
        for k in range(1, 4):
            sk = pltpu.roll(ext * mrows[:, k : k + 1], L + 8 - k, 0)[:L]
            dv = dv + taps[3 - k : 4 - k] * sk
            acc[8 + 8 * k : 16 + 8 * k, :] += eight(sk * v)
        out_ref[here, : 2 * N] = dv.astype(bf16)
        r1 = jnp.concatenate([r[k, here, 0:HG] for r in (rs0_ref, rs1_ref) for k in range(G // 2)], axis=1)
        r2 = jnp.concatenate([r[k, here, HG : 2 * HG] for r in (rs0_ref, rs1_ref) for k in range(G // 2)], axis=1)
        r3 = jnp.concatenate([r[k, here, 2 * HG : 3 * HG] for r in (rs0_ref, rs1_ref) for k in range(G // 2)], axis=1)
        da = dot(upper, r1, precision=HIGHEST) + dot(strict, r2, precision=HIGHEST) + kk_ref[pl.ds(c, 1), :]
        dt = dt_ref[here, :]
        raw = bcdt_ref[here, 2 * N : 2 * N + 128].astype(f32)[:, :H] + bias
        ddt = (r3 + da * rate) * sigmoid(raw)
        hacc[0:8, :] += eight(da * rate * dt)
        hacc[8:16, :] += eight(ddt)
        out_ref[here, 2 * N :] = jnp.concatenate([ddt, jnp.zeros((L, out_ref.shape[1] - 2 * N - H), f32)], axis=1).astype(bf16)
        return carry

    lax.fori_loop(0, nc, chunk, 0)
    for j in range(5):
        small_ref[j : j + 1, :] = jnp.sum(acc[8 * j : 8 * j + 8, :], axis=0, keepdims=True)
    small_ref[5:8, :] = jnp.zeros((3, 2 * N), f32)
    for j in range(2):
        hs_ref[j : j + 1, :] = jnp.sum(hacc[8 * j : 8 * j + 8, :], axis=0, keepdims=True)


def post(bcdt, pre, taps, heads, masks, segc, segr, b, c, first, second, kk, dt):
    T = bcdt.shape[0]
    N = b.shape[1]
    H = dt.shape[1]
    S = jax.ShapeDtypeStruct
    return pl.pallas_call(
        post_kernel,
        out_shape=(S(bcdt.shape, bf16), S((8, 2 * N), f32), S((2, H), f32)),
        scratch_shapes=[pltpu.VMEM((8, 2 * N), f32), pltpu.VMEM((40, 2 * N), f32), pltpu.VMEM((16, H), f32)],
        compiler_params=pltpu.CompilerParams(vmem_limit_bytes=60 << 20),
    )(bcdt, pre, taps, heads, masks, segc, segr, b, c, *first, *second, kk, dt)


NT = 256


def tail_kernel(nd, nf, parts, gg_tiles, *refs):
    g_refs, refs = refs[:parts], refs[parts:]
    wo_hbm, wg_hbm, wa_hbm, gg_ref, dz0_ref, dz1_ref, dbc_ref, hid_ref, go_ref, r_ref, gain_ref, sum_ref, out_ref, gin_ref, dn_ref = refs[:15]
    wo, wg, wa, acc, dn, sem = refs[15:21]
    sc = Scatter(nd, nf, g_refs, sum_ref, *refs[21:])
    D, E = wg.shape
    Eh = E // 2
    step = pl.program_id(0)
    tiles = gg_tiles
    blocks = D // NT
    ticks = sc.plan(*TAIL_PLAN)
    fetch = [pltpu.make_async_copy(src, dst, sem.at[k]) for k, (src, dst) in enumerate(((wo_hbm, wo), (wg_hbm, wg), (wa_hbm, wa)))]

    @pl.when(step == 0)
    def _():
        for cp in fetch:
            cp.start()
        dn[...] = jnp.zeros_like(dn)
        run_ticks(ticks, 0, 0)
        fetch[0].wait()

    @pl.when(step == tiles)
    def _():
        fetch[1].wait()
        fetch[2].wait()

    @pl.when(step < tiles)
    def _():
        def block(j, carry):
            now = step * blocks + j
            run_ticks({t: f for t, f in ticks.items() if 0 < t}, now, min(TAIL_TICKS, tiles * blocks - 1))
            cols = pl.ds(pl.multiple_of(j * NT, NT), NT)
            out_ref[:, cols] = (hid_ref[:, cols].astype(f32) + r_ref[...] * dot(gg_ref[...], wo[:, cols])).astype(bf16)
            return carry
        lax.fori_loop(0, blocks, block, 0)

    @pl.when(step >= tiles)
    def _():
        def block(j, carry):
            now = step * blocks + j
            run_ticks({t: f for t, f in ticks.items() if t >= tiles * blocks}, now, TAIL_TICKS)
            cols = pl.ds(pl.multiple_of(j * NT, NT), NT)
            part = dot(dz0_ref[0], wg[cols, :Eh], ((1,), (1,))) + dot(dz1_ref[0], wg[cols, Eh:], ((1,), (1,)))
            part = part + dot(dz0_ref[1], wa[cols, :Eh], ((1,), (1,))) + dot(dz1_ref[1], wa[cols, Eh:E], ((1,), (1,)))
            acc[:, cols] = part + dot(dbc_ref[...], wa[cols, E:], ((1,), (1,)))
            return carry
        lax.fori_loop(0, blocks, block, 0)
        gain = gain_ref[...]

        def rows_of(i, carry):
            here = pl.ds(pl.multiple_of(i * 64, 64), 64)
            rows = hid_ref[here, :].astype(f32)
            rinv = lax.rsqrt(jnp.mean(rows * rows, axis=-1, keepdims=True) + EPS)
            xhat = rows * rinv
            bn = acc[here, :]
            prod = bn * xhat
            dn[...] += jnp.sum(prod.reshape(8, 8, D), axis=0)
            mean = jnp.mean(prod * gain, axis=-1, keepdims=True)
            gin_ref[here, :] = (go_ref[here, :].astype(f32) + rinv * (bn * gain - xhat * mean)).astype(bf16)
            return carry
        lax.fori_loop(0, hid_ref.shape[0] // 64, rows_of, 0)

    @pl.when(step == 2 * tiles - 1)
    def _():
        dn_ref[...] = jnp.sum(dn[...], axis=0, keepdims=True)
        run_rest(ticks, TAIL_TICKS)
        sc.finish()


def tail(nd, nf, cid, gs, dz0, dz1, dbcdt, full_gate, full_a, gg, full_out, hidden, grad_out, r, norm_gain):
    T, D = hidden.shape
    E = full_out.shape[0]
    rows, cols = gs[0].shape[1], sum(g.shape[2] for g in gs)
    MT = 256 if rows % 16 == 0 else 128
    tiles = T // MT
    wide = dbcdt.shape[1]
    S = jax.ShapeDtypeStruct
    any_ = pl.BlockSpec(memory_space=pl.ANY)
    whole = lambda s: pl.BlockSpec(s, lambda k: (0,) * len(s), pipeline_mode=pl.Buffered(1))
    early = lambda w: pl.BlockSpec((MT, w), lambda k: (jnp.minimum(k, tiles - 1), 0))
    late = lambda w: pl.BlockSpec((MT, w), lambda k: (jnp.maximum(k - tiles, 0), 0))
    both = lambda w: pl.BlockSpec((MT, w), lambda k: (lax.rem(k, tiles), 0))
    half = pl.BlockSpec((2, MT, E // 2), lambda k: (0, jnp.maximum(k - tiles, 0), 0))
    return pl.pallas_call(
        functools.partial(tail_kernel, nd, nf, len(gs), tiles),
        grid=(2 * tiles,),
        in_specs=[any_] * (len(gs) + 3) + [early(E), half, half, late(wide), both(D), late(D), early(1), whole((1, D))],
        out_specs=[whole((rows, cols)), early(D), late(D), whole((1, D))],
        out_shape=(S((rows, cols), f32), S((T, D), bf16), S((T, D), bf16), S((1, D), f32)),
        scratch_shapes=[pltpu.VMEM((E, D), bf16), pltpu.VMEM((D, E), bf16), pltpu.VMEM((D, E + wide), bf16), pltpu.VMEM((MT, D), f32),
                        pltpu.VMEM((8, D), f32), pltpu.SemaphoreType.DMA((3,))] + Scatter.scratch(nd, rows, cols, len(gs)),
        compiler_params=pltpu.CompilerParams(collective_id=cid, has_side_effects=True, vmem_limit_bytes=67043328),
        cost_estimate=pl.CostEstimate(flops=2 * T * D * 3 * E, bytes_accessed=8 * D * E, transcendentals=0),
    )(*gs, full_out, full_gate, full_a, gg, dz0, dz1, dbcdt, hidden, grad_out, r, norm_gain)


def layer(nd, nf, hidden, grad_out, seg, shard_a, shard_gate, shard_out, head_params, sizes):
    n = nd * nf
    E, N, H, K1, S = sizes
    T, D = hidden.shape
    wide = 2 * N + 128
    full_gate = lax.all_gather(shard_gate, AXES, axis=0, tiled=True)
    full_out = lax.all_gather(shard_out, AXES, axis=0, tiled=True)
    full_a = gather_rows(shard_a, nd, nf, 0)
    off = E + 2 * N + H
    flat = full_a[:, :, off : off + S].reshape(n, -1)
    ncol, nrow, ngate = (E + 2 * N) // n, D // n, E // n
    conv = flat[:, : K1 * ncol].reshape(n, K1, ncol).transpose(1, 0, 2).reshape(K1, n * ncol).astype(f32)
    norm_gain = flat[:, K1 * ncol : K1 * ncol + nrow].reshape(-1).astype(f32)
    gate_gain = flat[:, K1 * ncol + nrow : K1 * ncol + nrow + ngate].reshape(-1).astype(f32)
    full_a = full_a.reshape(D, E + wide)
    rows = hidden.astype(f32)
    rinv = lax.rsqrt(jnp.mean(rows * rows, axis=-1, keepdims=True) + EPS)
    xhat = rows * rinv
    normed = (xhat * norm_gain).astype(bf16)
    ubc = dot(normed, full_a).astype(bf16)
    gate = dot(normed, full_gate).astype(bf16)
    bcdt = ubc[:, E:]
    pos = jnp.arange(T, dtype=jnp.int32)
    masks = jnp.stack([jnp.ones((T,), f32)] + [((jnp.roll(seg, k) == seg) & (pos >= k)).astype(f32) for k in range(1, 4)], axis=1)
    lastid = seg[L - 1 :: L]
    previd = jnp.concatenate([jnp.full((1,), -1, jnp.int32), lastid[:-1]])
    segc = jnp.stack([seg, jnp.repeat(previd, L), jnp.repeat(lastid, L)], axis=1)
    segr = seg[None, :]
    taps_u = jnp.concatenate([conv[:, :E], gate_gain[None], jnp.repeat(head_params[2], E // H)[None], jnp.zeros((1, E), f32)], axis=0)
    taps_bc = jnp.concatenate([conv[:, E:], jnp.zeros((3, 2 * N), f32)], axis=0)
    heads_p = jnp.pad(head_params, ((0, 5), (0, 128 - H)))
    b, c, bt, ct, pre_bc, gm, cum4, cumr, sc, dt = prep(bcdt, taps_bc, heads_p, masks, segc, segr, N, H)
    gg, ssq, pre, st = fwd(ubc, gate, taps_u, masks, b, c, bt, gm, cum4, cumr, sc)
    r = lax.rsqrt(jnp.sum(ssq, axis=1, keepdims=True) / E + EPS)
    gos = (grad_out.astype(f32) * r).astype(bf16)
    g_out = dot(gg, gos, ((0,), (0,))).astype(bf16)
    dm = dot(grad_out, full_out, ((1,), (1,))).astype(bf16)
    s = jnp.sum(gg.astype(f32) * dm.astype(f32), axis=1, keepdims=True)
    rq = jnp.concatenate([r, r * r * r * s / E], axis=1)
    masks8 = jnp.pad(masks, ((0, 8), (0, 0)))
    shape = lambda g: g.reshape(n, D // n, -1)
    grad = lambda dz: shape(dot(normed, dz, ((0,), (0,))).astype(bf16))
    back = functools.partial(bwd, u=ubc, gate=gate, pre=pre, dm=dm, rq=rq, taps=taps_u, masks=masks8, b=b, c=c, ct=ct, gm=gm, cum4=cum4,
                             cumr=cumr, sc=sc, st=st)
    dz0, dg0, db0, dc0, rs0, small0, kk0, s_out = back(0, 2, comm=(nd, nf, 4, (g_out.reshape(n, E // n, D),)))
    dz1, dg1, db1, dc1, rs1, small1, kk1, sum0 = back(1, 2, comm=(nd, nf, 3, (grad(dz0[0]), grad(dz0[1]))))
    small = jnp.concatenate([small0, small1], axis=1)
    kk = jnp.concatenate([kk0, kk1], axis=1)
    kkh = jnp.sum(kk.reshape(kk.shape[0], H, E // H), axis=2)
    dbcdt, small_bc, hs = post(bcdt, pre_bc, taps_bc, heads_p, masks8, segc, segr, b, c, (dg0, db0, dc0, rs0), (dg1, db1, dc1, rs1), kkh, dt)
    sum1, output, grad_in, d_norm = tail(nd, nf, 1, (grad(dz1[0]), grad(dz1[1]), grad(dbcdt)), dz0, dz1, dbcdt, full_gate, full_a, gg, full_out,
                                         hidden, grad_out, r, norm_gain[None])
    d_conv = jnp.concatenate([jnp.stack([small[6], small[5], small[4], small[3], small[2]]),
                              jnp.stack([small_bc[4], small_bc[3], small_bc[2], small_bc[1], small_bc[0]])], axis=1)
    d_heads = jnp.concatenate([hs, jnp.sum(small[1].reshape(1, H, E // H), axis=2)], axis=0)
    mine = jnp.concatenate([d_conv.reshape(K1, n, ncol).transpose(1, 0, 2).reshape(n, -1), d_norm.reshape(n, -1), small[0].reshape(n, -1),
                            jnp.broadcast_to(d_heads.reshape(1, -1), (n, d_heads.size))], axis=1)
    tiles = -(-mine.shape[1] // 1024)
    mine = jnp.pad(mine, ((0, 0), (0, tiles * 1024 - mine.shape[1]))).reshape(n, tiles * 8, 128)
    tot = exchange(mine, nd, nf, 2).reshape(-1)
    cut = [0, K1 * ncol, nrow, ngate, d_heads.size]
    ends = [sum(cut[: k + 1]) for k in range(5)]
    t_conv, t_norm, t_gate, t_heads = (tot[ends[k] : ends[k + 1]] for k in range(4))
    Eh = E // 2
    s_zx = jnp.concatenate([sum0[:, :Eh], sum1[:, :Eh], sum0[:, Eh:], sum1[:, Eh : 2 * Eh]], axis=1)
    return (output, grad_in, s_zx, sum1[:, 2 * Eh : 2 * Eh + 2 * N], sum1[:, 2 * Eh + 2 * N : 2 * Eh + 2 * N + H], s_out,
            t_conv.reshape(K1, ncol), t_norm, t_gate, t_heads.reshape(d_heads.shape))


def per_device(nd, nf, hidden, grad_out, segment_ids, w_zx, w_bc, w_dt, w_out, conv_params, norm_gain, gate_gain, head_params):
    n = nd * nf
    E, N2, H = w_out.shape[0] * n, w_bc.shape[1], w_dt.shape[1]
    rows = w_zx.shape[0]
    small = jnp.concatenate([conv_params.reshape(-1), norm_gain, gate_gain])
    S = -(-small.shape[0] // rows)
    assert S + H <= 128
    small = jnp.pad(small, (0, S * rows - small.shape[0])).reshape(rows, S)
    shard_a = jnp.concatenate([w_zx[:, E:], w_bc, w_dt, small, jnp.zeros((rows, 128 - H - S), bf16)], axis=1)
    return layer(nd, nf, hidden, grad_out, segment_ids, shard_a, w_zx[:, :E], w_out, head_params, (E, N2 // 2, H, conv_params.shape[0], S))


def solution(mesh):
    row, col, vec, rep = P(AXES, None), P(None, AXES), P(AXES), P()
    return jax.shard_map(
        functools.partial(per_device, mesh.shape["dp"], mesh.shape["fsdp"]),
        mesh=mesh,
        in_specs=(row, row, vec, row, row, row, row, col, vec, vec, rep),
        out_specs=(row, row, row, row, row, row, col, vec, vec, rep),
        check_vma=False,
    )
```

```python
import functools
import jax
import jax.numpy as jnp
from jax import lax
from jax.experimental import pallas as pl
from jax.experimental.pallas import tpu as pltpu
from jax.sharding import PartitionSpec as P

EPS = 1e-05
L = 128
HG = 8
LOG2E = 1.4426950408889634
BWD_PLAN = (2, 5, 2, 14, 2)
BWD_TICKS = 23
TAIL_PLAN = (6, 12, 4, 28, 4)
TAIL_TICKS = 47
bf16, f32 = jnp.bfloat16, jnp.float32
HIGHEST = lax.Precision.HIGHEST


AXES = ("dp", "fsdp")
MESH = pl.DeviceIdType.MESH


class Place:
    def __init__(self, nd, nf):
        self.zn, self.nf = nd // 2, nf
        d, f = lax.axis_index("dp"), lax.axis_index("fsdp")
        self.z, self.y = d // 2, d % 2
        self.x, self.c = f // 2, f % 2

    def dev(self, z, y, x, c):
        return (z * 2 + y, x * 2 + c)

    def idx(self, z, y, x, c):
        return (z * 2 + y) * self.nf + x * 2 + c

    def barrier(self):
        z, y, x, c, zn = self.z, self.y, self.x, self.c, self.zn
        sem = pltpu.get_barrier_semaphore()
        for there in ((z, y, 1 - x, c), (z, 1 - y, x, c), (z, y, x, 1 - c)):
            pl.semaphore_signal(sem, inc=1, device_id=self.dev(*there), device_id_type=MESH)

        @pl.when(z > 0)
        def _():
            pl.semaphore_signal(sem, inc=1, device_id=self.dev(z - 1, y, x, c), device_id_type=MESH)

        @pl.when(z < zn - 1)
        def _():
            pl.semaphore_signal(sem, inc=1, device_id=self.dev(z + 1, y, x, c), device_id_type=MESH)

        pl.semaphore_wait(sem, 3 + (z + zn - 1) // zn + (2 * zn - 2 - z) // zn)


def gather_kernel(nd, nf, src_ref, out_ref, own_sem, z_send, z_recv, x_send, x_recv, y_send, y_recv, dx_send, dx_recv, dy_send, dy_recv, c_send, c_recv):
    at = Place(nd, nf)
    z, y, x, c, zn = at.z, at.y, at.x, at.c, at.zn
    half = out_ref.shape[2] // 256 * 128
    lo, hi = pl.ds(0, half), pl.ds(half, out_ref.shape[2] - half)
    at.barrier()

    def copy(block, to, send, recv, cols=None, src=None):
        ref = out_ref.at[block] if cols is None else out_ref.at[block, :, cols]
        return pltpu.make_async_remote_copy(src_ref=ref if src is None else src, dst_ref=ref, send_sem=send, recv_sem=recv,
                                            device_id=at.dev(*to), device_id_type=MESH)

    def block(zs, col):
        return at.idx(zs, 1 - y if col & 2 else y, 1 - x if col & 1 else x, c)

    def up(zs, src=None):
        return copy(block(zs, 0), (z + 1, y, x, c), z_send.at[0, zs], z_recv.at[zs], src=src)

    def down(zs, src=None):
        return copy(block(zs, 0), (z - 1, y, x, c), z_send.at[1, zs], z_recv.at[zs], src=src)

    def to_x(zs, src=None):
        return copy(block(zs, 0), (z, y, 1 - x, c), x_send.at[zs], x_recv.at[zs], src=src)

    def to_y(zs, src=None):
        return copy(block(zs, 0), (z, 1 - y, x, c), y_send.at[zs], y_recv.at[zs], src=src)

    def diag_y(zs):
        return copy(block(zs, 1), (z, 1 - y, x, c), dy_send.at[zs], dy_recv.at[zs], lo)

    def diag_x(zs):
        return copy(block(zs, 2), (z, y, 1 - x, c), dx_send.at[zs], dx_recv.at[zs], hi)

    def to_core(zs, col, src=None):
        return copy(block(zs, col), (z, y, x, 1 - c), c_send.at[zs, col], c_recv.at[zs, col], src=src)

    own = pltpu.make_async_copy(src_ref, out_ref.at[block(z, 0)], own_sem)
    own.start()

    @pl.when(z < zn - 1)
    def _():
        up(z, src_ref).start()

    @pl.when(z > 0)
    def _():
        down(z, src_ref).start()

    to_x(z, src_ref).start()
    to_y(z, src_ref).start()
    to_core(z, 0, src_ref).start()

    def each(dist, fn):
        if dist == 0:
            fn(z, 0)
            return

        @pl.when(z - dist >= 0)
        def _():
            fn(z - dist, 1)

        @pl.when(z + dist < zn)
        def _():
            fn(z + dist, -1)

    def from_z(zs, way):
        copy(block(zs, 0), (z, y, x, c), z_send.at[0, zs], z_recv.at[zs]).wait_recv()
        if way > 0:
            @pl.when(z < zn - 1)
            def _():
                up(zs).start()
        else:
            @pl.when(z > 0)
            def _():
                down(zs).start()
        to_x(zs).start()
        to_y(zs).start()
        to_core(zs, 0).start()

    def from_xy(zs, way):
        to_x(zs).wait_recv()
        diag_y(zs).start()
        to_core(zs, 1).start()
        to_y(zs).wait_recv()
        diag_x(zs).start()
        to_core(zs, 2).start()

    def from_diag(zs, way):
        diag_y(zs).wait_recv()
        diag_x(zs).wait_recv()
        to_core(zs, 3).start()

    for dist in range(zn):
        if dist:
            each(dist, from_z)
        each(dist, from_xy)
    for dist in range(zn):
        each(dist, from_diag)
    own.wait()

    def sent(zs, way):
        for col in range(4):
            to_core(zs, col).wait_recv()
            to_core(zs, col).wait_send()
        to_x(zs).wait_send()
        to_y(zs).wait_send()
        diag_x(zs).wait_send()
        diag_y(zs).wait_send()
        if way >= 0:
            @pl.when(z < zn - 1)
            def _():
                up(zs).wait_send()
        if way <= 0:
            @pl.when(z > 0)
            def _():
                down(zs).wait_send()

    for dist in range(zn):
        each(dist, sent)


def gather_rows(shard, nd, nf, cid):
    zn = nd // 2
    D = pltpu.SemaphoreType.DMA
    return pl.pallas_call(
        functools.partial(gather_kernel, nd, nf),
        out_shape=jax.ShapeDtypeStruct((nd * nf,) + shard.shape, shard.dtype),
        in_specs=[pl.BlockSpec(memory_space=pl.ANY)],
        out_specs=pl.BlockSpec(memory_space=pl.ANY),
        scratch_shapes=[D(()), D((2, zn)), D((zn,)), D((zn,)), D((zn,)), D((zn,)), D((zn,)), D((zn,)), D((zn,)), D((zn,)), D((zn,)),
                        D((zn, 4)), D((zn, 4))],
        compiler_params=pltpu.CompilerParams(collective_id=cid, has_side_effects=True),
    )(shard)


class Scatter:
    def __init__(self, nd, nf, g_refs, out_ref, acc, c_in, d_in, xy_in, z_in,
                 load_sem, c_send, c_recv, dx_send, dx_recv, dy_send, dy_recv, x_send, x_recv, y_send, y_recv, z_send, z_recv):
        at = Place(nd, nf)
        z, y, x, c, zn = at.z, at.y, at.x, at.c, at.zn
        cols = out_ref.shape[1]
        offs = [sum(r.shape[2] for r in g_refs[:k]) for k in range(len(g_refs))]
        half = cols // 256 * 128
        lo, hi = pl.ds(0, half), pl.ds(half, cols - half)

        def idx(zs, col, core):
            return at.idx(zs, 1 - y if col & 2 else y, 1 - x if col & 1 else x, core)

        def remote(src, dst, to, send, recv):
            return pltpu.make_async_remote_copy(src_ref=src, dst_ref=dst, send_sem=send, recv_sem=recv, device_id=at.dev(*to), device_id_type=MESH)

        def load(zs, col):
            return [pltpu.make_async_copy(r.at[idx(zs, col, c)], acc.at[zs, col, :, pl.ds(o, r.shape[2])], load_sem.at[zs, col, k])
                    for k, (r, o) in enumerate(zip(g_refs, offs))]

        def core(zs, col):
            return [remote(r.at[idx(zs, col, 1 - c)], c_in.at[zs, col, :, pl.ds(o, r.shape[2])], (z, y, x, 1 - c),
                           c_send.at[zs, col, k], c_recv.at[zs, col, k])
                    for k, (r, o) in enumerate(zip(g_refs, offs))]

        def diag_x(zs):
            return remote(acc.at[zs, 3, :, lo], d_in.at[zs, :, lo], (z, y, 1 - x, c), dx_send.at[zs], dx_recv.at[zs])

        def diag_y(zs):
            return remote(acc.at[zs, 3, :, hi], d_in.at[zs, :, hi], (z, 1 - y, x, c), dy_send.at[zs], dy_recv.at[zs])

        def to_x(zs):
            return remote(acc.at[zs, 1], xy_in.at[0, zs], (z, y, 1 - x, c), x_send.at[zs], x_recv.at[zs])

        def to_y(zs):
            return remote(acc.at[zs, 2], xy_in.at[1, zs], (z, 1 - y, x, c), y_send.at[zs], y_recv.at[zs])

        def up(zs):
            return remote(acc.at[zs, 0], z_in.at[zs + 1], (z + 1, y, x, c), z_send.at[zs], z_recv.at[0, zs])

        def down(zs):
            return remote(acc.at[zs, 0], z_in.at[zs], (z - 1, y, x, c), z_send.at[zs], z_recv.at[1, zs])

        def each(dist, fn):
            if dist == 0:
                fn(z)
                return

            @pl.when(z - dist >= 0)
            def _():
                fn(z - dist)

            @pl.when(z + dist < zn)
            def _():
                fn(z + dist)

        order = list(range(zn - 1, -1, -1))

        def start(col):
            for dist in order:
                def one(zs):
                    for cp in core(zs, col) + load(zs, col):
                        cp.start()
                each(dist, one)

        def ready(zs, col):
            for cp in load(zs, col):
                cp.wait()
            for cp in core(zs, col):
                cp.wait_recv()

        def diag(zs):
            ready(zs, 3)
            acc[zs, 3] = acc[zs, 3] + c_in[zs, 3]
            diag_x(zs).start()
            diag_y(zs).start()

        def sides(zs):
            ready(zs, 1)
            diag_y(zs).wait_recv()
            acc[zs, 1, :, lo] = acc[zs, 1, :, lo] + c_in[zs, 1, :, lo]
            acc[zs, 1, :, hi] = acc[zs, 1, :, hi] + c_in[zs, 1, :, hi] + d_in[zs, :, hi]
            to_x(zs).start()
            ready(zs, 2)
            diag_x(zs).wait_recv()
            acc[zs, 2, :, lo] = acc[zs, 2, :, lo] + c_in[zs, 2, :, lo] + d_in[zs, :, lo]
            acc[zs, 2, :, hi] = acc[zs, 2, :, hi] + c_in[zs, 2, :, hi]
            to_y(zs).start()

        def column(zs):
            ready(zs, 0)
            to_x(zs).wait_recv()
            to_y(zs).wait_recv()
            return (acc[zs, 0] + c_in[zs, 0]).astype(f32) + (xy_in[0, zs] + xy_in[1, zs]).astype(f32)

        def pass_on(zs):
            total = column(zs)

            @pl.when(zs > z)
            def _():
                @pl.when(z > 0)
                def _():
                    up(zs).wait_recv()
                    acc[zs, 0] = (total + z_in[zs + 1].astype(f32)).astype(bf16)

                @pl.when(z == 0)
                def _():
                    acc[zs, 0] = total.astype(bf16)
                up(zs).start()

            @pl.when(zs < z)
            def _():
                @pl.when(z < zn - 1)
                def _():
                    down(zs).wait_recv()
                    acc[zs, 0] = (total + z_in[zs].astype(f32)).astype(bf16)

                @pl.when(z == zn - 1)
                def _():
                    acc[zs, 0] = total.astype(bf16)
                down(zs).start()

        def finish():
            out_ref[...] = column(z)

            @pl.when(z > 0)
            def _():
                up(z).wait_recv()
                out_ref[...] += z_in[z + 1].astype(f32)

            @pl.when(z < zn - 1)
            def _():
                down(z).wait_recv()
                out_ref[...] += z_in[z].astype(f32)

            def sent(zs):
                for col in range(4):
                    for cp in core(zs, col):
                        cp.wait_send()
                diag_x(zs).wait_send()
                diag_y(zs).wait_send()
                to_x(zs).wait_send()
                to_y(zs).wait_send()

            for dist in order:
                each(dist, sent)
                if dist:
                    each(dist, lambda zs: up(zs).wait_send())

        self.start, self.finish, self.barrier = start, finish, at.barrier
        self.diag = [functools.partial(each, dist, diag) for dist in order]
        self.sides = [functools.partial(each, dist, sides) for dist in order]
        self.pass_on = [functools.partial(each, dist, pass_on) for dist in order[:-1]]

    @staticmethod
    def scratch(nd, rows, cols, parts):
        zn = nd // 2
        D, V = pltpu.SemaphoreType.DMA, pltpu.VMEM
        return [V((zn, 4, rows, cols), bf16), V((zn, 4, rows, cols), bf16), V((zn, rows, cols), bf16), V((2, zn, rows, cols), bf16),
                V((zn + 1, rows, cols), bf16), D((zn, 4, parts)), D((zn, 4, parts)), D((zn, 4, parts))] + [D((zn,))] * 9 + [D((2, zn))]


def plan(pipes, barrier, diag, sides, side_gap, pass_on, pass_gap):
    ticks = {0: [barrier] + [functools.partial(p.start, col) for col in (3, 1, 2, 0) for p in pipes]}
    for m, p in enumerate(pipes):
        ticks.setdefault(diag + m, []).extend(p.diag)
        for k, fn in enumerate(p.sides):
            ticks.setdefault(sides + k * side_gap + m * (side_gap // 2), []).append(fn)
        for k, fn in enumerate(p.pass_on):
            ticks.setdefault(pass_on + k * pass_gap + m * (pass_gap // 2), []).append(fn)
    return ticks


def columns(refs, split):
    return [[refs[a].at[:, :, pl.ds(o, w)] for a, o, w in pipe] for pipe in split]


def pipes_of(nd, nf, g_refs, out_ref, split, scratch):
    pipes, off = [], 0
    per = len(scratch) // len(split)
    for m, (views, pipe) in enumerate(zip(columns(g_refs, split), split)):
        width = sum(w for _, _, w in pipe)
        pipes.append(Scatter(nd, nf, views, out_ref.at[:, pl.ds(off, width)], *scratch[per * m : per * (m + 1)]))
        off += width
    return pipes


def pipes_scratch(nd, rows, split):
    return [x for pipe in split for x in Scatter.scratch(nd, rows, sum(w for _, _, w in pipe), len(pipe))]


def run_ticks(ticks, now, last):
    for tick, fns in ticks.items():
        if tick <= last:
            @pl.when(now == tick)
            def _(fns=fns):
                for fn in fns:
                    fn()


def run_rest(ticks, last):
    for tick, fns in sorted(ticks.items()):
        if tick > last:
            for fn in fns:
                fn()


class Spread:
    def __init__(self, nd, nf, src, got, send, recv):
        self.n, self.nf = nd * nf, nf
        self.me = lax.axis_index("dp") * nf + lax.axis_index("fsdp")
        self.src, self.got, self.send, self.recv = src, got, send, recv

    def peer(self, k):
        return lax.rem(self.me + k, self.n)

    def loop(self, fn):
        def body(k, carry):
            fn(k)
            return carry
        lax.fori_loop(1, self.n, body, 0)

    def barrier(self):
        sem = pltpu.get_barrier_semaphore()

        def greet(k):
            pl.semaphore_signal(sem, inc=1, device_id=(self.peer(k) // self.nf, self.peer(k) % self.nf), device_id_type=MESH)
        self.loop(greet)
        pl.semaphore_wait(sem, self.n - 1)

    def copy(self, k):
        p = self.peer(k)
        src = self.src.at[p] if len(self.src.shape) == 3 else self.src
        return pltpu.make_async_remote_copy(src_ref=src, dst_ref=self.got.at[k], send_sem=self.send.at[k], recv_sem=self.recv.at[k],
                                            device_id=(p // self.nf, p % self.nf), device_id_type=MESH)

    def begin(self):
        self.loop(lambda k: self.copy(k).start())

    def total(self):
        own = self.src[self.me] if len(self.src.shape) == 3 else self.src[...]

        def add(k, total):
            self.copy(k).wait_recv()
            return total + self.got[k]
        total = lax.fori_loop(1, self.n, add, own)
        self.loop(lambda k: self.copy(k).wait_send())
        return total

    @staticmethod
    def scratch(n, tile):
        D = pltpu.SemaphoreType.DMA
        return [pltpu.VMEM((n,) + tile, f32), D((n,)), D((n,))]


def dot(a, b, dims=((1,), (0,)), precision=None):
    return lax.dot_general(a, b, (dims, ((), ())), preferred_element_type=f32, precision=precision)


def sigmoid(x):
    return 0.5 * jnp.tanh(0.5 * x) + 0.5


def conv_rows(ext, taps, masks, halo):
    rows = ext.shape[0] - halo
    width = 4
    v = ext[halo:]
    out = taps[4:5] + taps[3:4] * v
    for k in range(1, width):
        moved = pltpu.roll(ext, k, 0)[halo:]
        out = out + (taps[3 - k : 4 - k] * masks[:, k : k + 1]) * moved
    return out


def prep_kernel(bcdt_ref, taps_ref, heads_ref, m_ref, segc_ref, segr_ref,
                b_ref, c_ref, bt_ref, ct_ref, pre_ref, gm_ref, cum_ref, cumr_ref, sc_ref, dt_ref):
    T = bcdt_ref.shape[0]
    nc = T // L
    N = b_ref.shape[1]
    H = dt_ref.shape[1]
    groups = cumr_ref.shape[0]
    taps = taps_ref[...]
    tri = (lax.broadcasted_iota(jnp.int32, (L, L), 0) >= lax.broadcasted_iota(jnp.int32, (L, L), 1))
    trif = tri.astype(f32)
    neg_rate = -jnp.exp(heads_ref[0:1, :H]) * LOG2E
    bias = heads_ref[1:2, :H]

    def chunk(c, carry):
        t0 = pl.multiple_of(c * L, L)
        here = pl.ds(t0, L)
        h0 = pl.multiple_of(jnp.maximum(t0 - 16, 0), 16)
        before = bcdt_ref[pl.ds(h0, 16), : 2 * N].astype(f32)
        v = bcdt_ref[here, : 2 * N].astype(f32)
        pre = conv_rows(jnp.concatenate([before, v], axis=0), taps, m_ref[here, :], 16)
        pre_ref[here, :] = pre
        act = pre * sigmoid(pre)
        b = act[:, :N]
        cc = act[:, N:]
        bb = b.astype(bf16)
        cb = cc.astype(bf16)
        b_ref[here, :] = bb
        c_ref[here, :] = cb
        bt_ref[:, here] = b.T.astype(bf16)
        ct_ref[:, here] = cc.T.astype(bf16)
        segc = segc_ref[here, 0:1]
        prev = segc_ref[here, 1:2]
        last = segc_ref[here, 2:3]
        same = segc == segr_ref[:, here]
        g = dot(cb, bb, ((1,), (1,)))
        gm_ref[pl.ds(c, 1)] = jnp.where(tri & same, g, 0.0)[None]
        raw = bcdt_ref[here, 2 * N : 2 * N + 128].astype(f32)[:, :H] + bias
        dt = jnp.maximum(raw, 0.0) + jnp.log1p(jnp.exp(-jnp.abs(raw)))
        a2 = neg_rate * dt
        cum = dot(trif, a2, precision=HIGHEST)
        end = cum[L - 1 : L]
        ein = jnp.where(segc == prev, jnp.exp2(cum), 0.0)
        lv = jnp.where(segc == last, jnp.exp2(end - cum), 0.0)
        dt_ref[here, :] = dt
        wide = jnp.concatenate([cum, jnp.zeros((L, 128 - H), f32)], axis=1)
        cum_ref[here, :] = wide
        cumt = wide.T
        for k in range(groups):
            cumr_ref[k, :, here] = cumt[HG * k : HG * (k + 1)]
        s0 = pl.multiple_of(c * (3 * L), L)
        for k, part in enumerate((dt, ein, lv)):
            sc_ref[pl.ds(s0 + k * L, L), :] = jnp.concatenate([part, jnp.zeros((L, 128 - H), f32)], axis=1).astype(bf16)
        return carry

    lax.fori_loop(0, nc, chunk, 0)


def prep(bcdt, taps, heads, masks, segc, segr, N, H):
    T = bcdt.shape[0]
    nc = T // L
    G = H // HG
    S = jax.ShapeDtypeStruct
    full = lambda a: pl.BlockSpec(a.shape, lambda i: (0,) * a.ndim)
    outs = (S((T, N), bf16), S((T, N), bf16), S((N, T), bf16), S((N, T), bf16), S((T, 2 * N), f32),
            S((nc, L, L), f32), S((T, 128), f32), S((G, HG, T), f32), S((3 * T, 128), bf16), S((T, H), f32))
    wide = 2 * N + 128
    return pl.pallas_call(
        prep_kernel,
        grid=(1,),
        in_specs=[pl.BlockSpec((T, wide), lambda i: (0, bcdt.shape[1] // wide - 1))] + [full(a) for a in (taps, heads, masks, segc, segr)],
        out_specs=[full(o) for o in outs],
        out_shape=outs,
        compiler_params=pltpu.CompilerParams(vmem_limit_bytes=60 << 20),
    )(bcdt, taps, heads, masks, segc, segr)


def lane_onehot(group, width, per):
    shape = (128, width)
    return (group * HG + lax.broadcasted_iota(jnp.int32, shape, 1) // per == lax.broadcasted_iota(jnp.int32, shape, 0)).astype(bf16)


def half_masks(P):
    lane = lax.broadcasted_iota(jnp.int32, (1, 2 * P), 1)
    first = (lane < P).astype(f32)
    return first.astype(bf16), (1.0 - first).astype(bf16)


def decay(cum4, cumr, k):
    return jnp.exp2(jnp.minimum(cum4[:, k : k + 1] - cumr[k : k + 1, :], 0.0))


def fwd_kernel(u_ref, gate_ref, taps_ref, m_ref, b_ref, c_ref, bt_ref, gm_ref, cum_ref, cumr_ref, sc_ref,
               gg_ref, ssq_ref, pre_ref, st_ref, state):
    T, W = u_ref.shape
    P = W // HG
    nc = T // L
    step = pl.program_id(0)
    taps = taps_ref[...]
    gain = taps[5:6]
    skip = taps[6:7]
    onehot = lane_onehot(step, W, P)
    ma, mb = half_masks(P)
    state[...] = jnp.zeros_like(state)

    @pl.when(step == 0)
    def _():
        ssq_ref[...] = jnp.zeros_like(ssq_ref)

    def chunk(c, carry):
        t0 = pl.multiple_of(c * L, L)
        here = pl.ds(t0, L)
        h0 = pl.multiple_of(jnp.maximum(t0 - 16, 0), 16)
        ext = jnp.concatenate([u_ref[pl.ds(h0, 16), :], u_ref[here, :]], axis=0).astype(f32)
        pre = conv_rows(ext, taps, m_ref[here, :], 16)
        pre_ref[here, :] = pre.astype(bf16)
        x = pre * sigmoid(pre)
        s0 = pl.multiple_of(c * (3 * L), L)
        exp = dot(sc_ref[pl.ds(s0, 3 * L), :], onehot)
        dtx, einx, lvx = exp[:L], exp[L : 2 * L], exp[2 * L :]
        xd = x * dtx
        xdb = xd.astype(bf16)
        gm = gm_ref[c]
        cum4 = pltpu.roll(cum_ref[here, :], 128 - step * HG, 1)
        cumr = cumr_ref[0, :, here]
        sb = state[...].astype(bf16)
        st_ref[c] = sb
        inner = []
        for p in range(HG // 2):
            m0 = (decay(cum4, cumr, 2 * p) * gm).astype(bf16)
            m1 = (decay(cum4, cumr, 2 * p + 1) * gm).astype(bf16)
            xp = xdb[:, 2 * P * p : 2 * P * (p + 1)]
            inner.append(dot(jnp.concatenate([m0, m1], axis=1), jnp.concatenate([xp * ma, xp * mb], axis=0)))
        y = jnp.concatenate(inner, axis=1) + dot(c_ref[here, :], sb) * einx + skip * x
        state[...] = state[...] * einx[L - 1 : L] + dot(bt_ref[:, here], (xd * lvx).astype(bf16))
        gate = gate_ref[here, :].astype(f32)
        g = y * (gate * sigmoid(gate))
        gg_ref[here, :] = (g * gain).astype(bf16)
        g2 = g * g
        tot = g2[:, :128]
        for j in range(1, W // 128):
            tot = tot + g2[:, 128 * j : 128 * (j + 1)]
        ssq_ref[here, :] += tot
        return carry

    lax.fori_loop(0, nc, chunk, 0)


def fwd(u, gate, taps, masks, b, c, bt, gm, cum, cumr, sc):
    T, E = gate.shape
    N = b.shape[1]
    G = cumr.shape[0]
    W = E // G
    nc = T // L
    S = jax.ShapeDtypeStruct
    col = lambda off: pl.BlockSpec((T, W), lambda g: (0, g + off))
    full = lambda a: pl.BlockSpec(a.shape, lambda g: (0,) * a.ndim)
    grp = lambda a: pl.BlockSpec((1,) + a.shape[1:], lambda g: (g, 0, 0))
    return pl.pallas_call(
        fwd_kernel,
        grid=(G,),
        in_specs=[col(0), col(0), pl.BlockSpec((8, W), lambda g: (0, g)), full(masks), full(b), full(c), full(bt), full(gm),
                  full(cum), grp(cumr), full(sc)],
        out_specs=[col(0), pl.BlockSpec((T, 128), lambda g: (0, 0)), col(0), pl.BlockSpec((nc, N, W), lambda g: (0, 0, g))],
        out_shape=(S((T, E), bf16), S((T, 128), f32), S((T, E), bf16), S((nc, N, E), bf16)),
        scratch_shapes=[pltpu.VMEM((N, W), f32)],
        compiler_params=pltpu.CompilerParams(vmem_limit_bytes=60 << 20),
        cost_estimate=pl.CostEstimate(flops=T * E * (2 * L + 4 * N) * 2, bytes_accessed=T * E * 12, transcendentals=T * E * 4),
    )(u, gate, taps, masks, b, c, bt, gm, cum, cumr, sc)


def bwd_scatter_kernel(nd, nf, g0, arrays, split, *refs):
    g_refs, ins, outs = refs[:arrays], refs[arrays : arrays + 15], refs[arrays + 15 : arrays + 23]
    own, comm = refs[arrays + 23 : arrays + 26], refs[arrays + 26 :]
    pipes = pipes_of(nd, nf, g_refs, outs[7], split, comm)
    ticks = plan(pipes, pipes[0].barrier, *BWD_PLAN)
    bwd_body(lambda now: run_ticks(ticks, now, BWD_TICKS), g0, *ins, *outs[:7], *own)

    @pl.when(pl.program_id(0) == pl.num_programs(0) - 1)
    def _():
        run_rest(ticks, BWD_TICKS)
        for p in pipes:
            p.finish()


def bwd_body(tick, g0, u_ref, gate_ref, pre_ref, dm_ref, rq_ref, taps_ref, m_ref, b_ref, c_ref, ct_ref, gm_ref, cum_ref, cumr_ref, sc_ref, st_ref,
               dz_ref, dg_ref, db_ref, dc_ref, rs_ref, small_ref, kk_ref, ds, nxt, acc):
    T, W = u_ref.shape
    P = W // HG
    nc = T // L
    step = pl.program_id(0)
    taps = taps_ref[...]
    gain = taps[5:6]
    skip = taps[6:7]
    onehot = lane_onehot(step + g0, W, P)
    ma, mb = half_masks(P)
    ds[...] = jnp.zeros_like(ds)
    nxt[...] = jnp.zeros_like(nxt)
    acc[...] = jnp.zeros_like(acc)

    @pl.when(step == 0)
    def _():
        dg_ref[...] = jnp.zeros_like(dg_ref)
        db_ref[...] = jnp.zeros_like(db_ref)
        dc_ref[...] = jnp.zeros_like(dc_ref)
        rs_ref[...] = jnp.zeros_like(rs_ref)

    ri = lax.broadcasted_iota(jnp.int32, (4 * W, 128), 0)
    ci = lax.broadcasted_iota(jnp.int32, (4 * W, 128), 1)
    part = ri // W
    want = (jnp.maximum(part - 1, 0) * pl.num_programs(0) + step) * HG + (ri % W) // P
    fold = (want == ci).astype(bf16)

    def eight(z):
        return jnp.sum(z.reshape(L // 8, 8, W), axis=0)

    def chunk(i, carry):
        tick(step * nc + i)
        c = nc - 1 - i
        t0 = pl.multiple_of(c * L, L)
        here = pl.ds(t0, L)
        u = u_ref[here, :].astype(f32)
        pre = pre_ref[here, :].astype(f32)
        sig = sigmoid(pre)
        x = pre * sig
        dsilu = sig + x * (1.0 - sig)
        s0 = pl.multiple_of(c * (3 * L), L)
        exp = dot(sc_ref[pl.ds(s0, 3 * L), :], onehot)
        dtx, einx, lvx = exp[:L], exp[L : 2 * L], exp[2 * L :]
        xdb = (x * dtx).astype(bf16)
        xd = xdb.astype(f32)
        gm = gm_ref[c]
        cum4 = pltpu.roll(cum_ref[here, :], 128 - (step + g0) * HG, 1)
        cumr = cumr_ref[0, :, here]
        sb = st_ref[c]
        es, ms, inner = [], [], []
        for p in range(HG // 2):
            e0 = decay(cum4, cumr, 2 * p)
            e1 = decay(cum4, cumr, 2 * p + 1)
            m0 = (e0 * gm).astype(bf16)
            m1 = (e1 * gm).astype(bf16)
            xp = xdb[:, 2 * P * p : 2 * P * (p + 1)]
            inner.append(dot(jnp.concatenate([m0, m1], axis=1), jnp.concatenate([xp * ma, xp * mb], axis=0)))
            es.append((e0, e1))
            ms.append((m0, m1))
        yn = jnp.concatenate(inner, axis=1) + dot(c_ref[here, :], sb) * einx
        y = yn + skip * x
        gate = gate_ref[here, :].astype(f32)
        sgate = sigmoid(gate)
        silu_g = gate * sgate
        g = y * silu_g
        r = rq_ref[here, 0:1]
        q = rq_ref[here, 1:2]
        dmr = dm_ref[here, :].astype(f32) * r
        dgg = gain * dmr - g * q
        dyb = (dgg * silu_g).astype(bf16)
        dy = dyb.astype(f32)
        dz_ref[0, here, :] = (dgg * y * (sgate + silu_g * (1.0 - sgate))).astype(bf16)
        dxi = []
        dgc = dg_ref[c]
        for p in range(HG // 2):
            cols = slice(2 * P * p, 2 * P * (p + 1))
            dp = dyb[:, cols]
            dstack = jnp.concatenate([dp * ma, dp * mb], axis=0)
            dmm = dot(dstack, xdb[:, cols], ((1,), (1,)))
            dgc = dgc + dmm[:L] * es[p][0] + dmm[L:] * es[p][1]
            dxi.append(dot(jnp.concatenate(ms[p], axis=0), dstack, ((0,), (0,))))
        dg_ref[c] = dgc
        dxi = jnp.concatenate(dxi, axis=1)
        dsn = ds[...]
        dsb = dsn.astype(bf16)
        dye = (dy * einx).astype(bf16)
        dc_ref[here, :] += dot(dye, sb, ((1,), (1,)))
        kept = einx[L - 1 : L]
        kk_ref[pl.ds(c, 1), :] = kept * jnp.sum(sb.astype(f32) * dsn, axis=0, keepdims=True)
        db_ref[here, :] += dot((xd * lvx).astype(bf16), dsb, ((1,), (1,)))
        dxe = dot(b_ref[here, :], dsb) * lvx
        ds[...] = dsn * kept + dot(ct_ref[:, here], dye)
        dxd = dxi + dxe
        r1 = dy * yn - xd * dxi
        r1h = r1.astype(bf16)
        r1l = (r1 - r1h.astype(f32)).astype(bf16)
        rs_ref[here, :] += dot(jnp.concatenate([r1h, r1l, (xd * dxe).astype(bf16), (x * dxd).astype(bf16)], axis=1), fold)
        dpre = (dxd * dtx + skip * dy) * dsilu
        ext = jnp.concatenate([dpre, nxt[...]], axis=0)
        nxt[...] = dpre[:8]
        du = taps[3:4] * dpre
        acc[0:8, :] += eight(dmr * g)
        acc[8:16, :] += eight(dy * x)
        acc[16:24, :] += eight(dpre)
        acc[24:32, :] += eight(dpre * u)
        mrows = m_ref[pl.ds(t0, L + 8), :]
        for k in range(1, 4):
            sk = pltpu.roll(ext * mrows[:, k : k + 1], L + 8 - k, 0)[:L]
            du = du + taps[3 - k : 4 - k] * sk
            acc[24 + 8 * k : 32 + 8 * k, :] += eight(sk * u)
        dz_ref[1, here, :] = du.astype(bf16)
        return carry

    lax.fori_loop(0, nc, chunk, 0)
    for j in range(7):
        small_ref[j : j + 1, :] = jnp.sum(acc[8 * j : 8 * j + 8, :], axis=0, keepdims=True)
    small_ref[7:8, :] = jnp.zeros((1, W), f32)


def bwd(half, halves, u, gate, pre, dm, rq, taps, masks, b, c, ct, gm, cum, cumr, sc, st, comm):
    T, E = gate.shape
    N = b.shape[1]
    G = cumr.shape[0]
    W = E // G
    nc = T // L
    Gh = G // halves
    Eh = E // halves
    g0 = half * Gh
    S = jax.ShapeDtypeStruct
    col = pl.BlockSpec((T, W), lambda g: (0, g + g0))
    full = lambda a: pl.BlockSpec(a.shape, lambda g: (0,) * a.ndim)
    whole = lambda s: pl.BlockSpec(s, lambda g: (0,) * len(s))
    grp = lambda a: pl.BlockSpec((1,) + a.shape[1:], lambda g: (g + g0, 0, 0))
    in_specs = [col, col, col, col, full(rq), pl.BlockSpec((8, W), lambda g: (0, g + g0)), full(masks), full(b), full(c),
                full(ct), full(gm), full(cum), grp(cumr), full(sc), pl.BlockSpec((nc, N, W), lambda g: (0, 0, g + g0))]
    out_specs = [pl.BlockSpec((2, T, W), lambda g: (0, 0, g)), whole((nc, L, L)), whole((T, N)), whole((T, N)),
                 whole((T, 128)), pl.BlockSpec((8, W), lambda g: (0, g)), pl.BlockSpec((nc, W), lambda g: (0, g))]
    out_shape = [S((2, T, Eh), bf16), S((nc, L, L), f32), S((T, N), f32), S((T, N), f32), S((T, 128), f32), S((8, Eh), f32), S((nc, Eh), f32)]
    scratch = [pltpu.VMEM((N, W), f32), pltpu.VMEM((8, W), f32), pltpu.VMEM((56, W), f32)]
    nd, nf, cid, first, split = comm
    rows, cols = first[0].shape[1], sum(w for pipe in split for _, _, w in pipe)
    return pl.pallas_call(
        functools.partial(bwd_scatter_kernel, nd, nf, g0, len(first), split),
        grid=(Gh,),
        in_specs=[pl.BlockSpec(memory_space=pl.ANY)] * len(first) + in_specs,
        out_specs=out_specs + [whole((rows, cols))],
        out_shape=out_shape + [S((rows, cols), f32)],
        scratch_shapes=scratch + pipes_scratch(nd, rows, split),
        compiler_params=pltpu.CompilerParams(vmem_limit_bytes=60 << 20, collective_id=cid, has_side_effects=True),
        cost_estimate=pl.CostEstimate(flops=T * Eh * (8 * L + 12 * N), bytes_accessed=T * Eh * 16, transcendentals=T * Eh * 4),
    )(*first, u, gate, pre, dm, rq, taps, masks, b, c, ct, gm, cum, cumr, sc, st)


def post_kernel(bcdt_ref, pre_ref, taps_ref, heads_ref, m_ref, segc_ref, segr_ref, b_ref, c_ref, dg0_ref, db0_ref, dc0_ref, rs0_ref, dg1_ref, db1_ref, dc1_ref, rs1_ref, kk_ref, dt_ref,
                out_ref, small_ref, hs_ref, nxt, acc, hacc):
    T = bcdt_ref.shape[0]
    nc = T // L
    N = b_ref.shape[1]
    H = dt_ref.shape[1]
    taps = taps_ref[...]
    tri = (lax.broadcasted_iota(jnp.int32, (L, L), 0) >= lax.broadcasted_iota(jnp.int32, (L, L), 1))
    upper = (lax.broadcasted_iota(jnp.int32, (L, L), 0) <= lax.broadcasted_iota(jnp.int32, (L, L), 1)).astype(f32)
    strict = 1.0 - upper
    rate = -jnp.exp(heads_ref[0:1, :H])
    bias = heads_ref[1:2, :H]
    nxt[...] = jnp.zeros_like(nxt)
    acc[...] = jnp.zeros_like(acc)
    hacc[...] = jnp.zeros_like(hacc)

    def eight(z):
        return jnp.sum(z.reshape(L // 8, 8, z.shape[1]), axis=0)

    def chunk(i, carry):
        c = nc - 1 - i
        t0 = pl.multiple_of(c * L, L)
        here = pl.ds(t0, L)
        same = segc_ref[here, 0:1] == segr_ref[:, here]
        dg = jnp.where(tri & same, dg0_ref[c] + dg1_ref[c], 0.0)
        dgb = dg.astype(bf16)
        dcv = dc0_ref[here, :] + dc1_ref[here, :] + dot(dgb, b_ref[here, :])
        dbv = db0_ref[here, :] + db1_ref[here, :] + dot(dg.T.astype(bf16), c_ref[here, :])
        pre = pre_ref[here, :]
        sig = sigmoid(pre)
        dpre = jnp.concatenate([dbv, dcv], axis=1) * (sig + pre * sig * (1.0 - sig))
        v = bcdt_ref[here, : 2 * N].astype(f32)
        ext = jnp.concatenate([dpre, nxt[...]], axis=0)
        nxt[...] = dpre[:8]
        dv = taps[3:4] * dpre
        acc[0:8, :] += eight(dpre)
        acc[8:16, :] += eight(dpre * v)
        mrows = m_ref[pl.ds(t0, L + 8), :]
        for k in range(1, 4):
            sk = pltpu.roll(ext * mrows[:, k : k + 1], L + 8 - k, 0)[:L]
            dv = dv + taps[3 - k : 4 - k] * sk
            acc[8 + 8 * k : 16 + 8 * k, :] += eight(sk * v)
        out_ref[here, : 2 * N] = dv.astype(bf16)
        q = H // 2
        r0, r1 = rs0_ref[here, :], rs1_ref[here, :]
        r1, r2, r3 = (jnp.concatenate([r0[:, m * q : (m + 1) * q], r1[:, m * q : (m + 1) * q]], axis=1) for m in range(3))
        da = dot(upper, r1, precision=HIGHEST) + dot(strict, r2, precision=HIGHEST) + kk_ref[pl.ds(c, 1), :]
        dt = dt_ref[here, :]
        raw = bcdt_ref[here, 2 * N : 2 * N + 128].astype(f32)[:, :H] + bias
        ddt = (r3 + da * rate) * sigmoid(raw)
        hacc[0:8, :] += eight(da * rate * dt)
        hacc[8:16, :] += eight(ddt)
        out_ref[here, 2 * N :] = jnp.concatenate([ddt, jnp.zeros((L, out_ref.shape[1] - 2 * N - H), f32)], axis=1).astype(bf16)
        return carry

    lax.fori_loop(0, nc, chunk, 0)
    for j in range(5):
        small_ref[j : j + 1, :] = jnp.sum(acc[8 * j : 8 * j + 8, :], axis=0, keepdims=True)
    small_ref[5:8, :] = jnp.zeros((3, 2 * N), f32)
    for j in range(2):
        hs_ref[j : j + 1, :] = jnp.sum(hacc[8 * j : 8 * j + 8, :], axis=0, keepdims=True)


def post(bcdt, pre, taps, heads, masks, segc, segr, b, c, first, second, kk, dt):
    T = bcdt.shape[0]
    N = b.shape[1]
    H = dt.shape[1]
    S = jax.ShapeDtypeStruct
    wide = 2 * N + 128
    full = lambda a: pl.BlockSpec(a.shape, lambda i: (0,) * a.ndim)
    ins = (bcdt, pre, taps, heads, masks, segc, segr, b, c, *first, *second, kk, dt)
    outs = (S((T, wide), bf16), S((8, 2 * N), f32), S((2, H), f32))
    return pl.pallas_call(
        post_kernel,
        grid=(1,),
        in_specs=[pl.BlockSpec((T, wide), lambda i: (0, bcdt.shape[1] // wide - 1))] + [full(a) for a in ins[1:]],
        out_specs=[full(o) for o in outs],
        out_shape=outs,
        scratch_shapes=[pltpu.VMEM((8, 2 * N), f32), pltpu.VMEM((40, 2 * N), f32), pltpu.VMEM((16, H), f32)],
        compiler_params=pltpu.CompilerParams(vmem_limit_bytes=60 << 20),
    )(*ins)


NT = 256


def tail_kernel(nd, nf, arrays, split, tiles, *refs):
    g_refs, refs = refs[:arrays], refs[arrays:]
    (wo_hbm, wg_hbm, wa_hbm, gg_ref, dz0_ref, dz1_ref, dbc_ref, hid_ref, go_ref, r_ref, gain_ref, mine_ref,
     sum_ref, out_ref, gin_ref, small_ref, dnorm_ref) = refs[:17]
    wo, wg, wa, acc, dn, flat, sem = refs[17:24]
    mine = Spread(nd, nf, mine_ref, *refs[24:27])
    norm = Spread(nd, nf, flat, *refs[27:30])
    pipes = pipes_of(nd, nf, g_refs, sum_ref, split, refs[30:])
    D, E = wg.shape
    Eh = E // 2
    step = pl.program_id(0)
    early = tiles // 2
    blocks = D // NT
    ticks = plan(pipes, mine.barrier, *TAIL_PLAN)
    ticks[0].append(mine.begin)
    ticks.setdefault((early + tiles) * blocks + 2, []).append(norm.begin)
    fetch = [pltpu.make_async_copy(src, dst, sem.at[k]) for k, (src, dst) in enumerate(((wo_hbm, wo), (wg_hbm, wg), (wa_hbm, wa)))]

    @pl.when(step == 0)
    def _():
        for cp in fetch:
            cp.start()
        dn[...] = jnp.zeros_like(dn)
        run_ticks(ticks, 0, 0)
        fetch[0].wait()

    @pl.when(step == early)
    def _():
        fetch[1].wait()
        fetch[2].wait()

    back = (step >= early) & (step < early + tiles)
    in_back = lambda t: early * blocks <= t < (early + tiles) * blocks

    @pl.when(jnp.logical_not(back))
    def _():
        def block(j, carry):
            run_ticks({t: f for t, f in ticks.items() if t and not in_back(t)}, step * blocks + j, TAIL_TICKS)
            cols = pl.ds(pl.multiple_of(j * NT, NT), NT)
            out_ref[:, cols] = (hid_ref[:, cols].astype(f32) + r_ref[...] * dot(gg_ref[...], wo[:, cols])).astype(bf16)
            return carry
        lax.fori_loop(0, blocks, block, 0)

    @pl.when(back)
    def _():
        def block(j, carry):
            run_ticks({t: f for t, f in ticks.items() if in_back(t)}, step * blocks + j, TAIL_TICKS)
            cols = pl.ds(pl.multiple_of(j * NT, NT), NT)
            part = dot(dz0_ref[0], wg[cols, :Eh], ((1,), (1,))) + dot(dz1_ref[0], wg[cols, Eh:], ((1,), (1,)))
            part = part + dot(dz0_ref[1], wa[cols, :Eh], ((1,), (1,))) + dot(dz1_ref[1], wa[cols, Eh:E], ((1,), (1,)))
            acc[:, cols] = part + dot(dbc_ref[...], wa[cols, E:], ((1,), (1,)))
            return carry
        lax.fori_loop(0, blocks, block, 0)
        gain = gain_ref[...]

        def rows_of(i, carry):
            here = pl.ds(pl.multiple_of(i * 64, 64), 64)
            rows = hid_ref[here, :].astype(f32)
            rinv = lax.rsqrt(jnp.mean(rows * rows, axis=-1, keepdims=True) + EPS)
            xhat = rows * rinv
            bn = acc[here, :]
            prod = bn * xhat
            dn[...] += jnp.sum(prod.reshape(8, 8, D), axis=0)
            mean = jnp.mean(prod * gain, axis=-1, keepdims=True)
            gin_ref[here, :] = (go_ref[here, :].astype(f32) + rinv * (bn * gain - xhat * mean)).astype(bf16)
            return carry
        lax.fori_loop(0, hid_ref.shape[0] // 64, rows_of, 0)

    @pl.when(step == early + tiles - 1)
    def _():
        flat[...] = jnp.zeros_like(flat)
        for j in range(D // 128):
            flat[j : j + 1, :] = jnp.sum(dn[:, 128 * j : 128 * (j + 1)], axis=0, keepdims=True)

    @pl.when(step == 2 * tiles - 1)
    def _():
        run_rest(ticks, TAIL_TICKS)
        for p in pipes:
            p.finish()
        small_ref[...] = mine.total()
        dnorm_ref[...] = norm.total()


def tail(nd, nf, cid, gs, split, dz0, dz1, dbcdt, full_gate, full_a, gg, full_out, hidden, grad_out, r, norm_gain, mine):
    T, D = hidden.shape
    E = full_out.shape[0]
    n = nd * nf
    rows, cols = gs[0].shape[1], sum(w for pipe in split for _, _, w in pipe)
    MT = 256 if rows % 16 == 0 else 128
    tiles = T // MT
    early = tiles // 2
    wide = dbcdt.shape[1]
    S = jax.ShapeDtypeStruct
    any_ = pl.BlockSpec(memory_space=pl.ANY)
    whole = lambda s: pl.BlockSpec(s, lambda k: (0,) * len(s), pipeline_mode=pl.Buffered(1))
    at_out = lambda k: jnp.minimum(k, early - 1) + jnp.clip(k - tiles - early + 1, 0, tiles - early)
    at_back = lambda k: jnp.clip(k - early, 0, tiles - 1)
    at_row = lambda k: k - early * jnp.clip(k - early + 1, 0, 1) - (tiles - early) * jnp.clip(k - early - tiles + 1, 0, 1)
    out_tile = lambda w: pl.BlockSpec((MT, w), lambda k: (at_out(k), 0))
    back_tile = lambda w: pl.BlockSpec((MT, w), lambda k: (at_back(k), 0))
    half = pl.BlockSpec((2, MT, E // 2), lambda k: (0, at_back(k), 0))
    tile, ntile = mine.shape[1:], (-(-D // 1024) * 8, 128)
    return pl.pallas_call(
        functools.partial(tail_kernel, nd, nf, len(gs), split, tiles),
        grid=(2 * tiles,),
        in_specs=[any_] * (len(gs) + 3) + [out_tile(E), half, half, back_tile(wide), pl.BlockSpec((MT, D), lambda k: (at_row(k), 0)), back_tile(D),
                                           out_tile(1), whole((1, D)), whole(mine.shape)],
        out_specs=[whole((rows, cols)), out_tile(D), back_tile(D), whole(tile), whole(ntile)],
        out_shape=(S((rows, cols), f32), S((T, D), bf16), S((T, D), bf16), S(tile, f32), S(ntile, f32)),
        scratch_shapes=[pltpu.VMEM((E, D), bf16), pltpu.VMEM((D, E), bf16), pltpu.VMEM((D, E + wide), bf16), pltpu.VMEM((MT, D), f32),
                        pltpu.VMEM((8, D), f32), pltpu.VMEM(ntile, f32), pltpu.SemaphoreType.DMA((3,))]
        + Spread.scratch(n, tile) + Spread.scratch(n, ntile) + pipes_scratch(nd, rows, split),
        compiler_params=pltpu.CompilerParams(collective_id=cid, has_side_effects=True, vmem_limit_bytes=67043328),
        cost_estimate=pl.CostEstimate(flops=2 * T * D * 3 * E, bytes_accessed=8 * D * E, transcendentals=0),
    )(*gs, full_out, full_gate, full_a, gg, dz0, dz1, dbcdt, hidden, grad_out, r, norm_gain, mine)


def layer(nd, nf, hidden, grad_out, seg, shard_a, shard_gate, shard_out, head_params, sizes):
    n = nd * nf
    E, N, H, K1, S = sizes
    T, D = hidden.shape
    wide = 2 * N + 128
    full_gate = lax.all_gather(shard_gate, AXES, axis=0, tiled=True)
    full_out = lax.all_gather(shard_out, AXES, axis=0, tiled=True)
    full_a = gather_rows(shard_a, nd, nf, 0)
    off = E + 2 * N + H
    flat = full_a[:, :, off : off + S].reshape(n, -1)
    ncol, nrow, ngate = (E + 2 * N) // n, D // n, E // n
    conv = flat[:, : K1 * ncol].reshape(n, K1, ncol).transpose(1, 0, 2).reshape(K1, n * ncol).astype(f32)
    norm_gain = flat[:, K1 * ncol : K1 * ncol + nrow].reshape(-1).astype(f32)
    gate_gain = flat[:, K1 * ncol + nrow : K1 * ncol + nrow + ngate].reshape(-1).astype(f32)
    full_a = full_a.reshape(D, E + wide)
    rows = hidden.astype(f32)
    rinv = lax.rsqrt(jnp.mean(rows * rows, axis=-1, keepdims=True) + EPS)
    xhat = rows * rinv
    normed = (xhat * norm_gain).astype(bf16)
    ubc = dot(normed, full_a).astype(bf16)
    gate = dot(normed, full_gate).astype(bf16)
    pos = jnp.arange(T, dtype=jnp.int32)
    masks = jnp.stack([jnp.ones((T,), f32)] + [((jnp.roll(seg, k) == seg) & (pos >= k)).astype(f32) for k in range(1, 4)], axis=1)
    lastid = seg[L - 1 :: L]
    previd = jnp.concatenate([jnp.full((1,), -1, jnp.int32), lastid[:-1]])
    segc = jnp.stack([seg, jnp.repeat(previd, L), jnp.repeat(lastid, L)], axis=1)
    segr = seg[None, :]
    taps_u = jnp.concatenate([conv[:, :E], gate_gain[None], jnp.repeat(head_params[2], E // H)[None], jnp.zeros((1, E), f32)], axis=0)
    taps_bc = jnp.concatenate([conv[:, E:], jnp.zeros((3, 2 * N), f32)], axis=0)
    heads_p = jnp.pad(head_params, ((0, 5), (0, 128 - H)))
    b, c, bt, ct, pre_bc, gm, cum, cumr, sc, dt = prep(ubc, taps_bc, heads_p, masks, segc, segr, N, H)
    gg, ssq, pre, st = fwd(ubc, gate, taps_u, masks, b, c, bt, gm, cum, cumr, sc)
    r = lax.rsqrt(jnp.sum(ssq, axis=1, keepdims=True) / E + EPS)
    gos = (grad_out.astype(f32) * r).astype(bf16)
    g_out = dot(gg, gos, ((0,), (0,))).astype(bf16)
    dm = dot(grad_out, full_out, ((1,), (1,))).astype(bf16)
    s = jnp.sum(gg.astype(f32) * dm.astype(f32), axis=1, keepdims=True)
    rq = jnp.concatenate([r, r * r * r * s / E], axis=1)
    masks8 = jnp.pad(masks, ((0, 8), (0, 0)))
    shape = lambda g: g.reshape(n, D // n, -1)
    grad = lambda dz: shape(dot(normed, dz, ((0,), (0,))).astype(bf16))
    back = functools.partial(bwd, u=ubc, gate=gate, pre=pre, dm=dm, rq=rq, taps=taps_u, masks=masks8, b=b, c=c, ct=ct, gm=gm, cum=cum,
                             cumr=cumr, sc=sc, st=st)
    dz0, dg0, db0, dc0, rs0, small0, kk0, s_out = back(0, 2, comm=(nd, nf, 4, (g_out.reshape(n, E // n, D),), (((0, 0, D // 2),), ((0, D // 2, D // 2),))))
    dz1, dg1, db1, dc1, rs1, small1, kk1, sum0 = back(1, 2, comm=(nd, nf, 3, (grad(dz0[0]), grad(dz0[1])), (((0, 0, E // 2),), ((1, 0, E // 2),))))
    small = jnp.concatenate([small0, small1], axis=1)
    kk = jnp.concatenate([kk0, kk1], axis=1)
    kkh = jnp.sum(kk.reshape(kk.shape[0], H, E // H), axis=2)
    dbcdt, small_bc, hs = post(ubc, pre_bc, taps_bc, heads_p, masks8, segc, segr, b, c, (dg0, db0, dc0, rs0), (dg1, db1, dc1, rs1), kkh, dt)
    d_conv = jnp.concatenate([jnp.stack([small[6], small[5], small[4], small[3], small[2]]),
                              jnp.stack([small_bc[4], small_bc[3], small_bc[2], small_bc[1], small_bc[0]])], axis=1)
    d_heads = jnp.concatenate([hs, jnp.sum(small[1].reshape(1, H, E // H), axis=2)], axis=0)
    mine = jnp.concatenate([d_conv.reshape(K1, n, ncol).transpose(1, 0, 2).reshape(n, -1), small[0].reshape(n, -1),
                            jnp.broadcast_to(d_heads.reshape(1, -1), (n, d_heads.size))], axis=1)
    tiles = -(-mine.shape[1] // 1024)
    mine = jnp.pad(mine, ((0, 0), (0, tiles * 1024 - mine.shape[1]))).reshape(n, tiles * 8, 128)
    split = (((0, 0, E // 2),), ((1, 0, E // 2), (2, 0, wide)))
    sum1, output, grad_in, tot, d_norm = tail(nd, nf, 1, (grad(dz1[0]), grad(dz1[1]), grad(dbcdt)), split, dz0, dz1, dbcdt, full_gate, full_a, gg,
                                              full_out, hidden, grad_out, r, norm_gain[None], mine)
    tot = tot.reshape(-1)
    me = lax.axis_index("dp") * nf + lax.axis_index("fsdp")
    t_norm = lax.dynamic_slice(d_norm.reshape(-1), (me * nrow,), (nrow,))
    cut = [0, K1 * ncol, ngate, d_heads.size]
    ends = [sum(cut[: k + 1]) for k in range(4)]
    t_conv, t_gate, t_heads = (tot[ends[k] : ends[k + 1]] for k in range(3))
    Eh = E // 2
    s_zx = jnp.concatenate([sum0[:, :Eh], sum1[:, :Eh], sum0[:, Eh:], sum1[:, Eh : 2 * Eh]], axis=1)
    return (output, grad_in, s_zx, sum1[:, 2 * Eh : 2 * Eh + 2 * N], sum1[:, 2 * Eh + 2 * N : 2 * Eh + 2 * N + H], s_out,
            t_conv.reshape(K1, ncol), t_norm, t_gate, t_heads.reshape(d_heads.shape))


def per_device(nd, nf, hidden, grad_out, segment_ids, w_zx, w_bc, w_dt, w_out, conv_params, norm_gain, gate_gain, head_params):
    n = nd * nf
    E, N2, H = w_out.shape[0] * n, w_bc.shape[1], w_dt.shape[1]
    rows = w_zx.shape[0]
    small = jnp.concatenate([conv_params.reshape(-1), norm_gain, gate_gain])
    S = -(-small.shape[0] // rows)
    assert S + H <= 128
    small = jnp.pad(small, (0, S * rows - small.shape[0])).reshape(rows, S)
    shard_a = jnp.concatenate([w_zx[:, E:], w_bc, w_dt, small, jnp.zeros((rows, 128 - H - S), bf16)], axis=1)
    return layer(nd, nf, hidden, grad_out, segment_ids, shard_a, w_zx[:, :E], w_out, head_params, (E, N2 // 2, H, conv_params.shape[0], S))


def solution(mesh):
    row, col, vec, rep = P(AXES, None), P(None, AXES), P(AXES), P()
    return jax.shard_map(
        functools.partial(per_device, mesh.shape["dp"], mesh.shape["fsdp"]),
        mesh=mesh,
        in_specs=(row, row, vec, row, row, row, row, col, vec, vec, rep),
        out_specs=(row, row, row, row, row, row, col, vec, vec, rep),
        check_vma=False,
    )
```

```python
import functools
import jax
import jax.numpy as jnp
from jax import lax
from jax.experimental import pallas as pl
from jax.experimental.pallas import tpu as pltpu
from jax.sharding import PartitionSpec as P

EPS = 1e-05
L = 128
HG = 8
LOG2E = 1.4426950408889634
MB = 512
BWD_SPOTS = ((5.0, 10.0, 2.0, 26.0, 3.2), (7.0, 16.5, 2.0, 39.0, 3.2))
TAIL_SPOTS = ((7.0, 13.0, 3.0, 30.0, 4.0), (9.0, 22.0, 3.0, 46.0, 3.0))
bf16, f32 = jnp.bfloat16, jnp.float32
HIGHEST = lax.Precision.HIGHEST


AXES = ("dp", "fsdp")
MESH = pl.DeviceIdType.MESH


class Place:
    def __init__(self, nd, nf):
        self.zn, self.nf = nd // 2, nf
        d, f = lax.axis_index("dp"), lax.axis_index("fsdp")
        self.z, self.y = d // 2, d % 2
        self.x, self.c = f // 2, f % 2

    def dev(self, z, y, x, c):
        return (z * 2 + y, x * 2 + c)

    def idx(self, z, y, x, c):
        return (z * 2 + y) * self.nf + x * 2 + c

    def barrier(self):
        z, y, x, c, zn = self.z, self.y, self.x, self.c, self.zn
        sem = pltpu.get_barrier_semaphore()
        for there in ((z, y, 1 - x, c), (z, 1 - y, x, c), (z, y, x, 1 - c)):
            pl.semaphore_signal(sem, inc=1, device_id=self.dev(*there), device_id_type=MESH)

        @pl.when(z > 0)
        def _():
            pl.semaphore_signal(sem, inc=1, device_id=self.dev(z - 1, y, x, c), device_id_type=MESH)

        @pl.when(z < zn - 1)
        def _():
            pl.semaphore_signal(sem, inc=1, device_id=self.dev(z + 1, y, x, c), device_id_type=MESH)

        pl.semaphore_wait(sem, 3 + (z + zn - 1) // zn + (2 * zn - 2 - z) // zn)


def gather_kernel(nd, nf, src_ref, out_ref, own_sem, z_send, z_recv, x_send, x_recv, y_send, y_recv, dx_send, dx_recv, dy_send, dy_recv, c_send, c_recv):
    at = Place(nd, nf)
    z, y, x, c, zn = at.z, at.y, at.x, at.c, at.zn
    half = out_ref.shape[2] // 256 * 128
    lo, hi = pl.ds(0, half), pl.ds(half, out_ref.shape[2] - half)
    at.barrier()

    def copy(block, to, send, recv, cols=None, src=None):
        ref = out_ref.at[block] if cols is None else out_ref.at[block, :, cols]
        return pltpu.make_async_remote_copy(src_ref=ref if src is None else src, dst_ref=ref, send_sem=send, recv_sem=recv,
                                            device_id=at.dev(*to), device_id_type=MESH)

    def block(zs, col):
        return at.idx(zs, 1 - y if col & 2 else y, 1 - x if col & 1 else x, c)

    def up(zs, src=None):
        return copy(block(zs, 0), (z + 1, y, x, c), z_send.at[0, zs], z_recv.at[zs], src=src)

    def down(zs, src=None):
        return copy(block(zs, 0), (z - 1, y, x, c), z_send.at[1, zs], z_recv.at[zs], src=src)

    def to_x(zs, src=None):
        return copy(block(zs, 0), (z, y, 1 - x, c), x_send.at[zs], x_recv.at[zs], src=src)

    def to_y(zs, src=None):
        return copy(block(zs, 0), (z, 1 - y, x, c), y_send.at[zs], y_recv.at[zs], src=src)

    def diag_y(zs):
        return copy(block(zs, 1), (z, 1 - y, x, c), dy_send.at[zs], dy_recv.at[zs], lo)

    def diag_x(zs):
        return copy(block(zs, 2), (z, y, 1 - x, c), dx_send.at[zs], dx_recv.at[zs], hi)

    def to_core(zs, col, src=None):
        return copy(block(zs, col), (z, y, x, 1 - c), c_send.at[zs, col], c_recv.at[zs, col], src=src)

    own = pltpu.make_async_copy(src_ref, out_ref.at[block(z, 0)], own_sem)
    own.start()

    @pl.when(z < zn - 1)
    def _():
        up(z, src_ref).start()

    @pl.when(z > 0)
    def _():
        down(z, src_ref).start()

    to_x(z, src_ref).start()
    to_y(z, src_ref).start()
    to_core(z, 0, src_ref).start()

    def each(dist, fn):
        if dist == 0:
            fn(z, 0)
            return

        @pl.when(z - dist >= 0)
        def _():
            fn(z - dist, 1)

        @pl.when(z + dist < zn)
        def _():
            fn(z + dist, -1)

    def from_z(zs, way):
        copy(block(zs, 0), (z, y, x, c), z_send.at[0, zs], z_recv.at[zs]).wait_recv()
        if way > 0:
            @pl.when(z < zn - 1)
            def _():
                up(zs).start()
        else:
            @pl.when(z > 0)
            def _():
                down(zs).start()
        to_x(zs).start()
        to_y(zs).start()
        to_core(zs, 0).start()

    def from_xy(zs, way):
        to_x(zs).wait_recv()
        diag_y(zs).start()
        to_core(zs, 1).start()
        to_y(zs).wait_recv()
        diag_x(zs).start()
        to_core(zs, 2).start()

    def from_diag(zs, way):
        diag_y(zs).wait_recv()
        diag_x(zs).wait_recv()
        to_core(zs, 3).start()

    for dist in range(zn):
        if dist:
            each(dist, from_z)
        each(dist, from_xy)
    for dist in range(zn):
        each(dist, from_diag)
    own.wait()

    def sent(zs, way):
        for col in range(4):
            to_core(zs, col).wait_recv()
            to_core(zs, col).wait_send()
        to_x(zs).wait_send()
        to_y(zs).wait_send()
        diag_x(zs).wait_send()
        diag_y(zs).wait_send()
        if way >= 0:
            @pl.when(z < zn - 1)
            def _():
                up(zs).wait_send()
        if way <= 0:
            @pl.when(z > 0)
            def _():
                down(zs).wait_send()

    for dist in range(zn):
        each(dist, sent)


def gather_rows(shard, nd, nf, cid):
    zn = nd // 2
    D = pltpu.SemaphoreType.DMA
    return pl.pallas_call(
        functools.partial(gather_kernel, nd, nf),
        out_shape=jax.ShapeDtypeStruct((nd * nf,) + shard.shape, shard.dtype),
        in_specs=[pl.BlockSpec(memory_space=pl.ANY)],
        out_specs=pl.BlockSpec(memory_space=pl.ANY),
        scratch_shapes=[D(()), D((2, zn)), D((zn,)), D((zn,)), D((zn,)), D((zn,)), D((zn,)), D((zn,)), D((zn,)), D((zn,)), D((zn,)),
                        D((zn, 4)), D((zn, 4))],
        compiler_params=pltpu.CompilerParams(collective_id=cid, has_side_effects=True),
    )(shard)


class Scatter:
    def __init__(self, nd, nf, g_refs, out_ref, acc, c_in, d_in, xy_in, z_in,
                 load_sem, c_send, c_recv, dx_send, dx_recv, dy_send, dy_recv, x_send, x_recv, y_send, y_recv, z_send, z_recv):
        at = Place(nd, nf)
        z, y, x, c, zn = at.z, at.y, at.x, at.c, at.zn
        cols = out_ref.shape[1]
        wids = [r.shape[3] for r in g_refs]
        offs = [sum(wids[:k]) for k in range(len(wids))]
        half = cols // 256 * 128
        lo, hi = pl.ds(0, half), pl.ds(half, cols - half)

        def inner(col, core):
            return at.idx(0, 1 - y if col & 2 else y, 1 - x if col & 1 else x, core)

        def remote(src, dst, to, send, recv):
            return pltpu.make_async_remote_copy(src_ref=src, dst_ref=dst, send_sem=send, recv_sem=recv, device_id=at.dev(*to), device_id_type=MESH)

        def load(col):
            return [pltpu.make_async_copy(r.at[:, inner(col, c)], acc.at[col, :, :, pl.ds(o, w)], load_sem.at[col, k])
                    for k, (r, o, w) in enumerate(zip(g_refs, offs, wids))]

        def core(col):
            return [remote(r.at[:, inner(col, 1 - c)], c_in.at[col, :, :, pl.ds(o, w)], (z, y, x, 1 - c), c_send.at[col, k], c_recv.at[col, k])
                    for k, (r, o, w) in enumerate(zip(g_refs, offs, wids))]

        def diag_x(zs):
            return remote(acc.at[3, zs, :, lo], d_in.at[zs, :, lo], (z, y, 1 - x, c), dx_send.at[zs], dx_recv.at[zs])

        def diag_y(zs):
            return remote(acc.at[3, zs, :, hi], d_in.at[zs, :, hi], (z, 1 - y, x, c), dy_send.at[zs], dy_recv.at[zs])

        def to_x(zs):
            return remote(acc.at[1, zs], xy_in.at[0, zs], (z, y, 1 - x, c), x_send.at[zs], x_recv.at[zs])

        def to_y(zs):
            return remote(acc.at[2, zs], xy_in.at[1, zs], (z, 1 - y, x, c), y_send.at[zs], y_recv.at[zs])

        def up(zs):
            return remote(acc.at[0, zs], z_in.at[zs + 1], (z + 1, y, x, c), z_send.at[zs], z_recv.at[0, zs])

        def down(zs):
            return remote(acc.at[0, zs], z_in.at[zs], (z - 1, y, x, c), z_send.at[zs], z_recv.at[1, zs])

        def each(dist, fn):
            if dist == 0:
                fn(z)
                return

            @pl.when(z - dist >= 0)
            def _():
                fn(z - dist)

            @pl.when(z + dist < zn)
            def _():
                fn(z + dist)

        order = list(range(zn - 1, -1, -1))

        def start(col):
            for cp in core(col) + load(col):
                cp.start()

        def ready(col):
            for cp in load(col):
                cp.wait()
            for cp in core(col):
                cp.wait_recv()

        def diag(zs):
            acc[3, zs] = acc[3, zs] + c_in[3, zs]
            diag_x(zs).start()
            diag_y(zs).start()

        def sides(zs):
            diag_y(zs).wait_recv()
            acc[1, zs, :, lo] = acc[1, zs, :, lo] + c_in[1, zs, :, lo]
            acc[1, zs, :, hi] = acc[1, zs, :, hi] + c_in[1, zs, :, hi] + d_in[zs, :, hi]
            to_x(zs).start()
            diag_x(zs).wait_recv()
            acc[2, zs, :, lo] = acc[2, zs, :, lo] + c_in[2, zs, :, lo] + d_in[zs, :, lo]
            acc[2, zs, :, hi] = acc[2, zs, :, hi] + c_in[2, zs, :, hi]
            to_y(zs).start()

        def column(zs):
            to_x(zs).wait_recv()
            to_y(zs).wait_recv()
            return (acc[0, zs] + c_in[0, zs]).astype(f32) + (xy_in[0, zs] + xy_in[1, zs]).astype(f32)

        def pass_on(zs):
            total = column(zs)

            @pl.when(zs > z)
            def _():
                @pl.when(z > 0)
                def _():
                    up(zs).wait_recv()
                    acc[0, zs] = (total + z_in[zs + 1].astype(f32)).astype(bf16)

                @pl.when(z == 0)
                def _():
                    acc[0, zs] = total.astype(bf16)
                up(zs).start()

            @pl.when(zs < z)
            def _():
                @pl.when(z < zn - 1)
                def _():
                    down(zs).wait_recv()
                    acc[0, zs] = (total + z_in[zs].astype(f32)).astype(bf16)

                @pl.when(z == zn - 1)
                def _():
                    acc[0, zs] = total.astype(bf16)
                down(zs).start()

        def finish():
            out_ref[...] = column(z)

            @pl.when(z > 0)
            def _():
                up(z).wait_recv()
                out_ref[...] += z_in[z + 1].astype(f32)

            @pl.when(z < zn - 1)
            def _():
                down(z).wait_recv()
                out_ref[...] += z_in[z].astype(f32)

            def sent(zs):
                diag_x(zs).wait_send()
                diag_y(zs).wait_send()
                to_x(zs).wait_send()
                to_y(zs).wait_send()

            for col in range(4):
                for cp in core(col):
                    cp.wait_send()
            for dist in order:
                each(dist, sent)
                if dist:
                    each(dist, lambda zs: up(zs).wait_send())

        self.start, self.finish, self.barrier = start, finish, at.barrier
        self.diag = [functools.partial(ready, 3)] + [functools.partial(each, dist, diag) for dist in order]
        self.sides = [functools.partial(each, dist, sides) for dist in order]
        self.pass_on = [functools.partial(each, dist, pass_on) for dist in order[:-1]]
        self.ready = lambda: (ready(1), ready(2), ready(0))

    @staticmethod
    def scratch(nd, rows, cols, parts):
        zn = nd // 2
        D, V = pltpu.SemaphoreType.DMA, pltpu.VMEM
        return [V((4, zn, rows, cols), bf16), V((4, zn, rows, cols), bf16), V((zn, rows, cols), bf16), V((2, zn, rows, cols), bf16),
                V((zn + 1, rows, cols), bf16), D((4, parts)), D((4, parts)), D((4, parts))] + [D((zn,))] * 9 + [D((2, zn))]


def plan(pipes, barrier, time_of, spots):
    ticks = {0: [barrier] + [functools.partial(p.start, col) for col in (3, 1, 2, 0) for p in pipes]}

    def put(when, fn):
        tick = next((t for t, us in enumerate(time_of) if us >= when), len(time_of))
        ticks.setdefault(tick, []).append(fn)

    todo = []
    for p, (diag, sides, side_gap, pass_on, pass_gap) in zip(pipes, spots):
        todo += [(diag, fn) for fn in p.diag] + [(sides, p.ready)]
        todo += [(sides + k * side_gap * 4 / len(p.sides), fn) for k, fn in enumerate(p.sides)]
        todo += [(pass_on + k * pass_gap * 4 / len(p.sides), fn) for k, fn in enumerate(p.pass_on)]
    for when, fn in sorted(todo, key=lambda e: e[0]):
        put(when, fn)
    return ticks


def pipes_of(nd, nf, g_refs, out_refs, split, scratch):
    def view(a, lead, o, w):
        return g_refs[a].at[:, :, :, pl.ds(o, w)] if lead is None else g_refs[a].at[lead, :, :, :, pl.ds(o, w)]
    per = len(scratch) // len(split)
    return [Scatter(nd, nf, [view(*v) for v in pipe], out_ref, *scratch[per * m : per * (m + 1)])
            for m, (pipe, out_ref) in enumerate(zip(split, out_refs))]


def widths(split):
    return [sum(v[3] for v in pipe) for pipe in split]


def pipes_scratch(nd, rows, split):
    return [x for pipe, w in zip(split, widths(split)) for x in Scatter.scratch(nd, rows, w, len(pipe))]


def run_ticks(ticks, now, last):
    planned = sorted((t, fns) for t, fns in ticks.items() if t <= last)

    def search(items):
        if len(items) == 1:
            tick, fns = items[0]

            @pl.when(now == tick)
            def _():
                for fn in fns:
                    fn()
            return
        mid = len(items) // 2
        lax.cond(now < items[mid][0], lambda: search(items[:mid]), lambda: search(items[mid:]))

    if planned:
        search(planned)


def run_rest(ticks, last):
    for tick, fns in sorted(ticks.items()):
        if tick > last:
            for fn in fns:
                fn()


class Spread:
    def __init__(self, nd, nf, src, got, send, recv):
        self.n, self.nf = nd * nf, nf
        self.me = lax.axis_index("dp") * nf + lax.axis_index("fsdp")
        self.src, self.got, self.send, self.recv = src, got, send, recv

    def peer(self, k):
        return lax.rem(self.me + k, self.n)

    def loop(self, fn):
        def body(k, carry):
            fn(k)
            return carry
        lax.fori_loop(1, self.n, body, 0)

    def barrier(self):
        sem = pltpu.get_barrier_semaphore()

        def greet(k):
            pl.semaphore_signal(sem, inc=1, device_id=(self.peer(k) // self.nf, self.peer(k) % self.nf), device_id_type=MESH)
        self.loop(greet)
        pl.semaphore_wait(sem, self.n - 1)

    def copy(self, k):
        p = self.peer(k)
        src = self.src.at[p] if len(self.src.shape) == 3 else self.src
        return pltpu.make_async_remote_copy(src_ref=src, dst_ref=self.got.at[k], send_sem=self.send.at[k], recv_sem=self.recv.at[k],
                                            device_id=(p // self.nf, p % self.nf), device_id_type=MESH)

    def begin(self):
        self.loop(lambda k: self.copy(k).start())

    def total(self):
        own = self.src[self.me] if len(self.src.shape) == 3 else self.src[...]

        def add(k, total):
            self.copy(k).wait_recv()
            return total + self.got[k]
        total = lax.fori_loop(1, self.n, add, own)
        self.loop(lambda k: self.copy(k).wait_send())
        return total

    @staticmethod
    def scratch(n, tile):
        D = pltpu.SemaphoreType.DMA
        return [pltpu.VMEM((n,) + tile, f32), D((n,)), D((n,))]


def dot(a, b, dims=((1,), (0,)), precision=None):
    return lax.dot_general(a, b, (dims, ((), ())), preferred_element_type=f32, precision=precision)


def sigmoid(x):
    return 0.5 * jnp.tanh(0.5 * x) + 0.5


def conv_rows(ext, taps, masks, halo):
    rows = ext.shape[0] - halo
    width = 4
    v = ext[halo:]
    out = taps[4:5] + taps[3:4] * v
    for k in range(1, width):
        moved = pltpu.roll(ext, k, 0)[halo:]
        out = out + (taps[3 - k : 4 - k] * masks[:, k : k + 1]) * moved
    return out


def prep_kernel(bcdt_ref, taps_ref, heads_ref, segc_ref, segr_ref,
                m_ref, b_ref, c_ref, bt_ref, ct_ref, pre_ref, gm_ref, cum_ref, cumr_ref, sc_ref, dt_ref):
    T = bcdt_ref.shape[0]
    nc = T // L
    N = b_ref.shape[1]
    H = dt_ref.shape[1]
    groups = cumr_ref.shape[0]
    taps = taps_ref[...]
    tri = (lax.broadcasted_iota(jnp.int32, (L, L), 0) >= lax.broadcasted_iota(jnp.int32, (L, L), 1))
    trif = tri.astype(f32)
    neg_rate = -jnp.exp(heads_ref[0:1, :H]) * LOG2E
    m_ref[T : T + 8, :] = jnp.zeros((8, 4), f32)
    bias = heads_ref[1:2, :H]

    def chunk(c, carry):
        t0 = pl.multiple_of(c * L, L)
        here = pl.ds(t0, L)
        h0 = pl.multiple_of(jnp.maximum(t0 - 16, 0), 16)
        before = bcdt_ref[pl.ds(h0, 16), : 2 * N].astype(f32)
        v = bcdt_ref[here, : 2 * N].astype(f32)
        segc = segc_ref[here, :].astype(f32)
        seg_ext = jnp.concatenate([segc_ref[pl.ds(h0, 16), :].astype(f32), segc], axis=0)
        at = t0 + lax.broadcasted_iota(jnp.int32, (L, 1), 0)
        masks = [jnp.ones((L, 1), f32)]
        for k in range(1, 4):
            masks.append(((pltpu.roll(seg_ext, k, 0)[16:] == segc) & (at >= k)).astype(f32))
        masks = jnp.concatenate(masks, axis=1)
        m_ref[here, :] = masks
        pre = conv_rows(jnp.concatenate([before, v], axis=0), taps, masks, 16)
        pre_ref[here, :] = pre
        act = pre * sigmoid(pre)
        b = act[:, :N]
        cc = act[:, N:]
        bb = b.astype(bf16)
        cb = cc.astype(bf16)
        b_ref[here, :] = bb
        c_ref[here, :] = cb
        bt_ref[:, here] = b.T.astype(bf16)
        ct_ref[:, here] = cc.T.astype(bf16)
        prev = jnp.where(c > 0, seg_ext[15:16], -1.0)
        last = segc[L - 1 : L]
        same = segc == segr_ref[:, here].astype(f32)
        g = dot(cb, bb, ((1,), (1,)))
        gm_ref[pl.ds(c, 1)] = jnp.where(tri & same, g, 0.0)[None]
        raw = bcdt_ref[here, 2 * N : 2 * N + 128].astype(f32)[:, :H] + bias
        dt = jnp.maximum(raw, 0.0) + jnp.log1p(jnp.exp(-jnp.abs(raw)))
        a2 = neg_rate * dt
        cum = dot(trif, a2, precision=HIGHEST)
        end = cum[L - 1 : L]
        ein = jnp.where(segc == prev, jnp.exp2(cum), 0.0)
        lv = jnp.where(segc == last, jnp.exp2(end - cum), 0.0)
        dt_ref[here, :] = dt
        wide = jnp.concatenate([cum, jnp.zeros((L, 128 - H), f32)], axis=1)
        cum_ref[here, :] = wide
        cumt = wide.T
        for k in range(groups):
            cumr_ref[k, :, here] = cumt[HG * k : HG * (k + 1)]
        s0 = pl.multiple_of(c * (3 * L), L)
        for k, part in enumerate((dt, ein, lv)):
            sc_ref[pl.ds(s0 + k * L, L), :] = jnp.concatenate([part, jnp.zeros((L, 128 - H), f32)], axis=1).astype(bf16)
        return carry

    lax.fori_loop(0, nc, chunk, 0)


def prep(bcdt, taps, heads, segc, segr, N, H):
    T = bcdt.shape[0]
    nc = T // L
    G = H // HG
    S = jax.ShapeDtypeStruct
    full = lambda a: pl.BlockSpec(a.shape, lambda i: (0,) * a.ndim)
    outs = (S((T + 8, 4), f32), S((T, N), bf16), S((T, N), bf16), S((N, T), bf16), S((N, T), bf16), S((T, 2 * N), f32),
            S((nc, L, L), f32), S((T, 128), f32), S((G, HG, T), f32), S((3 * T, 128), bf16), S((T, H), f32))
    wide = 2 * N + 128
    return pl.pallas_call(
        prep_kernel,
        grid=(1,),
        in_specs=[pl.BlockSpec((T, wide), lambda i: (0, bcdt.shape[1] // wide - 1))] + [full(a) for a in (taps, heads, segc, segr)],
        out_specs=[full(o) for o in outs],
        out_shape=outs,
        compiler_params=pltpu.CompilerParams(vmem_limit_bytes=60 << 20),
    )(bcdt, taps, heads, segc, segr)


def lane_onehot(group, width, per):
    shape = (128, width)
    return (group * HG + lax.broadcasted_iota(jnp.int32, shape, 1) // per == lax.broadcasted_iota(jnp.int32, shape, 0)).astype(bf16)


def half_masks(P):
    lane = lax.broadcasted_iota(jnp.int32, (1, 2 * P), 1)
    first = (lane < P).astype(f32)
    return first.astype(bf16), (1.0 - first).astype(bf16)


def decay(cum4, cumr, k):
    return jnp.exp2(jnp.minimum(cum4[:, k : k + 1] - cumr[k : k + 1, :], 0.0))


def fwd_kernel(u_ref, gate_ref, taps_ref, m_ref, b_ref, c_ref, bt_ref, gm_ref, cum_ref, cumr_ref, sc_ref,
               gg_ref, ssq_ref, pre_ref, st_ref, state):
    T, W = u_ref.shape
    P = W // HG
    nc = T // L
    step = pl.program_id(0)
    taps = taps_ref[...]
    gain = taps[5:6]
    skip = taps[6:7]
    onehot = lane_onehot(step, W, P)
    ma, mb = half_masks(P)
    state[...] = jnp.zeros_like(state)

    @pl.when(step == 0)
    def _():
        ssq_ref[...] = jnp.zeros_like(ssq_ref)

    def chunk(c, carry):
        t0 = pl.multiple_of(c * L, L)
        here = pl.ds(t0, L)
        h0 = pl.multiple_of(jnp.maximum(t0 - 16, 0), 16)
        ext = jnp.concatenate([u_ref[pl.ds(h0, 16), :], u_ref[here, :]], axis=0).astype(f32)
        pre = conv_rows(ext, taps, m_ref[here, :], 16)
        pre_ref[here, :] = pre.astype(bf16)
        x = pre * sigmoid(pre)
        s0 = pl.multiple_of(c * (3 * L), L)
        exp = dot(sc_ref[pl.ds(s0, 3 * L), :], onehot)
        dtx, einx, lvx = exp[:L], exp[L : 2 * L], exp[2 * L :]
        xd = x * dtx
        xdb = xd.astype(bf16)
        gm = gm_ref[c]
        cum4 = pltpu.roll(cum_ref[here, :], 128 - step * HG, 1)
        cumr = cumr_ref[0, :, here]
        sb = state[...].astype(bf16)
        st_ref[c] = sb
        inner = []
        for p in range(HG // 2):
            m0 = (decay(cum4, cumr, 2 * p) * gm).astype(bf16)
            m1 = (decay(cum4, cumr, 2 * p + 1) * gm).astype(bf16)
            xp = xdb[:, 2 * P * p : 2 * P * (p + 1)]
            inner.append(dot(jnp.concatenate([m0, m1], axis=1), jnp.concatenate([xp * ma, xp * mb], axis=0)))
        y = jnp.concatenate(inner, axis=1) + dot(c_ref[here, :], sb) * einx + skip * x
        state[...] = state[...] * einx[L - 1 : L] + dot(bt_ref[:, here], (xd * lvx).astype(bf16))
        gate = gate_ref[here, :].astype(f32)
        g = y * (gate * sigmoid(gate))
        gg_ref[here, :] = (g * gain).astype(bf16)
        g2 = g * g
        tot = g2[:, :128]
        for j in range(1, W // 128):
            tot = tot + g2[:, 128 * j : 128 * (j + 1)]
        ssq_ref[here, :] += tot
        return carry

    lax.fori_loop(0, nc, chunk, 0)


def fwd(u, gate, taps, masks, b, c, bt, gm, cum, cumr, sc):
    T, E = gate.shape
    N = b.shape[1]
    G = cumr.shape[0]
    W = E // G
    nc = T // L
    S = jax.ShapeDtypeStruct
    col = lambda off: pl.BlockSpec((T, W), lambda g: (0, g + off))
    full = lambda a: pl.BlockSpec(a.shape, lambda g: (0,) * a.ndim)
    grp = lambda a: pl.BlockSpec((1,) + a.shape[1:], lambda g: (g, 0, 0))
    return pl.pallas_call(
        fwd_kernel,
        grid=(G,),
        in_specs=[col(0), col(0), pl.BlockSpec((8, W), lambda g: (0, g)), full(masks), full(b), full(c), full(bt), full(gm),
                  full(cum), grp(cumr), full(sc)],
        out_specs=[col(0), pl.BlockSpec((T, 128), lambda g: (0, 0)), col(0), pl.BlockSpec((nc, N, W), lambda g: (0, 0, g))],
        out_shape=(S((T, E), bf16), S((T, 128), f32), S((T, E), bf16), S((nc, N, E), bf16)),
        scratch_shapes=[pltpu.VMEM((N, W), f32)],
        compiler_params=pltpu.CompilerParams(vmem_limit_bytes=60 << 20),
        cost_estimate=pl.CostEstimate(flops=T * E * (2 * L + 4 * N) * 2, bytes_accessed=T * E * 12, transcendentals=T * E * 4),
    )(u, gate, taps, masks, b, c, bt, gm, cum, cumr, sc)


def bwd_scatter_kernel(nd, nf, g0, Gh, nc, arrays, split, *refs):
    g_refs, ins, outs = refs[:arrays], refs[arrays : arrays + 16], refs[arrays + 16 : arrays + 24]
    refs = refs[arrays + 24 :]
    sums, own, comm = refs[: len(split)], refs[len(split) : len(split) + 3], refs[len(split) + 3 :]
    pipes = pipes_of(nd, nf, g_refs, sums, split, comm)
    nb = ins[15].shape[0] // MB
    time_of = [21.0 * g + (1.9 * i if i < nc else 1.9 * nc + 1.9 * (i - nc)) for g in range(Gh) for i in range(nc + nb)]
    ticks = plan(pipes, pipes[0].barrier, time_of, BWD_SPOTS)
    last = len(time_of) - 1
    bwd_body(lambda i: run_ticks(ticks, pl.program_id(0) * (nc + nb) + i, last), g0, *ins, *outs, *own)

    @pl.when(pl.program_id(0) == pl.num_programs(0) - 1)
    def _():
        run_rest(ticks, last)
        for p in pipes:
            p.finish()


def bwd_body(tick, g0, u_ref, gate_ref, pre_ref, dm_ref, rq_ref, taps_ref, m_ref, b_ref, c_ref, ct_ref, gm_ref, cum_ref, cumr_ref, sc_ref, st_ref, normt_ref,
             dz_ref, gw_ref, dg_ref, db_ref, dc_ref, rs_ref, small_ref, kk_ref, ds, nxt, acc):
    T, W = u_ref.shape
    P = W // HG
    nc = T // L
    step = pl.program_id(0)
    taps = taps_ref[...]
    gain = taps[5:6]
    skip = taps[6:7]
    onehot = lane_onehot(step + g0, W, P)
    ma, mb = half_masks(P)
    ds[...] = jnp.zeros_like(ds)
    nxt[...] = jnp.zeros_like(nxt)
    acc[...] = jnp.zeros_like(acc)

    @pl.when(step == 0)
    def _():
        dg_ref[...] = jnp.zeros_like(dg_ref)
        db_ref[...] = jnp.zeros_like(db_ref)
        dc_ref[...] = jnp.zeros_like(dc_ref)
        rs_ref[...] = jnp.zeros_like(rs_ref)

    ri = lax.broadcasted_iota(jnp.int32, (4 * W, 128), 0)
    ci = lax.broadcasted_iota(jnp.int32, (4 * W, 128), 1)
    part = ri // W
    want = (jnp.maximum(part - 1, 0) * pl.num_programs(0) + step) * HG + (ri % W) // P
    fold = (want == ci).astype(bf16)

    def eight(z):
        return jnp.sum(z.reshape(L // 8, 8, W), axis=0)

    def chunk(i, carry):
        tick(i)
        c = nc - 1 - i
        t0 = pl.multiple_of(c * L, L)
        here = pl.ds(t0, L)
        u = u_ref[here, :].astype(f32)
        pre = pre_ref[here, :].astype(f32)
        sig = sigmoid(pre)
        x = pre * sig
        dsilu = sig + x * (1.0 - sig)
        s0 = pl.multiple_of(c * (3 * L), L)
        exp = dot(sc_ref[pl.ds(s0, 3 * L), :], onehot)
        dtx, einx, lvx = exp[:L], exp[L : 2 * L], exp[2 * L :]
        xdb = (x * dtx).astype(bf16)
        xd = xdb.astype(f32)
        gm = gm_ref[c]
        cum4 = pltpu.roll(cum_ref[here, :], 128 - (step + g0) * HG, 1)
        cumr = cumr_ref[0, :, here]
        sb = st_ref[c]
        es, ms, inner = [], [], []
        for p in range(HG // 2):
            e0 = decay(cum4, cumr, 2 * p)
            e1 = decay(cum4, cumr, 2 * p + 1)
            m0 = (e0 * gm).astype(bf16)
            m1 = (e1 * gm).astype(bf16)
            xp = xdb[:, 2 * P * p : 2 * P * (p + 1)]
            inner.append(dot(jnp.concatenate([m0, m1], axis=1), jnp.concatenate([xp * ma, xp * mb], axis=0)))
            es.append((e0, e1))
            ms.append((m0, m1))
        yn = jnp.concatenate(inner, axis=1) + dot(c_ref[here, :], sb) * einx
        y = yn + skip * x
        gate = gate_ref[here, :].astype(f32)
        sgate = sigmoid(gate)
        silu_g = gate * sgate
        g = y * silu_g
        r = rq_ref[here, 0:1]
        q = rq_ref[here, 1:2]
        dmr = dm_ref[here, :].astype(f32) * r
        dgg = gain * dmr - g * q
        dyb = (dgg * silu_g).astype(bf16)
        dy = dyb.astype(f32)
        dz_ref[0, here, :] = (dgg * y * (sgate + silu_g * (1.0 - sgate))).astype(bf16)
        dxi = []
        dgc = dg_ref[c]
        for p in range(HG // 2):
            cols = slice(2 * P * p, 2 * P * (p + 1))
            dp = dyb[:, cols]
            dstack = jnp.concatenate([dp * ma, dp * mb], axis=0)
            dmm = dot(dstack, xdb[:, cols], ((1,), (1,)))
            dgc = dgc + dmm[:L] * es[p][0] + dmm[L:] * es[p][1]
            dxi.append(dot(jnp.concatenate(ms[p], axis=0), dstack, ((0,), (0,))))
        dg_ref[c] = dgc
        dxi = jnp.concatenate(dxi, axis=1)
        dsn = ds[...]
        dsb = dsn.astype(bf16)
        dye = (dy * einx).astype(bf16)
        dc_ref[here, :] += dot(dye, sb, ((1,), (1,)))
        kept = einx[L - 1 : L]
        kk_ref[pl.ds(c, 1), :] = kept * jnp.sum(sb.astype(f32) * dsn, axis=0, keepdims=True)
        db_ref[here, :] += dot((xd * lvx).astype(bf16), dsb, ((1,), (1,)))
        dxe = dot(b_ref[here, :], dsb) * lvx
        ds[...] = dsn * kept + dot(ct_ref[:, here], dye)
        dxd = dxi + dxe
        r1 = dy * yn - xd * dxi
        r1h = r1.astype(bf16)
        r1l = (r1 - r1h.astype(f32)).astype(bf16)
        rs_ref[here, :] += dot(jnp.concatenate([r1h, r1l, (xd * dxe).astype(bf16), (x * dxd).astype(bf16)], axis=1), fold)
        dpre = (dxd * dtx + skip * dy) * dsilu
        ext = jnp.concatenate([dpre, nxt[...]], axis=0)
        nxt[...] = dpre[:8]
        du = taps[3:4] * dpre
        acc[0:8, :] += eight(dmr * g)
        acc[8:16, :] += eight(dy * x)
        acc[16:24, :] += eight(dpre)
        acc[24:32, :] += eight(dpre * u)
        mrows = m_ref[pl.ds(t0, L + 8), :]
        for k in range(1, 4):
            sk = pltpu.roll(ext * mrows[:, k : k + 1], L + 8 - k, 0)[:L]
            du = du + taps[3 - k : 4 - k] * sk
            acc[24 + 8 * k : 32 + 8 * k, :] += eight(sk * u)
        dz_ref[1, here, :] = du.astype(bf16)
        return carry

    lax.fori_loop(0, nc, chunk, 0)
    for j in range(7):
        small_ref[j : j + 1, :] = jnp.sum(acc[8 * j : 8 * j + 8, :], axis=0, keepdims=True)
    small_ref[7:8, :] = jnp.zeros((1, W), f32)

    def weights(i, carry):
        tick(nc + i)
        rows = pl.ds(pl.multiple_of(i * MB, MB), MB)
        for kind in range(2):
            gw_ref[kind, rows, :] = dot(normt_ref[rows, :], dz_ref[kind]).astype(bf16)
        return carry

    lax.fori_loop(0, normt_ref.shape[0] // MB, weights, 0)


def bwd(half, halves, u, gate, pre, dm, rq, taps, masks, b, c, ct, gm, cum, cumr, sc, st, normt, comm):
    T, E = gate.shape
    N = b.shape[1]
    G = cumr.shape[0]
    W = E // G
    nc = T // L
    Gh = G // halves
    Eh = E // halves
    g0 = half * Gh
    S = jax.ShapeDtypeStruct
    col = pl.BlockSpec((T, W), lambda g: (0, g + g0))
    full = lambda a: pl.BlockSpec(a.shape, lambda g: (0,) * a.ndim)
    whole = lambda s: pl.BlockSpec(s, lambda g: (0,) * len(s))
    grp = lambda a: pl.BlockSpec((1,) + a.shape[1:], lambda g: (g + g0, 0, 0))
    in_specs = [col, col, col, col, full(rq), pl.BlockSpec((8, W), lambda g: (0, g + g0)), full(masks), full(b), full(c),
                full(ct), full(gm), full(cum), grp(cumr), full(sc), pl.BlockSpec((nc, N, W), lambda g: (0, 0, g + g0)), full(normt)]
    D = normt.shape[0]
    out_specs = [pl.BlockSpec((2, T, W), lambda g: (0, 0, g)), pl.BlockSpec((2, D, W), lambda g: (0, 0, g)), whole((nc, L, L)), whole((T, N)), whole((T, N)),
                 whole((T, 128)), pl.BlockSpec((8, W), lambda g: (0, g)), pl.BlockSpec((nc, W), lambda g: (0, g))]
    out_shape = [S((2, T, Eh), bf16), S((2, D, Eh), bf16), S((nc, L, L), f32), S((T, N), f32), S((T, N), f32), S((T, 128), f32), S((8, Eh), f32), S((nc, Eh), f32)]
    scratch = [pltpu.VMEM((N, W), f32), pltpu.VMEM((8, W), f32), pltpu.VMEM((56, W), f32)]
    nd, nf, cid, first, split = comm
    rows = first[0].shape[-2]
    return pl.pallas_call(
        functools.partial(bwd_scatter_kernel, nd, nf, g0, Gh, nc, len(first), split),
        grid=(Gh,),
        in_specs=[pl.BlockSpec(memory_space=pl.ANY)] * len(first) + in_specs,
        out_specs=out_specs + [whole((rows, w)) for w in widths(split)],
        out_shape=out_shape + [S((rows, w), f32) for w in widths(split)],
        scratch_shapes=scratch + pipes_scratch(nd, rows, split),
        compiler_params=pltpu.CompilerParams(vmem_limit_bytes=60 << 20, collective_id=cid, has_side_effects=True),
        cost_estimate=pl.CostEstimate(flops=T * Eh * (8 * L + 12 * N + 4 * D), bytes_accessed=T * Eh * 16, transcendentals=T * Eh * 4),
    )(*first, u, gate, pre, dm, rq, taps, masks, b, c, ct, gm, cum, cumr, sc, st, normt)


def post_kernel(bcdt_ref, pre_ref, taps_ref, heads_ref, m_ref, segc_ref, segr_ref, b_ref, c_ref, dg0_ref, db0_ref, dc0_ref, rs0_ref, dg1_ref, db1_ref, dc1_ref, rs1_ref, kk_ref, dt_ref,
                out_ref, small_ref, hs_ref, nxt, acc, hacc):
    T = bcdt_ref.shape[0]
    nc = T // L
    N = b_ref.shape[1]
    H = dt_ref.shape[1]
    taps = taps_ref[...]
    tri = (lax.broadcasted_iota(jnp.int32, (L, L), 0) >= lax.broadcasted_iota(jnp.int32, (L, L), 1))
    upper = (lax.broadcasted_iota(jnp.int32, (L, L), 0) <= lax.broadcasted_iota(jnp.int32, (L, L), 1)).astype(f32)
    strict = 1.0 - upper
    rate = -jnp.exp(heads_ref[0:1, :H])
    bias = heads_ref[1:2, :H]
    nxt[...] = jnp.zeros_like(nxt)
    acc[...] = jnp.zeros_like(acc)
    hacc[...] = jnp.zeros_like(hacc)

    def eight(z):
        return jnp.sum(z.reshape(L // 8, 8, z.shape[1]), axis=0)

    def chunk(i, carry):
        c = nc - 1 - i
        t0 = pl.multiple_of(c * L, L)
        here = pl.ds(t0, L)
        same = segc_ref[here, :] == segr_ref[:, here]
        dg = jnp.where(tri & same, dg0_ref[c] + dg1_ref[c], 0.0)
        dgb = dg.astype(bf16)
        dcv = dc0_ref[here, :] + dc1_ref[here, :] + dot(dgb, b_ref[here, :])
        dbv = db0_ref[here, :] + db1_ref[here, :] + dot(dg.T.astype(bf16), c_ref[here, :])
        pre = pre_ref[here, :]
        sig = sigmoid(pre)
        dpre = jnp.concatenate([dbv, dcv], axis=1) * (sig + pre * sig * (1.0 - sig))
        v = bcdt_ref[here, : 2 * N].astype(f32)
        ext = jnp.concatenate([dpre, nxt[...]], axis=0)
        nxt[...] = dpre[:8]
        dv = taps[3:4] * dpre
        acc[0:8, :] += eight(dpre)
        acc[8:16, :] += eight(dpre * v)
        mrows = m_ref[pl.ds(t0, L + 8), :]
        for k in range(1, 4):
            sk = pltpu.roll(ext * mrows[:, k : k + 1], L + 8 - k, 0)[:L]
            dv = dv + taps[3 - k : 4 - k] * sk
            acc[8 + 8 * k : 16 + 8 * k, :] += eight(sk * v)
        out_ref[here, : 2 * N] = dv.astype(bf16)
        q = H // 2
        r0, r1 = rs0_ref[here, :], rs1_ref[here, :]
        r1, r2, r3 = (jnp.concatenate([r0[:, m * q : (m + 1) * q], r1[:, m * q : (m + 1) * q]], axis=1) for m in range(3))
        da = dot(upper, r1, precision=HIGHEST) + dot(strict, r2, precision=HIGHEST) + kk_ref[pl.ds(c, 1), :]
        dt = dt_ref[here, :]
        raw = bcdt_ref[here, 2 * N : 2 * N + 128].astype(f32)[:, :H] + bias
        ddt = (r3 + da * rate) * sigmoid(raw)
        hacc[0:8, :] += eight(da * rate * dt)
        hacc[8:16, :] += eight(ddt)
        out_ref[here, 2 * N :] = jnp.concatenate([ddt, jnp.zeros((L, out_ref.shape[1] - 2 * N - H), f32)], axis=1).astype(bf16)
        return carry

    lax.fori_loop(0, nc, chunk, 0)
    for j in range(5):
        small_ref[j : j + 1, :] = jnp.sum(acc[8 * j : 8 * j + 8, :], axis=0, keepdims=True)
    small_ref[5:8, :] = jnp.zeros((3, 2 * N), f32)
    for j in range(2):
        hs_ref[j : j + 1, :] = jnp.sum(hacc[8 * j : 8 * j + 8, :], axis=0, keepdims=True)


def post(bcdt, pre, taps, heads, masks, segc, segr, b, c, first, second, kk, dt):
    T = bcdt.shape[0]
    N = b.shape[1]
    H = dt.shape[1]
    S = jax.ShapeDtypeStruct
    wide = 2 * N + 128
    full = lambda a: pl.BlockSpec(a.shape, lambda i: (0,) * a.ndim)
    ins = (bcdt, pre, taps, heads, masks, segc, segr, b, c, *first, *second, kk, dt)
    outs = (S((T, wide), bf16), S((8, 2 * N), f32), S((2, H), f32))
    return pl.pallas_call(
        post_kernel,
        grid=(1,),
        in_specs=[pl.BlockSpec((T, wide), lambda i: (0, bcdt.shape[1] // wide - 1))] + [full(a) for a in ins[1:]],
        out_specs=[full(o) for o in outs],
        out_shape=outs,
        scratch_shapes=[pltpu.VMEM((8, 2 * N), f32), pltpu.VMEM((40, 2 * N), f32), pltpu.VMEM((16, H), f32)],
        compiler_params=pltpu.CompilerParams(vmem_limit_bytes=60 << 20),
    )(*ins)


NT = 256


def tail_kernel(nd, nf, arrays, split, tiles, *refs):
    g_refs, refs = refs[:arrays], refs[arrays:]
    (wo_hbm, wg_hbm, wa_hbm, gg_ref, dz0_ref, dz1_ref, dbc_ref, hid_ref, go_ref, r_ref, gain_ref, mine_ref,
     suma_ref, sumb_ref, out_ref, gin_ref, small_ref, dnorm_ref) = refs[:18]
    refs = refs[1:]
    wo, wg, wa, acc, dn, flat, sem = refs[17:24]
    mine = Spread(nd, nf, mine_ref, *refs[24:27])
    norm = Spread(nd, nf, flat, *refs[27:30])
    pipes = pipes_of(nd, nf, g_refs, (suma_ref, sumb_ref), split, refs[30:])
    D, E = wg.shape
    Eh = E // 2
    step = pl.program_id(0)
    early = tiles // 2
    blocks = D // NT
    mid = (early + tiles) * blocks
    scale = 4 / tiles
    time_of = [4 + 0.75 * scale * t if t < early * blocks else
               (13 + 1.65 * scale * (t - early * blocks) if t < mid else 52.6 + 0.65 * scale * (t - mid)) for t in range(2 * tiles * blocks)]
    ticks = plan(pipes, mine.barrier, time_of, TAIL_SPOTS)
    last = len(time_of) - 1
    ticks[0].append(mine.begin)
    ticks.setdefault((early + tiles) * blocks + 2, []).append(norm.begin)
    fetch = [pltpu.make_async_copy(src, dst, sem.at[k]) for k, (src, dst) in enumerate(((wo_hbm, wo), (wg_hbm, wg), (wa_hbm, wa)))]

    @pl.when(step == 0)
    def _():
        for cp in fetch:
            cp.start()
        dn[...] = jnp.zeros_like(dn)
        run_ticks(ticks, 0, 0)
        fetch[0].wait()

    @pl.when(step == early)
    def _():
        fetch[1].wait()
        fetch[2].wait()

    back = (step >= early) & (step < early + tiles)
    in_back = lambda t: early * blocks <= t < (early + tiles) * blocks

    @pl.when(jnp.logical_not(back))
    def _():
        def block(j, carry):
            run_ticks({t: f for t, f in ticks.items() if t and not in_back(t)}, step * blocks + j, last)
            cols = pl.ds(pl.multiple_of(j * NT, NT), NT)
            out_ref[:, cols] = (hid_ref[:, cols].astype(f32) + r_ref[...] * dot(gg_ref[...], wo[:, cols])).astype(bf16)
            return carry
        lax.fori_loop(0, blocks, block, 0)

    @pl.when(back)
    def _():
        def block(j, carry):
            run_ticks({t: f for t, f in ticks.items() if in_back(t)}, step * blocks + j, last)
            cols = pl.ds(pl.multiple_of(j * NT, NT), NT)
            part = dot(dz0_ref[0], wg[cols, :Eh], ((1,), (1,))) + dot(dz1_ref[0], wg[cols, Eh:], ((1,), (1,)))
            part = part + dot(dz0_ref[1], wa[cols, :Eh], ((1,), (1,))) + dot(dz1_ref[1], wa[cols, Eh:E], ((1,), (1,)))
            acc[:, cols] = part + dot(dbc_ref[...], wa[cols, E:], ((1,), (1,)))
            return carry
        lax.fori_loop(0, blocks, block, 0)
        gain = gain_ref[...]

        def rows_of(i, carry):
            here = pl.ds(pl.multiple_of(i * 64, 64), 64)
            rows = hid_ref[here, :].astype(f32)
            rinv = lax.rsqrt(jnp.mean(rows * rows, axis=-1, keepdims=True) + EPS)
            xhat = rows * rinv
            bn = acc[here, :]
            prod = bn * xhat
            dn[...] += jnp.sum(prod.reshape(8, 8, D), axis=0)
            mean = jnp.mean(prod * gain, axis=-1, keepdims=True)
            gin_ref[here, :] = (go_ref[here, :].astype(f32) + rinv * (bn * gain - xhat * mean)).astype(bf16)
            return carry
        lax.fori_loop(0, hid_ref.shape[0] // 64, rows_of, 0)

    @pl.when(step == early + tiles - 1)
    def _():
        flat[...] = jnp.zeros_like(flat)
        for j in range(D // 128):
            flat[j : j + 1, :] = jnp.sum(dn[:, 128 * j : 128 * (j + 1)], axis=0, keepdims=True)

    @pl.when(step == 2 * tiles - 1)
    def _():
        run_rest(ticks, last)
        for p in pipes:
            p.finish()
        small_ref[...] = mine.total()
        dnorm_ref[...] = norm.total()


def tail(nd, nf, cid, gs, split, dz0, dz1, dbcdt, full_gate, full_a, gg, full_out, hidden, grad_out, r, norm_gain, mine):
    T, D = hidden.shape
    E = full_out.shape[0]
    n = nd * nf
    rows = gs[0].shape[-2]
    MT = 256 if rows % 16 == 0 else 128
    tiles = T // MT
    early = tiles // 2
    wide = dbcdt.shape[1]
    S = jax.ShapeDtypeStruct
    any_ = pl.BlockSpec(memory_space=pl.ANY)
    whole = lambda s: pl.BlockSpec(s, lambda k: (0,) * len(s), pipeline_mode=pl.Buffered(1))
    at_out = lambda k: jnp.minimum(k, early - 1) + jnp.clip(k - tiles - early + 1, 0, tiles - early)
    at_back = lambda k: jnp.clip(k - early, 0, tiles - 1)
    at_row = lambda k: k - early * jnp.clip(k - early + 1, 0, 1) - (tiles - early) * jnp.clip(k - early - tiles + 1, 0, 1)
    out_tile = lambda w: pl.BlockSpec((MT, w), lambda k: (at_out(k), 0))
    back_tile = lambda w: pl.BlockSpec((MT, w), lambda k: (at_back(k), 0))
    half = pl.BlockSpec((2, MT, E // 2), lambda k: (0, at_back(k), 0))
    tile, ntile = mine.shape[1:], (-(-D // 1024) * 8, 128)
    return pl.pallas_call(
        functools.partial(tail_kernel, nd, nf, len(gs), split, tiles),
        grid=(2 * tiles,),
        in_specs=[any_] * (len(gs) + 3) + [out_tile(E), half, half, back_tile(wide), pl.BlockSpec((MT, D), lambda k: (at_row(k), 0)), back_tile(D),
                                           out_tile(1), whole((1, D)), whole(mine.shape)],
        out_specs=[whole((rows, w)) for w in widths(split)] + [out_tile(D), back_tile(D), whole(tile), whole(ntile)],
        out_shape=[S((rows, w), f32) for w in widths(split)] + [S((T, D), bf16), S((T, D), bf16), S(tile, f32), S(ntile, f32)],
        scratch_shapes=[pltpu.VMEM((E, D), bf16), pltpu.VMEM((D, E), bf16), pltpu.VMEM((D, E + wide), bf16), pltpu.VMEM((MT, D), f32),
                        pltpu.VMEM((8, D), f32), pltpu.VMEM(ntile, f32), pltpu.SemaphoreType.DMA((3,))]
        + Spread.scratch(n, tile) + Spread.scratch(n, ntile) + pipes_scratch(nd, rows, split),
        compiler_params=pltpu.CompilerParams(collective_id=cid, has_side_effects=True, vmem_limit_bytes=67043328),
        cost_estimate=pl.CostEstimate(flops=2 * T * D * 3 * E, bytes_accessed=8 * D * E, transcendentals=0),
    )(*gs, full_out, full_gate, full_a, gg, dz0, dz1, dbcdt, hidden, grad_out, r, norm_gain, mine)


def finish_kernel(nd, nf, gate0_ref, gate1_ref, u0_ref, u1_ref, oa_ref, ob_ref, tot_ref, norm_ref,
                  zx_ref, bc_ref, dt_ref, out_ref, conv_ref, n_ref, gg_ref, heads_ref):
    Eh = gate0_ref.shape[1]
    for k, ref in enumerate((gate0_ref, gate1_ref, u0_ref)):
        zx_ref[:, k * Eh : (k + 1) * Eh] = ref[...]
    zx_ref[:, 3 * Eh :] = u1_ref[:, :Eh]
    wide = bc_ref.shape[1]
    bc_ref[...] = u1_ref[:, Eh : Eh + wide]
    dt_ref[...] = u1_ref[:, Eh + wide : Eh + wide + 128][:, : dt_ref.shape[1]]
    half = oa_ref.shape[1]
    out_ref[:, :half] = oa_ref[...]
    out_ref[:, half:] = ob_ref[...]
    k1 = conv_ref.shape[0]
    conv_ref[...] = tot_ref[:k1, : conv_ref.shape[1]]
    gg_ref[...] = tot_ref[k1 : k1 + 1, : gg_ref.shape[1]]
    heads_ref[...] = tot_ref[k1 + 1 : k1 + 1 + heads_ref.shape[0], : heads_ref.shape[1]]
    me = lax.axis_index("dp") * nf + lax.axis_index("fsdp")
    nrow = n_ref.shape[1]
    D = nrow * nd * nf
    row = jnp.concatenate([norm_ref[j : j + 1, :] for j in range(D // 128)], axis=1)
    row = pltpu.roll(jnp.broadcast_to(row, (8, D)), lax.rem(D - me * nrow, D), 1)
    n_ref[...] = row[:1, :nrow]


def finish(nd, nf, gate0, gate1, u0, u1, s_out, tot, d_norm, shapes):
    S = jax.ShapeDtypeStruct
    return pl.pallas_call(
        functools.partial(finish_kernel, nd, nf),
        out_shape=[S(s, f32) for s in shapes],
        compiler_params=pltpu.CompilerParams(vmem_limit_bytes=40 << 20),
    )(gate0, gate1, u0, u1, *s_out, tot, d_norm)


def layer(nd, nf, hidden, grad_out, seg, shard_a, shard_gate, shard_out, head_params, sizes):
    n = nd * nf
    E, N, H, K1, S = sizes
    T, D = hidden.shape
    wide = 2 * N + 128
    full_gate = lax.all_gather(shard_gate, AXES, axis=0, tiled=True)
    full_out = lax.all_gather(shard_out, AXES, axis=0, tiled=True)
    full_a = gather_rows(shard_a, nd, nf, 0)
    off = E + 2 * N + H
    flat = full_a[:, :, off : off + S].reshape(n, -1)
    ncol, nrow, ngate = (E + 2 * N) // n, D // n, E // n
    conv = flat[:, : K1 * ncol].reshape(n, K1, ncol).transpose(1, 0, 2).reshape(K1, n * ncol).astype(f32)
    norm_gain = flat[:, K1 * ncol : K1 * ncol + nrow].reshape(-1).astype(f32)
    gate_gain = flat[:, K1 * ncol + nrow : K1 * ncol + nrow + ngate].reshape(-1).astype(f32)
    full_a = full_a.reshape(D, E + wide)
    rows = hidden.astype(f32)
    rinv = lax.rsqrt(jnp.mean(rows * rows, axis=-1, keepdims=True) + EPS)
    xhat = rows * rinv
    normed = lax.optimization_barrier((xhat * norm_gain).astype(bf16))
    normt = normed.T
    ubc = dot(normed, full_a).astype(bf16)
    gate = dot(normed, full_gate).astype(bf16)
    segc, segr = seg[:, None], seg[None, :]
    taps_u = jnp.concatenate([conv[:, :E], gate_gain[None], jnp.repeat(head_params[2], E // H)[None], jnp.zeros((1, E), f32)], axis=0)
    taps_bc = jnp.concatenate([conv[:, E:], jnp.zeros((3, 2 * N), f32)], axis=0)
    masks, b, c, bt, ct, pre_bc, gm, cum, cumr, sc, dt = prep(ubc, taps_bc, head_params, segc, segr, N, H)
    gg, ssq, pre, st = fwd(ubc, gate, taps_u, masks, b, c, bt, gm, cum, cumr, sc)
    r = lax.rsqrt(jnp.sum(ssq, axis=1, keepdims=True) / E + EPS)
    gos = (grad_out.astype(f32) * r).astype(bf16)
    g_out = dot(gg, gos, ((0,), (0,))).astype(bf16)
    dm = dot(grad_out, full_out, ((1,), (1,))).astype(bf16)
    s = jnp.sum(gg.astype(f32) * dm.astype(f32), axis=1, keepdims=True)
    rq = jnp.concatenate([r, r * r * r * s / E], axis=1)
    back = functools.partial(bwd, u=ubc, gate=gate, pre=pre, dm=dm, rq=rq, taps=taps_u, masks=masks, b=b, c=c, ct=ct, gm=gm, cum=cum,
                             cumr=cumr, sc=sc, st=st, normt=normt)
    zn = max(nd // 2, 1)
    rows_of = lambda g: g.reshape(g.shape[:-2] + (zn, n // zn, g.shape[-2] // n, g.shape[-1]))
    Eh = E // 2
    dz0, gw0, dg0, db0, dc0, rs0, small0, kk0, *s_out = back(
        0, 2, comm=(nd, nf, 4, (rows_of(g_out),), (((0, None, 0, D // 2),), ((0, None, D // 2, D // 2),))))
    dz1, gw1, dg1, db1, dc1, rs1, small1, kk1, gate0, u0 = back(1, 2, comm=(nd, nf, 3, (rows_of(gw0),), (((0, 0, 0, Eh),), ((0, 1, 0, Eh),))))
    small = jnp.concatenate([small0, small1], axis=1)
    kk = jnp.concatenate([kk0, kk1], axis=1)
    kkh = jnp.sum(kk.reshape(kk.shape[0], H, E // H), axis=2)
    dbcdt, small_bc, hs = post(ubc, pre_bc, taps_bc, head_params, masks, segc, segr, b, c, (dg0, db0, dc0, rs0), (dg1, db1, dc1, rs1), kkh, dt)
    d_conv = jnp.concatenate([jnp.stack([small[6], small[5], small[4], small[3], small[2]]),
                              jnp.stack([small_bc[4], small_bc[3], small_bc[2], small_bc[1], small_bc[0]])], axis=1)
    d_heads = jnp.concatenate([hs, jnp.sum(small[1].reshape(1, H, E // H), axis=2)], axis=0)
    lanes = -(-max(ncol, ngate, H) // 128) * 128
    cols = lambda a: jnp.pad(a.reshape(-1, n, a.shape[1] // n).transpose(1, 0, 2), ((0, 0), (0, 0), (0, lanes - a.shape[1] // n)))
    heads_row = jnp.broadcast_to(jnp.pad(d_heads, ((0, 0), (0, lanes - H)))[None], (n, d_heads.shape[0], lanes))
    used = K1 + 1 + d_heads.shape[0]
    mine = jnp.concatenate([cols(d_conv), cols(small[:1]), heads_row, jnp.zeros((n, -(-used // 8) * 8 - used, lanes), f32)], axis=1)
    g_bcdt = dot(normt, dbcdt).astype(bf16)
    split = (((0, 0, 0, Eh),), ((0, 1, 0, Eh), (1, None, 0, wide)))
    gate1, u1, output, grad_in, tot, d_norm = tail(nd, nf, 1, (rows_of(gw1), rows_of(g_bcdt)), split, dz0, dz1, dbcdt, full_gate, full_a, gg,
                                                   full_out, hidden, grad_out, r, norm_gain[None], mine)
    s_zx, s_bc, s_dt, s_w, t_conv, t_norm, t_gate, t_heads = finish(
        nd, nf, gate0, gate1, u0, u1, s_out, tot, d_norm,
        ((nrow, 2 * E), (nrow, 2 * N), (nrow, H), (E // n, D), (K1, ncol), (1, nrow), (1, ngate), d_heads.shape))
    return output, grad_in, s_zx, s_bc, s_dt, s_w, t_conv, t_norm.reshape(-1), t_gate.reshape(-1), t_heads


def per_device(nd, nf, hidden, grad_out, segment_ids, w_zx, w_bc, w_dt, w_out, conv_params, norm_gain, gate_gain, head_params):
    n = nd * nf
    E, N2, H = w_out.shape[0] * n, w_bc.shape[1], w_dt.shape[1]
    rows = w_zx.shape[0]
    small = jnp.concatenate([conv_params.reshape(-1), norm_gain, gate_gain])
    S = -(-small.shape[0] // rows)
    assert S + H <= 128
    small = jnp.pad(small, (0, S * rows - small.shape[0])).reshape(rows, S)
    shard_a = jnp.concatenate([w_zx[:, E:], w_bc, w_dt, small, jnp.zeros((rows, 128 - H - S), bf16)], axis=1)
    return layer(nd, nf, hidden, grad_out, segment_ids, shard_a, w_zx[:, :E], w_out, head_params, (E, N2 // 2, H, conv_params.shape[0], S))


def solution(mesh):
    row, col, vec, rep = P(AXES, None), P(None, AXES), P(AXES), P()
    return jax.shard_map(
        functools.partial(per_device, mesh.shape["dp"], mesh.shape["fsdp"]),
        mesh=mesh,
        in_specs=(row, row, vec, row, row, row, row, col, vec, vec, rep),
        out_specs=(row, row, row, row, row, row, col, vec, vec, rep),
        check_vma=False,
    )
```

```python
import functools
import jax
import jax.numpy as jnp
from jax import lax
from jax.experimental import pallas as pl
from jax.experimental.pallas import tpu as pltpu
from jax.sharding import PartitionSpec as P

EPS = 1e-05
L = 128
HG = 8
LOG2E = 1.4426950408889634
MB = 512
BWD_SPOTS = ((5.0, 10.0, 2.0, 26.0, 3.2), (7.0, 16.5, 2.0, 39.0, 3.2))
TAIL_SPOTS = ((7.0, 13.0, 3.0, 30.0, 4.0), (9.0, 22.0, 3.0, 46.0, 3.0))
bf16, f32 = jnp.bfloat16, jnp.float32
HIGHEST = lax.Precision.HIGHEST


AXES = ("dp", "fsdp")
MESH = pl.DeviceIdType.MESH


class Place:
    def __init__(self, nd, nf):
        self.zn, self.nf = nd // 2, nf
        d, f = lax.axis_index("dp"), lax.axis_index("fsdp")
        self.z, self.y = d // 2, d % 2
        self.x, self.c = f // 2, f % 2

    def dev(self, z, y, x, c):
        return (z * 2 + y, x * 2 + c)

    def idx(self, z, y, x, c):
        return (z * 2 + y) * self.nf + x * 2 + c

    def meet(self):
        z, zn = self.z, self.zn
        pl.semaphore_wait(pltpu.get_barrier_semaphore(), 3 + (z + zn - 1) // zn + (2 * zn - 2 - z) // zn)

    def greet(self):
        z, y, x, c, zn = self.z, self.y, self.x, self.c, self.zn
        sem = pltpu.get_barrier_semaphore()
        for there in ((z, y, 1 - x, c), (z, 1 - y, x, c), (z, y, x, 1 - c)):
            pl.semaphore_signal(sem, inc=1, device_id=self.dev(*there), device_id_type=MESH)

        @pl.when(z > 0)
        def _():
            pl.semaphore_signal(sem, inc=1, device_id=self.dev(z - 1, y, x, c), device_id_type=MESH)

        @pl.when(z < zn - 1)
        def _():
            pl.semaphore_signal(sem, inc=1, device_id=self.dev(z + 1, y, x, c), device_id_type=MESH)


def gather_kernel(nd, nf, src_ref, out_ref, own_sem, z_send, z_recv, x_send, x_recv, y_send, y_recv, dx_send, dx_recv, dy_send, dy_recv, c_send, c_recv):
    at = Place(nd, nf)
    z, y, x, c, zn = at.z, at.y, at.x, at.c, at.zn
    half = out_ref.shape[2] // 256 * 128
    lo, hi = pl.ds(0, half), pl.ds(half, out_ref.shape[2] - half)
    at.greet()
    at.meet()

    def copy(block, to, send, recv, cols=None, src=None):
        ref = out_ref.at[block] if cols is None else out_ref.at[block, :, cols]
        return pltpu.make_async_remote_copy(src_ref=ref if src is None else src, dst_ref=ref, send_sem=send, recv_sem=recv,
                                            device_id=at.dev(*to), device_id_type=MESH)

    def block(zs, col):
        return at.idx(zs, 1 - y if col & 2 else y, 1 - x if col & 1 else x, c)

    def up(zs, src=None):
        return copy(block(zs, 0), (z + 1, y, x, c), z_send.at[0, zs], z_recv.at[zs], src=src)

    def down(zs, src=None):
        return copy(block(zs, 0), (z - 1, y, x, c), z_send.at[1, zs], z_recv.at[zs], src=src)

    def to_x(zs, src=None):
        return copy(block(zs, 0), (z, y, 1 - x, c), x_send.at[zs], x_recv.at[zs], src=src)

    def to_y(zs, src=None):
        return copy(block(zs, 0), (z, 1 - y, x, c), y_send.at[zs], y_recv.at[zs], src=src)

    def diag_y(zs):
        return copy(block(zs, 1), (z, 1 - y, x, c), dy_send.at[zs], dy_recv.at[zs], lo)

    def diag_x(zs):
        return copy(block(zs, 2), (z, y, 1 - x, c), dx_send.at[zs], dx_recv.at[zs], hi)

    def to_core(zs, col, src=None):
        return copy(block(zs, col), (z, y, x, 1 - c), c_send.at[zs, col], c_recv.at[zs, col], src=src)

    own = pltpu.make_async_copy(src_ref, out_ref.at[block(z, 0)], own_sem)
    own.start()

    @pl.when(z < zn - 1)
    def _():
        up(z, src_ref).start()

    @pl.when(z > 0)
    def _():
        down(z, src_ref).start()

    to_x(z, src_ref).start()
    to_y(z, src_ref).start()
    to_core(z, 0, src_ref).start()

    def each(dist, fn):
        if dist == 0:
            fn(z, 0)
            return

        @pl.when(z - dist >= 0)
        def _():
            fn(z - dist, 1)

        @pl.when(z + dist < zn)
        def _():
            fn(z + dist, -1)

    def from_z(zs, way):
        copy(block(zs, 0), (z, y, x, c), z_send.at[0, zs], z_recv.at[zs]).wait_recv()
        if way > 0:
            @pl.when(z < zn - 1)
            def _():
                up(zs).start()
        else:
            @pl.when(z > 0)
            def _():
                down(zs).start()
        to_x(zs).start()
        to_y(zs).start()
        to_core(zs, 0).start()

    def from_xy(zs, way):
        to_x(zs).wait_recv()
        diag_y(zs).start()
        to_core(zs, 1).start()
        to_y(zs).wait_recv()
        diag_x(zs).start()
        to_core(zs, 2).start()

    def from_diag(zs, way):
        diag_y(zs).wait_recv()
        diag_x(zs).wait_recv()
        to_core(zs, 3).start()

    for dist in range(zn):
        if dist:
            each(dist, from_z)
        each(dist, from_xy)
    for dist in range(zn):
        each(dist, from_diag)
    own.wait()

    def sent(zs, way):
        for col in range(4):
            to_core(zs, col).wait_recv()
            to_core(zs, col).wait_send()
        to_x(zs).wait_send()
        to_y(zs).wait_send()
        diag_x(zs).wait_send()
        diag_y(zs).wait_send()
        if way >= 0:
            @pl.when(z < zn - 1)
            def _():
                up(zs).wait_send()
        if way <= 0:
            @pl.when(z > 0)
            def _():
                down(zs).wait_send()

    for dist in range(zn):
        each(dist, sent)


def gather_rows(shard, nd, nf, cid):
    zn = nd // 2
    D = pltpu.SemaphoreType.DMA
    return pl.pallas_call(
        functools.partial(gather_kernel, nd, nf),
        out_shape=jax.ShapeDtypeStruct((nd * nf,) + shard.shape, shard.dtype),
        in_specs=[pl.BlockSpec(memory_space=pl.ANY)],
        out_specs=pl.BlockSpec(memory_space=pl.ANY),
        scratch_shapes=[D(()), D((2, zn)), D((zn,)), D((zn,)), D((zn,)), D((zn,)), D((zn,)), D((zn,)), D((zn,)), D((zn,)), D((zn,)),
                        D((zn, 4)), D((zn, 4))],
        compiler_params=pltpu.CompilerParams(collective_id=cid, has_side_effects=True),
    )(shard)


class Scatter:
    def __init__(self, nd, nf, g_refs, out_ref, acc, c_in, d_in, xy_in, z_in,
                 load_sem, c_send, c_recv, dx_send, dx_recv, dy_send, dy_recv, x_send, x_recv, y_send, y_recv, z_send, z_recv):
        at = Place(nd, nf)
        z, y, x, c, zn = at.z, at.y, at.x, at.c, at.zn
        cols = out_ref.shape[1]
        wids = [r.shape[3] for r in g_refs]
        offs = [sum(wids[:k]) for k in range(len(wids))]
        half = cols // 256 * 128
        lo, hi = pl.ds(0, half), pl.ds(half, cols - half)

        def inner(col, core):
            return at.idx(0, 1 - y if col & 2 else y, 1 - x if col & 1 else x, core)

        def remote(src, dst, to, send, recv):
            return pltpu.make_async_remote_copy(src_ref=src, dst_ref=dst, send_sem=send, recv_sem=recv, device_id=at.dev(*to), device_id_type=MESH)

        def load(col):
            return [pltpu.make_async_copy(r.at[:, inner(col, c)], acc.at[col, :, :, pl.ds(o, w)], load_sem.at[col, k])
                    for k, (r, o, w) in enumerate(zip(g_refs, offs, wids))]

        def core(col):
            return [remote(r.at[:, inner(col, 1 - c)], c_in.at[col, :, :, pl.ds(o, w)], (z, y, x, 1 - c), c_send.at[col, k], c_recv.at[col, k])
                    for k, (r, o, w) in enumerate(zip(g_refs, offs, wids))]

        def diag_x(zs):
            return remote(acc.at[3, zs, :, lo], d_in.at[zs, :, lo], (z, y, 1 - x, c), dx_send.at[zs], dx_recv.at[zs])

        def diag_y(zs):
            return remote(acc.at[3, zs, :, hi], d_in.at[zs, :, hi], (z, 1 - y, x, c), dy_send.at[zs], dy_recv.at[zs])

        def to_x(zs):
            return remote(acc.at[1, zs], xy_in.at[0, zs], (z, y, 1 - x, c), x_send.at[zs], x_recv.at[zs])

        def to_y(zs):
            return remote(acc.at[2, zs], xy_in.at[1, zs], (z, 1 - y, x, c), y_send.at[zs], y_recv.at[zs])

        def up(zs):
            return remote(acc.at[0, zs], z_in.at[zs + 1], (z + 1, y, x, c), z_send.at[zs], z_recv.at[0, zs])

        def down(zs):
            return remote(acc.at[0, zs], z_in.at[zs], (z - 1, y, x, c), z_send.at[zs], z_recv.at[1, zs])

        def each(dist, fn):
            if dist == 0:
                fn(z)
                return

            @pl.when(z - dist >= 0)
            def _():
                fn(z - dist)

            @pl.when(z + dist < zn)
            def _():
                fn(z + dist)

        order = list(range(zn - 1, -1, -1))

        def start(col):
            for cp in core(col) + load(col):
                cp.start()

        def ready(col):
            for cp in load(col):
                cp.wait()
            for cp in core(col):
                cp.wait_recv()

        def diag(zs):
            acc[3, zs] = acc[3, zs] + c_in[3, zs]
            diag_x(zs).start()
            diag_y(zs).start()

        def sides(zs):
            diag_y(zs).wait_recv()
            acc[1, zs, :, lo] = acc[1, zs, :, lo] + c_in[1, zs, :, lo]
            acc[1, zs, :, hi] = acc[1, zs, :, hi] + c_in[1, zs, :, hi] + d_in[zs, :, hi]
            to_x(zs).start()
            diag_x(zs).wait_recv()
            acc[2, zs, :, lo] = acc[2, zs, :, lo] + c_in[2, zs, :, lo] + d_in[zs, :, lo]
            acc[2, zs, :, hi] = acc[2, zs, :, hi] + c_in[2, zs, :, hi]
            to_y(zs).start()

        def column(zs):
            to_x(zs).wait_recv()
            to_y(zs).wait_recv()
            return (acc[0, zs] + c_in[0, zs]).astype(f32) + (xy_in[0, zs] + xy_in[1, zs]).astype(f32)

        def pass_on(zs):
            total = column(zs)

            @pl.when(zs > z)
            def _():
                @pl.when(z > 0)
                def _():
                    up(zs).wait_recv()
                    acc[0, zs] = (total + z_in[zs + 1].astype(f32)).astype(bf16)

                @pl.when(z == 0)
                def _():
                    acc[0, zs] = total.astype(bf16)
                up(zs).start()

            @pl.when(zs < z)
            def _():
                @pl.when(z < zn - 1)
                def _():
                    down(zs).wait_recv()
                    acc[0, zs] = (total + z_in[zs].astype(f32)).astype(bf16)

                @pl.when(z == zn - 1)
                def _():
                    acc[0, zs] = total.astype(bf16)
                down(zs).start()

        def finish():
            out_ref[...] = column(z)

            @pl.when(z > 0)
            def _():
                up(z).wait_recv()
                out_ref[...] += z_in[z + 1].astype(f32)

            @pl.when(z < zn - 1)
            def _():
                down(z).wait_recv()
                out_ref[...] += z_in[z].astype(f32)

            def sent(zs):
                diag_x(zs).wait_send()
                diag_y(zs).wait_send()
                to_x(zs).wait_send()
                to_y(zs).wait_send()

            for col in range(4):
                for cp in core(col):
                    cp.wait_send()
            for dist in order:
                each(dist, sent)
                if dist:
                    each(dist, lambda zs: up(zs).wait_send())

        self.start, self.finish, self.greet, self.meet = start, finish, at.greet, at.meet
        self.diag = [functools.partial(ready, 3)] + [functools.partial(each, dist, diag) for dist in order]
        self.sides = [functools.partial(each, dist, sides) for dist in order]
        self.pass_on = [functools.partial(each, dist, pass_on) for dist in order[:-1]]
        self.ready = lambda: (ready(1), ready(2), ready(0))

    @staticmethod
    def scratch(nd, rows, cols, parts):
        zn = nd // 2
        D, V = pltpu.SemaphoreType.DMA, pltpu.VMEM
        return [V((4, zn, rows, cols), bf16), V((4, zn, rows, cols), bf16), V((zn, rows, cols), bf16), V((2, zn, rows, cols), bf16),
                V((zn + 1, rows, cols), bf16), D((4, parts)), D((4, parts)), D((4, parts))] + [D((zn,))] * 9 + [D((2, zn))]


def plan(pipes, place, time_of, spots):
    ticks = {0: [place.greet], 1: [place.meet] + [functools.partial(p.start, col) for col in (3, 1, 2, 0) for p in pipes]}

    def put(when, fn):
        tick = next((t for t, us in enumerate(time_of) if us >= when), len(time_of))
        ticks.setdefault(tick, []).append(fn)

    todo = []
    for p, (diag, sides, side_gap, pass_on, pass_gap) in zip(pipes, spots):
        todo += [(diag, fn) for fn in p.diag] + [(sides, p.ready)]
        todo += [(sides + k * side_gap * 4 / len(p.sides), fn) for k, fn in enumerate(p.sides)]
        todo += [(pass_on + k * pass_gap * 4 / len(p.sides), fn) for k, fn in enumerate(p.pass_on)]
    for when, fn in sorted(todo, key=lambda e: e[0]):
        put(when, fn)
    return ticks


def pipes_of(nd, nf, g_refs, out_refs, split, scratch):
    def view(a, lead, o, w):
        return g_refs[a].at[:, :, :, pl.ds(o, w)] if lead is None else g_refs[a].at[lead, :, :, :, pl.ds(o, w)]
    per = len(scratch) // len(split)
    return [Scatter(nd, nf, [view(*v) for v in pipe], out_ref, *scratch[per * m : per * (m + 1)])
            for m, (pipe, out_ref) in enumerate(zip(split, out_refs))]


def widths(split):
    return [sum(v[3] for v in pipe) for pipe in split]


def pipes_scratch(nd, rows, split):
    return [x for pipe, w in zip(split, widths(split)) for x in Scatter.scratch(nd, rows, w, len(pipe))]


def run_ticks(ticks, now, last):
    planned = sorted((t, fns) for t, fns in ticks.items() if t <= last)

    def search(items):
        if len(items) == 1:
            tick, fns = items[0]

            @pl.when(now == tick)
            def _():
                for fn in fns:
                    fn()
            return
        mid = len(items) // 2
        lax.cond(now < items[mid][0], lambda: search(items[:mid]), lambda: search(items[mid:]))

    if planned:
        search(planned)


def run_rest(ticks, last):
    for tick, fns in sorted(ticks.items()):
        if tick > last:
            for fn in fns:
                fn()


class Spread:
    def __init__(self, nd, nf, src, got, send, recv):
        self.n, self.nf = nd * nf, nf
        self.me = lax.axis_index("dp") * nf + lax.axis_index("fsdp")
        self.src, self.got, self.send, self.recv = src, got, send, recv

    def peer(self, k):
        return lax.rem(self.me + k, self.n)

    def loop(self, fn):
        def body(k, carry):
            fn(k)
            return carry
        lax.fori_loop(1, self.n, body, 0)

    def greet(self):
        sem = pltpu.get_barrier_semaphore()

        def one(k):
            pl.semaphore_signal(sem, inc=1, device_id=(self.peer(k) // self.nf, self.peer(k) % self.nf), device_id_type=MESH)
        self.loop(one)

    def meet(self):
        pl.semaphore_wait(pltpu.get_barrier_semaphore(), self.n - 1)

    def copy(self, k):
        p = self.peer(k)
        src = self.src.at[p] if len(self.src.shape) == 3 else self.src
        return pltpu.make_async_remote_copy(src_ref=src, dst_ref=self.got.at[k], send_sem=self.send.at[k], recv_sem=self.recv.at[k],
                                            device_id=(p // self.nf, p % self.nf), device_id_type=MESH)

    def begin(self):
        self.loop(lambda k: self.copy(k).start())

    def total(self):
        own = self.src[self.me] if len(self.src.shape) == 3 else self.src[...]

        def add(k, total):
            self.copy(k).wait_recv()
            return total + self.got[k]
        total = lax.fori_loop(1, self.n, add, own)
        self.loop(lambda k: self.copy(k).wait_send())
        return total

    @staticmethod
    def scratch(n, tile):
        D = pltpu.SemaphoreType.DMA
        return [pltpu.VMEM((n,) + tile, f32), D((n,)), D((n,))]


def dot(a, b, dims=((1,), (0,)), precision=None):
    return lax.dot_general(a, b, (dims, ((), ())), preferred_element_type=f32, precision=precision)


def sigmoid(x):
    return 0.5 * jnp.tanh(0.5 * x) + 0.5


def conv_rows(ext, taps, masks, halo):
    rows = ext.shape[0] - halo
    width = 4
    v = ext[halo:]
    out = taps[4:5] + taps[3:4] * v
    for k in range(1, width):
        moved = pltpu.roll(ext, k, 0)[halo:]
        out = out + (taps[3 - k : 4 - k] * masks[:, k : k + 1]) * moved
    return out


def prep_kernel(bcdt_ref, taps_ref, heads_ref, segc_ref, segr_ref,
                m_ref, b_ref, c_ref, bt_ref, ct_ref, pre_ref, gm_ref, cum_ref, cumr_ref, sc_ref, dt_ref):
    T = bcdt_ref.shape[0]
    nc = T // L
    N = b_ref.shape[1]
    H = dt_ref.shape[1]
    groups = cumr_ref.shape[0]
    taps = taps_ref[...]
    tri = (lax.broadcasted_iota(jnp.int32, (L, L), 0) >= lax.broadcasted_iota(jnp.int32, (L, L), 1))
    trif = tri.astype(f32)
    neg_rate = -jnp.exp(heads_ref[0:1, :H]) * LOG2E
    m_ref[T : T + 8, :] = jnp.zeros((8, 4), f32)
    bias = heads_ref[1:2, :H]

    def chunk(c, carry):
        t0 = pl.multiple_of(c * L, L)
        here = pl.ds(t0, L)
        h0 = pl.multiple_of(jnp.maximum(t0 - 16, 0), 16)
        before = bcdt_ref[pl.ds(h0, 16), : 2 * N].astype(f32)
        v = bcdt_ref[here, : 2 * N].astype(f32)
        segc = segc_ref[here, :].astype(f32)
        seg_ext = jnp.concatenate([segc_ref[pl.ds(h0, 16), :].astype(f32), segc], axis=0)
        at = t0 + lax.broadcasted_iota(jnp.int32, (L, 1), 0)
        masks = [jnp.ones((L, 1), f32)]
        for k in range(1, 4):
            masks.append(((pltpu.roll(seg_ext, k, 0)[16:] == segc) & (at >= k)).astype(f32))
        masks = jnp.concatenate(masks, axis=1)
        m_ref[here, :] = masks
        pre = conv_rows(jnp.concatenate([before, v], axis=0), taps, masks, 16)
        pre_ref[here, :] = pre
        act = pre * sigmoid(pre)
        b = act[:, :N]
        cc = act[:, N:]
        bb = b.astype(bf16)
        cb = cc.astype(bf16)
        b_ref[here, :] = bb
        c_ref[here, :] = cb
        bt_ref[:, here] = b.T.astype(bf16)
        ct_ref[:, here] = cc.T.astype(bf16)
        prev = jnp.where(c > 0, seg_ext[15:16], -1.0)
        last = segc[L - 1 : L]
        same = segc == segr_ref[:, here].astype(f32)
        g = dot(cb, bb, ((1,), (1,)))
        gm_ref[pl.ds(c, 1)] = jnp.where(tri & same, g, 0.0)[None]
        raw = bcdt_ref[here, 2 * N : 2 * N + 128].astype(f32)[:, :H] + bias
        dt = jnp.maximum(raw, 0.0) + jnp.log1p(jnp.exp(-jnp.abs(raw)))
        a2 = neg_rate * dt
        cum = dot(trif, a2, precision=HIGHEST)
        end = cum[L - 1 : L]
        ein = jnp.where(segc == prev, jnp.exp2(cum), 0.0)
        lv = jnp.where(segc == last, jnp.exp2(end - cum), 0.0)
        dt_ref[here, :] = dt
        wide = jnp.concatenate([cum, jnp.zeros((L, 128 - H), f32)], axis=1)
        cum_ref[here, :] = wide
        cumt = wide.T
        for k in range(groups):
            cumr_ref[k, :, here] = cumt[HG * k : HG * (k + 1)]
        s0 = pl.multiple_of(c * (3 * L), L)
        for k, part in enumerate((dt, ein, lv)):
            sc_ref[pl.ds(s0 + k * L, L), :] = jnp.concatenate([part, jnp.zeros((L, 128 - H), f32)], axis=1).astype(bf16)
        return carry

    lax.fori_loop(0, nc, chunk, 0)


def prep(bcdt, taps, heads, segc, segr, N, H):
    T = bcdt.shape[0]
    nc = T // L
    G = H // HG
    S = jax.ShapeDtypeStruct
    full = lambda a: pl.BlockSpec(a.shape, lambda i: (0,) * a.ndim)
    outs = (S((T + 8, 4), f32), S((T, N), bf16), S((T, N), bf16), S((N, T), bf16), S((N, T), bf16), S((T, 2 * N), f32),
            S((nc, L, L), f32), S((T, 128), f32), S((G, HG, T), f32), S((3 * T, 128), bf16), S((T, H), f32))
    wide = 2 * N + 128
    return pl.pallas_call(
        prep_kernel,
        grid=(1,),
        in_specs=[pl.BlockSpec((T, wide), lambda i: (0, bcdt.shape[1] // wide - 1))] + [full(a) for a in (taps, heads, segc, segr)],
        out_specs=[full(o) for o in outs],
        out_shape=outs,
        compiler_params=pltpu.CompilerParams(vmem_limit_bytes=60 << 20),
    )(bcdt, taps, heads, segc, segr)


def lane_onehot(group, width, per):
    shape = (128, width)
    return (group * HG + lax.broadcasted_iota(jnp.int32, shape, 1) // per == lax.broadcasted_iota(jnp.int32, shape, 0)).astype(bf16)


def half_masks(P):
    lane = lax.broadcasted_iota(jnp.int32, (1, 2 * P), 1)
    first = (lane < P).astype(f32)
    return first.astype(bf16), (1.0 - first).astype(bf16)


def decay(cum4, cumr, k):
    return jnp.exp2(jnp.minimum(cum4[:, k : k + 1] - cumr[k : k + 1, :], 0.0))


def fwd_kernel(u_ref, gate_ref, taps_ref, m_ref, b_ref, c_ref, bt_ref, gm_ref, cum_ref, cumr_ref, sc_ref,
               gg_ref, r_ref, pre_ref, st_ref, state, move, ssq_ref):
    T, W = u_ref.shape
    P = W // HG
    nc = T // L
    step = pl.program_id(0)
    taps = taps_ref[...]
    gain = taps[5:6]
    skip = taps[6:7]
    onehot = lane_onehot(step, W, P)
    ma, mb = half_masks(P)
    state[...] = jnp.zeros_like(state)

    @pl.when(step == 0)
    def _():
        ssq_ref[...] = jnp.zeros_like(ssq_ref)

    @pl.when(step == 0)
    def _():
        def make(c, carry):
            here = pl.ds(pl.multiple_of(c * L, L), L)
            lag = lax.broadcasted_iota(jnp.int32, (L, L + 16), 0) + 16 - lax.broadcasted_iota(jnp.int32, (L, L + 16), 1)
            for k in range(1, 4):
                move[c, (k - 1) * L : k * L, :] = jnp.where(lag == k, m_ref[here, k : k + 1], 0.0).astype(bf16)
            return carry
        lax.fori_loop(0, nc, make, 0)

    def chunk(c, carry):
        t0 = pl.multiple_of(c * L, L)
        here = pl.ds(t0, L)
        h0 = pl.multiple_of(jnp.maximum(t0 - 16, 0), 16)
        v = u_ref[here, :]
        moved = dot(move[c], jnp.concatenate([u_ref[pl.ds(h0, 16), :], v], axis=0))
        pre = taps[4:5] + taps[3:4] * v.astype(f32)
        for k in range(1, 4):
            pre = pre + taps[3 - k : 4 - k] * moved[(k - 1) * L : k * L]
        pre_ref[here, :] = pre.astype(bf16)
        x = pre * sigmoid(pre)
        s0 = pl.multiple_of(c * (3 * L), L)
        exp = dot(sc_ref[pl.ds(s0, 3 * L), :], onehot)
        dtx, einx, lvx = exp[:L], exp[L : 2 * L], exp[2 * L :]
        xd = x * dtx
        xdb = xd.astype(bf16)
        gm = gm_ref[c]
        cum4 = pltpu.roll(cum_ref[here, :], 128 - step * HG, 1)
        cumr = cumr_ref[0, :, here]
        sb = state[...].astype(bf16)
        st_ref[c] = sb
        inner = []
        for p in range(HG // 2):
            m0 = (decay(cum4, cumr, 2 * p) * gm).astype(bf16)
            m1 = (decay(cum4, cumr, 2 * p + 1) * gm).astype(bf16)
            xp = xdb[:, 2 * P * p : 2 * P * (p + 1)]
            inner.append(dot(jnp.concatenate([m0, m1], axis=1), jnp.concatenate([xp * ma, xp * mb], axis=0)))
        y = jnp.concatenate(inner, axis=1) + dot(c_ref[here, :], sb) * einx + skip * x
        state[...] = state[...] * einx[L - 1 : L] + dot(bt_ref[:, here], (xd * lvx).astype(bf16))
        gate = gate_ref[here, :].astype(f32)
        g = y * (gate * sigmoid(gate))
        gg_ref[here, :] = (g * gain).astype(bf16)
        g2 = g * g
        tot = g2[:, :128]
        for j in range(1, W // 128):
            tot = tot + g2[:, 128 * j : 128 * (j + 1)]
        ssq_ref[here, :] += tot
        return carry

    lax.fori_loop(0, nc, chunk, 0, unroll=4)

    @pl.when(step == pl.num_programs(0) - 1)
    def _():
        def root(c, carry):
            here = pl.ds(pl.multiple_of(c * L, L), L)
            total = jnp.sum(ssq_ref[here, :], axis=1, keepdims=True)
            r_ref[here, :] = lax.rsqrt(total / (W * pl.num_programs(0)) + EPS)
            return carry
        lax.fori_loop(0, nc, root, 0)


def fwd(u, gate, taps, masks, b, c, bt, gm, cum, cumr, sc):
    T, E = gate.shape
    N = b.shape[1]
    G = cumr.shape[0]
    W = E // G
    nc = T // L
    S = jax.ShapeDtypeStruct
    col = lambda off: pl.BlockSpec((T, W), lambda g: (0, g + off))
    full = lambda a: pl.BlockSpec(a.shape, lambda g: (0,) * a.ndim)
    grp = lambda a: pl.BlockSpec((1,) + a.shape[1:], lambda g: (g, 0, 0))
    return pl.pallas_call(
        fwd_kernel,
        grid=(G,),
        in_specs=[col(0), col(0), pl.BlockSpec((8, W), lambda g: (0, g)), full(masks), full(b), full(c), full(bt), full(gm),
                  full(cum), grp(cumr), full(sc)],
        out_specs=[col(0), pl.BlockSpec((T, 1), lambda g: (0, 0)), col(0), pl.BlockSpec((nc, N, W), lambda g: (0, 0, g))],
        out_shape=(S((T, E), bf16), S((T, 1), f32), S((T, E), bf16), S((nc, N, E), bf16)),
        scratch_shapes=[pltpu.VMEM((N, W), f32), pltpu.VMEM((nc, 3 * L, L + 16), bf16), pltpu.VMEM((T, 128), f32)],
        compiler_params=pltpu.CompilerParams(vmem_limit_bytes=60 << 20),
        cost_estimate=pl.CostEstimate(flops=T * E * (2 * L + 4 * N) * 2, bytes_accessed=T * E * 12, transcendentals=T * E * 4),
    )(u, gate, taps, masks, b, c, bt, gm, cum, cumr, sc)


def bwd_scatter_kernel(nd, nf, g0, Gh, nc, arrays, split, *refs):
    g_refs, ins, outs = refs[:arrays], refs[arrays : arrays + 16], refs[arrays + 16 : arrays + 24]
    refs = refs[arrays + 24 :]
    sums, own, comm = refs[: len(split)], refs[len(split) : len(split) + 3], refs[len(split) + 3 :]
    pipes = pipes_of(nd, nf, g_refs, sums, split, comm)
    nb = ins[15].shape[0] // MB
    time_of = [21.0 * g + (1.9 * i if i < nc else 1.9 * nc + 1.9 * (i - nc)) for g in range(Gh) for i in range(nc + nb)]
    ticks = plan(pipes, pipes[0], time_of, BWD_SPOTS)
    last = len(time_of) - 1
    bwd_body(lambda i: run_ticks(ticks, pl.program_id(0) * (nc + nb) + i, last), g0, *ins, *outs, *own)

    @pl.when(pl.program_id(0) == pl.num_programs(0) - 1)
    def _():
        run_rest(ticks, last)
        for p in pipes:
            p.finish()


def bwd_body(tick, g0, u_ref, gate_ref, pre_ref, dm_ref, rq_ref, taps_ref, m_ref, b_ref, c_ref, ct_ref, gm_ref, cum_ref, cumr_ref, sc_ref, st_ref, normt_ref,
             dz_ref, gw_ref, dg_ref, db_ref, dc_ref, rs_ref, small_ref, kk_ref, ds, nxt, acc):
    T, W = u_ref.shape
    P = W // HG
    nc = T // L
    step = pl.program_id(0)
    taps = taps_ref[...]
    gain = taps[5:6]
    skip = taps[6:7]
    onehot = lane_onehot(step + g0, W, P)
    ma, mb = half_masks(P)
    ds[...] = jnp.zeros_like(ds)
    nxt[...] = jnp.zeros_like(nxt)
    acc[...] = jnp.zeros_like(acc)

    @pl.when(step == 0)
    def _():
        dg_ref[...] = jnp.zeros_like(dg_ref)
        db_ref[...] = jnp.zeros_like(db_ref)
        dc_ref[...] = jnp.zeros_like(dc_ref)
        rs_ref[...] = jnp.zeros_like(rs_ref)

    ri = lax.broadcasted_iota(jnp.int32, (4 * W, 128), 0)
    ci = lax.broadcasted_iota(jnp.int32, (4 * W, 128), 1)
    part = ri // W
    want = (jnp.maximum(part - 1, 0) * pl.num_programs(0) + step) * HG + (ri % W) // P
    fold = (want == ci).astype(bf16)

    def eight(z):
        return jnp.sum(z.reshape(L // 8, 8, W), axis=0)

    def chunk(i, carry):
        tick(i)
        c = nc - 1 - i
        t0 = pl.multiple_of(c * L, L)
        here = pl.ds(t0, L)
        u = u_ref[here, :].astype(f32)
        pre = pre_ref[here, :].astype(f32)
        sig = sigmoid(pre)
        x = pre * sig
        dsilu = sig + x * (1.0 - sig)
        s0 = pl.multiple_of(c * (3 * L), L)
        exp = dot(sc_ref[pl.ds(s0, 3 * L), :], onehot)
        dtx, einx, lvx = exp[:L], exp[L : 2 * L], exp[2 * L :]
        xdb = (x * dtx).astype(bf16)
        xd = xdb.astype(f32)
        gm = gm_ref[c]
        cum4 = pltpu.roll(cum_ref[here, :], 128 - (step + g0) * HG, 1)
        cumr = cumr_ref[0, :, here]
        sb = st_ref[c]
        es, ms, inner = [], [], []
        for p in range(HG // 2):
            e0 = decay(cum4, cumr, 2 * p)
            e1 = decay(cum4, cumr, 2 * p + 1)
            m0 = (e0 * gm).astype(bf16)
            m1 = (e1 * gm).astype(bf16)
            xp = xdb[:, 2 * P * p : 2 * P * (p + 1)]
            inner.append(dot(jnp.concatenate([m0, m1], axis=1), jnp.concatenate([xp * ma, xp * mb], axis=0)))
            es.append((e0, e1))
            ms.append((m0, m1))
        yn = jnp.concatenate(inner, axis=1) + dot(c_ref[here, :], sb) * einx
        y = yn + skip * x
        gate = gate_ref[here, :].astype(f32)
        sgate = sigmoid(gate)
        silu_g = gate * sgate
        g = y * silu_g
        r = rq_ref[here, 0:1]
        q = rq_ref[here, 1:2]
        dmr = dm_ref[here, :].astype(f32) * r
        dgg = gain * dmr - g * q
        dyb = (dgg * silu_g).astype(bf16)
        dy = dyb.astype(f32)
        dz_ref[0, here, :] = (dgg * y * (sgate + silu_g * (1.0 - sgate))).astype(bf16)
        dxi = []
        dgc = dg_ref[c]
        for p in range(HG // 2):
            cols = slice(2 * P * p, 2 * P * (p + 1))
            dp = dyb[:, cols]
            dstack = jnp.concatenate([dp * ma, dp * mb], axis=0)
            dmm = dot(dstack, xdb[:, cols], ((1,), (1,)))
            dgc = dgc + dmm[:L] * es[p][0] + dmm[L:] * es[p][1]
            dxi.append(dot(jnp.concatenate(ms[p], axis=0), dstack, ((0,), (0,))))
        dg_ref[c] = dgc
        dxi = jnp.concatenate(dxi, axis=1)
        dsn = ds[...]
        dsb = dsn.astype(bf16)
        dye = (dy * einx).astype(bf16)
        dc_ref[here, :] += dot(dye, sb, ((1,), (1,)))
        kept = einx[L - 1 : L]
        kk_ref[pl.ds(c, 1), :] = kept * jnp.sum(sb.astype(f32) * dsn, axis=0, keepdims=True)
        db_ref[here, :] += dot((xd * lvx).astype(bf16), dsb, ((1,), (1,)))
        dxe = dot(b_ref[here, :], dsb) * lvx
        ds[...] = dsn * kept + dot(ct_ref[:, here], dye)
        dxd = dxi + dxe
        r1 = dy * yn - xd * dxi
        r1h = r1.astype(bf16)
        r1l = (r1 - r1h.astype(f32)).astype(bf16)
        rs_ref[here, :] += dot(jnp.concatenate([r1h, r1l, (xd * dxe).astype(bf16), (x * dxd).astype(bf16)], axis=1), fold)
        dpre = (dxd * dtx + skip * dy) * dsilu
        ext = jnp.concatenate([dpre, nxt[...]], axis=0)
        nxt[...] = dpre[:8]
        du = taps[3:4] * dpre
        acc[0:8, :] += eight(dmr * g)
        acc[8:16, :] += eight(dy * x)
        acc[16:24, :] += eight(dpre)
        acc[24:32, :] += eight(dpre * u)
        mrows = m_ref[pl.ds(t0, L + 8), :]
        for k in range(1, 4):
            sk = pltpu.roll(ext * mrows[:, k : k + 1], L + 8 - k, 0)[:L]
            du = du + taps[3 - k : 4 - k] * sk
            acc[24 + 8 * k : 32 + 8 * k, :] += eight(sk * u)
        dz_ref[1, here, :] = du.astype(bf16)
        return carry

    lax.fori_loop(0, nc, chunk, 0)
    for j in range(7):
        small_ref[j : j + 1, :] = jnp.sum(acc[8 * j : 8 * j + 8, :], axis=0, keepdims=True)
    small_ref[7:8, :] = jnp.zeros((1, W), f32)

    def weights(i, carry):
        tick(nc + i)
        rows = pl.ds(pl.multiple_of(i * MB, MB), MB)
        for kind in range(2):
            gw_ref[kind, rows, :] = dot(normt_ref[rows, :], dz_ref[kind]).astype(bf16)
        return carry

    lax.fori_loop(0, normt_ref.shape[0] // MB, weights, 0)


def bwd(half, halves, u, gate, pre, dm, rq, taps, masks, b, c, ct, gm, cum, cumr, sc, st, normt, comm):
    T, E = gate.shape
    N = b.shape[1]
    G = cumr.shape[0]
    W = E // G
    nc = T // L
    Gh = G // halves
    Eh = E // halves
    g0 = half * Gh
    S = jax.ShapeDtypeStruct
    col = pl.BlockSpec((T, W), lambda g: (0, g + g0))
    full = lambda a: pl.BlockSpec(a.shape, lambda g: (0,) * a.ndim)
    whole = lambda s: pl.BlockSpec(s, lambda g: (0,) * len(s))
    grp = lambda a: pl.BlockSpec((1,) + a.shape[1:], lambda g: (g + g0, 0, 0))
    in_specs = [col, col, col, col, full(rq), pl.BlockSpec((8, W), lambda g: (0, g + g0)), full(masks), full(b), full(c),
                full(ct), full(gm), full(cum), grp(cumr), full(sc), pl.BlockSpec((nc, N, W), lambda g: (0, 0, g + g0)), full(normt)]
    D = normt.shape[0]
    out_specs = [pl.BlockSpec((2, T, W), lambda g: (0, 0, g)), pl.BlockSpec((2, D, W), lambda g: (0, 0, g)), whole((nc, L, L)), whole((T, N)), whole((T, N)),
                 whole((T, 128)), pl.BlockSpec((8, W), lambda g: (0, g)), pl.BlockSpec((nc, W), lambda g: (0, g))]
    out_shape = [S((2, T, Eh), bf16), S((2, D, Eh), bf16), S((nc, L, L), f32), S((T, N), f32), S((T, N), f32), S((T, 128), f32), S((8, Eh), f32), S((nc, Eh), f32)]
    scratch = [pltpu.VMEM((N, W), f32), pltpu.VMEM((8, W), f32), pltpu.VMEM((56, W), f32)]
    nd, nf, cid, first, split = comm
    rows = first[0].shape[-2]
    return pl.pallas_call(
        functools.partial(bwd_scatter_kernel, nd, nf, g0, Gh, nc, len(first), split),
        grid=(Gh,),
        in_specs=[pl.BlockSpec(memory_space=pl.ANY)] * len(first) + in_specs,
        out_specs=out_specs + [whole((rows, w)) for w in widths(split)],
        out_shape=out_shape + [S((rows, w), f32) for w in widths(split)],
        scratch_shapes=scratch + pipes_scratch(nd, rows, split),
        compiler_params=pltpu.CompilerParams(vmem_limit_bytes=60 << 20, collective_id=cid, has_side_effects=True),
        cost_estimate=pl.CostEstimate(flops=T * Eh * (8 * L + 12 * N + 4 * D), bytes_accessed=T * Eh * 16, transcendentals=T * Eh * 4),
    )(*first, u, gate, pre, dm, rq, taps, masks, b, c, ct, gm, cum, cumr, sc, st, normt)


def post_kernel(bcdt_ref, pre_ref, taps_ref, heads_ref, m_ref, segc_ref, segr_ref, b_ref, c_ref, dg0_ref, db0_ref, dc0_ref, rs0_ref, dg1_ref, db1_ref, dc1_ref, rs1_ref, kk_ref, dt_ref,
                out_ref, small_ref, hs_ref, nxt, acc, hacc):
    T = bcdt_ref.shape[0]
    nc = T // L
    N = b_ref.shape[1]
    H = dt_ref.shape[1]
    taps = taps_ref[...]
    tri = (lax.broadcasted_iota(jnp.int32, (L, L), 0) >= lax.broadcasted_iota(jnp.int32, (L, L), 1))
    upper = (lax.broadcasted_iota(jnp.int32, (L, L), 0) <= lax.broadcasted_iota(jnp.int32, (L, L), 1)).astype(f32)
    strict = 1.0 - upper
    rate = -jnp.exp(heads_ref[0:1, :H])
    bias = heads_ref[1:2, :H]
    nxt[...] = jnp.zeros_like(nxt)
    acc[...] = jnp.zeros_like(acc)
    hacc[...] = jnp.zeros_like(hacc)

    def eight(z):
        return jnp.sum(z.reshape(L // 8, 8, z.shape[1]), axis=0)

    def chunk(i, carry):
        c = nc - 1 - i
        t0 = pl.multiple_of(c * L, L)
        here = pl.ds(t0, L)
        same = segc_ref[here, :] == segr_ref[:, here]
        dg = jnp.where(tri & same, dg0_ref[c] + dg1_ref[c], 0.0)
        dgb = dg.astype(bf16)
        dcv = dc0_ref[here, :] + dc1_ref[here, :] + dot(dgb, b_ref[here, :])
        dbv = db0_ref[here, :] + db1_ref[here, :] + dot(dg.T.astype(bf16), c_ref[here, :])
        pre = pre_ref[here, :]
        sig = sigmoid(pre)
        dpre = jnp.concatenate([dbv, dcv], axis=1) * (sig + pre * sig * (1.0 - sig))
        v = bcdt_ref[here, : 2 * N].astype(f32)
        ext = jnp.concatenate([dpre, nxt[...]], axis=0)
        nxt[...] = dpre[:8]
        dv = taps[3:4] * dpre
        acc[0:8, :] += eight(dpre)
        acc[8:16, :] += eight(dpre * v)
        mrows = m_ref[pl.ds(t0, L + 8), :]
        for k in range(1, 4):
            sk = pltpu.roll(ext * mrows[:, k : k + 1], L + 8 - k, 0)[:L]
            dv = dv + taps[3 - k : 4 - k] * sk
            acc[8 + 8 * k : 16 + 8 * k, :] += eight(sk * v)
        out_ref[here, : 2 * N] = dv.astype(bf16)
        q = H // 2
        r0, r1 = rs0_ref[here, :], rs1_ref[here, :]
        r1, r2, r3 = (jnp.concatenate([r0[:, m * q : (m + 1) * q], r1[:, m * q : (m + 1) * q]], axis=1) for m in range(3))
        da = dot(upper, r1, precision=HIGHEST) + dot(strict, r2, precision=HIGHEST) + kk_ref[pl.ds(c, 1), :]
        dt = dt_ref[here, :]
        raw = bcdt_ref[here, 2 * N : 2 * N + 128].astype(f32)[:, :H] + bias
        ddt = (r3 + da * rate) * sigmoid(raw)
        hacc[0:8, :] += eight(da * rate * dt)
        hacc[8:16, :] += eight(ddt)
        out_ref[here, 2 * N :] = jnp.concatenate([ddt, jnp.zeros((L, out_ref.shape[1] - 2 * N - H), f32)], axis=1).astype(bf16)
        return carry

    lax.fori_loop(0, nc, chunk, 0)
    for j in range(5):
        small_ref[j : j + 1, :] = jnp.sum(acc[8 * j : 8 * j + 8, :], axis=0, keepdims=True)
    small_ref[5:8, :] = jnp.zeros((3, 2 * N), f32)
    for j in range(2):
        hs_ref[j : j + 1, :] = jnp.sum(hacc[8 * j : 8 * j + 8, :], axis=0, keepdims=True)


def post(bcdt, pre, taps, heads, masks, segc, segr, b, c, first, second, kk, dt):
    T = bcdt.shape[0]
    N = b.shape[1]
    H = dt.shape[1]
    S = jax.ShapeDtypeStruct
    wide = 2 * N + 128
    full = lambda a: pl.BlockSpec(a.shape, lambda i: (0,) * a.ndim)
    ins = (bcdt, pre, taps, heads, masks, segc, segr, b, c, *first, *second, kk, dt)
    outs = (S((T, wide), bf16), S((8, 2 * N), f32), S((2, H), f32))
    return pl.pallas_call(
        post_kernel,
        grid=(1,),
        in_specs=[pl.BlockSpec((T, wide), lambda i: (0, bcdt.shape[1] // wide - 1))] + [full(a) for a in ins[1:]],
        out_specs=[full(o) for o in outs],
        out_shape=outs,
        scratch_shapes=[pltpu.VMEM((8, 2 * N), f32), pltpu.VMEM((40, 2 * N), f32), pltpu.VMEM((16, H), f32)],
        compiler_params=pltpu.CompilerParams(vmem_limit_bytes=60 << 20),
    )(*ins)


NT = 256


def tail_kernel(nd, nf, arrays, split, tiles, *refs):
    g_refs, refs = refs[:arrays], refs[arrays:]
    (wo_hbm, wg_hbm, wa_hbm, gg_ref, dz0_ref, dz1_ref, dbc_ref, hid_ref, go_ref, r_ref, gain_ref, mine_ref,
     suma_ref, sumb_ref, out_ref, gin_ref, small_ref, dnorm_ref) = refs[:18]
    refs = refs[1:]
    wo, wg, wa, acc, dn, flat, sem = refs[17:24]
    mine = Spread(nd, nf, mine_ref, *refs[24:27])
    norm = Spread(nd, nf, flat, *refs[27:30])
    pipes = pipes_of(nd, nf, g_refs, (suma_ref, sumb_ref), split, refs[30:])
    D, E = wg.shape
    Eh = E // 2
    step = pl.program_id(0)
    early = tiles // 2
    blocks = D // NT
    mid = (early + tiles) * blocks
    scale = 4 / tiles
    time_of = [4 + 0.75 * scale * t if t < early * blocks else
               (13 + 1.65 * scale * (t - early * blocks) if t < mid else 52.6 + 0.65 * scale * (t - mid)) for t in range(2 * tiles * blocks)]
    ticks = plan(pipes, mine, time_of, TAIL_SPOTS)
    last = len(time_of) - 1
    ticks[1].append(mine.begin)
    ticks.setdefault((early + tiles) * blocks + 2, []).append(norm.begin)
    fetch = [pltpu.make_async_copy(src, dst, sem.at[k]) for k, (src, dst) in enumerate(((wo_hbm, wo), (wg_hbm, wg), (wa_hbm, wa)))]

    @pl.when(step == 0)
    def _():
        for cp in fetch:
            cp.start()
        dn[...] = jnp.zeros_like(dn)
        run_ticks(ticks, 0, 0)
        fetch[0].wait()

    @pl.when(step == early)
    def _():
        fetch[1].wait()
        fetch[2].wait()

    back = (step >= early) & (step < early + tiles)
    in_back = lambda t: early * blocks <= t < (early + tiles) * blocks

    @pl.when(jnp.logical_not(back))
    def _():
        def block(j, carry):
            run_ticks({t: f for t, f in ticks.items() if t and not in_back(t)}, step * blocks + j, last)
            cols = pl.ds(pl.multiple_of(j * NT, NT), NT)
            out_ref[:, cols] = (hid_ref[:, cols].astype(f32) + r_ref[...] * dot(gg_ref[...], wo[:, cols])).astype(bf16)
            return carry
        lax.fori_loop(0, blocks, block, 0)

    @pl.when(back)
    def _():
        def block(j, carry):
            run_ticks({t: f for t, f in ticks.items() if in_back(t)}, step * blocks + j, last)
            cols = pl.ds(pl.multiple_of(j * NT, NT), NT)
            part = dot(dz0_ref[0], wg[cols, :Eh], ((1,), (1,))) + dot(dz1_ref[0], wg[cols, Eh:], ((1,), (1,)))
            part = part + dot(dz0_ref[1], wa[cols, :Eh], ((1,), (1,))) + dot(dz1_ref[1], wa[cols, Eh:E], ((1,), (1,)))
            acc[:, cols] = part + dot(dbc_ref[...], wa[cols, E:], ((1,), (1,)))
            return carry
        lax.fori_loop(0, blocks, block, 0)
        gain = gain_ref[...]

        def rows_of(i, carry):
            here = pl.ds(pl.multiple_of(i * 64, 64), 64)
            rows = hid_ref[here, :].astype(f32)
            rinv = lax.rsqrt(jnp.mean(rows * rows, axis=-1, keepdims=True) + EPS)
            xhat = rows * rinv
            bn = acc[here, :]
            prod = bn * xhat
            dn[...] += jnp.sum(prod.reshape(8, 8, D), axis=0)
            mean = jnp.mean(prod * gain, axis=-1, keepdims=True)
            gin_ref[here, :] = (go_ref[here, :].astype(f32) + rinv * (bn * gain - xhat * mean)).astype(bf16)
            return carry
        lax.fori_loop(0, hid_ref.shape[0] // 64, rows_of, 0)

    @pl.when(step == early + tiles - 1)
    def _():
        flat[...] = jnp.zeros_like(flat)
        for j in range(D // 128):
            flat[j : j + 1, :] = jnp.sum(dn[:, 128 * j : 128 * (j + 1)], axis=0, keepdims=True)

    @pl.when(step == 2 * tiles - 1)
    def _():
        run_rest(ticks, last)
        for p in pipes:
            p.finish()
        small_ref[...] = mine.total()
        dnorm_ref[...] = norm.total()


def tail(nd, nf, cid, gs, split, dz0, dz1, dbcdt, full_gate, full_a, gg, full_out, hidden, grad_out, r, norm_gain, mine):
    T, D = hidden.shape
    E = full_out.shape[0]
    n = nd * nf
    rows = gs[0].shape[-2]
    MT = 256 if rows % 16 == 0 else 128
    tiles = T // MT
    early = tiles // 2
    wide = dbcdt.shape[1]
    S = jax.ShapeDtypeStruct
    any_ = pl.BlockSpec(memory_space=pl.ANY)
    whole = lambda s: pl.BlockSpec(s, lambda k: (0,) * len(s), pipeline_mode=pl.Buffered(1))
    at_out = lambda k: jnp.minimum(k, early - 1) + jnp.clip(k - tiles - early + 1, 0, tiles - early)
    at_back = lambda k: jnp.clip(k - early, 0, tiles - 1)
    at_row = lambda k: k - early * jnp.clip(k - early + 1, 0, 1) - (tiles - early) * jnp.clip(k - early - tiles + 1, 0, 1)
    out_tile = lambda w: pl.BlockSpec((MT, w), lambda k: (at_out(k), 0))
    back_tile = lambda w: pl.BlockSpec((MT, w), lambda k: (at_back(k), 0))
    half = pl.BlockSpec((2, MT, E // 2), lambda k: (0, at_back(k), 0))
    tile, ntile = mine.shape[1:], (-(-D // 1024) * 8, 128)
    return pl.pallas_call(
        functools.partial(tail_kernel, nd, nf, len(gs), split, tiles),
        grid=(2 * tiles,),
        in_specs=[any_] * (len(gs) + 3) + [out_tile(E), half, half, back_tile(wide), pl.BlockSpec((MT, D), lambda k: (at_row(k), 0)), back_tile(D),
                                           out_tile(1), whole((1, D)), whole(mine.shape)],
        out_specs=[whole((rows, w)) for w in widths(split)] + [out_tile(D), back_tile(D), whole(tile), whole(ntile)],
        out_shape=[S((rows, w), f32) for w in widths(split)] + [S((T, D), bf16), S((T, D), bf16), S(tile, f32), S(ntile, f32)],
        scratch_shapes=[pltpu.VMEM((E, D), bf16), pltpu.VMEM((D, E), bf16), pltpu.VMEM((D, E + wide), bf16), pltpu.VMEM((MT, D), f32),
                        pltpu.VMEM((8, D), f32), pltpu.VMEM(ntile, f32), pltpu.SemaphoreType.DMA((3,))]
        + Spread.scratch(n, tile) + Spread.scratch(n, ntile) + pipes_scratch(nd, rows, split),
        compiler_params=pltpu.CompilerParams(collective_id=cid, has_side_effects=True, vmem_limit_bytes=67043328),
        cost_estimate=pl.CostEstimate(flops=2 * T * D * 3 * E, bytes_accessed=8 * D * E, transcendentals=0),
    )(*gs, full_out, full_gate, full_a, gg, dz0, dz1, dbcdt, hidden, grad_out, r, norm_gain, mine)


def finish_kernel(nd, nf, gate0_ref, gate1_ref, u0_ref, u1_ref, oa_ref, ob_ref, tot_ref, norm_ref, o_ref, gi_ref,
                  oo_ref, go_ref, zx_ref, bc_ref, dt_ref, out_ref, conv_ref, n_ref, gg_ref, heads_ref):
    oo_ref[...] = o_ref[...]
    go_ref[...] = gi_ref[...]

    @pl.when(pl.program_id(0) == 0)
    def _():
        Eh = gate0_ref.shape[1]
        for k, ref in enumerate((gate0_ref, gate1_ref, u0_ref)):
            zx_ref[:, k * Eh : (k + 1) * Eh] = ref[...]
        zx_ref[:, 3 * Eh :] = u1_ref[:, :Eh]
        wide = bc_ref.shape[1]
        bc_ref[...] = u1_ref[:, Eh : Eh + wide]
        dt_ref[...] = u1_ref[:, Eh + wide : Eh + wide + 128][:, : dt_ref.shape[1]]
        half = oa_ref.shape[1]
        out_ref[:, :half] = oa_ref[...]
        out_ref[:, half:] = ob_ref[...]
        k1 = conv_ref.shape[0]
        conv_ref[...] = tot_ref[:k1, : conv_ref.shape[1]]
        gg_ref[...] = tot_ref[k1 : k1 + 1, : gg_ref.shape[1]]
        heads_ref[...] = tot_ref[k1 + 1 : k1 + 1 + heads_ref.shape[0], : heads_ref.shape[1]]
        me = lax.axis_index("dp") * nf + lax.axis_index("fsdp")
        nrow = n_ref.shape[1]
        D = nrow * nd * nf
        row = jnp.concatenate([norm_ref[j : j + 1, :] for j in range(D // 128)], axis=1)
        row = pltpu.roll(jnp.broadcast_to(row, (8, D)), lax.rem(D - me * nrow, D), 1)
        n_ref[...] = row[:1, :nrow]


def finish(nd, nf, gate0, gate1, u0, u1, s_out, tot, d_norm, output, grad_in, shapes):
    S = jax.ShapeDtypeStruct
    tile = pl.BlockSpec((256, output.shape[1]), lambda i: (i, 0))
    return pl.pallas_call(
        functools.partial(finish_kernel, nd, nf),
        grid=(output.shape[0] // 256,),
        in_specs=[pl.BlockSpec(a.shape, lambda i: (0, 0)) for a in (gate0, gate1, u0, u1, *s_out, tot, d_norm)] + [tile, tile],
        out_specs=[tile, tile] + [pl.BlockSpec(s, lambda i: (0, 0)) for s in shapes],
        out_shape=[S(output.shape, bf16), S(output.shape, bf16)] + [S(s, f32) for s in shapes],
        compiler_params=pltpu.CompilerParams(vmem_limit_bytes=63 << 20),
    )(gate0, gate1, u0, u1, *s_out, tot, d_norm, output, grad_in)


def norm_kernel(hid_ref, gain_ref, normed_ref, normt_ref):
    rows = hid_ref[...].astype(f32)
    normed = rows * lax.rsqrt(jnp.mean(rows * rows, axis=-1, keepdims=True) + EPS) * gain_ref[...]
    normed_ref[...] = normed.astype(bf16)
    normt_ref[...] = normed.T.astype(bf16)


def norm(hidden, gain):
    T, D = hidden.shape
    S = jax.ShapeDtypeStruct
    row = pl.BlockSpec((256, D), lambda i: (i, 0))
    return pl.pallas_call(
        norm_kernel,
        grid=(T // 256,),
        in_specs=[row, pl.BlockSpec((1, D), lambda i: (0, 0))],
        out_specs=[row, pl.BlockSpec((D, 256), lambda i: (0, i))],
        out_shape=(S((T, D), bf16), S((D, T), bf16)),
        compiler_params=pltpu.CompilerParams(vmem_limit_bytes=40 << 20),
    )(hidden, gain)


def layer(nd, nf, hidden, grad_out, seg, shard_a, shard_gate, shard_out, head_params, sizes):
    n = nd * nf
    E, N, H, K1, S = sizes
    T, D = hidden.shape
    wide = 2 * N + 128
    full_gate = lax.all_gather(shard_gate, AXES, axis=0, tiled=True)
    full_out = lax.all_gather(shard_out, AXES, axis=0, tiled=True)
    full_a = gather_rows(shard_a, nd, nf, 0)
    off = E + 2 * N + H
    flat = full_a[:, :, off : off + S].reshape(n, -1)
    ncol, nrow, ngate = (E + 2 * N) // n, D // n, E // n
    conv = flat[:, : K1 * ncol].reshape(n, K1, ncol).transpose(1, 0, 2).reshape(K1, n * ncol).astype(f32)
    norm_gain = flat[:, K1 * ncol : K1 * ncol + nrow].reshape(-1).astype(f32)
    gate_gain = flat[:, K1 * ncol + nrow : K1 * ncol + nrow + ngate].reshape(-1).astype(f32)
    full_a = full_a.reshape(D, E + wide)
    normed, normt = norm(hidden, norm_gain[None])
    ubc = dot(normed, full_a).astype(bf16)
    gate = dot(normed, full_gate).astype(bf16)
    segc, segr = seg[:, None], seg[None, :]
    taps_u = jnp.concatenate([conv[:, :E], gate_gain[None], jnp.repeat(head_params[2], E // H)[None], jnp.zeros((1, E), f32)], axis=0)
    taps_bc = jnp.concatenate([conv[:, E:], jnp.zeros((3, 2 * N), f32)], axis=0)
    masks, b, c, bt, ct, pre_bc, gm, cum, cumr, sc, dt = prep(ubc, taps_bc, head_params, segc, segr, N, H)
    gg, r, pre, st = fwd(ubc, gate, taps_u, masks, b, c, bt, gm, cum, cumr, sc)
    gos = (grad_out.astype(f32) * r).astype(bf16)
    g_out = dot(gg, gos, ((0,), (0,))).astype(bf16)
    dm = dot(grad_out, full_out, ((1,), (1,))).astype(bf16)
    s = jnp.sum(gg.astype(f32) * dm.astype(f32), axis=1, keepdims=True)
    rq = jnp.concatenate([r, r * r * r * s / E], axis=1)
    back = functools.partial(bwd, u=ubc, gate=gate, pre=pre, dm=dm, rq=rq, taps=taps_u, masks=masks, b=b, c=c, ct=ct, gm=gm, cum=cum,
                             cumr=cumr, sc=sc, st=st, normt=normt)
    zn = max(nd // 2, 1)
    rows_of = lambda g: g.reshape(g.shape[:-2] + (zn, n // zn, g.shape[-2] // n, g.shape[-1]))
    Eh = E // 2
    dz0, gw0, dg0, db0, dc0, rs0, small0, kk0, *s_out = back(
        0, 2, comm=(nd, nf, 4, (rows_of(g_out),), (((0, None, 0, D // 2),), ((0, None, D // 2, D // 2),))))
    dz1, gw1, dg1, db1, dc1, rs1, small1, kk1, gate0, u0 = back(1, 2, comm=(nd, nf, 3, (rows_of(gw0),), (((0, 0, 0, Eh),), ((0, 1, 0, Eh),))))
    small = jnp.concatenate([small0, small1], axis=1)
    kk = jnp.concatenate([kk0, kk1], axis=1)
    kkh = jnp.sum(kk.reshape(kk.shape[0], H, E // H), axis=2)
    dbcdt, small_bc, hs = post(ubc, pre_bc, taps_bc, head_params, masks, segc, segr, b, c, (dg0, db0, dc0, rs0), (dg1, db1, dc1, rs1), kkh, dt)
    d_conv = jnp.concatenate([jnp.stack([small[6], small[5], small[4], small[3], small[2]]),
                              jnp.stack([small_bc[4], small_bc[3], small_bc[2], small_bc[1], small_bc[0]])], axis=1)
    d_heads = jnp.concatenate([hs, jnp.sum(small[1].reshape(1, H, E // H), axis=2)], axis=0)
    lanes = -(-max(ncol, ngate, H) // 128) * 128
    cols = lambda a: jnp.pad(a.reshape(-1, n, a.shape[1] // n).transpose(1, 0, 2), ((0, 0), (0, 0), (0, lanes - a.shape[1] // n)))
    heads_row = jnp.broadcast_to(jnp.pad(d_heads, ((0, 0), (0, lanes - H)))[None], (n, d_heads.shape[0], lanes))
    used = K1 + 1 + d_heads.shape[0]
    mine = jnp.concatenate([cols(d_conv), cols(small[:1]), heads_row, jnp.zeros((n, -(-used // 8) * 8 - used, lanes), f32)], axis=1)
    g_bcdt = dot(normt, dbcdt).astype(bf16)
    split = (((0, 0, 0, Eh),), ((0, 1, 0, Eh), (1, None, 0, wide)))
    gate1, u1, output, grad_in, tot, d_norm = tail(nd, nf, 1, (rows_of(gw1), rows_of(g_bcdt)), split, dz0, dz1, dbcdt, full_gate, full_a, gg,
                                                   full_out, hidden, grad_out, r, norm_gain[None], mine)
    output, grad_in, s_zx, s_bc, s_dt, s_w, t_conv, t_norm, t_gate, t_heads = finish(
        nd, nf, gate0, gate1, u0, u1, s_out, tot, d_norm, output, grad_in,
        ((nrow, 2 * E), (nrow, 2 * N), (nrow, H), (E // n, D), (K1, ncol), (1, nrow), (1, ngate), d_heads.shape))
    return output, grad_in, s_zx, s_bc, s_dt, s_w, t_conv, t_norm.reshape(-1), t_gate.reshape(-1), t_heads


def per_device(nd, nf, hidden, grad_out, segment_ids, w_zx, w_bc, w_dt, w_out, conv_params, norm_gain, gate_gain, head_params):
    n = nd * nf
    E, N2, H = w_out.shape[0] * n, w_bc.shape[1], w_dt.shape[1]
    rows = w_zx.shape[0]
    small = jnp.concatenate([conv_params.reshape(-1), norm_gain, gate_gain])
    S = -(-small.shape[0] // rows)
    assert S + H <= 128
    small = jnp.pad(small, (0, S * rows - small.shape[0])).reshape(rows, S)
    shard_a = jnp.concatenate([w_zx[:, E:], w_bc, w_dt, small, jnp.zeros((rows, 128 - H - S), bf16)], axis=1)
    return layer(nd, nf, hidden, grad_out, segment_ids, shard_a, w_zx[:, :E], w_out, head_params, (E, N2 // 2, H, conv_params.shape[0], S))


def solution(mesh):
    row, col, vec, rep = P(AXES, None), P(None, AXES), P(AXES), P()
    return jax.shard_map(
        functools.partial(per_device, mesh.shape["dp"], mesh.shape["fsdp"]),
        mesh=mesh,
        in_specs=(row, row, vec, row, row, row, row, col, vec, vec, rep),
        out_specs=(row, row, row, row, row, row, col, vec, vec, rep),
        check_vma=False,
    )
```

```python
import functools
import jax
import jax.numpy as jnp
from jax import lax
from jax.experimental import pallas as pl
from jax.experimental.pallas import tpu as pltpu
from jax.sharding import PartitionSpec as P

EPS = 1e-05
L = 128
HG = 8
LOG2E = 1.4426950408889634
MB = 512
BWD_SPOTS = ((5.0, 10.0, 2.0, 26.0, 3.2), (7.0, 16.5, 2.0, 39.0, 3.2))
TAIL_SPOTS = ((7.0, 13.0, 3.0, 30.0, 4.0), (9.0, 22.0, 3.0, 46.0, 3.0))
bf16, f32 = jnp.bfloat16, jnp.float32
HIGHEST = lax.Precision.HIGHEST


AXES = ("dp", "fsdp")
MESH = pl.DeviceIdType.MESH


class Place:
    def __init__(self, nd, nf):
        self.zn, self.nf = nd // 2, nf
        d, f = lax.axis_index("dp"), lax.axis_index("fsdp")
        self.z, self.y = d // 2, d % 2
        self.x, self.c = f // 2, f % 2

    def dev(self, z, y, x, c):
        return (z * 2 + y, x * 2 + c)

    def idx(self, z, y, x, c):
        return (z * 2 + y) * self.nf + x * 2 + c

    def meet(self):
        z, zn = self.z, self.zn
        pl.semaphore_wait(pltpu.get_barrier_semaphore(), 3 + (z + zn - 1) // zn + (2 * zn - 2 - z) // zn)

    def greet(self):
        z, y, x, c, zn = self.z, self.y, self.x, self.c, self.zn
        sem = pltpu.get_barrier_semaphore()
        for there in ((z, y, 1 - x, c), (z, 1 - y, x, c), (z, y, x, 1 - c)):
            pl.semaphore_signal(sem, inc=1, device_id=self.dev(*there), device_id_type=MESH)

        @pl.when(z > 0)
        def _():
            pl.semaphore_signal(sem, inc=1, device_id=self.dev(z - 1, y, x, c), device_id_type=MESH)

        @pl.when(z < zn - 1)
        def _():
            pl.semaphore_signal(sem, inc=1, device_id=self.dev(z + 1, y, x, c), device_id_type=MESH)


def gather_kernel(nd, nf, src_ref, out_ref, own_sem, z_send, z_recv, x_send, x_recv, y_send, y_recv, dx_send, dx_recv, dy_send, dy_recv, c_send, c_recv):
    at = Place(nd, nf)
    z, y, x, c, zn = at.z, at.y, at.x, at.c, at.zn
    half = out_ref.shape[2] // 256 * 128
    lo, hi = pl.ds(0, half), pl.ds(half, out_ref.shape[2] - half)
    at.greet()
    at.meet()

    def copy(block, to, send, recv, cols=None, src=None):
        ref = out_ref.at[block] if cols is None else out_ref.at[block, :, cols]
        return pltpu.make_async_remote_copy(src_ref=ref if src is None else src, dst_ref=ref, send_sem=send, recv_sem=recv,
                                            device_id=at.dev(*to), device_id_type=MESH)

    def block(zs, col):
        return at.idx(zs, 1 - y if col & 2 else y, 1 - x if col & 1 else x, c)

    def up(zs, src=None):
        return copy(block(zs, 0), (z + 1, y, x, c), z_send.at[0, zs], z_recv.at[zs], src=src)

    def down(zs, src=None):
        return copy(block(zs, 0), (z - 1, y, x, c), z_send.at[1, zs], z_recv.at[zs], src=src)

    def to_x(zs, src=None):
        return copy(block(zs, 0), (z, y, 1 - x, c), x_send.at[zs], x_recv.at[zs], src=src)

    def to_y(zs, src=None):
        return copy(block(zs, 0), (z, 1 - y, x, c), y_send.at[zs], y_recv.at[zs], src=src)

    def diag_y(zs):
        return copy(block(zs, 1), (z, 1 - y, x, c), dy_send.at[zs], dy_recv.at[zs], lo)

    def diag_x(zs):
        return copy(block(zs, 2), (z, y, 1 - x, c), dx_send.at[zs], dx_recv.at[zs], hi)

    def to_core(zs, col, src=None):
        return copy(block(zs, col), (z, y, x, 1 - c), c_send.at[zs, col], c_recv.at[zs, col], src=src)

    own = pltpu.make_async_copy(src_ref, out_ref.at[block(z, 0)], own_sem)
    own.start()

    @pl.when(z < zn - 1)
    def _():
        up(z, src_ref).start()

    @pl.when(z > 0)
    def _():
        down(z, src_ref).start()

    to_x(z, src_ref).start()
    to_y(z, src_ref).start()
    to_core(z, 0, src_ref).start()

    def each(dist, fn):
        if dist == 0:
            fn(z, 0)
            return

        @pl.when(z - dist >= 0)
        def _():
            fn(z - dist, 1)

        @pl.when(z + dist < zn)
        def _():
            fn(z + dist, -1)

    def from_z(zs, way):
        copy(block(zs, 0), (z, y, x, c), z_send.at[0, zs], z_recv.at[zs]).wait_recv()
        if way > 0:
            @pl.when(z < zn - 1)
            def _():
                up(zs).start()
        else:
            @pl.when(z > 0)
            def _():
                down(zs).start()
        to_x(zs).start()
        to_y(zs).start()
        to_core(zs, 0).start()

    def from_xy(zs, way):
        to_x(zs).wait_recv()
        diag_y(zs).start()
        to_core(zs, 1).start()
        to_y(zs).wait_recv()
        diag_x(zs).start()
        to_core(zs, 2).start()

    def from_diag(zs, way):
        diag_y(zs).wait_recv()
        diag_x(zs).wait_recv()
        to_core(zs, 3).start()

    for dist in range(zn):
        if dist:
            each(dist, from_z)
        each(dist, from_xy)
    for dist in range(zn):
        each(dist, from_diag)
    own.wait()

    def sent(zs, way):
        for col in range(4):
            to_core(zs, col).wait_recv()
            to_core(zs, col).wait_send()
        to_x(zs).wait_send()
        to_y(zs).wait_send()
        diag_x(zs).wait_send()
        diag_y(zs).wait_send()
        if way >= 0:
            @pl.when(z < zn - 1)
            def _():
                up(zs).wait_send()
        if way <= 0:
            @pl.when(z > 0)
            def _():
                down(zs).wait_send()

    for dist in range(zn):
        each(dist, sent)


def gather_rows(shard, nd, nf, cid):
    zn = nd // 2
    D = pltpu.SemaphoreType.DMA
    return pl.pallas_call(
        functools.partial(gather_kernel, nd, nf),
        out_shape=jax.ShapeDtypeStruct((nd * nf,) + shard.shape, shard.dtype),
        in_specs=[pl.BlockSpec(memory_space=pl.ANY)],
        out_specs=pl.BlockSpec(memory_space=pl.ANY),
        scratch_shapes=[D(()), D((2, zn)), D((zn,)), D((zn,)), D((zn,)), D((zn,)), D((zn,)), D((zn,)), D((zn,)), D((zn,)), D((zn,)),
                        D((zn, 4)), D((zn, 4))],
        compiler_params=pltpu.CompilerParams(collective_id=cid, has_side_effects=True),
    )(shard)


class Scatter:
    def __init__(self, nd, nf, g_refs, out_ref, acc, c_in, d_in, xy_in, z_in,
                 load_sem, c_send, c_recv, dx_send, dx_recv, dy_send, dy_recv, x_send, x_recv, y_send, y_recv, z_send, z_recv):
        at = Place(nd, nf)
        z, y, x, c, zn = at.z, at.y, at.x, at.c, at.zn
        cols = out_ref.shape[1]
        wids = [r.shape[3] for r in g_refs]
        offs = [sum(wids[:k]) for k in range(len(wids))]
        half = cols // 256 * 128
        lo, hi = pl.ds(0, half), pl.ds(half, cols - half)

        def inner(col, core):
            return at.idx(0, 1 - y if col & 2 else y, 1 - x if col & 1 else x, core)

        def remote(src, dst, to, send, recv):
            return pltpu.make_async_remote_copy(src_ref=src, dst_ref=dst, send_sem=send, recv_sem=recv, device_id=at.dev(*to), device_id_type=MESH)

        def load(col):
            return [pltpu.make_async_copy(r.at[:, inner(col, c)], acc.at[col, :, :, pl.ds(o, w)], load_sem.at[col, k])
                    for k, (r, o, w) in enumerate(zip(g_refs, offs, wids))]

        def core(col):
            return [remote(r.at[:, inner(col, 1 - c)], c_in.at[col, :, :, pl.ds(o, w)], (z, y, x, 1 - c), c_send.at[col, k], c_recv.at[col, k])
                    for k, (r, o, w) in enumerate(zip(g_refs, offs, wids))]

        def diag_x(zs):
            return remote(acc.at[3, zs, :, lo], d_in.at[zs, :, lo], (z, y, 1 - x, c), dx_send.at[zs], dx_recv.at[zs])

        def diag_y(zs):
            return remote(acc.at[3, zs, :, hi], d_in.at[zs, :, hi], (z, 1 - y, x, c), dy_send.at[zs], dy_recv.at[zs])

        def to_x(zs):
            return remote(acc.at[1, zs], xy_in.at[0, zs], (z, y, 1 - x, c), x_send.at[zs], x_recv.at[zs])

        def to_y(zs):
            return remote(acc.at[2, zs], xy_in.at[1, zs], (z, 1 - y, x, c), y_send.at[zs], y_recv.at[zs])

        def up(zs):
            return remote(acc.at[0, zs], z_in.at[zs + 1], (z + 1, y, x, c), z_send.at[zs], z_recv.at[0, zs])

        def down(zs):
            return remote(acc.at[0, zs], z_in.at[zs], (z - 1, y, x, c), z_send.at[zs], z_recv.at[1, zs])

        def each(dist, fn):
            if dist == 0:
                fn(z)
                return

            @pl.when(z - dist >= 0)
            def _():
                fn(z - dist)

            @pl.when(z + dist < zn)
            def _():
                fn(z + dist)

        order = list(range(zn - 1, -1, -1))

        def start(col):
            for cp in core(col) + load(col):
                cp.start()

        def ready(col):
            for cp in load(col):
                cp.wait()
            for cp in core(col):
                cp.wait_recv()

        def diag(zs):
            acc[3, zs] = acc[3, zs] + c_in[3, zs]
            diag_x(zs).start()
            diag_y(zs).start()

        def sides(zs):
            diag_y(zs).wait_recv()
            acc[1, zs, :, lo] = acc[1, zs, :, lo] + c_in[1, zs, :, lo]
            acc[1, zs, :, hi] = acc[1, zs, :, hi] + c_in[1, zs, :, hi] + d_in[zs, :, hi]
            to_x(zs).start()
            diag_x(zs).wait_recv()
            acc[2, zs, :, lo] = acc[2, zs, :, lo] + c_in[2, zs, :, lo] + d_in[zs, :, lo]
            acc[2, zs, :, hi] = acc[2, zs, :, hi] + c_in[2, zs, :, hi]
            to_y(zs).start()

        def column(zs):
            to_x(zs).wait_recv()
            to_y(zs).wait_recv()
            return (acc[0, zs] + c_in[0, zs]).astype(f32) + (xy_in[0, zs] + xy_in[1, zs]).astype(f32)

        def pass_on(zs):
            total = column(zs)

            @pl.when(zs > z)
            def _():
                @pl.when(z > 0)
                def _():
                    up(zs).wait_recv()
                    acc[0, zs] = (total + z_in[zs + 1].astype(f32)).astype(bf16)

                @pl.when(z == 0)
                def _():
                    acc[0, zs] = total.astype(bf16)
                up(zs).start()

            @pl.when(zs < z)
            def _():
                @pl.when(z < zn - 1)
                def _():
                    down(zs).wait_recv()
                    acc[0, zs] = (total + z_in[zs].astype(f32)).astype(bf16)

                @pl.when(z == zn - 1)
                def _():
                    acc[0, zs] = total.astype(bf16)
                down(zs).start()

        def finish():
            out_ref[...] = column(z)

            @pl.when(z > 0)
            def _():
                up(z).wait_recv()
                out_ref[...] += z_in[z + 1].astype(f32)

            @pl.when(z < zn - 1)
            def _():
                down(z).wait_recv()
                out_ref[...] += z_in[z].astype(f32)

            def sent(zs):
                diag_x(zs).wait_send()
                diag_y(zs).wait_send()
                to_x(zs).wait_send()
                to_y(zs).wait_send()

            for col in range(4):
                for cp in core(col):
                    cp.wait_send()
            for dist in order:
                each(dist, sent)
                if dist:
                    each(dist, lambda zs: up(zs).wait_send())

        self.start, self.finish, self.greet, self.meet = start, finish, at.greet, at.meet
        self.diag = [functools.partial(ready, 3)] + [functools.partial(each, dist, diag) for dist in order]
        self.sides = [functools.partial(each, dist, sides) for dist in order]
        self.pass_on = [functools.partial(each, dist, pass_on) for dist in order[:-1]]
        self.ready = lambda: (ready(1), ready(2), ready(0))

    @staticmethod
    def scratch(nd, rows, cols, parts):
        zn = nd // 2
        D, V = pltpu.SemaphoreType.DMA, pltpu.VMEM
        return [V((4, zn, rows, cols), bf16), V((4, zn, rows, cols), bf16), V((zn, rows, cols), bf16), V((2, zn, rows, cols), bf16),
                V((zn + 1, rows, cols), bf16), D((4, parts)), D((4, parts)), D((4, parts))] + [D((zn,))] * 9 + [D((2, zn))]


def plan(pipes, place, time_of, spots):
    ticks = {0: [place.greet], 1: [place.meet] + [functools.partial(p.start, col) for col in (3, 1, 2, 0) for p in pipes]}

    def put(when, fn):
        tick = next((t for t, us in enumerate(time_of) if us >= when), len(time_of))
        ticks.setdefault(tick, []).append(fn)

    todo = []
    for p, (diag, sides, side_gap, pass_on, pass_gap) in zip(pipes, spots):
        todo += [(diag, fn) for fn in p.diag] + [(sides, p.ready)]
        todo += [(sides + k * side_gap * 4 / len(p.sides), fn) for k, fn in enumerate(p.sides)]
        todo += [(pass_on + k * pass_gap * 4 / len(p.sides), fn) for k, fn in enumerate(p.pass_on)]
    for when, fn in sorted(todo, key=lambda e: e[0]):
        put(when, fn)
    return ticks


def pipes_of(nd, nf, g_refs, out_refs, split, scratch):
    def view(a, lead, o, w):
        return g_refs[a].at[:, :, :, pl.ds(o, w)] if lead is None else g_refs[a].at[lead, :, :, :, pl.ds(o, w)]
    per = len(scratch) // len(split)
    return [Scatter(nd, nf, [view(*v) for v in pipe], out_ref, *scratch[per * m : per * (m + 1)])
            for m, (pipe, out_ref) in enumerate(zip(split, out_refs))]


def widths(split):
    return [sum(v[3] for v in pipe) for pipe in split]


def pipes_scratch(nd, rows, split):
    return [x for pipe, w in zip(split, widths(split)) for x in Scatter.scratch(nd, rows, w, len(pipe))]


def run_ticks(ticks, now, last):
    planned = sorted((t, fns) for t, fns in ticks.items() if t <= last)

    def search(items):
        if len(items) == 1:
            tick, fns = items[0]

            @pl.when(now == tick)
            def _():
                for fn in fns:
                    fn()
            return
        mid = len(items) // 2
        lax.cond(now < items[mid][0], lambda: search(items[:mid]), lambda: search(items[mid:]))

    if planned:
        search(planned)


def run_rest(ticks, last):
    for tick, fns in sorted(ticks.items()):
        if tick > last:
            for fn in fns:
                fn()


class Spread:
    def __init__(self, nd, nf, src, got, send, recv):
        self.n, self.nf = nd * nf, nf
        self.me = lax.axis_index("dp") * nf + lax.axis_index("fsdp")
        self.src, self.got, self.send, self.recv = src, got, send, recv

    def peer(self, k):
        return lax.rem(self.me + k, self.n)

    def loop(self, fn):
        def body(k, carry):
            fn(k)
            return carry
        lax.fori_loop(1, self.n, body, 0)

    def greet(self):
        sem = pltpu.get_barrier_semaphore()

        def one(k):
            pl.semaphore_signal(sem, inc=1, device_id=(self.peer(k) // self.nf, self.peer(k) % self.nf), device_id_type=MESH)
        self.loop(one)

    def meet(self):
        pl.semaphore_wait(pltpu.get_barrier_semaphore(), self.n - 1)

    def copy(self, k):
        p = self.peer(k)
        src = self.src.at[p] if len(self.src.shape) == 3 else self.src
        return pltpu.make_async_remote_copy(src_ref=src, dst_ref=self.got.at[k], send_sem=self.send.at[k], recv_sem=self.recv.at[k],
                                            device_id=(p // self.nf, p % self.nf), device_id_type=MESH)

    def begin(self):
        self.loop(lambda k: self.copy(k).start())

    def total(self):
        own = self.src[self.me] if len(self.src.shape) == 3 else self.src[...]

        def add(k, total):
            self.copy(k).wait_recv()
            return total + self.got[k]
        total = lax.fori_loop(1, self.n, add, own)
        self.loop(lambda k: self.copy(k).wait_send())
        return total

    @staticmethod
    def scratch(n, tile):
        D = pltpu.SemaphoreType.DMA
        return [pltpu.VMEM((n,) + tile, f32), D((n,)), D((n,))]


def dot(a, b, dims=((1,), (0,)), precision=None):
    return lax.dot_general(a, b, (dims, ((), ())), preferred_element_type=f32, precision=precision)


def sigmoid(x):
    return 0.5 * jnp.tanh(0.5 * x) + 0.5


def conv_rows(ext, taps, masks, halo):
    rows = ext.shape[0] - halo
    width = 4
    v = ext[halo:]
    out = taps[4:5] + taps[3:4] * v
    for k in range(1, width):
        moved = pltpu.roll(ext, k, 0)[halo:]
        out = out + (taps[3 - k : 4 - k] * masks[:, k : k + 1]) * moved
    return out


def prep_kernel(bcdt_ref, taps_ref, heads_ref, segc_ref, segr_ref,
                m_ref, b_ref, c_ref, bt_ref, ct_ref, pre_ref, gm_ref, cum_ref, cumr_ref, sc_ref, dt_ref):
    T = bcdt_ref.shape[0]
    nc = T // L
    N = b_ref.shape[1]
    H = dt_ref.shape[1]
    groups = cumr_ref.shape[0]
    taps = taps_ref[...]
    tri = (lax.broadcasted_iota(jnp.int32, (L, L), 0) >= lax.broadcasted_iota(jnp.int32, (L, L), 1))
    trif = tri.astype(f32)
    neg_rate = -jnp.exp(heads_ref[0:1, :H]) * LOG2E
    m_ref[T : T + 8, :] = jnp.zeros((8, 4), f32)
    bias = heads_ref[1:2, :H]

    def chunk(c, carry):
        t0 = pl.multiple_of(c * L, L)
        here = pl.ds(t0, L)
        h0 = pl.multiple_of(jnp.maximum(t0 - 16, 0), 16)
        before = bcdt_ref[pl.ds(h0, 16), : 2 * N].astype(f32)
        v = bcdt_ref[here, : 2 * N].astype(f32)
        segc = segc_ref[here, :].astype(f32)
        seg_ext = jnp.concatenate([segc_ref[pl.ds(h0, 16), :].astype(f32), segc], axis=0)
        at = t0 + lax.broadcasted_iota(jnp.int32, (L, 1), 0)
        masks = [jnp.ones((L, 1), f32)]
        for k in range(1, 4):
            masks.append(((pltpu.roll(seg_ext, k, 0)[16:] == segc) & (at >= k)).astype(f32))
        masks = jnp.concatenate(masks, axis=1)
        m_ref[here, :] = masks
        pre = conv_rows(jnp.concatenate([before, v], axis=0), taps, masks, 16)
        pre_ref[here, :] = pre
        act = pre * sigmoid(pre)
        b = act[:, :N]
        cc = act[:, N:]
        bb = b.astype(bf16)
        cb = cc.astype(bf16)
        b_ref[here, :] = bb
        c_ref[here, :] = cb
        bt_ref[:, here] = b.T.astype(bf16)
        ct_ref[:, here] = cc.T.astype(bf16)
        prev = jnp.where(c > 0, seg_ext[15:16], -1.0)
        last = segc[L - 1 : L]
        same = segc == segr_ref[:, here].astype(f32)
        g = dot(cb, bb, ((1,), (1,)))
        gm_ref[pl.ds(c, 1)] = jnp.where(tri & same, g, 0.0)[None]
        raw = bcdt_ref[here, 2 * N : 2 * N + 128].astype(f32)[:, :H] + bias
        dt = jnp.maximum(raw, 0.0) + jnp.log1p(jnp.exp(-jnp.abs(raw)))
        a2 = neg_rate * dt
        cum = dot(trif, a2, precision=HIGHEST)
        end = cum[L - 1 : L]
        ein = jnp.where(segc == prev, jnp.exp2(cum), 0.0)
        lv = jnp.where(segc == last, jnp.exp2(end - cum), 0.0)
        dt_ref[here, :] = dt
        wide = jnp.concatenate([cum, jnp.zeros((L, 128 - H), f32)], axis=1)
        cum_ref[here, :] = wide
        cumt = wide.T
        for k in range(groups):
            cumr_ref[k, :, here] = cumt[HG * k : HG * (k + 1)]
        s0 = pl.multiple_of(c * (3 * L), L)
        for k, part in enumerate((dt, ein, lv)):
            sc_ref[pl.ds(s0 + k * L, L), :] = jnp.concatenate([part, jnp.zeros((L, 128 - H), f32)], axis=1).astype(bf16)
        return carry

    lax.fori_loop(0, nc, chunk, 0)


def prep(bcdt, taps, heads, segc, segr, N, H):
    T = bcdt.shape[0]
    nc = T // L
    G = H // HG
    S = jax.ShapeDtypeStruct
    full = lambda a: pl.BlockSpec(a.shape, lambda i: (0,) * a.ndim)
    outs = (S((T + 8, 4), f32), S((T, N), bf16), S((T, N), bf16), S((N, T), bf16), S((N, T), bf16), S((T, 2 * N), f32),
            S((nc, L, L), f32), S((T, 128), f32), S((G, HG, T), f32), S((3 * T, 128), bf16), S((T, H), f32))
    wide = 2 * N + 128
    return pl.pallas_call(
        prep_kernel,
        grid=(1,),
        in_specs=[pl.BlockSpec((T, wide), lambda i: (0, bcdt.shape[1] // wide - 1))] + [full(a) for a in (taps, heads, segc, segr)],
        out_specs=[full(o) for o in outs],
        out_shape=outs,
        compiler_params=pltpu.CompilerParams(vmem_limit_bytes=60 << 20),
    )(bcdt, taps, heads, segc, segr)


def lane_onehot(group, width, per):
    shape = (128, width)
    return (group * HG + lax.broadcasted_iota(jnp.int32, shape, 1) // per == lax.broadcasted_iota(jnp.int32, shape, 0)).astype(bf16)


def half_masks(P):
    lane = lax.broadcasted_iota(jnp.int32, (1, 2 * P), 1)
    first = (lane < P).astype(f32)
    return first.astype(bf16), (1.0 - first).astype(bf16)


def decay(cum4, cumr, k):
    return jnp.exp2(jnp.minimum(cum4[:, k : k + 1] - cumr[k : k + 1, :], 0.0))


def fwd_kernel(u_ref, gate_ref, taps_ref, m_ref, b_ref, c_ref, bt_ref, gm_ref, cum_ref, cumr_ref, sc_ref,
               gg_ref, r_ref, pre_ref, st_ref, state, move, ssq_ref):
    T, W = u_ref.shape
    P = W // HG
    nc = T // L
    step = pl.program_id(0)
    taps = taps_ref[...]
    gain = taps[5:6]
    skip = taps[6:7]
    onehot = lane_onehot(step, W, P)
    ma, mb = half_masks(P)
    state[...] = jnp.zeros_like(state)

    @pl.when(step == 0)
    def _():
        ssq_ref[...] = jnp.zeros_like(ssq_ref)

    @pl.when(step == 0)
    def _():
        def make(c, carry):
            here = pl.ds(pl.multiple_of(c * L, L), L)
            lag = lax.broadcasted_iota(jnp.int32, (L, L + 16), 0) + 16 - lax.broadcasted_iota(jnp.int32, (L, L + 16), 1)
            for k in range(1, 4):
                move[c, (k - 1) * L : k * L, :] = jnp.where(lag == k, m_ref[here, k : k + 1], 0.0).astype(bf16)
            return carry
        lax.fori_loop(0, nc, make, 0)

    def chunk(c, carry):
        t0 = pl.multiple_of(c * L, L)
        here = pl.ds(t0, L)
        h0 = pl.multiple_of(jnp.maximum(t0 - 16, 0), 16)
        v = u_ref[here, :]
        moved = dot(move[c], jnp.concatenate([u_ref[pl.ds(h0, 16), :], v], axis=0))
        pre = taps[4:5] + taps[3:4] * v.astype(f32)
        for k in range(1, 4):
            pre = pre + taps[3 - k : 4 - k] * moved[(k - 1) * L : k * L]
        pre_ref[here, :] = pre.astype(bf16)
        x = pre * sigmoid(pre)
        s0 = pl.multiple_of(c * (3 * L), L)
        exp = dot(sc_ref[pl.ds(s0, 3 * L), :], onehot)
        dtx, einx, lvx = exp[:L], exp[L : 2 * L], exp[2 * L :]
        xd = x * dtx
        xdb = xd.astype(bf16)
        gm = gm_ref[c]
        cum4 = pltpu.roll(cum_ref[here, :], 128 - step * HG, 1)
        cumr = cumr_ref[0, :, here]
        sb = state[...].astype(bf16)
        st_ref[c] = sb
        inner = []
        for p in range(HG // 2):
            m0 = (decay(cum4, cumr, 2 * p) * gm).astype(bf16)
            m1 = (decay(cum4, cumr, 2 * p + 1) * gm).astype(bf16)
            xp = xdb[:, 2 * P * p : 2 * P * (p + 1)]
            inner.append(dot(jnp.concatenate([m0, m1], axis=1), jnp.concatenate([xp * ma, xp * mb], axis=0)))
        y = jnp.concatenate(inner, axis=1) + dot(c_ref[here, :], sb) * einx + skip * x
        state[...] = state[...] * einx[L - 1 : L] + dot(bt_ref[:, here], (xd * lvx).astype(bf16))
        gate = gate_ref[here, :].astype(f32)
        g = y * (gate * sigmoid(gate))
        gg_ref[here, :] = (g * gain).astype(bf16)
        g2 = g * g
        tot = g2[:, :128]
        for j in range(1, W // 128):
            tot = tot + g2[:, 128 * j : 128 * (j + 1)]
        ssq_ref[here, :] += tot
        return carry

    lax.fori_loop(0, nc, chunk, 0, unroll=4)

    @pl.when(step == pl.num_programs(0) - 1)
    def _():
        def root(c, carry):
            here = pl.ds(pl.multiple_of(c * L, L), L)
            total = jnp.sum(ssq_ref[here, :], axis=1, keepdims=True)
            r_ref[here, :] = lax.rsqrt(total / (W * pl.num_programs(0)) + EPS)
            return carry
        lax.fori_loop(0, nc, root, 0)


def fwd(u, gate, taps, masks, b, c, bt, gm, cum, cumr, sc):
    T, E = gate.shape
    N = b.shape[1]
    G = cumr.shape[0]
    W = E // G
    nc = T // L
    S = jax.ShapeDtypeStruct
    col = lambda off: pl.BlockSpec((T, W), lambda g: (0, g + off))
    full = lambda a: pl.BlockSpec(a.shape, lambda g: (0,) * a.ndim)
    grp = lambda a: pl.BlockSpec((1,) + a.shape[1:], lambda g: (g, 0, 0))
    return pl.pallas_call(
        fwd_kernel,
        grid=(G,),
        in_specs=[col(0), col(0), pl.BlockSpec((8, W), lambda g: (0, g)), full(masks), full(b), full(c), full(bt), full(gm),
                  full(cum), grp(cumr), full(sc)],
        out_specs=[col(0), pl.BlockSpec((T, 1), lambda g: (0, 0)), col(0), pl.BlockSpec((nc, N, W), lambda g: (0, 0, g))],
        out_shape=(S((T, E), bf16), S((T, 1), f32), S((T, E), bf16), S((nc, N, E), bf16)),
        scratch_shapes=[pltpu.VMEM((N, W), f32), pltpu.VMEM((nc, 3 * L, L + 16), bf16), pltpu.VMEM((T, 128), f32)],
        compiler_params=pltpu.CompilerParams(vmem_limit_bytes=60 << 20),
        cost_estimate=pl.CostEstimate(flops=T * E * (2 * L + 4 * N) * 2, bytes_accessed=T * E * 12, transcendentals=T * E * 4),
    )(u, gate, taps, masks, b, c, bt, gm, cum, cumr, sc)


def bwd_scatter_kernel(nd, nf, g0, Gh, nc, arrays, split, *refs):
    g_refs, ins, outs = refs[:arrays], refs[arrays : arrays + 16], refs[arrays + 16 : arrays + 24]
    refs = refs[arrays + 24 :]
    sums, own, comm = refs[: len(split)], refs[len(split) : len(split) + 3], refs[len(split) + 3 :]
    pipes = pipes_of(nd, nf, g_refs, sums, split, comm)
    nb = ins[15].shape[0] // MB
    time_of = [21.0 * g + (1.9 * i if i < nc else 1.9 * nc + 1.9 * (i - nc)) for g in range(Gh) for i in range(nc + nb)]
    ticks = plan(pipes, pipes[0], time_of, BWD_SPOTS)
    last = len(time_of) - 1
    bwd_body(lambda i: run_ticks(ticks, pl.program_id(0) * (nc + nb) + i, last), g0, *ins, *outs, *own)

    @pl.when(pl.program_id(0) == pl.num_programs(0) - 1)
    def _():
        run_rest(ticks, last)
        for p in pipes:
            p.finish()


def bwd_body(tick, g0, u_ref, gate_ref, pre_ref, dm_ref, rq_ref, taps_ref, m_ref, b_ref, c_ref, ct_ref, gm_ref, cum_ref, cumr_ref, sc_ref, st_ref, normt_ref,
             dz_ref, gw_ref, dg_ref, db_ref, dc_ref, rs_ref, small_ref, kk_ref, ds, nxt, acc):
    T, W = u_ref.shape
    P = W // HG
    nc = T // L
    step = pl.program_id(0)
    taps = taps_ref[...]
    gain = taps[5:6]
    skip = taps[6:7]
    onehot = lane_onehot(step + g0, W, P)
    ma, mb = half_masks(P)
    ds[...] = jnp.zeros_like(ds)
    nxt[...] = jnp.zeros_like(nxt)
    acc[...] = jnp.zeros_like(acc)

    @pl.when(step == 0)
    def _():
        dg_ref[...] = jnp.zeros_like(dg_ref)
        db_ref[...] = jnp.zeros_like(db_ref)
        dc_ref[...] = jnp.zeros_like(dc_ref)
        rs_ref[...] = jnp.zeros_like(rs_ref)

    ri = lax.broadcasted_iota(jnp.int32, (4 * W, 128), 0)
    ci = lax.broadcasted_iota(jnp.int32, (4 * W, 128), 1)
    part = ri // W
    want = (jnp.maximum(part - 1, 0) * pl.num_programs(0) + step) * HG + (ri % W) // P
    fold = (want == ci).astype(bf16)

    def eight(z):
        return jnp.sum(z.reshape(L // 8, 8, W), axis=0)

    def chunk(i, carry):
        tick(i)
        c = nc - 1 - i
        t0 = pl.multiple_of(c * L, L)
        here = pl.ds(t0, L)
        u = u_ref[here, :].astype(f32)
        pre = pre_ref[here, :].astype(f32)
        sig = sigmoid(pre)
        x = pre * sig
        dsilu = sig + x * (1.0 - sig)
        s0 = pl.multiple_of(c * (3 * L), L)
        exp = dot(sc_ref[pl.ds(s0, 3 * L), :], onehot)
        dtx, einx, lvx = exp[:L], exp[L : 2 * L], exp[2 * L :]
        xdb = (x * dtx).astype(bf16)
        xd = xdb.astype(f32)
        gm = gm_ref[c]
        cum4 = pltpu.roll(cum_ref[here, :], 128 - (step + g0) * HG, 1)
        cumr = cumr_ref[0, :, here]
        sb = st_ref[c]
        es, ms, inner = [], [], []
        for p in range(HG // 2):
            e0 = decay(cum4, cumr, 2 * p)
            e1 = decay(cum4, cumr, 2 * p + 1)
            m0 = (e0 * gm).astype(bf16)
            m1 = (e1 * gm).astype(bf16)
            xp = xdb[:, 2 * P * p : 2 * P * (p + 1)]
            inner.append(dot(jnp.concatenate([m0, m1], axis=1), jnp.concatenate([xp * ma, xp * mb], axis=0)))
            es.append((e0, e1))
            ms.append((m0, m1))
        yn = jnp.concatenate(inner, axis=1) + dot(c_ref[here, :], sb) * einx
        y = yn + skip * x
        gate = gate_ref[here, :].astype(f32)
        sgate = sigmoid(gate)
        silu_g = gate * sgate
        g = y * silu_g
        r = rq_ref[here, 0:1]
        q = rq_ref[here, 1:2]
        dmr = dm_ref[here, :].astype(f32) * r
        dgg = gain * dmr - g * q
        dyb = (dgg * silu_g).astype(bf16)
        dy = dyb.astype(f32)
        dz_ref[0, here, :] = (dgg * y * (sgate + silu_g * (1.0 - sgate))).astype(bf16)
        dxi = []
        dgc = dg_ref[c]
        for p in range(HG // 2):
            cols = slice(2 * P * p, 2 * P * (p + 1))
            dp = dyb[:, cols]
            dstack = jnp.concatenate([dp * ma, dp * mb], axis=0)
            dmm = dot(dstack, xdb[:, cols], ((1,), (1,)))
            dgc = dgc + dmm[:L] * es[p][0] + dmm[L:] * es[p][1]
            dxi.append(dot(jnp.concatenate(ms[p], axis=0), dstack, ((0,), (0,))))
        dg_ref[c] = dgc
        dxi = jnp.concatenate(dxi, axis=1)
        dsn = ds[...]
        dsb = dsn.astype(bf16)
        dye = (dy * einx).astype(bf16)
        dc_ref[here, :] += dot(dye, sb, ((1,), (1,)))
        kept = einx[L - 1 : L]
        kk_ref[pl.ds(c, 1), :] = kept * jnp.sum(sb.astype(f32) * dsn, axis=0, keepdims=True)
        db_ref[here, :] += dot((xd * lvx).astype(bf16), dsb, ((1,), (1,)))
        dxe = dot(b_ref[here, :], dsb) * lvx
        ds[...] = dsn * kept + dot(ct_ref[:, here], dye)
        dxd = dxi + dxe
        r1 = dy * yn - xd * dxi
        r1h = r1.astype(bf16)
        r1l = (r1 - r1h.astype(f32)).astype(bf16)
        rs_ref[here, :] += dot(jnp.concatenate([r1h, r1l, (xd * dxe).astype(bf16), (x * dxd).astype(bf16)], axis=1), fold)
        dpre = (dxd * dtx + skip * dy) * dsilu
        ext = jnp.concatenate([dpre, nxt[...]], axis=0)
        nxt[...] = dpre[:8]
        du = taps[3:4] * dpre
        acc[0:8, :] += eight(dmr * g)
        acc[8:16, :] += eight(dy * x)
        acc[16:24, :] += eight(dpre)
        acc[24:32, :] += eight(dpre * u)
        mrows = m_ref[pl.ds(t0, L + 8), :]
        for k in range(1, 4):
            sk = pltpu.roll(ext * mrows[:, k : k + 1], L + 8 - k, 0)[:L]
            du = du + taps[3 - k : 4 - k] * sk
            acc[24 + 8 * k : 32 + 8 * k, :] += eight(sk * u)
        dz_ref[1, here, :] = du.astype(bf16)
        return carry

    lax.fori_loop(0, nc, chunk, 0)
    for j in range(7):
        small_ref[j : j + 1, :] = jnp.sum(acc[8 * j : 8 * j + 8, :], axis=0, keepdims=True)
    small_ref[7:8, :] = jnp.zeros((1, W), f32)

    def weights(i, carry):
        tick(nc + i)
        rows = pl.ds(pl.multiple_of(i * MB, MB), MB)
        for kind in range(2):
            gw_ref[kind, rows, :] = dot(normt_ref[rows, :], dz_ref[kind]).astype(bf16)
        return carry

    lax.fori_loop(0, normt_ref.shape[0] // MB, weights, 0)


def bwd(half, halves, u, gate, pre, dm, rq, taps, masks, b, c, ct, gm, cum, cumr, sc, st, normt, comm):
    T, E = gate.shape
    N = b.shape[1]
    G = cumr.shape[0]
    W = E // G
    nc = T // L
    Gh = G // halves
    Eh = E // halves
    g0 = half * Gh
    S = jax.ShapeDtypeStruct
    col = pl.BlockSpec((T, W), lambda g: (0, g + g0))
    full = lambda a: pl.BlockSpec(a.shape, lambda g: (0,) * a.ndim)
    whole = lambda s: pl.BlockSpec(s, lambda g: (0,) * len(s))
    grp = lambda a: pl.BlockSpec((1,) + a.shape[1:], lambda g: (g + g0, 0, 0))
    in_specs = [col, col, col, col, full(rq), pl.BlockSpec((8, W), lambda g: (0, g + g0)), full(masks), full(b), full(c),
                full(ct), full(gm), full(cum), grp(cumr), full(sc), pl.BlockSpec((nc, N, W), lambda g: (0, 0, g + g0)), full(normt)]
    D = normt.shape[0]
    out_specs = [pl.BlockSpec((2, T, W), lambda g: (0, 0, g)), pl.BlockSpec((2, D, W), lambda g: (0, 0, g)), whole((nc, L, L)), whole((T, N)), whole((T, N)),
                 whole((T, 128)), pl.BlockSpec((8, W), lambda g: (0, g)), pl.BlockSpec((nc, W), lambda g: (0, g))]
    out_shape = [S((2, T, Eh), bf16), S((2, D, Eh), bf16), S((nc, L, L), f32), S((T, N), f32), S((T, N), f32), S((T, 128), f32), S((8, Eh), f32), S((nc, Eh), f32)]
    scratch = [pltpu.VMEM((N, W), f32), pltpu.VMEM((8, W), f32), pltpu.VMEM((56, W), f32)]
    nd, nf, cid, first, split = comm
    rows = first[0].shape[-2]
    return pl.pallas_call(
        functools.partial(bwd_scatter_kernel, nd, nf, g0, Gh, nc, len(first), split),
        grid=(Gh,),
        in_specs=[pl.BlockSpec(memory_space=pl.ANY)] * len(first) + in_specs,
        out_specs=out_specs + [whole((rows, w)) for w in widths(split)],
        out_shape=out_shape + [S((rows, w), f32) for w in widths(split)],
        scratch_shapes=scratch + pipes_scratch(nd, rows, split),
        compiler_params=pltpu.CompilerParams(vmem_limit_bytes=60 << 20, collective_id=cid, has_side_effects=True),
        cost_estimate=pl.CostEstimate(flops=T * Eh * (8 * L + 12 * N + 4 * D), bytes_accessed=T * Eh * 16, transcendentals=T * Eh * 4),
    )(*first, u, gate, pre, dm, rq, taps, masks, b, c, ct, gm, cum, cumr, sc, st, normt)


def post_kernel(bcdt_ref, pre_ref, taps_ref, heads_ref, m_ref, segc_ref, segr_ref, b_ref, c_ref, dg0_ref, db0_ref, dc0_ref, rs0_ref, dg1_ref, db1_ref, dc1_ref, rs1_ref, kk_ref, dt_ref,
                out_ref, small_ref, hs_ref, nxt, acc, hacc):
    T = bcdt_ref.shape[0]
    nc = T // L
    N = b_ref.shape[1]
    H = dt_ref.shape[1]
    taps = taps_ref[...]
    tri = (lax.broadcasted_iota(jnp.int32, (L, L), 0) >= lax.broadcasted_iota(jnp.int32, (L, L), 1))
    upper = (lax.broadcasted_iota(jnp.int32, (L, L), 0) <= lax.broadcasted_iota(jnp.int32, (L, L), 1)).astype(f32)
    strict = 1.0 - upper
    rate = -jnp.exp(heads_ref[0:1, :H])
    bias = heads_ref[1:2, :H]
    nxt[...] = jnp.zeros_like(nxt)
    acc[...] = jnp.zeros_like(acc)
    hacc[...] = jnp.zeros_like(hacc)

    def eight(z):
        return jnp.sum(z.reshape(L // 8, 8, z.shape[1]), axis=0)

    def chunk(i, carry):
        c = nc - 1 - i
        t0 = pl.multiple_of(c * L, L)
        here = pl.ds(t0, L)
        same = segc_ref[here, :] == segr_ref[:, here]
        dg = jnp.where(tri & same, dg0_ref[c] + dg1_ref[c], 0.0)
        dgb = dg.astype(bf16)
        dcv = dc0_ref[here, :] + dc1_ref[here, :] + dot(dgb, b_ref[here, :])
        dbv = db0_ref[here, :] + db1_ref[here, :] + dot(dg.T.astype(bf16), c_ref[here, :])
        pre = pre_ref[here, :]
        sig = sigmoid(pre)
        dpre = jnp.concatenate([dbv, dcv], axis=1) * (sig + pre * sig * (1.0 - sig))
        v = bcdt_ref[here, : 2 * N].astype(f32)
        ext = jnp.concatenate([dpre, nxt[...]], axis=0)
        nxt[...] = dpre[:8]
        dv = taps[3:4] * dpre
        acc[0:8, :] += eight(dpre)
        acc[8:16, :] += eight(dpre * v)
        mrows = m_ref[pl.ds(t0, L + 8), :]
        for k in range(1, 4):
            sk = pltpu.roll(ext * mrows[:, k : k + 1], L + 8 - k, 0)[:L]
            dv = dv + taps[3 - k : 4 - k] * sk
            acc[8 + 8 * k : 16 + 8 * k, :] += eight(sk * v)
        out_ref[here, : 2 * N] = dv.astype(bf16)
        q = H // 2
        r0, r1 = rs0_ref[here, :], rs1_ref[here, :]
        r1, r2, r3 = (jnp.concatenate([r0[:, m * q : (m + 1) * q], r1[:, m * q : (m + 1) * q]], axis=1) for m in range(3))
        da = dot(upper, r1, precision=HIGHEST) + dot(strict, r2, precision=HIGHEST) + kk_ref[pl.ds(c, 1), :]
        dt = dt_ref[here, :]
        raw = bcdt_ref[here, 2 * N : 2 * N + 128].astype(f32)[:, :H] + bias
        ddt = (r3 + da * rate) * sigmoid(raw)
        hacc[0:8, :] += eight(da * rate * dt)
        hacc[8:16, :] += eight(ddt)
        out_ref[here, 2 * N :] = jnp.concatenate([ddt, jnp.zeros((L, out_ref.shape[1] - 2 * N - H), f32)], axis=1).astype(bf16)
        return carry

    lax.fori_loop(0, nc, chunk, 0)
    for j in range(5):
        small_ref[j : j + 1, :] = jnp.sum(acc[8 * j : 8 * j + 8, :], axis=0, keepdims=True)
    small_ref[5:8, :] = jnp.zeros((3, 2 * N), f32)
    for j in range(2):
        hs_ref[j : j + 1, :] = jnp.sum(hacc[8 * j : 8 * j + 8, :], axis=0, keepdims=True)


def post(bcdt, pre, taps, heads, masks, segc, segr, b, c, first, second, kk, dt):
    T = bcdt.shape[0]
    N = b.shape[1]
    H = dt.shape[1]
    S = jax.ShapeDtypeStruct
    wide = 2 * N + 128
    full = lambda a: pl.BlockSpec(a.shape, lambda i: (0,) * a.ndim)
    ins = (bcdt, pre, taps, heads, masks, segc, segr, b, c, *first, *second, kk, dt)
    outs = (S((T, wide), bf16), S((8, 2 * N), f32), S((2, H), f32))
    return pl.pallas_call(
        post_kernel,
        grid=(1,),
        in_specs=[pl.BlockSpec((T, wide), lambda i: (0, bcdt.shape[1] // wide - 1))] + [full(a) for a in ins[1:]],
        out_specs=[full(o) for o in outs],
        out_shape=outs,
        scratch_shapes=[pltpu.VMEM((8, 2 * N), f32), pltpu.VMEM((40, 2 * N), f32), pltpu.VMEM((16, H), f32)],
        compiler_params=pltpu.CompilerParams(vmem_limit_bytes=60 << 20),
    )(*ins)


NT = 256


def tail_kernel(nd, nf, arrays, split, tiles, *refs):
    g_refs, refs = refs[:arrays], refs[arrays:]
    (wo_hbm, wg_hbm, wa_hbm, gg_ref, dz0_ref, dz1_ref, dbc_ref, hid_ref, go_ref, r_ref, gain_ref, mine_ref,
     suma_ref, sumb_ref, out_ref, gin_ref, small_ref) = refs[:17]
    wo, wg, wa, acc, sem = refs[17:22]
    mine = Spread(nd, nf, mine_ref, *refs[22:25])
    pipes = pipes_of(nd, nf, g_refs, (suma_ref, sumb_ref), split, refs[25:])
    D, E = wg.shape
    Eh = E // 2
    step = pl.program_id(0)
    early = tiles // 2
    blocks = D // NT
    mid = (early + tiles) * blocks
    scale = 4 / tiles
    time_of = [4 + 0.75 * scale * t if t < early * blocks else
               (13 + 1.65 * scale * (t - early * blocks) if t < mid else 52.6 + 0.65 * scale * (t - mid)) for t in range(2 * tiles * blocks)]
    ticks = plan(pipes, mine, time_of, TAIL_SPOTS)
    last = len(time_of) - 1
    ticks[1].append(mine.begin)
    fetch = [pltpu.make_async_copy(src, dst, sem.at[k]) for k, (src, dst) in enumerate(((wo_hbm, wo), (wg_hbm, wg), (wa_hbm, wa)))]

    @pl.when(step == 0)
    def _():
        for cp in fetch:
            cp.start()
        run_ticks(ticks, 0, 0)
        fetch[0].wait()

    @pl.when(step == early)
    def _():
        fetch[1].wait()
        fetch[2].wait()

    back = (step >= early) & (step < early + tiles)
    in_back = lambda t: early * blocks <= t < (early + tiles) * blocks

    @pl.when(jnp.logical_not(back))
    def _():
        def block(j, carry):
            run_ticks({t: f for t, f in ticks.items() if t and not in_back(t)}, step * blocks + j, last)
            cols = pl.ds(pl.multiple_of(j * NT, NT), NT)
            out_ref[:, cols] = (hid_ref[:, cols].astype(f32) + r_ref[...] * dot(gg_ref[...], wo[:, cols])).astype(bf16)
            return carry
        lax.fori_loop(0, blocks, block, 0)

    @pl.when(back)
    def _():
        def block(j, carry):
            run_ticks({t: f for t, f in ticks.items() if in_back(t)}, step * blocks + j, last)
            cols = pl.ds(pl.multiple_of(j * NT, NT), NT)
            part = dot(dz0_ref[0], wg[cols, :Eh], ((1,), (1,))) + dot(dz1_ref[0], wg[cols, Eh:], ((1,), (1,)))
            part = part + dot(dz0_ref[1], wa[cols, :Eh], ((1,), (1,))) + dot(dz1_ref[1], wa[cols, Eh:E], ((1,), (1,)))
            acc[:, cols] = part + dot(dbc_ref[...], wa[cols, E:], ((1,), (1,)))
            return carry
        lax.fori_loop(0, blocks, block, 0)
        gain = gain_ref[...]

        def rows_of(i, carry):
            here = pl.ds(pl.multiple_of(i * 64, 64), 64)
            rows = hid_ref[here, :].astype(f32)
            rinv = lax.rsqrt(jnp.mean(rows * rows, axis=-1, keepdims=True) + EPS)
            xhat = rows * rinv
            bn = acc[here, :]
            gb = bn * gain
            mean = jnp.mean(gb * xhat, axis=-1, keepdims=True)
            gin_ref[here, :] = (go_ref[here, :].astype(f32) + rinv * (gb - xhat * mean)).astype(bf16)
            return carry
        lax.fori_loop(0, hid_ref.shape[0] // 64, rows_of, 0)

    @pl.when(step == 2 * tiles - 1)
    def _():
        run_rest(ticks, last)
        for p in pipes:
            p.finish()
        small_ref[...] = mine.total()


def tail(nd, nf, cid, gs, split, dz0, dz1, dbcdt, full_gate, full_a, gg, full_out, hidden, grad_out, r, norm_gain, mine):
    T, D = hidden.shape
    E = full_out.shape[0]
    n = nd * nf
    rows = gs[0].shape[-2]
    MT = 256 if rows % 16 == 0 else 128
    tiles = T // MT
    early = tiles // 2
    wide = dbcdt.shape[1]
    S = jax.ShapeDtypeStruct
    any_ = pl.BlockSpec(memory_space=pl.ANY)
    whole = lambda s: pl.BlockSpec(s, lambda k: (0,) * len(s), pipeline_mode=pl.Buffered(1))
    at_out = lambda k: jnp.minimum(k, early - 1) + jnp.clip(k - tiles - early + 1, 0, tiles - early)
    at_back = lambda k: jnp.clip(k - early, 0, tiles - 1)
    at_row = lambda k: k - early * jnp.clip(k - early + 1, 0, 1) - (tiles - early) * jnp.clip(k - early - tiles + 1, 0, 1)
    out_tile = lambda w: pl.BlockSpec((MT, w), lambda k: (at_out(k), 0))
    back_tile = lambda w: pl.BlockSpec((MT, w), lambda k: (at_back(k), 0))
    half = pl.BlockSpec((2, MT, E // 2), lambda k: (0, at_back(k), 0))
    tile = mine.shape[1:]
    return pl.pallas_call(
        functools.partial(tail_kernel, nd, nf, len(gs), split, tiles),
        grid=(2 * tiles,),
        in_specs=[any_] * (len(gs) + 3) + [out_tile(E), half, half, back_tile(wide), pl.BlockSpec((MT, D), lambda k: (at_row(k), 0)), back_tile(D),
                                           out_tile(1), whole((1, D)), whole(mine.shape)],
        out_specs=[whole((rows, w)) for w in widths(split)] + [out_tile(D), back_tile(D), whole(tile)],
        out_shape=[S((rows, w), f32) for w in widths(split)] + [S((T, D), bf16), S((T, D), bf16), S(tile, f32)],
        scratch_shapes=[pltpu.VMEM((E, D), bf16), pltpu.VMEM((D, E), bf16), pltpu.VMEM((D, E + wide), bf16), pltpu.VMEM((MT, D), f32),
                        pltpu.SemaphoreType.DMA((3,))]
        + Spread.scratch(n, tile) + pipes_scratch(nd, rows, split),
        compiler_params=pltpu.CompilerParams(collective_id=cid, has_side_effects=True, vmem_limit_bytes=67043328),
        cost_estimate=pl.CostEstimate(flops=2 * T * D * 3 * E, bytes_accessed=8 * D * E, transcendentals=0),
    )(*gs, full_out, full_gate, full_a, gg, dz0, dz1, dbcdt, hidden, grad_out, r, norm_gain, mine)


def finish_kernel(gate0_ref, gate1_ref, u0_ref, u1_ref, oa_ref, ob_ref, tot_ref, wzx_ref, wbc_ref, wdt_ref, gain_ref, o_ref, gi_ref,
                  oo_ref, go_ref, zx_ref, bc_ref, dt_ref, out_ref, conv_ref, n_ref, gg_ref, heads_ref):
    oo_ref[...] = o_ref[...]
    go_ref[...] = gi_ref[...]

    @pl.when(pl.program_id(0) == 0)
    def _():
        Eh = gate0_ref.shape[1]
        for k, ref in enumerate((gate0_ref, gate1_ref, u0_ref)):
            zx_ref[:, k * Eh : (k + 1) * Eh] = ref[...]
        zx_ref[:, 3 * Eh :] = u1_ref[:, :Eh]
        wide = bc_ref.shape[1]
        bc_ref[...] = u1_ref[:, Eh : Eh + wide]
        dt_ref[...] = u1_ref[:, Eh + wide : Eh + wide + 128][:, : dt_ref.shape[1]]
        half = oa_ref.shape[1]
        out_ref[:, :half] = oa_ref[...]
        out_ref[:, half:] = ob_ref[...]
        k1 = conv_ref.shape[0]
        conv_ref[...] = tot_ref[:k1, : conv_ref.shape[1]]
        gg_ref[...] = tot_ref[k1 : k1 + 1, : gg_ref.shape[1]]
        heads_ref[...] = tot_ref[k1 + 1 : k1 + 1 + heads_ref.shape[0], : heads_ref.shape[1]]
        dots = lambda w, g: jnp.sum(w.astype(f32) * g, axis=1, keepdims=True)
        total = dots(wzx_ref[...], zx_ref[...]) + dots(wbc_ref[...], bc_ref[...]) + dots(wdt_ref[...], dt_ref[...])
        n_ref[...] = total / gain_ref[...].astype(f32)


def finish(gate0, gate1, u0, u1, s_out, tot, w_zx, w_bc, w_dt, gain, output, grad_in, shapes):
    S = jax.ShapeDtypeStruct
    tile = pl.BlockSpec((256, output.shape[1]), lambda i: (i, 0))
    return pl.pallas_call(
        finish_kernel,
        grid=(output.shape[0] // 256,),
        in_specs=[pl.BlockSpec(a.shape, lambda i: (0, 0)) for a in (gate0, gate1, u0, u1, *s_out, tot, w_zx, w_bc, w_dt, gain)] + [tile, tile],
        out_specs=[tile, tile] + [pl.BlockSpec(s, lambda i: (0, 0)) for s in shapes],
        out_shape=[S(output.shape, bf16), S(output.shape, bf16)] + [S(s, f32) for s in shapes],
        compiler_params=pltpu.CompilerParams(vmem_limit_bytes=63 << 20),
    )(gate0, gate1, u0, u1, *s_out, tot, w_zx, w_bc, w_dt, gain, output, grad_in)


def norm_kernel(hid_ref, gain_ref, normed_ref, normt_ref):
    rows = hid_ref[...].astype(f32)
    normed = rows * lax.rsqrt(jnp.mean(rows * rows, axis=-1, keepdims=True) + EPS) * gain_ref[...]
    normed_ref[...] = normed.astype(bf16)
    normt_ref[...] = normed.T.astype(bf16)


def norm(hidden, gain):
    T, D = hidden.shape
    S = jax.ShapeDtypeStruct
    row = pl.BlockSpec((256, D), lambda i: (i, 0))
    return pl.pallas_call(
        norm_kernel,
        grid=(T // 256,),
        in_specs=[row, pl.BlockSpec((1, D), lambda i: (0, 0))],
        out_specs=[row, pl.BlockSpec((D, 256), lambda i: (0, i))],
        out_shape=(S((T, D), bf16), S((D, T), bf16)),
        compiler_params=pltpu.CompilerParams(vmem_limit_bytes=40 << 20),
    )(hidden, gain)


def layer(nd, nf, hidden, grad_out, seg, shard_a, shard_gate, shard_out, head_params, owned, sizes):
    w_zx, w_bc, w_dt, own_gain = owned
    n = nd * nf
    E, N, H, K1, S = sizes
    T, D = hidden.shape
    wide = 2 * N + 128
    full_gate = lax.all_gather(shard_gate, AXES, axis=0, tiled=True)
    full_out = lax.all_gather(shard_out, AXES, axis=0, tiled=True)
    full_a = gather_rows(shard_a, nd, nf, 0)
    off = E + 2 * N + H
    flat = full_a[:, :, off : off + S].reshape(n, -1)
    ncol, nrow, ngate = (E + 2 * N) // n, D // n, E // n
    conv = flat[:, : K1 * ncol].reshape(n, K1, ncol).transpose(1, 0, 2).reshape(K1, n * ncol).astype(f32)
    norm_gain = flat[:, K1 * ncol : K1 * ncol + nrow].reshape(-1).astype(f32)
    gate_gain = flat[:, K1 * ncol + nrow : K1 * ncol + nrow + ngate].reshape(-1).astype(f32)
    full_a = full_a.reshape(D, E + wide)
    normed, normt = norm(hidden, norm_gain[None])
    ubc = dot(normed, full_a).astype(bf16)
    gate = dot(normed, full_gate).astype(bf16)
    segc, segr = seg[:, None], seg[None, :]
    taps_u = jnp.concatenate([conv[:, :E], gate_gain[None], jnp.repeat(head_params[2], E // H)[None], jnp.zeros((1, E), f32)], axis=0)
    taps_bc = jnp.concatenate([conv[:, E:], jnp.zeros((3, 2 * N), f32)], axis=0)
    masks, b, c, bt, ct, pre_bc, gm, cum, cumr, sc, dt = prep(ubc, taps_bc, head_params, segc, segr, N, H)
    gg, r, pre, st = fwd(ubc, gate, taps_u, masks, b, c, bt, gm, cum, cumr, sc)
    gos = (grad_out.astype(f32) * r).astype(bf16)
    g_out = dot(gg, gos, ((0,), (0,))).astype(bf16)
    g_out, full_out = lax.optimization_barrier((g_out, full_out))
    dm = dot(grad_out, full_out, ((1,), (1,))).astype(bf16)
    s = jnp.sum(gg.astype(f32) * dm.astype(f32), axis=1, keepdims=True)
    rq = jnp.concatenate([r, r * r * r * s / E], axis=1)
    back = functools.partial(bwd, u=ubc, gate=gate, pre=pre, dm=dm, rq=rq, taps=taps_u, masks=masks, b=b, c=c, ct=ct, gm=gm, cum=cum,
                             cumr=cumr, sc=sc, st=st, normt=normt)
    zn = max(nd // 2, 1)
    rows_of = lambda g: g.reshape(g.shape[:-2] + (zn, n // zn, g.shape[-2] // n, g.shape[-1]))
    Eh = E // 2
    dz0, gw0, dg0, db0, dc0, rs0, small0, kk0, *s_out = back(
        0, 2, comm=(nd, nf, 4, (rows_of(g_out),), (((0, None, 0, D // 2),), ((0, None, D // 2, D // 2),))))
    dz1, gw1, dg1, db1, dc1, rs1, small1, kk1, gate0, u0 = back(1, 2, comm=(nd, nf, 3, (rows_of(gw0),), (((0, 0, 0, Eh),), ((0, 1, 0, Eh),))))
    small = jnp.concatenate([small0, small1], axis=1)
    kk = jnp.concatenate([kk0, kk1], axis=1)
    kkh = jnp.sum(kk.reshape(kk.shape[0], H, E // H), axis=2)
    dbcdt, small_bc, hs = post(ubc, pre_bc, taps_bc, head_params, masks, segc, segr, b, c, (dg0, db0, dc0, rs0), (dg1, db1, dc1, rs1), kkh, dt)
    d_conv = jnp.concatenate([jnp.stack([small[6], small[5], small[4], small[3], small[2]]),
                              jnp.stack([small_bc[4], small_bc[3], small_bc[2], small_bc[1], small_bc[0]])], axis=1)
    d_heads = jnp.concatenate([hs, jnp.sum(small[1].reshape(1, H, E // H), axis=2)], axis=0)
    lanes = -(-max(ncol, ngate, H) // 128) * 128
    cols = lambda a: jnp.pad(a.reshape(-1, n, a.shape[1] // n).transpose(1, 0, 2), ((0, 0), (0, 0), (0, lanes - a.shape[1] // n)))
    heads_row = jnp.broadcast_to(jnp.pad(d_heads, ((0, 0), (0, lanes - H)))[None], (n, d_heads.shape[0], lanes))
    used = K1 + 1 + d_heads.shape[0]
    mine = jnp.concatenate([cols(d_conv), cols(small[:1]), heads_row, jnp.zeros((n, -(-used // 8) * 8 - used, lanes), f32)], axis=1)
    g_bcdt = dot(normt, dbcdt).astype(bf16)
    split = (((0, 0, 0, Eh),), ((0, 1, 0, Eh), (1, None, 0, wide)))
    gate1, u1, output, grad_in, tot = tail(nd, nf, 1, (rows_of(gw1), rows_of(g_bcdt)), split, dz0, dz1, dbcdt, full_gate, full_a, gg,
                                                   full_out, hidden, grad_out, r, norm_gain[None], mine)
    output, grad_in, s_zx, s_bc, s_dt, s_w, t_conv, t_norm, t_gate, t_heads = finish(
        gate0, gate1, u0, u1, s_out, tot, w_zx, w_bc, w_dt, own_gain, output, grad_in,
        ((nrow, 2 * E), (nrow, 2 * N), (nrow, H), (E // n, D), (K1, ncol), (nrow, 1), (1, ngate), d_heads.shape))
    return output, grad_in, s_zx, s_bc, s_dt, s_w, t_conv, t_norm.reshape(-1), t_gate.reshape(-1), t_heads


def per_device(nd, nf, hidden, grad_out, segment_ids, w_zx, w_bc, w_dt, w_out, conv_params, norm_gain, gate_gain, head_params):
    n = nd * nf
    E, N2, H = w_out.shape[0] * n, w_bc.shape[1], w_dt.shape[1]
    rows = w_zx.shape[0]
    small = jnp.concatenate([conv_params.reshape(-1), norm_gain, gate_gain])
    S = -(-small.shape[0] // rows)
    assert S + H <= 128
    small = jnp.pad(small, (0, S * rows - small.shape[0])).reshape(rows, S)
    shard_a = jnp.concatenate([w_zx[:, E:], w_bc, w_dt, small, jnp.zeros((rows, 128 - H - S), bf16)], axis=1)
    return layer(nd, nf, hidden, grad_out, segment_ids, shard_a, w_zx[:, :E], w_out, head_params, (w_zx, w_bc, w_dt, norm_gain[:, None]),
                 (E, N2 // 2, H, conv_params.shape[0], S))


def solution(mesh):
    row, col, vec, rep = P(AXES, None), P(None, AXES), P(AXES), P()
    return jax.shard_map(
        functools.partial(per_device, mesh.shape["dp"], mesh.shape["fsdp"]),
        mesh=mesh,
        in_specs=(row, row, vec, row, row, row, row, col, vec, vec, rep),
        out_specs=(row, row, row, row, row, row, col, vec, vec, rep),
        check_vma=False,
    )
```

```python
import functools
import jax
import jax.numpy as jnp
from jax import lax
from jax.experimental import pallas as pl
from jax.experimental.pallas import tpu as pltpu
from jax.sharding import PartitionSpec as P

EPS = 1e-05
L = 128
HG = 8
LOG2E = 1.4426950408889634
MB = 512
BWD_SPOTS = ((5.0, 10.0, 2.0, 26.0, 3.2), (7.0, 16.5, 2.0, 39.0, 3.2))
TAIL_SPOTS = ((7.0, 13.0, 3.0, 30.0, 4.0), (9.0, 22.0, 3.0, 46.0, 3.0))
bf16, f32 = jnp.bfloat16, jnp.float32
HIGHEST = lax.Precision.HIGHEST


AXES = ("dp", "fsdp")
MESH = pl.DeviceIdType.MESH


class Place:
    def __init__(self, nd, nf):
        self.zn, self.nf = nd // 2, nf
        d, f = lax.axis_index("dp"), lax.axis_index("fsdp")
        self.z, self.y = d // 2, d % 2
        self.x, self.c = f // 2, f % 2

    def dev(self, z, y, x, c):
        return (z * 2 + y, x * 2 + c)

    def idx(self, z, y, x, c):
        return (z * 2 + y) * self.nf + x * 2 + c

    def meet(self):
        z, zn = self.z, self.zn
        pl.semaphore_wait(pltpu.get_barrier_semaphore(), 3 + (z + zn - 1) // zn + (2 * zn - 2 - z) // zn)

    def greet(self):
        z, y, x, c, zn = self.z, self.y, self.x, self.c, self.zn
        sem = pltpu.get_barrier_semaphore()
        for there in ((z, y, 1 - x, c), (z, 1 - y, x, c), (z, y, x, 1 - c)):
            pl.semaphore_signal(sem, inc=1, device_id=self.dev(*there), device_id_type=MESH)

        @pl.when(z > 0)
        def _():
            pl.semaphore_signal(sem, inc=1, device_id=self.dev(z - 1, y, x, c), device_id_type=MESH)

        @pl.when(z < zn - 1)
        def _():
            pl.semaphore_signal(sem, inc=1, device_id=self.dev(z + 1, y, x, c), device_id_type=MESH)


def gather_kernel(nd, nf, src_ref, out_ref, own_sem, z_send, z_recv, x_send, x_recv, y_send, y_recv, dx_send, dx_recv, dy_send, dy_recv, c_send, c_recv):
    at = Place(nd, nf)
    z, y, x, c, zn = at.z, at.y, at.x, at.c, at.zn
    half = out_ref.shape[2] // 256 * 128
    lo, hi = pl.ds(0, half), pl.ds(half, out_ref.shape[2] - half)
    at.greet()
    at.meet()

    def copy(block, to, send, recv, cols=None, src=None):
        ref = out_ref.at[block] if cols is None else out_ref.at[block, :, cols]
        return pltpu.make_async_remote_copy(src_ref=ref if src is None else src, dst_ref=ref, send_sem=send, recv_sem=recv,
                                            device_id=at.dev(*to), device_id_type=MESH)

    def block(zs, col):
        return at.idx(zs, 1 - y if col & 2 else y, 1 - x if col & 1 else x, c)

    def up(zs, src=None):
        return copy(block(zs, 0), (z + 1, y, x, c), z_send.at[0, zs], z_recv.at[zs], src=src)

    def down(zs, src=None):
        return copy(block(zs, 0), (z - 1, y, x, c), z_send.at[1, zs], z_recv.at[zs], src=src)

    def to_x(zs, src=None):
        return copy(block(zs, 0), (z, y, 1 - x, c), x_send.at[zs], x_recv.at[zs], src=src)

    def to_y(zs, src=None):
        return copy(block(zs, 0), (z, 1 - y, x, c), y_send.at[zs], y_recv.at[zs], src=src)

    def diag_y(zs):
        return copy(block(zs, 1), (z, 1 - y, x, c), dy_send.at[zs], dy_recv.at[zs], lo)

    def diag_x(zs):
        return copy(block(zs, 2), (z, y, 1 - x, c), dx_send.at[zs], dx_recv.at[zs], hi)

    def to_core(zs, col, src=None):
        return copy(block(zs, col), (z, y, x, 1 - c), c_send.at[zs, col], c_recv.at[zs, col], src=src)

    own = pltpu.make_async_copy(src_ref, out_ref.at[block(z, 0)], own_sem)
    own.start()

    @pl.when(z < zn - 1)
    def _():
        up(z, src_ref).start()

    @pl.when(z > 0)
    def _():
        down(z, src_ref).start()

    to_x(z, src_ref).start()
    to_y(z, src_ref).start()
    to_core(z, 0, src_ref).start()

    def each(dist, fn):
        if dist == 0:
            fn(z, 0)
            return

        @pl.when(z - dist >= 0)
        def _():
            fn(z - dist, 1)

        @pl.when(z + dist < zn)
        def _():
            fn(z + dist, -1)

    def from_z(zs, way):
        copy(block(zs, 0), (z, y, x, c), z_send.at[0, zs], z_recv.at[zs]).wait_recv()
        if way > 0:
            @pl.when(z < zn - 1)
            def _():
                up(zs).start()
        else:
            @pl.when(z > 0)
            def _():
                down(zs).start()
        to_x(zs).start()
        to_y(zs).start()
        to_core(zs, 0).start()

    def from_xy(zs, way):
        to_x(zs).wait_recv()
        diag_y(zs).start()
        to_core(zs, 1).start()
        to_y(zs).wait_recv()
        diag_x(zs).start()
        to_core(zs, 2).start()

    def from_diag(zs, way):
        diag_y(zs).wait_recv()
        diag_x(zs).wait_recv()
        to_core(zs, 3).start()

    for dist in range(zn):
        if dist:
            each(dist, from_z)
        each(dist, from_xy)
    for dist in range(zn):
        each(dist, from_diag)
    own.wait()

    def sent(zs, way):
        for col in range(4):
            to_core(zs, col).wait_recv()
            to_core(zs, col).wait_send()
        to_x(zs).wait_send()
        to_y(zs).wait_send()
        diag_x(zs).wait_send()
        diag_y(zs).wait_send()
        if way >= 0:
            @pl.when(z < zn - 1)
            def _():
                up(zs).wait_send()
        if way <= 0:
            @pl.when(z > 0)
            def _():
                down(zs).wait_send()

    for dist in range(zn):
        each(dist, sent)


def gather_rows(shard, nd, nf, cid):
    zn = nd // 2
    D = pltpu.SemaphoreType.DMA
    return pl.pallas_call(
        functools.partial(gather_kernel, nd, nf),
        out_shape=jax.ShapeDtypeStruct((nd * nf,) + shard.shape, shard.dtype),
        in_specs=[pl.BlockSpec(memory_space=pl.ANY)],
        out_specs=pl.BlockSpec(memory_space=pl.ANY),
        scratch_shapes=[D(()), D((2, zn)), D((zn,)), D((zn,)), D((zn,)), D((zn,)), D((zn,)), D((zn,)), D((zn,)), D((zn,)), D((zn,)),
                        D((zn, 4)), D((zn, 4))],
        compiler_params=pltpu.CompilerParams(collective_id=cid, has_side_effects=True),
    )(shard)


class Scatter:
    def __init__(self, nd, nf, g_refs, out_ref, acc, c_in, d_in, xy_in, z_in,
                 load_sem, c_send, c_recv, dx_send, dx_recv, dy_send, dy_recv, x_send, x_recv, y_send, y_recv, z_send, z_recv):
        at = Place(nd, nf)
        z, y, x, c, zn = at.z, at.y, at.x, at.c, at.zn
        cols = out_ref.shape[1]
        wids = [r.shape[3] for r in g_refs]
        offs = [sum(wids[:k]) for k in range(len(wids))]
        half = cols // 256 * 128
        lo, hi = pl.ds(0, half), pl.ds(half, cols - half)

        def inner(col, core):
            return at.idx(0, 1 - y if col & 2 else y, 1 - x if col & 1 else x, core)

        def remote(src, dst, to, send, recv):
            return pltpu.make_async_remote_copy(src_ref=src, dst_ref=dst, send_sem=send, recv_sem=recv, device_id=at.dev(*to), device_id_type=MESH)

        def load(col):
            return [pltpu.make_async_copy(r.at[:, inner(col, c)], acc.at[col, :, :, pl.ds(o, w)], load_sem.at[col, k])
                    for k, (r, o, w) in enumerate(zip(g_refs, offs, wids))]

        def core(col):
            return [remote(r.at[:, inner(col, 1 - c)], c_in.at[col, :, :, pl.ds(o, w)], (z, y, x, 1 - c), c_send.at[col, k], c_recv.at[col, k])
                    for k, (r, o, w) in enumerate(zip(g_refs, offs, wids))]

        def diag_x(zs):
            return remote(acc.at[3, zs, :, lo], d_in.at[zs, :, lo], (z, y, 1 - x, c), dx_send.at[zs], dx_recv.at[zs])

        def diag_y(zs):
            return remote(acc.at[3, zs, :, hi], d_in.at[zs, :, hi], (z, 1 - y, x, c), dy_send.at[zs], dy_recv.at[zs])

        def to_x(zs):
            return remote(acc.at[1, zs], xy_in.at[0, zs], (z, y, 1 - x, c), x_send.at[zs], x_recv.at[zs])

        def to_y(zs):
            return remote(acc.at[2, zs], xy_in.at[1, zs], (z, 1 - y, x, c), y_send.at[zs], y_recv.at[zs])

        def up(zs):
            return remote(acc.at[0, zs], z_in.at[zs + 1], (z + 1, y, x, c), z_send.at[zs], z_recv.at[0, zs])

        def down(zs):
            return remote(acc.at[0, zs], z_in.at[zs], (z - 1, y, x, c), z_send.at[zs], z_recv.at[1, zs])

        def each(dist, fn):
            if dist == 0:
                fn(z)
                return

            @pl.when(z - dist >= 0)
            def _():
                fn(z - dist)

            @pl.when(z + dist < zn)
            def _():
                fn(z + dist)

        order = list(range(zn - 1, -1, -1))

        def start(col):
            for cp in core(col) + load(col):
                cp.start()

        def ready(col):
            for cp in load(col):
                cp.wait()
            for cp in core(col):
                cp.wait_recv()

        def diag(zs):
            acc[3, zs] = acc[3, zs] + c_in[3, zs]
            diag_x(zs).start()
            diag_y(zs).start()

        def sides(zs):
            diag_y(zs).wait_recv()
            acc[1, zs, :, lo] = acc[1, zs, :, lo] + c_in[1, zs, :, lo]
            acc[1, zs, :, hi] = acc[1, zs, :, hi] + c_in[1, zs, :, hi] + d_in[zs, :, hi]
            to_x(zs).start()
            diag_x(zs).wait_recv()
            acc[2, zs, :, lo] = acc[2, zs, :, lo] + c_in[2, zs, :, lo] + d_in[zs, :, lo]
            acc[2, zs, :, hi] = acc[2, zs, :, hi] + c_in[2, zs, :, hi]
            to_y(zs).start()

        def column(zs):
            to_x(zs).wait_recv()
            to_y(zs).wait_recv()
            return (acc[0, zs] + c_in[0, zs]).astype(f32) + (xy_in[0, zs] + xy_in[1, zs]).astype(f32)

        def pass_on(zs):
            total = column(zs)

            @pl.when(zs > z)
            def _():
                @pl.when(z > 0)
                def _():
                    up(zs).wait_recv()
                    acc[0, zs] = (total + z_in[zs + 1].astype(f32)).astype(bf16)

                @pl.when(z == 0)
                def _():
                    acc[0, zs] = total.astype(bf16)
                up(zs).start()

            @pl.when(zs < z)
            def _():
                @pl.when(z < zn - 1)
                def _():
                    down(zs).wait_recv()
                    acc[0, zs] = (total + z_in[zs].astype(f32)).astype(bf16)

                @pl.when(z == zn - 1)
                def _():
                    acc[0, zs] = total.astype(bf16)
                down(zs).start()

        def finish():
            out_ref[...] = column(z)

            @pl.when(z > 0)
            def _():
                up(z).wait_recv()
                out_ref[...] += z_in[z + 1].astype(f32)

            @pl.when(z < zn - 1)
            def _():
                down(z).wait_recv()
                out_ref[...] += z_in[z].astype(f32)

            def sent(zs):
                diag_x(zs).wait_send()
                diag_y(zs).wait_send()
                to_x(zs).wait_send()
                to_y(zs).wait_send()

            for col in range(4):
                for cp in core(col):
                    cp.wait_send()
            for dist in order:
                each(dist, sent)
                if dist:
                    each(dist, lambda zs: up(zs).wait_send())

        self.start, self.finish, self.greet, self.meet = start, finish, at.greet, at.meet
        self.diag = [functools.partial(ready, 3)] + [functools.partial(each, dist, diag) for dist in order]
        self.sides = [functools.partial(each, dist, sides) for dist in order]
        self.pass_on = [functools.partial(each, dist, pass_on) for dist in order[:-1]]
        self.ready = lambda: (ready(1), ready(2), ready(0))

    @staticmethod
    def scratch(nd, rows, cols, parts):
        zn = nd // 2
        D, V = pltpu.SemaphoreType.DMA, pltpu.VMEM
        return [V((4, zn, rows, cols), bf16), V((4, zn, rows, cols), bf16), V((zn, rows, cols), bf16), V((2, zn, rows, cols), bf16),
                V((zn + 1, rows, cols), bf16), D((4, parts)), D((4, parts)), D((4, parts))] + [D((zn,))] * 9 + [D((2, zn))]


def plan(pipes, place, time_of, spots):
    ticks = {0: [place.greet], 1: [place.meet] + [functools.partial(p.start, col) for col in (3, 1, 2, 0) for p in pipes]}

    def put(when, fn):
        tick = next((t for t, us in enumerate(time_of) if us >= when), len(time_of))
        ticks.setdefault(tick, []).append(fn)

    todo = []
    for p, (diag, sides, side_gap, pass_on, pass_gap) in zip(pipes, spots):
        todo += [(diag, fn) for fn in p.diag] + [(sides, p.ready)]
        todo += [(sides + k * side_gap * 4 / len(p.sides), fn) for k, fn in enumerate(p.sides)]
        todo += [(pass_on + k * pass_gap * 4 / len(p.sides), fn) for k, fn in enumerate(p.pass_on)]
    for when, fn in sorted(todo, key=lambda e: e[0]):
        put(when, fn)
    return ticks


def pipes_of(nd, nf, g_refs, out_refs, split, scratch):
    def view(a, lead, o, w):
        return g_refs[a].at[:, :, :, pl.ds(o, w)] if lead is None else g_refs[a].at[lead, :, :, :, pl.ds(o, w)]
    per = len(scratch) // len(split)
    return [Scatter(nd, nf, [view(*v) for v in pipe], out_ref, *scratch[per * m : per * (m + 1)])
            for m, (pipe, out_ref) in enumerate(zip(split, out_refs))]


def widths(split):
    return [sum(v[3] for v in pipe) for pipe in split]


def pipes_scratch(nd, rows, split):
    return [x for pipe, w in zip(split, widths(split)) for x in Scatter.scratch(nd, rows, w, len(pipe))]


def run_ticks(ticks, now, last):
    planned = sorted((t, fns) for t, fns in ticks.items() if t <= last)

    def search(items):
        if len(items) == 1:
            tick, fns = items[0]

            @pl.when(now == tick)
            def _():
                for fn in fns:
                    fn()
            return
        mid = len(items) // 2
        lax.cond(now < items[mid][0], lambda: search(items[:mid]), lambda: search(items[mid:]))

    if planned:
        search(planned)


def run_rest(ticks, last):
    for tick, fns in sorted(ticks.items()):
        if tick > last:
            for fn in fns:
                fn()


class Spread:
    def __init__(self, nd, nf, src, got, send, recv):
        self.n, self.nf = nd * nf, nf
        self.me = lax.axis_index("dp") * nf + lax.axis_index("fsdp")
        self.src, self.got, self.send, self.recv = src, got, send, recv

    def peer(self, k):
        return lax.rem(self.me + k, self.n)

    def loop(self, fn):
        def body(k, carry):
            fn(k)
            return carry
        lax.fori_loop(1, self.n, body, 0)

    def greet(self):
        sem = pltpu.get_barrier_semaphore()

        def one(k):
            pl.semaphore_signal(sem, inc=1, device_id=(self.peer(k) // self.nf, self.peer(k) % self.nf), device_id_type=MESH)
        self.loop(one)

    def meet(self):
        pl.semaphore_wait(pltpu.get_barrier_semaphore(), self.n - 1)

    def copy(self, k):
        p = self.peer(k)
        src = self.src.at[p] if len(self.src.shape) == 3 else self.src
        return pltpu.make_async_remote_copy(src_ref=src, dst_ref=self.got.at[k], send_sem=self.send.at[k], recv_sem=self.recv.at[k],
                                            device_id=(p // self.nf, p % self.nf), device_id_type=MESH)

    def begin(self):
        self.loop(lambda k: self.copy(k).start())

    def total(self):
        own = self.src[self.me] if len(self.src.shape) == 3 else self.src[...]

        def add(k, total):
            self.copy(k).wait_recv()
            return total + self.got[k]
        total = lax.fori_loop(1, self.n, add, own)
        self.loop(lambda k: self.copy(k).wait_send())
        return total

    @staticmethod
    def scratch(n, tile):
        D = pltpu.SemaphoreType.DMA
        return [pltpu.VMEM((n,) + tile, f32), D((n,)), D((n,))]


def dot(a, b, dims=((1,), (0,)), precision=None):
    return lax.dot_general(a, b, (dims, ((), ())), preferred_element_type=f32, precision=precision)


def sigmoid(x):
    return 0.5 * jnp.tanh(0.5 * x) + 0.5


def conv_rows(ext, taps, masks, halo):
    rows = ext.shape[0] - halo
    width = 4
    v = ext[halo:]
    out = taps[4:5] + taps[3:4] * v
    for k in range(1, width):
        moved = pltpu.roll(ext, k, 0)[halo:]
        out = out + (taps[3 - k : 4 - k] * masks[:, k : k + 1]) * moved
    return out


def prep_kernel(bcdt_ref, taps_ref, heads_ref, segc_ref, segr_ref,
                m_ref, b_ref, c_ref, bt_ref, ct_ref, pre_ref, gm_ref, cum_ref, cumr_ref, sc_ref, dt_ref):
    T = bcdt_ref.shape[0]
    nc = T // L
    N = b_ref.shape[1]
    H = dt_ref.shape[1]
    groups = cumr_ref.shape[0]
    taps = taps_ref[...]
    tri = (lax.broadcasted_iota(jnp.int32, (L, L), 0) >= lax.broadcasted_iota(jnp.int32, (L, L), 1))
    trif = tri.astype(f32)
    neg_rate = -jnp.exp(heads_ref[0:1, :H]) * LOG2E
    m_ref[T : T + 8, :] = jnp.zeros((8, 4), f32)
    bias = heads_ref[1:2, :H]

    def chunk(c, carry):
        t0 = pl.multiple_of(c * L, L)
        here = pl.ds(t0, L)
        h0 = pl.multiple_of(jnp.maximum(t0 - 16, 0), 16)
        before = bcdt_ref[pl.ds(h0, 16), : 2 * N].astype(f32)
        v = bcdt_ref[here, : 2 * N].astype(f32)
        segc = segc_ref[here, :].astype(f32)
        seg_ext = jnp.concatenate([segc_ref[pl.ds(h0, 16), :].astype(f32), segc], axis=0)
        at = t0 + lax.broadcasted_iota(jnp.int32, (L, 1), 0)
        masks = [jnp.ones((L, 1), f32)]
        for k in range(1, 4):
            masks.append(((pltpu.roll(seg_ext, k, 0)[16:] == segc) & (at >= k)).astype(f32))
        masks = jnp.concatenate(masks, axis=1)
        m_ref[here, :] = masks
        pre = conv_rows(jnp.concatenate([before, v], axis=0), taps, masks, 16)
        pre_ref[here, :] = pre
        act = pre * sigmoid(pre)
        b = act[:, :N]
        cc = act[:, N:]
        bb = b.astype(bf16)
        cb = cc.astype(bf16)
        b_ref[here, :] = bb
        c_ref[here, :] = cb
        bt_ref[:, here] = b.T.astype(bf16)
        ct_ref[:, here] = cc.T.astype(bf16)
        prev = jnp.where(c > 0, seg_ext[15:16], -1.0)
        last = segc[L - 1 : L]
        same = segc == segr_ref[:, here].astype(f32)
        g = dot(cb, bb, ((1,), (1,)))
        gm_ref[pl.ds(c, 1)] = jnp.where(tri & same, g, 0.0)[None]
        raw = bcdt_ref[here, 2 * N : 2 * N + 128].astype(f32)[:, :H] + bias
        dt = jnp.maximum(raw, 0.0) + jnp.log1p(jnp.exp(-jnp.abs(raw)))
        a2 = neg_rate * dt
        cum = dot(trif, a2, precision=HIGHEST)
        end = cum[L - 1 : L]
        ein = jnp.where(segc == prev, jnp.exp2(cum), 0.0)
        lv = jnp.where(segc == last, jnp.exp2(end - cum), 0.0)
        dt_ref[here, :] = dt
        wide = jnp.concatenate([cum, jnp.zeros((L, 128 - H), f32)], axis=1)
        cum_ref[here, :] = wide
        cumt = wide.T
        for k in range(groups):
            cumr_ref[k, :, here] = cumt[HG * k : HG * (k + 1)]
        s0 = pl.multiple_of(c * (3 * L), L)
        for k, part in enumerate((dt, ein, lv)):
            sc_ref[pl.ds(s0 + k * L, L), :] = jnp.concatenate([part, jnp.zeros((L, 128 - H), f32)], axis=1).astype(bf16)
        return carry

    lax.fori_loop(0, nc, chunk, 0, unroll=2)


def prep(bcdt, taps, heads, segc, segr, N, H):
    T = bcdt.shape[0]
    nc = T // L
    G = H // HG
    S = jax.ShapeDtypeStruct
    full = lambda a: pl.BlockSpec(a.shape, lambda i: (0,) * a.ndim)
    outs = (S((T + 8, 4), f32), S((T, N), bf16), S((T, N), bf16), S((N, T), bf16), S((N, T), bf16), S((T, 2 * N), f32),
            S((nc, L, L), f32), S((T, 128), f32), S((G, HG, T), f32), S((3 * T, 128), bf16), S((T, H), f32))
    wide = 2 * N + 128
    return pl.pallas_call(
        prep_kernel,
        grid=(1,),
        in_specs=[pl.BlockSpec((T, wide), lambda i: (0, bcdt.shape[1] // wide - 1))] + [full(a) for a in (taps, heads, segc, segr)],
        out_specs=[full(o) for o in outs],
        out_shape=outs,
        compiler_params=pltpu.CompilerParams(vmem_limit_bytes=60 << 20),
    )(bcdt, taps, heads, segc, segr)


def lane_onehot(group, width, per):
    shape = (128, width)
    return (group * HG + lax.broadcasted_iota(jnp.int32, shape, 1) // per == lax.broadcasted_iota(jnp.int32, shape, 0)).astype(bf16)


def half_masks(P):
    lane = lax.broadcasted_iota(jnp.int32, (1, 2 * P), 1)
    first = (lane < P).astype(f32)
    return first.astype(bf16), (1.0 - first).astype(bf16)


def decay(cum4, cumr, k):
    return jnp.exp2(jnp.minimum(cum4[:, k : k + 1] - cumr[k : k + 1, :], 0.0))


def fwd_kernel(u_ref, gate_ref, taps_ref, m_ref, b_ref, c_ref, bt_ref, gm_ref, cum_ref, cumr_ref, sc_ref,
               gg_ref, r_ref, pre_ref, st_ref, state, move, ssq_ref):
    T, W = u_ref.shape
    P = W // HG
    nc = T // L
    step = pl.program_id(0)
    taps = taps_ref[...]
    gain = taps[5:6]
    skip = taps[6:7]
    onehot = lane_onehot(step, W, P)
    ma, mb = half_masks(P)
    state[...] = jnp.zeros_like(state)

    @pl.when(step == 0)
    def _():
        ssq_ref[...] = jnp.zeros_like(ssq_ref)

    @pl.when(step == 0)
    def _():
        def make(c, carry):
            here = pl.ds(pl.multiple_of(c * L, L), L)
            lag = lax.broadcasted_iota(jnp.int32, (L, L + 16), 0) + 16 - lax.broadcasted_iota(jnp.int32, (L, L + 16), 1)
            for k in range(1, 4):
                move[c, (k - 1) * L : k * L, :] = jnp.where(lag == k, m_ref[here, k : k + 1], 0.0).astype(bf16)
            return carry
        lax.fori_loop(0, nc, make, 0)

    def chunk(c, carry):
        t0 = pl.multiple_of(c * L, L)
        here = pl.ds(t0, L)
        h0 = pl.multiple_of(jnp.maximum(t0 - 16, 0), 16)
        v = u_ref[here, :]
        moved = dot(move[c], jnp.concatenate([u_ref[pl.ds(h0, 16), :], v], axis=0))
        pre = taps[4:5] + taps[3:4] * v.astype(f32)
        for k in range(1, 4):
            pre = pre + taps[3 - k : 4 - k] * moved[(k - 1) * L : k * L]
        pre_ref[here, :] = pre.astype(bf16)
        x = pre * sigmoid(pre)
        s0 = pl.multiple_of(c * (3 * L), L)
        exp = dot(sc_ref[pl.ds(s0, 3 * L), :], onehot)
        dtx, einx, lvx = exp[:L], exp[L : 2 * L], exp[2 * L :]
        xd = x * dtx
        xdb = xd.astype(bf16)
        gm = gm_ref[c]
        cum4 = pltpu.roll(cum_ref[here, :], 128 - step * HG, 1)
        cumr = cumr_ref[0, :, here]
        sb = state[...].astype(bf16)
        st_ref[c] = sb
        inner = []
        for p in range(HG // 2):
            m0 = (decay(cum4, cumr, 2 * p) * gm).astype(bf16)
            m1 = (decay(cum4, cumr, 2 * p + 1) * gm).astype(bf16)
            xp = xdb[:, 2 * P * p : 2 * P * (p + 1)]
            inner.append(dot(jnp.concatenate([m0, m1], axis=1), jnp.concatenate([xp * ma, xp * mb], axis=0)))
        y = jnp.concatenate(inner, axis=1) + dot(c_ref[here, :], sb) * einx + skip * x
        state[...] = state[...] * einx[L - 1 : L] + dot(bt_ref[:, here], (xd * lvx).astype(bf16))
        gate = gate_ref[here, :].astype(f32)
        g = y * (gate * sigmoid(gate))
        gg_ref[here, :] = (g * gain).astype(bf16)
        g2 = g * g
        tot = g2[:, :128]
        for j in range(1, W // 128):
            tot = tot + g2[:, 128 * j : 128 * (j + 1)]
        ssq_ref[here, :] += tot
        return carry

    lax.fori_loop(0, nc, chunk, 0, unroll=4)

    @pl.when(step == pl.num_programs(0) - 1)
    def _():
        def root(c, carry):
            here = pl.ds(pl.multiple_of(c * L, L), L)
            total = jnp.sum(ssq_ref[here, :], axis=1, keepdims=True)
            r_ref[here, :] = lax.rsqrt(total / (W * pl.num_programs(0)) + EPS)
            return carry
        lax.fori_loop(0, nc, root, 0)


def fwd(u, gate, taps, masks, b, c, bt, gm, cum, cumr, sc):
    T, E = gate.shape
    N = b.shape[1]
    G = cumr.shape[0]
    W = E // G
    nc = T // L
    S = jax.ShapeDtypeStruct
    col = lambda off: pl.BlockSpec((T, W), lambda g: (0, g + off))
    full = lambda a: pl.BlockSpec(a.shape, lambda g: (0,) * a.ndim)
    grp = lambda a: pl.BlockSpec((1,) + a.shape[1:], lambda g: (g, 0, 0))
    return pl.pallas_call(
        fwd_kernel,
        grid=(G,),
        in_specs=[col(0), col(0), pl.BlockSpec((8, W), lambda g: (0, g)), full(masks), full(b), full(c), full(bt), full(gm),
                  full(cum), grp(cumr), full(sc)],
        out_specs=[col(0), pl.BlockSpec((T, 1), lambda g: (0, 0)), col(0), pl.BlockSpec((nc, N, W), lambda g: (0, 0, g))],
        out_shape=(S((T, E), bf16), S((T, 1), f32), S((T, E), bf16), S((nc, N, E), bf16)),
        scratch_shapes=[pltpu.VMEM((N, W), f32), pltpu.VMEM((nc, 3 * L, L + 16), bf16), pltpu.VMEM((T, 128), f32)],
        compiler_params=pltpu.CompilerParams(vmem_limit_bytes=60 << 20),
        cost_estimate=pl.CostEstimate(flops=T * E * (2 * L + 4 * N) * 2, bytes_accessed=T * E * 12, transcendentals=T * E * 4),
    )(u, gate, taps, masks, b, c, bt, gm, cum, cumr, sc)


def bwd_scatter_kernel(nd, nf, g0, Gh, nc, arrays, split, *refs):
    g_refs, ins, outs = refs[:arrays], refs[arrays : arrays + 16], refs[arrays + 16 : arrays + 24]
    refs = refs[arrays + 24 :]
    sums, own, comm = refs[: len(split)], refs[len(split) : len(split) + 4], refs[len(split) + 4 :]
    pipes = pipes_of(nd, nf, g_refs, sums, split, comm)
    nb = ins[15].shape[0] // MB
    pairs = nc // 2
    time_of = [20.0 * g + (3.7 * i if i < pairs else 3.7 * pairs + 1.7 * (i - pairs)) for g in range(Gh) for i in range(pairs + nb)]
    ticks = plan(pipes, pipes[0], time_of, BWD_SPOTS)
    last = len(time_of) - 1
    bwd_body(lambda i: run_ticks(ticks, pl.program_id(0) * (pairs + nb) + i, last), g0, *ins, *outs, *own)

    @pl.when(pl.program_id(0) == pl.num_programs(0) - 1)
    def _():
        run_rest(ticks, last)
        for p in pipes:
            p.finish()


def bwd_body(tick, g0, u_ref, gate_ref, pre_ref, dm_ref, rq_ref, taps_ref, m_ref, b_ref, c_ref, ct_ref, gm_ref, cum_ref, cumr_ref, sc_ref, st_ref, normt_ref,
             dz_ref, gw_ref, dg_ref, db_ref, dc_ref, rs_ref, small_ref, kk_ref, ds, nxt, acc, move):
    T, W = u_ref.shape
    P = W // HG
    nc = T // L
    step = pl.program_id(0)
    taps = taps_ref[...]
    gain = taps[5:6]
    skip = taps[6:7]
    onehot = lane_onehot(step + g0, W, P)
    ma, mb = half_masks(P)
    ds[...] = jnp.zeros_like(ds)
    nxt[...] = jnp.zeros_like(nxt)
    acc[...] = jnp.zeros_like(acc)

    @pl.when(step == 0)
    def _():
        dg_ref[...] = jnp.zeros_like(dg_ref)
        db_ref[...] = jnp.zeros_like(db_ref)
        dc_ref[...] = jnp.zeros_like(dc_ref)
        rs_ref[...] = jnp.zeros_like(rs_ref)

    @pl.when(step == 0)
    def _():
        def make(c, carry):
            mrows = m_ref[pl.ds(pl.multiple_of(c * L, L), L + 8), :]
            lag = lax.broadcasted_iota(jnp.int32, (2 * L, L), 0) - lax.broadcasted_iota(jnp.int32, (2 * L, L), 1)
            for k in range(1, 4):
                col = jnp.concatenate([mrows[:, k : k + 1], jnp.zeros((L - 8, 1), f32)], axis=0)
                move[c, (k - 1) * L : k * L, :] = jnp.where(lag == k, col, 0.0).T[:, : L + 16].astype(bf16)
            return carry
        lax.fori_loop(0, nc, make, 0)

    ri = lax.broadcasted_iota(jnp.int32, (4 * W, 128), 0)
    ci = lax.broadcasted_iota(jnp.int32, (4 * W, 128), 1)
    part = ri // W
    want = (jnp.maximum(part - 1, 0) * pl.num_programs(0) + step) * HG + (ri % W) // P
    fold = (want == ci).astype(bf16)

    def eight(z):
        return jnp.sum(z.reshape(L // 8, 8, W), axis=0)

    def chunk(i, carry):
        c = nc - 1 - i
        t0 = pl.multiple_of(c * L, L)
        here = pl.ds(t0, L)
        u = u_ref[here, :].astype(f32)
        pre = pre_ref[here, :].astype(f32)
        sig = sigmoid(pre)
        x = pre * sig
        dsilu = sig + x * (1.0 - sig)
        s0 = pl.multiple_of(c * (3 * L), L)
        exp = dot(sc_ref[pl.ds(s0, 3 * L), :], onehot)
        dtx, einx, lvx = exp[:L], exp[L : 2 * L], exp[2 * L :]
        xdb = (x * dtx).astype(bf16)
        xd = xdb.astype(f32)
        gm = gm_ref[c]
        cum4 = pltpu.roll(cum_ref[here, :], 128 - (step + g0) * HG, 1)
        cumr = cumr_ref[0, :, here]
        sb = st_ref[c]
        es, ms, inner = [], [], []
        for p in range(HG // 2):
            e0 = decay(cum4, cumr, 2 * p)
            e1 = decay(cum4, cumr, 2 * p + 1)
            m0 = (e0 * gm).astype(bf16)
            m1 = (e1 * gm).astype(bf16)
            xp = xdb[:, 2 * P * p : 2 * P * (p + 1)]
            inner.append(dot(jnp.concatenate([m0, m1], axis=1), jnp.concatenate([xp * ma, xp * mb], axis=0)))
            es.append((e0, e1))
            ms.append((m0, m1))
        yn = jnp.concatenate(inner, axis=1) + dot(c_ref[here, :], sb) * einx
        y = yn + skip * x
        gate = gate_ref[here, :].astype(f32)
        sgate = sigmoid(gate)
        silu_g = gate * sgate
        g = y * silu_g
        r = rq_ref[here, 0:1]
        q = rq_ref[here, 1:2]
        dmr = dm_ref[here, :].astype(f32) * r
        dgg = gain * dmr - g * q
        dyb = (dgg * silu_g).astype(bf16)
        dy = dyb.astype(f32)
        dz_ref[0, here, :] = (dgg * y * (sgate + silu_g * (1.0 - sgate))).astype(bf16)
        dxi = []
        dgc = dg_ref[c]
        for p in range(HG // 2):
            cols = slice(2 * P * p, 2 * P * (p + 1))
            dp = dyb[:, cols]
            dstack = jnp.concatenate([dp * ma, dp * mb], axis=0)
            dmm = dot(dstack, xdb[:, cols], ((1,), (1,)))
            dgc = dgc + dmm[:L] * es[p][0] + dmm[L:] * es[p][1]
            dxi.append(dot(jnp.concatenate(ms[p], axis=0), dstack, ((0,), (0,))))
        dg_ref[c] = dgc
        dxi = jnp.concatenate(dxi, axis=1)
        dsn = ds[...]
        dsb = dsn.astype(bf16)
        dye = (dy * einx).astype(bf16)
        dc_ref[here, :] += dot(dye, sb, ((1,), (1,)))
        kept = einx[L - 1 : L]
        kk_ref[pl.ds(c, 1), :] = kept * jnp.sum(sb.astype(f32) * dsn, axis=0, keepdims=True)
        db_ref[here, :] += dot((xd * lvx).astype(bf16), dsb, ((1,), (1,)))
        dxe = dot(b_ref[here, :], dsb) * lvx
        ds[...] = dsn * kept + dot(ct_ref[:, here], dye)
        dxd = dxi + dxe
        r1 = dy * yn - xd * dxi
        r1h = r1.astype(bf16)
        r1l = (r1 - r1h.astype(f32)).astype(bf16)
        rs_ref[here, :] += dot(jnp.concatenate([r1h, r1l, (xd * dxe).astype(bf16), (x * dxd).astype(bf16)], axis=1), fold)
        dpre = (dxd * dtx + skip * dy) * dsilu
        dpb = dpre.astype(bf16)
        moved = dot(move[c], jnp.concatenate([dpb, nxt[...]], axis=0))
        nxt[...] = dpb[:16]
        du = taps[3:4] * dpre
        acc[0:8, :] += eight(dmr * g)
        acc[8:16, :] += eight(dy * x)
        acc[16:24, :] += eight(dpre)
        acc[24:32, :] += eight(dpre * u)
        for k in range(1, 4):
            sk = moved[(k - 1) * L : k * L]
            du = du + taps[3 - k : 4 - k] * sk
            acc[24 + 8 * k : 32 + 8 * k, :] += eight(sk * u)
        dz_ref[1, here, :] = du.astype(bf16)
        return carry

    def pair(i, carry):
        tick(i)
        chunk(2 * i, carry)
        return chunk(2 * i + 1, carry)

    lax.fori_loop(0, nc // 2, pair, 0)
    for j in range(7):
        small_ref[j : j + 1, :] = jnp.sum(acc[8 * j : 8 * j + 8, :], axis=0, keepdims=True)
    small_ref[7:8, :] = jnp.zeros((1, W), f32)

    def weights(i, carry):
        tick(nc // 2 + i)
        rows = pl.ds(pl.multiple_of(i * MB, MB), MB)
        for kind in range(2):
            gw_ref[kind, rows, :] = dot(normt_ref[rows, :], dz_ref[kind]).astype(bf16)
        return carry

    lax.fori_loop(0, normt_ref.shape[0] // MB, weights, 0)


def bwd(half, halves, u, gate, pre, dm, rq, taps, masks, b, c, ct, gm, cum, cumr, sc, st, normt, comm):
    T, E = gate.shape
    N = b.shape[1]
    G = cumr.shape[0]
    W = E // G
    nc = T // L
    Gh = G // halves
    Eh = E // halves
    g0 = half * Gh
    S = jax.ShapeDtypeStruct
    col = pl.BlockSpec((T, W), lambda g: (0, g + g0))
    full = lambda a: pl.BlockSpec(a.shape, lambda g: (0,) * a.ndim)
    whole = lambda s: pl.BlockSpec(s, lambda g: (0,) * len(s))
    grp = lambda a: pl.BlockSpec((1,) + a.shape[1:], lambda g: (g + g0, 0, 0))
    in_specs = [col, col, col, col, full(rq), pl.BlockSpec((8, W), lambda g: (0, g + g0)), full(masks), full(b), full(c),
                full(ct), full(gm), full(cum), grp(cumr), full(sc), pl.BlockSpec((nc, N, W), lambda g: (0, 0, g + g0)), full(normt)]
    D = normt.shape[0]
    out_specs = [pl.BlockSpec((2, T, W), lambda g: (0, 0, g)), pl.BlockSpec((2, D, W), lambda g: (0, 0, g)), whole((nc, L, L)), whole((T, N)), whole((T, N)),
                 whole((T, 128)), pl.BlockSpec((8, W), lambda g: (0, g)), pl.BlockSpec((nc, W), lambda g: (0, g))]
    out_shape = [S((2, T, Eh), bf16), S((2, D, Eh), bf16), S((nc, L, L), f32), S((T, N), f32), S((T, N), f32), S((T, 128), f32), S((8, Eh), f32), S((nc, Eh), f32)]
    scratch = [pltpu.VMEM((N, W), f32), pltpu.VMEM((16, W), bf16), pltpu.VMEM((56, W), f32), pltpu.VMEM((nc, 3 * L, L + 16), bf16)]
    nd, nf, cid, first, split = comm
    rows = first[0].shape[-2]
    return pl.pallas_call(
        functools.partial(bwd_scatter_kernel, nd, nf, g0, Gh, nc, len(first), split),
        grid=(Gh,),
        in_specs=[pl.BlockSpec(memory_space=pl.ANY)] * len(first) + in_specs,
        out_specs=out_specs + [whole((rows, w)) for w in widths(split)],
        out_shape=out_shape + [S((rows, w), f32) for w in widths(split)],
        scratch_shapes=scratch + pipes_scratch(nd, rows, split),
        compiler_params=pltpu.CompilerParams(vmem_limit_bytes=60 << 20, collective_id=cid, has_side_effects=True),
        cost_estimate=pl.CostEstimate(flops=T * Eh * (8 * L + 12 * N + 4 * D), bytes_accessed=T * Eh * 16, transcendentals=T * Eh * 4),
    )(*first, u, gate, pre, dm, rq, taps, masks, b, c, ct, gm, cum, cumr, sc, st, normt)


def post_kernel(bcdt_ref, pre_ref, taps_ref, heads_ref, m_ref, segc_ref, segr_ref, b_ref, c_ref, dg0_ref, db0_ref, dc0_ref, rs0_ref, dg1_ref, db1_ref, dc1_ref, rs1_ref, kk_ref, dt_ref,
                out_ref, small_ref, hs_ref, nxt, acc, hacc):
    T = bcdt_ref.shape[0]
    nc = T // L
    N = b_ref.shape[1]
    H = dt_ref.shape[1]
    taps = taps_ref[...]
    tri = (lax.broadcasted_iota(jnp.int32, (L, L), 0) >= lax.broadcasted_iota(jnp.int32, (L, L), 1))
    upper = (lax.broadcasted_iota(jnp.int32, (L, L), 0) <= lax.broadcasted_iota(jnp.int32, (L, L), 1)).astype(f32)
    strict = 1.0 - upper
    rate = -jnp.exp(heads_ref[0:1, :H])
    bias = heads_ref[1:2, :H]
    nxt[...] = jnp.zeros_like(nxt)
    acc[...] = jnp.zeros_like(acc)
    hacc[...] = jnp.zeros_like(hacc)

    def eight(z):
        return jnp.sum(z.reshape(L // 8, 8, z.shape[1]), axis=0)

    def chunk(i, carry):
        c = nc - 1 - i
        t0 = pl.multiple_of(c * L, L)
        here = pl.ds(t0, L)
        same = segc_ref[here, :] == segr_ref[:, here]
        dg = jnp.where(tri & same, dg0_ref[c] + dg1_ref[c], 0.0)
        dgb = dg.astype(bf16)
        dcv = dc0_ref[here, :] + dc1_ref[here, :] + dot(dgb, b_ref[here, :])
        dbv = db0_ref[here, :] + db1_ref[here, :] + dot(dg.T.astype(bf16), c_ref[here, :])
        pre = pre_ref[here, :]
        sig = sigmoid(pre)
        dpre = jnp.concatenate([dbv, dcv], axis=1) * (sig + pre * sig * (1.0 - sig))
        v = bcdt_ref[here, : 2 * N].astype(f32)
        ext = jnp.concatenate([dpre, nxt[...]], axis=0)
        nxt[...] = dpre[:8]
        dv = taps[3:4] * dpre
        acc[0:8, :] += eight(dpre)
        acc[8:16, :] += eight(dpre * v)
        mrows = m_ref[pl.ds(t0, L + 8), :]
        for k in range(1, 4):
            sk = pltpu.roll(ext * mrows[:, k : k + 1], L + 8 - k, 0)[:L]
            dv = dv + taps[3 - k : 4 - k] * sk
            acc[8 + 8 * k : 16 + 8 * k, :] += eight(sk * v)
        out_ref[here, : 2 * N] = dv.astype(bf16)
        q = H // 2
        r0, r1 = rs0_ref[here, :], rs1_ref[here, :]
        r1, r2, r3 = (jnp.concatenate([r0[:, m * q : (m + 1) * q], r1[:, m * q : (m + 1) * q]], axis=1) for m in range(3))
        da = dot(upper, r1, precision=HIGHEST) + dot(strict, r2, precision=HIGHEST) + kk_ref[pl.ds(c, 1), :]
        dt = dt_ref[here, :]
        raw = bcdt_ref[here, 2 * N : 2 * N + 128].astype(f32)[:, :H] + bias
        ddt = (r3 + da * rate) * sigmoid(raw)
        hacc[0:8, :] += eight(da * rate * dt)
        hacc[8:16, :] += eight(ddt)
        out_ref[here, 2 * N :] = jnp.concatenate([ddt, jnp.zeros((L, out_ref.shape[1] - 2 * N - H), f32)], axis=1).astype(bf16)
        return carry

    lax.fori_loop(0, nc, chunk, 0, unroll=2)
    for j in range(5):
        small_ref[j : j + 1, :] = jnp.sum(acc[8 * j : 8 * j + 8, :], axis=0, keepdims=True)
    small_ref[5:8, :] = jnp.zeros((3, 2 * N), f32)
    for j in range(2):
        hs_ref[j : j + 1, :] = jnp.sum(hacc[8 * j : 8 * j + 8, :], axis=0, keepdims=True)


def post(bcdt, pre, taps, heads, masks, segc, segr, b, c, first, second, kk, dt):
    T = bcdt.shape[0]
    N = b.shape[1]
    H = dt.shape[1]
    S = jax.ShapeDtypeStruct
    wide = 2 * N + 128
    full = lambda a: pl.BlockSpec(a.shape, lambda i: (0,) * a.ndim)
    ins = (bcdt, pre, taps, heads, masks, segc, segr, b, c, *first, *second, kk, dt)
    outs = (S((T, wide), bf16), S((8, 2 * N), f32), S((2, H), f32))
    return pl.pallas_call(
        post_kernel,
        grid=(1,),
        in_specs=[pl.BlockSpec((T, wide), lambda i: (0, bcdt.shape[1] // wide - 1))] + [full(a) for a in ins[1:]],
        out_specs=[full(o) for o in outs],
        out_shape=outs,
        scratch_shapes=[pltpu.VMEM((8, 2 * N), f32), pltpu.VMEM((40, 2 * N), f32), pltpu.VMEM((16, H), f32)],
        compiler_params=pltpu.CompilerParams(vmem_limit_bytes=60 << 20),
    )(*ins)


NT = 256


def tail_kernel(nd, nf, arrays, split, tiles, *refs):
    g_refs, refs = refs[:arrays], refs[arrays:]
    (wo_hbm, wg_hbm, wa_hbm, gg_ref, dz0_ref, dz1_ref, dbc_ref, hid_ref, go_ref, r_ref, gain_ref, mine_ref,
     suma_ref, sumb_ref, out_ref, gin_ref, small_ref) = refs[:17]
    wo, wg, wa, acc, sem = refs[17:22]
    mine = Spread(nd, nf, mine_ref, *refs[22:25])
    pipes = pipes_of(nd, nf, g_refs, (suma_ref, sumb_ref), split, refs[25:])
    D, E = wg.shape
    Eh = E // 2
    step = pl.program_id(0)
    early = tiles // 2
    blocks = D // NT
    mid = (early + tiles) * blocks
    scale = 4 / tiles
    time_of = [4 + 0.75 * scale * t if t < early * blocks else
               (13 + 1.65 * scale * (t - early * blocks) if t < mid else 52.6 + 0.65 * scale * (t - mid)) for t in range(2 * tiles * blocks)]
    ticks = plan(pipes, mine, time_of, TAIL_SPOTS)
    last = len(time_of) - 1
    ticks[1].append(mine.begin)
    fetch = [pltpu.make_async_copy(src, dst, sem.at[k]) for k, (src, dst) in enumerate(((wo_hbm, wo), (wg_hbm, wg), (wa_hbm, wa)))]

    @pl.when(step == 0)
    def _():
        for cp in fetch:
            cp.start()
        run_ticks(ticks, 0, 0)
        fetch[0].wait()

    @pl.when(step == early)
    def _():
        fetch[1].wait()
        fetch[2].wait()

    back = (step >= early) & (step < early + tiles)
    in_back = lambda t: early * blocks <= t < (early + tiles) * blocks

    @pl.when(jnp.logical_not(back))
    def _():
        def block(j, carry):
            run_ticks({t: f for t, f in ticks.items() if t and not in_back(t)}, step * blocks + j, last)
            cols = pl.ds(pl.multiple_of(j * NT, NT), NT)
            out_ref[:, cols] = (hid_ref[:, cols].astype(f32) + r_ref[...] * dot(gg_ref[...], wo[:, cols])).astype(bf16)
            return carry
        lax.fori_loop(0, blocks, block, 0)

    @pl.when(back)
    def _():
        def block(j, carry):
            run_ticks({t: f for t, f in ticks.items() if in_back(t)}, step * blocks + j, last)
            cols = pl.ds(pl.multiple_of(j * NT, NT), NT)
            part = dot(dz0_ref[0], wg[cols, :Eh], ((1,), (1,))) + dot(dz1_ref[0], wg[cols, Eh:], ((1,), (1,)))
            part = part + dot(dz0_ref[1], wa[cols, :Eh], ((1,), (1,))) + dot(dz1_ref[1], wa[cols, Eh:E], ((1,), (1,)))
            acc[:, cols] = part + dot(dbc_ref[...], wa[cols, E:], ((1,), (1,)))
            return carry
        lax.fori_loop(0, blocks, block, 0)
        gain = gain_ref[...]

        def rows_of(i, carry):
            here = pl.ds(pl.multiple_of(i * 64, 64), 64)
            rows = hid_ref[here, :].astype(f32)
            rinv = lax.rsqrt(jnp.mean(rows * rows, axis=-1, keepdims=True) + EPS)
            xhat = rows * rinv
            bn = acc[here, :]
            gb = bn * gain
            mean = jnp.mean(gb * xhat, axis=-1, keepdims=True)
            gin_ref[here, :] = (go_ref[here, :].astype(f32) + rinv * (gb - xhat * mean)).astype(bf16)
            return carry
        lax.fori_loop(0, hid_ref.shape[0] // 64, rows_of, 0)

    @pl.when(step == 2 * tiles - 1)
    def _():
        run_rest(ticks, last)
        for p in pipes:
            p.finish()
        small_ref[...] = mine.total()


def tail(nd, nf, cid, gs, split, dz0, dz1, dbcdt, full_gate, full_a, gg, full_out, hidden, grad_out, r, norm_gain, mine):
    T, D = hidden.shape
    E = full_out.shape[0]
    n = nd * nf
    rows = gs[0].shape[-2]
    MT = 256 if rows % 16 == 0 else 128
    tiles = T // MT
    early = tiles // 2
    wide = dbcdt.shape[1]
    S = jax.ShapeDtypeStruct
    any_ = pl.BlockSpec(memory_space=pl.ANY)
    whole = lambda s: pl.BlockSpec(s, lambda k: (0,) * len(s), pipeline_mode=pl.Buffered(1))
    at_out = lambda k: jnp.minimum(k, early - 1) + jnp.clip(k - tiles - early + 1, 0, tiles - early)
    at_back = lambda k: jnp.clip(k - early, 0, tiles - 1)
    at_row = lambda k: k - early * jnp.clip(k - early + 1, 0, 1) - (tiles - early) * jnp.clip(k - early - tiles + 1, 0, 1)
    out_tile = lambda w: pl.BlockSpec((MT, w), lambda k: (at_out(k), 0))
    back_tile = lambda w: pl.BlockSpec((MT, w), lambda k: (at_back(k), 0))
    half = pl.BlockSpec((2, MT, E // 2), lambda k: (0, at_back(k), 0))
    tile = mine.shape[1:]
    return pl.pallas_call(
        functools.partial(tail_kernel, nd, nf, len(gs), split, tiles),
        grid=(2 * tiles,),
        in_specs=[any_] * (len(gs) + 3) + [out_tile(E), half, half, back_tile(wide), pl.BlockSpec((MT, D), lambda k: (at_row(k), 0)), back_tile(D),
                                           out_tile(1), whole((1, D)), whole(mine.shape)],
        out_specs=[whole((rows, w)) for w in widths(split)] + [out_tile(D), back_tile(D), whole(tile)],
        out_shape=[S((rows, w), f32) for w in widths(split)] + [S((T, D), bf16), S((T, D), bf16), S(tile, f32)],
        scratch_shapes=[pltpu.VMEM((E, D), bf16), pltpu.VMEM((D, E), bf16), pltpu.VMEM((D, E + wide), bf16), pltpu.VMEM((MT, D), f32),
                        pltpu.SemaphoreType.DMA((3,))]
        + Spread.scratch(n, tile) + pipes_scratch(nd, rows, split),
        compiler_params=pltpu.CompilerParams(collective_id=cid, has_side_effects=True, vmem_limit_bytes=67043328),
        cost_estimate=pl.CostEstimate(flops=2 * T * D * 3 * E, bytes_accessed=8 * D * E, transcendentals=0),
    )(*gs, full_out, full_gate, full_a, gg, dz0, dz1, dbcdt, hidden, grad_out, r, norm_gain, mine)


def finish_kernel(gate0_ref, gate1_ref, u0_ref, u1_ref, oa_ref, ob_ref, tot_ref, wzx_ref, wbc_ref, wdt_ref, gain_ref, o_ref, gi_ref,
                  oo_ref, go_ref, zx_ref, bc_ref, dt_ref, out_ref, conv_ref, n_ref, gg_ref, heads_ref):
    oo_ref[...] = o_ref[...]
    go_ref[...] = gi_ref[...]

    @pl.when(pl.program_id(0) == 0)
    def _():
        Eh = gate0_ref.shape[1]
        for k, ref in enumerate((gate0_ref, gate1_ref, u0_ref)):
            zx_ref[:, k * Eh : (k + 1) * Eh] = ref[...]
        zx_ref[:, 3 * Eh :] = u1_ref[:, :Eh]
        wide = bc_ref.shape[1]
        bc_ref[...] = u1_ref[:, Eh : Eh + wide]
        dt_ref[...] = u1_ref[:, Eh + wide : Eh + wide + 128][:, : dt_ref.shape[1]]
        half = oa_ref.shape[1]
        out_ref[:, :half] = oa_ref[...]
        out_ref[:, half:] = ob_ref[...]
        k1 = conv_ref.shape[0]
        conv_ref[...] = tot_ref[:k1, : conv_ref.shape[1]]
        gg_ref[...] = tot_ref[k1 : k1 + 1, : gg_ref.shape[1]]
        heads_ref[...] = tot_ref[k1 + 1 : k1 + 1 + heads_ref.shape[0], : heads_ref.shape[1]]
        dots = lambda w, g: jnp.sum(w.astype(f32) * g, axis=1, keepdims=True)
        total = dots(wzx_ref[...], zx_ref[...]) + dots(wbc_ref[...], bc_ref[...]) + dots(wdt_ref[...], dt_ref[...])
        n_ref[...] = total / gain_ref[...].astype(f32)


def finish(gate0, gate1, u0, u1, s_out, tot, w_zx, w_bc, w_dt, gain, output, grad_in, shapes):
    S = jax.ShapeDtypeStruct
    tile = pl.BlockSpec((256, output.shape[1]), lambda i: (i, 0))
    return pl.pallas_call(
        finish_kernel,
        grid=(output.shape[0] // 256,),
        in_specs=[pl.BlockSpec(a.shape, lambda i: (0, 0)) for a in (gate0, gate1, u0, u1, *s_out, tot, w_zx, w_bc, w_dt, gain)] + [tile, tile],
        out_specs=[tile, tile] + [pl.BlockSpec(s, lambda i: (0, 0)) for s in shapes],
        out_shape=[S(output.shape, bf16), S(output.shape, bf16)] + [S(s, f32) for s in shapes],
        compiler_params=pltpu.CompilerParams(vmem_limit_bytes=63 << 20),
    )(gate0, gate1, u0, u1, *s_out, tot, w_zx, w_bc, w_dt, gain, output, grad_in)


def norm_kernel(hid_ref, gain_ref, normed_ref, normt_ref):
    rows = hid_ref[...].astype(f32)
    normed = rows * lax.rsqrt(jnp.mean(rows * rows, axis=-1, keepdims=True) + EPS) * gain_ref[...]
    normed_ref[...] = normed.astype(bf16)
    normt_ref[...] = normed.T.astype(bf16)


def norm(hidden, gain):
    T, D = hidden.shape
    S = jax.ShapeDtypeStruct
    row = pl.BlockSpec((256, D), lambda i: (i, 0))
    return pl.pallas_call(
        norm_kernel,
        grid=(T // 256,),
        in_specs=[row, pl.BlockSpec((1, D), lambda i: (0, 0))],
        out_specs=[row, pl.BlockSpec((D, 256), lambda i: (0, i))],
        out_shape=(S((T, D), bf16), S((D, T), bf16)),
        compiler_params=pltpu.CompilerParams(vmem_limit_bytes=40 << 20),
    )(hidden, gain)


def layer(nd, nf, hidden, grad_out, seg, shard_a, shard_gate, shard_out, head_params, owned, sizes):
    w_zx, w_bc, w_dt, own_gain = owned
    n = nd * nf
    E, N, H, K1, S = sizes
    T, D = hidden.shape
    wide = 2 * N + 128
    full_gate = lax.all_gather(shard_gate, AXES, axis=0, tiled=True)
    full_out = lax.all_gather(shard_out, AXES, axis=0, tiled=True)
    full_a = gather_rows(shard_a, nd, nf, 0)
    off = E + 2 * N + H
    flat = full_a[:, :, off : off + S].reshape(n, -1)
    ncol, nrow, ngate = (E + 2 * N) // n, D // n, E // n
    conv = flat[:, : K1 * ncol].reshape(n, K1, ncol).transpose(1, 0, 2).reshape(K1, n * ncol).astype(f32)
    norm_gain = flat[:, K1 * ncol : K1 * ncol + nrow].reshape(-1).astype(f32)
    gate_gain = flat[:, K1 * ncol + nrow : K1 * ncol + nrow + ngate].reshape(-1).astype(f32)
    full_a = full_a.reshape(D, E + wide)
    normed, normt = norm(hidden, norm_gain[None])
    ubc = dot(normed, full_a).astype(bf16)
    gate = dot(normed, full_gate).astype(bf16)
    segc, segr = seg[:, None], seg[None, :]
    taps_u = jnp.concatenate([conv[:, :E], gate_gain[None], jnp.repeat(head_params[2], E // H)[None], jnp.zeros((1, E), f32)], axis=0)
    taps_bc = jnp.concatenate([conv[:, E:], jnp.zeros((3, 2 * N), f32)], axis=0)
    masks, b, c, bt, ct, pre_bc, gm, cum, cumr, sc, dt = prep(ubc, taps_bc, head_params, segc, segr, N, H)
    gg, r, pre, st = fwd(ubc, gate, taps_u, masks, b, c, bt, gm, cum, cumr, sc)
    gos = (grad_out.astype(f32) * r).astype(bf16)
    g_out = dot(gg, gos, ((0,), (0,))).astype(bf16)
    g_out, full_out = lax.optimization_barrier((g_out, full_out))
    dm = dot(grad_out, full_out, ((1,), (1,))).astype(bf16)
    s = jnp.sum(gg.astype(f32) * dm.astype(f32), axis=1, keepdims=True)
    rq = jnp.concatenate([r, r * r * r * s / E], axis=1)
    back = functools.partial(bwd, u=ubc, gate=gate, pre=pre, dm=dm, rq=rq, taps=taps_u, masks=masks, b=b, c=c, ct=ct, gm=gm, cum=cum,
                             cumr=cumr, sc=sc, st=st, normt=normt)
    zn = max(nd // 2, 1)
    rows_of = lambda g: g.reshape(g.shape[:-2] + (zn, n // zn, g.shape[-2] // n, g.shape[-1]))
    Eh = E // 2
    dz0, gw0, dg0, db0, dc0, rs0, small0, kk0, *s_out = back(
        0, 2, comm=(nd, nf, 4, (rows_of(g_out),), (((0, None, 0, D // 2),), ((0, None, D // 2, D // 2),))))
    dz1, gw1, dg1, db1, dc1, rs1, small1, kk1, gate0, u0 = back(1, 2, comm=(nd, nf, 3, (rows_of(gw0),), (((0, 0, 0, Eh),), ((0, 1, 0, Eh),))))
    small = jnp.concatenate([small0, small1], axis=1)
    kk = jnp.concatenate([kk0, kk1], axis=1)
    kkh = jnp.sum(kk.reshape(kk.shape[0], H, E // H), axis=2)
    dbcdt, small_bc, hs = post(ubc, pre_bc, taps_bc, head_params, masks, segc, segr, b, c, (dg0, db0, dc0, rs0), (dg1, db1, dc1, rs1), kkh, dt)
    d_conv = jnp.concatenate([jnp.stack([small[6], small[5], small[4], small[3], small[2]]),
                              jnp.stack([small_bc[4], small_bc[3], small_bc[2], small_bc[1], small_bc[0]])], axis=1)
    d_heads = jnp.concatenate([hs, jnp.sum(small[1].reshape(1, H, E // H), axis=2)], axis=0)
    lanes = -(-max(ncol, ngate, H) // 128) * 128
    cols = lambda a: jnp.pad(a.reshape(-1, n, a.shape[1] // n).transpose(1, 0, 2), ((0, 0), (0, 0), (0, lanes - a.shape[1] // n)))
    heads_row = jnp.broadcast_to(jnp.pad(d_heads, ((0, 0), (0, lanes - H)))[None], (n, d_heads.shape[0], lanes))
    used = K1 + 1 + d_heads.shape[0]
    mine = jnp.concatenate([cols(d_conv), cols(small[:1]), heads_row, jnp.zeros((n, -(-used // 8) * 8 - used, lanes), f32)], axis=1)
    g_bcdt = dot(normt, dbcdt).astype(bf16)
    split = (((0, 0, 0, Eh),), ((0, 1, 0, Eh), (1, None, 0, wide)))
    gate1, u1, output, grad_in, tot = tail(nd, nf, 1, (rows_of(gw1), rows_of(g_bcdt)), split, dz0, dz1, dbcdt, full_gate, full_a, gg,
                                                   full_out, hidden, grad_out, r, norm_gain[None], mine)
    output, grad_in, s_zx, s_bc, s_dt, s_w, t_conv, t_norm, t_gate, t_heads = finish(
        gate0, gate1, u0, u1, s_out, tot, w_zx, w_bc, w_dt, own_gain, output, grad_in,
        ((nrow, 2 * E), (nrow, 2 * N), (nrow, H), (E // n, D), (K1, ncol), (nrow, 1), (1, ngate), d_heads.shape))
    return output, grad_in, s_zx, s_bc, s_dt, s_w, t_conv, t_norm.reshape(-1), t_gate.reshape(-1), t_heads


def per_device(nd, nf, hidden, grad_out, segment_ids, w_zx, w_bc, w_dt, w_out, conv_params, norm_gain, gate_gain, head_params):
    n = nd * nf
    E, N2, H = w_out.shape[0] * n, w_bc.shape[1], w_dt.shape[1]
    rows = w_zx.shape[0]
    small = jnp.concatenate([conv_params.reshape(-1), norm_gain, gate_gain])
    S = -(-small.shape[0] // rows)
    assert S + H <= 128
    small = jnp.pad(small, (0, S * rows - small.shape[0])).reshape(rows, S)
    shard_a = jnp.concatenate([w_zx[:, E:], w_bc, w_dt, small, jnp.zeros((rows, 128 - H - S), bf16)], axis=1)
    return layer(nd, nf, hidden, grad_out, segment_ids, shard_a, w_zx[:, :E], w_out, head_params, (w_zx, w_bc, w_dt, norm_gain[:, None]),
                 (E, N2 // 2, H, conv_params.shape[0], S))


def solution(mesh):
    row, col, vec, rep = P(AXES, None), P(None, AXES), P(AXES), P()
    return jax.shard_map(
        functools.partial(per_device, mesh.shape["dp"], mesh.shape["fsdp"]),
        mesh=mesh,
        in_specs=(row, row, vec, row, row, row, row, col, vec, vec, rep),
        out_specs=(row, row, row, row, row, row, col, vec, vec, rep),
        check_vma=False,
    )
```

```python
import functools
import jax
import jax.numpy as jnp
from jax import lax
from jax.experimental import pallas as pl
from jax.experimental.pallas import tpu as pltpu
from jax.sharding import PartitionSpec as P

EPS = 1e-05
L = 128
HG = 8
LOG2E = 1.4426950408889634
MB = 512
BWD_SPOTS = ((5.0, 10.0, 2.0, 26.0, 3.2), (7.0, 16.5, 2.0, 39.0, 3.2))
TAIL_SPOTS = ((7.0, 13.0, 3.0, 30.0, 4.0), (9.0, 22.0, 3.0, 46.0, 3.0))
bf16, f32 = jnp.bfloat16, jnp.float32
HIGHEST = lax.Precision.HIGHEST


AXES = ("dp", "fsdp")
MESH = pl.DeviceIdType.MESH


class Place:
    def __init__(self, nd, nf):
        self.zn, self.nf = nd // 2, nf
        d, f = lax.axis_index("dp"), lax.axis_index("fsdp")
        self.z, self.y = d // 2, d % 2
        self.x, self.c = f // 2, f % 2

    def dev(self, z, y, x, c):
        return (z * 2 + y, x * 2 + c)

    def idx(self, z, y, x, c):
        return (z * 2 + y) * self.nf + x * 2 + c

    def meet(self):
        z, zn = self.z, self.zn
        pl.semaphore_wait(pltpu.get_barrier_semaphore(), 3 + (z + zn - 1) // zn + (2 * zn - 2 - z) // zn)

    def greet(self):
        z, y, x, c, zn = self.z, self.y, self.x, self.c, self.zn
        sem = pltpu.get_barrier_semaphore()
        for there in ((z, y, 1 - x, c), (z, 1 - y, x, c), (z, y, x, 1 - c)):
            pl.semaphore_signal(sem, inc=1, device_id=self.dev(*there), device_id_type=MESH)

        @pl.when(z > 0)
        def _():
            pl.semaphore_signal(sem, inc=1, device_id=self.dev(z - 1, y, x, c), device_id_type=MESH)

        @pl.when(z < zn - 1)
        def _():
            pl.semaphore_signal(sem, inc=1, device_id=self.dev(z + 1, y, x, c), device_id_type=MESH)


def gather_kernel(nd, nf, src_ref, out_ref, own_sem, z_send, z_recv, x_send, x_recv, y_send, y_recv, dx_send, dx_recv, dy_send, dy_recv, c_send, c_recv):
    at = Place(nd, nf)
    z, y, x, c, zn = at.z, at.y, at.x, at.c, at.zn
    half = out_ref.shape[2] // 256 * 128
    lo, hi = pl.ds(0, half), pl.ds(half, out_ref.shape[2] - half)
    at.greet()
    at.meet()

    def copy(block, to, send, recv, cols=None, src=None):
        ref = out_ref.at[block] if cols is None else out_ref.at[block, :, cols]
        return pltpu.make_async_remote_copy(src_ref=ref if src is None else src, dst_ref=ref, send_sem=send, recv_sem=recv,
                                            device_id=at.dev(*to), device_id_type=MESH)

    def block(zs, col):
        return at.idx(zs, 1 - y if col & 2 else y, 1 - x if col & 1 else x, c)

    def up(zs, src=None):
        return copy(block(zs, 0), (z + 1, y, x, c), z_send.at[0, zs], z_recv.at[zs], src=src)

    def down(zs, src=None):
        return copy(block(zs, 0), (z - 1, y, x, c), z_send.at[1, zs], z_recv.at[zs], src=src)

    def to_x(zs, src=None):
        return copy(block(zs, 0), (z, y, 1 - x, c), x_send.at[zs], x_recv.at[zs], src=src)

    def to_y(zs, src=None):
        return copy(block(zs, 0), (z, 1 - y, x, c), y_send.at[zs], y_recv.at[zs], src=src)

    def diag_y(zs):
        return copy(block(zs, 1), (z, 1 - y, x, c), dy_send.at[zs], dy_recv.at[zs], lo)

    def diag_x(zs):
        return copy(block(zs, 2), (z, y, 1 - x, c), dx_send.at[zs], dx_recv.at[zs], hi)

    def to_core(zs, col, src=None):
        return copy(block(zs, col), (z, y, x, 1 - c), c_send.at[zs, col], c_recv.at[zs, col], src=src)

    own = pltpu.make_async_copy(src_ref, out_ref.at[block(z, 0)], own_sem)
    own.start()

    @pl.when(z < zn - 1)
    def _():
        up(z, src_ref).start()

    @pl.when(z > 0)
    def _():
        down(z, src_ref).start()

    to_x(z, src_ref).start()
    to_y(z, src_ref).start()
    to_core(z, 0, src_ref).start()

    def each(dist, fn):
        if dist == 0:
            fn(z, 0)
            return

        @pl.when(z - dist >= 0)
        def _():
            fn(z - dist, 1)

        @pl.when(z + dist < zn)
        def _():
            fn(z + dist, -1)

    def from_z(zs, way):
        copy(block(zs, 0), (z, y, x, c), z_send.at[0, zs], z_recv.at[zs]).wait_recv()
        if way > 0:
            @pl.when(z < zn - 1)
            def _():
                up(zs).start()
        else:
            @pl.when(z > 0)
            def _():
                down(zs).start()
        to_x(zs).start()
        to_y(zs).start()
        to_core(zs, 0).start()

    def from_xy(zs, way):
        to_x(zs).wait_recv()
        diag_y(zs).start()
        to_core(zs, 1).start()
        to_y(zs).wait_recv()
        diag_x(zs).start()
        to_core(zs, 2).start()

    def from_diag(zs, way):
        diag_y(zs).wait_recv()
        diag_x(zs).wait_recv()
        to_core(zs, 3).start()

    for dist in range(zn):
        if dist:
            each(dist, from_z)
        each(dist, from_xy)
    for dist in range(zn):
        each(dist, from_diag)
    own.wait()

    def sent(zs, way):
        for col in range(4):
            to_core(zs, col).wait_recv()
            to_core(zs, col).wait_send()
        to_x(zs).wait_send()
        to_y(zs).wait_send()
        diag_x(zs).wait_send()
        diag_y(zs).wait_send()
        if way >= 0:
            @pl.when(z < zn - 1)
            def _():
                up(zs).wait_send()
        if way <= 0:
            @pl.when(z > 0)
            def _():
                down(zs).wait_send()

    for dist in range(zn):
        each(dist, sent)


def gather_rows(shard, nd, nf, cid):
    zn = nd // 2
    D = pltpu.SemaphoreType.DMA
    return pl.pallas_call(
        functools.partial(gather_kernel, nd, nf),
        out_shape=jax.ShapeDtypeStruct((nd * nf,) + shard.shape, shard.dtype),
        in_specs=[pl.BlockSpec(memory_space=pl.ANY)],
        out_specs=pl.BlockSpec(memory_space=pl.ANY),
        scratch_shapes=[D(()), D((2, zn)), D((zn,)), D((zn,)), D((zn,)), D((zn,)), D((zn,)), D((zn,)), D((zn,)), D((zn,)), D((zn,)),
                        D((zn, 4)), D((zn, 4))],
        compiler_params=pltpu.CompilerParams(collective_id=cid, has_side_effects=True),
    )(shard)


class Scatter:
    def __init__(self, nd, nf, g_refs, out_ref, acc, c_in, d_in, xy_in, z_in,
                 load_sem, c_send, c_recv, dx_send, dx_recv, dy_send, dy_recv, x_send, x_recv, y_send, y_recv, z_send, z_recv):
        at = Place(nd, nf)
        z, y, x, c, zn = at.z, at.y, at.x, at.c, at.zn
        cols = out_ref.shape[1]
        wids = [r.shape[3] for r in g_refs]
        offs = [sum(wids[:k]) for k in range(len(wids))]
        half = cols // 256 * 128
        lo, hi = pl.ds(0, half), pl.ds(half, cols - half)

        def inner(col, core):
            return at.idx(0, 1 - y if col & 2 else y, 1 - x if col & 1 else x, core)

        def remote(src, dst, to, send, recv):
            return pltpu.make_async_remote_copy(src_ref=src, dst_ref=dst, send_sem=send, recv_sem=recv, device_id=at.dev(*to), device_id_type=MESH)

        def load(col):
            return [pltpu.make_async_copy(r.at[:, inner(col, c)], acc.at[col, :, :, pl.ds(o, w)], load_sem.at[col, k])
                    for k, (r, o, w) in enumerate(zip(g_refs, offs, wids))]

        def core(col):
            return [remote(r.at[:, inner(col, 1 - c)], c_in.at[col, :, :, pl.ds(o, w)], (z, y, x, 1 - c), c_send.at[col, k], c_recv.at[col, k])
                    for k, (r, o, w) in enumerate(zip(g_refs, offs, wids))]

        def diag_x(zs):
            return remote(acc.at[3, zs, :, lo], d_in.at[zs, :, lo], (z, y, 1 - x, c), dx_send.at[zs], dx_recv.at[zs])

        def diag_y(zs):
            return remote(acc.at[3, zs, :, hi], d_in.at[zs, :, hi], (z, 1 - y, x, c), dy_send.at[zs], dy_recv.at[zs])

        def to_x(zs):
            return remote(acc.at[1, zs], xy_in.at[0, zs], (z, y, 1 - x, c), x_send.at[zs], x_recv.at[zs])

        def to_y(zs):
            return remote(acc.at[2, zs], xy_in.at[1, zs], (z, 1 - y, x, c), y_send.at[zs], y_recv.at[zs])

        def up(zs):
            return remote(acc.at[0, zs], z_in.at[zs + 1], (z + 1, y, x, c), z_send.at[zs], z_recv.at[0, zs])

        def down(zs):
            return remote(acc.at[0, zs], z_in.at[zs], (z - 1, y, x, c), z_send.at[zs], z_recv.at[1, zs])

        def each(dist, fn):
            if dist == 0:
                fn(z)
                return

            @pl.when(z - dist >= 0)
            def _():
                fn(z - dist)

            @pl.when(z + dist < zn)
            def _():
                fn(z + dist)

        order = list(range(zn - 1, -1, -1))

        def start(col):
            for cp in core(col) + load(col):
                cp.start()

        def ready(col):
            for cp in load(col):
                cp.wait()
            for cp in core(col):
                cp.wait_recv()

        def diag(zs):
            acc[3, zs] = acc[3, zs] + c_in[3, zs]
            diag_x(zs).start()
            diag_y(zs).start()

        def sides(zs):
            diag_y(zs).wait_recv()
            acc[1, zs, :, lo] = acc[1, zs, :, lo] + c_in[1, zs, :, lo]
            acc[1, zs, :, hi] = acc[1, zs, :, hi] + c_in[1, zs, :, hi] + d_in[zs, :, hi]
            to_x(zs).start()
            diag_x(zs).wait_recv()
            acc[2, zs, :, lo] = acc[2, zs, :, lo] + c_in[2, zs, :, lo] + d_in[zs, :, lo]
            acc[2, zs, :, hi] = acc[2, zs, :, hi] + c_in[2, zs, :, hi]
            to_y(zs).start()

        def column(zs):
            to_x(zs).wait_recv()
            to_y(zs).wait_recv()
            return (acc[0, zs] + c_in[0, zs]).astype(f32) + (xy_in[0, zs] + xy_in[1, zs]).astype(f32)

        def pass_on(zs):
            total = column(zs)

            @pl.when(zs > z)
            def _():
                @pl.when(z > 0)
                def _():
                    up(zs).wait_recv()
                    acc[0, zs] = (total + z_in[zs + 1].astype(f32)).astype(bf16)

                @pl.when(z == 0)
                def _():
                    acc[0, zs] = total.astype(bf16)
                up(zs).start()

            @pl.when(zs < z)
            def _():
                @pl.when(z < zn - 1)
                def _():
                    down(zs).wait_recv()
                    acc[0, zs] = (total + z_in[zs].astype(f32)).astype(bf16)

                @pl.when(z == zn - 1)
                def _():
                    acc[0, zs] = total.astype(bf16)
                down(zs).start()

        def finish():
            out_ref[...] = column(z)

            @pl.when(z > 0)
            def _():
                up(z).wait_recv()
                out_ref[...] += z_in[z + 1].astype(f32)

            @pl.when(z < zn - 1)
            def _():
                down(z).wait_recv()
                out_ref[...] += z_in[z].astype(f32)

            def sent(zs):
                diag_x(zs).wait_send()
                diag_y(zs).wait_send()
                to_x(zs).wait_send()
                to_y(zs).wait_send()

            for col in range(4):
                for cp in core(col):
                    cp.wait_send()
            for dist in order:
                each(dist, sent)
                if dist:
                    each(dist, lambda zs: up(zs).wait_send())

        self.start, self.finish, self.greet, self.meet = start, finish, at.greet, at.meet
        self.diag = [functools.partial(ready, 3)] + [functools.partial(each, dist, diag) for dist in order]
        self.sides = [functools.partial(each, dist, sides) for dist in order]
        self.pass_on = [functools.partial(each, dist, pass_on) for dist in order[:-1]]
        self.ready = lambda: (ready(1), ready(2), ready(0))

    @staticmethod
    def scratch(nd, rows, cols, parts):
        zn = nd // 2
        D, V = pltpu.SemaphoreType.DMA, pltpu.VMEM
        return [V((4, zn, rows, cols), bf16), V((4, zn, rows, cols), bf16), V((zn, rows, cols), bf16), V((2, zn, rows, cols), bf16),
                V((zn + 1, rows, cols), bf16), D((4, parts)), D((4, parts)), D((4, parts))] + [D((zn,))] * 9 + [D((2, zn))]


def plan(pipes, place, time_of, spots):
    ticks = {0: [place.greet], 1: [place.meet] + [functools.partial(p.start, col) for col in (3, 1, 2, 0) for p in pipes]}

    def put(when, fn):
        tick = next((t for t, us in enumerate(time_of) if us >= when), len(time_of))
        ticks.setdefault(tick, []).append(fn)

    todo = []
    for p, (diag, sides, side_gap, pass_on, pass_gap) in zip(pipes, spots):
        todo += [(diag, fn) for fn in p.diag] + [(sides, p.ready)]
        todo += [(sides + k * side_gap * 4 / len(p.sides), fn) for k, fn in enumerate(p.sides)]
        todo += [(pass_on + k * pass_gap * 4 / len(p.sides), fn) for k, fn in enumerate(p.pass_on)]
    for when, fn in sorted(todo, key=lambda e: e[0]):
        put(when, fn)
    return ticks


def pipes_of(nd, nf, g_refs, out_refs, split, scratch):
    def view(a, lead, o, w):
        return g_refs[a].at[:, :, :, pl.ds(o, w)] if lead is None else g_refs[a].at[lead, :, :, :, pl.ds(o, w)]
    per = len(scratch) // len(split)
    return [Scatter(nd, nf, [view(*v) for v in pipe], out_ref, *scratch[per * m : per * (m + 1)])
            for m, (pipe, out_ref) in enumerate(zip(split, out_refs))]


def widths(split):
    return [sum(v[3] for v in pipe) for pipe in split]


def pipes_scratch(nd, rows, split):
    return [x for pipe, w in zip(split, widths(split)) for x in Scatter.scratch(nd, rows, w, len(pipe))]


def run_ticks(ticks, now, last):
    planned = sorted((t, fns) for t, fns in ticks.items() if t <= last)

    def search(items):
        if len(items) == 1:
            tick, fns = items[0]

            @pl.when(now == tick)
            def _():
                for fn in fns:
                    fn()
            return
        mid = len(items) // 2
        lax.cond(now < items[mid][0], lambda: search(items[:mid]), lambda: search(items[mid:]))

    if planned:
        search(planned)


def run_rest(ticks, last):
    for tick, fns in sorted(ticks.items()):
        if tick > last:
            for fn in fns:
                fn()


class Spread:
    def __init__(self, nd, nf, src, got, send, recv):
        self.n, self.nf = nd * nf, nf
        self.me = lax.axis_index("dp") * nf + lax.axis_index("fsdp")
        self.src, self.got, self.send, self.recv = src, got, send, recv

    def peer(self, k):
        return lax.rem(self.me + k, self.n)

    def loop(self, fn):
        def body(k, carry):
            fn(k)
            return carry
        lax.fori_loop(1, self.n, body, 0)

    def greet(self):
        sem = pltpu.get_barrier_semaphore()

        def one(k):
            pl.semaphore_signal(sem, inc=1, device_id=(self.peer(k) // self.nf, self.peer(k) % self.nf), device_id_type=MESH)
        self.loop(one)

    def meet(self):
        pl.semaphore_wait(pltpu.get_barrier_semaphore(), self.n - 1)

    def copy(self, k):
        p = self.peer(k)
        src = self.src.at[p] if len(self.src.shape) == 3 else self.src
        return pltpu.make_async_remote_copy(src_ref=src, dst_ref=self.got.at[k], send_sem=self.send.at[k], recv_sem=self.recv.at[k],
                                            device_id=(p // self.nf, p % self.nf), device_id_type=MESH)

    def begin(self):
        self.loop(lambda k: self.copy(k).start())

    def total(self):
        own = self.src[self.me] if len(self.src.shape) == 3 else self.src[...]

        def add(k, total):
            self.copy(k).wait_recv()
            return total + self.got[k]
        total = lax.fori_loop(1, self.n, add, own)
        self.loop(lambda k: self.copy(k).wait_send())
        return total

    @staticmethod
    def scratch(n, tile):
        D = pltpu.SemaphoreType.DMA
        return [pltpu.VMEM((n,) + tile, f32), D((n,)), D((n,))]


def dot(a, b, dims=((1,), (0,)), precision=None):
    return lax.dot_general(a, b, (dims, ((), ())), preferred_element_type=f32, precision=precision)


def sigmoid(x):
    return 0.5 * jnp.tanh(0.5 * x) + 0.5


def conv_rows(ext, taps, masks, halo):
    rows = ext.shape[0] - halo
    width = 4
    v = ext[halo:]
    out = taps[4:5] + taps[3:4] * v
    for k in range(1, width):
        moved = pltpu.roll(ext, k, 0)[halo:]
        out = out + (taps[3 - k : 4 - k] * masks[:, k : k + 1]) * moved
    return out


def prep_kernel(bcdt_ref, taps_ref, heads_ref, segc_ref, segr_ref,
                m_ref, b_ref, c_ref, bt_ref, ct_ref, pre_ref, gm_ref, cum_ref, cumr_ref, sc_ref, dt_ref):
    T = bcdt_ref.shape[0]
    nc = T // L
    N = b_ref.shape[1]
    H = dt_ref.shape[1]
    groups = cumr_ref.shape[0]
    taps = taps_ref[...]
    tri = (lax.broadcasted_iota(jnp.int32, (L, L), 0) >= lax.broadcasted_iota(jnp.int32, (L, L), 1))
    trif = tri.astype(f32)
    neg_rate = -jnp.exp(heads_ref[0:1, :H]) * LOG2E
    m_ref[T : T + 8, :] = jnp.zeros((8, 4), f32)
    bias = heads_ref[1:2, :H]

    def chunk(c, carry):
        t0 = pl.multiple_of(c * L, L)
        here = pl.ds(t0, L)
        h0 = pl.multiple_of(jnp.maximum(t0 - 16, 0), 16)
        before = bcdt_ref[pl.ds(h0, 16), : 2 * N].astype(f32)
        v = bcdt_ref[here, : 2 * N].astype(f32)
        segc = segc_ref[here, :].astype(f32)
        seg_ext = jnp.concatenate([segc_ref[pl.ds(h0, 16), :].astype(f32), segc], axis=0)
        at = t0 + lax.broadcasted_iota(jnp.int32, (L, 1), 0)
        masks = [jnp.ones((L, 1), f32)]
        for k in range(1, 4):
            masks.append(((pltpu.roll(seg_ext, k, 0)[16:] == segc) & (at >= k)).astype(f32))
        masks = jnp.concatenate(masks, axis=1)
        m_ref[here, :] = masks
        pre = conv_rows(jnp.concatenate([before, v], axis=0), taps, masks, 16)
        pre_ref[here, :] = pre
        act = pre * sigmoid(pre)
        b = act[:, :N]
        cc = act[:, N:]
        bb = b.astype(bf16)
        cb = cc.astype(bf16)
        b_ref[here, :] = bb
        c_ref[here, :] = cb
        bt_ref[:, here] = b.T.astype(bf16)
        ct_ref[:, here] = cc.T.astype(bf16)
        prev = jnp.where(c > 0, seg_ext[15:16], -1.0)
        last = segc[L - 1 : L]
        same = segc == segr_ref[:, here].astype(f32)
        g = dot(cb, bb, ((1,), (1,)))
        gm_ref[pl.ds(c, 1)] = jnp.where(tri & same, g, 0.0)[None]
        raw = bcdt_ref[here, 2 * N : 2 * N + 128].astype(f32)[:, :H] + bias
        dt = jnp.maximum(raw, 0.0) + jnp.log1p(jnp.exp(-jnp.abs(raw)))
        a2 = neg_rate * dt
        cum = dot(trif, a2, precision=HIGHEST)
        end = cum[L - 1 : L]
        ein = jnp.where(segc == prev, jnp.exp2(cum), 0.0)
        lv = jnp.where(segc == last, jnp.exp2(end - cum), 0.0)
        dt_ref[here, :] = dt
        wide = jnp.concatenate([cum, jnp.zeros((L, 128 - H), f32)], axis=1)
        cum_ref[here, :] = wide
        cumt = wide.T
        for k in range(groups):
            cumr_ref[k, :, here] = cumt[HG * k : HG * (k + 1)]
        s0 = pl.multiple_of(c * (3 * L), L)
        for k, part in enumerate((dt, ein, lv)):
            sc_ref[pl.ds(s0 + k * L, L), :] = jnp.concatenate([part, jnp.zeros((L, 128 - H), f32)], axis=1).astype(bf16)
        return carry

    lax.fori_loop(0, nc, chunk, 0, unroll=2)


def prep(bcdt, taps, heads, segc, segr, N, H):
    T = bcdt.shape[0]
    nc = T // L
    G = H // HG
    S = jax.ShapeDtypeStruct
    full = lambda a: pl.BlockSpec(a.shape, lambda i: (0,) * a.ndim)
    outs = (S((T + 8, 4), f32), S((T, N), bf16), S((T, N), bf16), S((N, T), bf16), S((N, T), bf16), S((T, 2 * N), f32),
            S((nc, L, L), f32), S((T, 128), f32), S((G, HG, T), f32), S((3 * T, 128), bf16), S((T, H), f32))
    wide = 2 * N + 128
    return pl.pallas_call(
        prep_kernel,
        grid=(1,),
        in_specs=[pl.BlockSpec((T, wide), lambda i: (0, bcdt.shape[1] // wide - 1))] + [full(a) for a in (taps, heads, segc, segr)],
        out_specs=[full(o) for o in outs],
        out_shape=outs,
        compiler_params=pltpu.CompilerParams(vmem_limit_bytes=60 << 20),
    )(bcdt, taps, heads, segc, segr)


def lane_onehot(group, width, per):
    shape = (128, width)
    return (group * HG + lax.broadcasted_iota(jnp.int32, shape, 1) // per == lax.broadcasted_iota(jnp.int32, shape, 0)).astype(bf16)


def half_masks(P):
    lane = lax.broadcasted_iota(jnp.int32, (1, 2 * P), 1)
    first = (lane < P).astype(f32)
    return first.astype(bf16), (1.0 - first).astype(bf16)


def decay(cum4, cumr, k):
    return jnp.exp2(jnp.minimum(cum4[:, k : k + 1] - cumr[k : k + 1, :], 0.0))


def fwd_kernel(u_ref, gate_ref, taps_ref, m_ref, b_ref, c_ref, bt_ref, gm_ref, cum_ref, cumr_ref, sc_ref,
               gg_ref, r_ref, pre_ref, st_ref, state, move, ssq_ref):
    T, W = u_ref.shape
    P = W // HG
    nc = T // L
    step = pl.program_id(0)
    taps = taps_ref[...]
    gain = taps[5:6]
    skip = taps[6:7]
    onehot = lane_onehot(step, W, P)
    ma, mb = half_masks(P)
    state[...] = jnp.zeros_like(state)

    @pl.when(step == 0)
    def _():
        ssq_ref[...] = jnp.zeros_like(ssq_ref)

    @pl.when(step == 0)
    def _():
        def make(c, carry):
            here = pl.ds(pl.multiple_of(c * L, L), L)
            lag = lax.broadcasted_iota(jnp.int32, (L, L + 16), 0) + 16 - lax.broadcasted_iota(jnp.int32, (L, L + 16), 1)
            for k in range(1, 4):
                move[c, (k - 1) * L : k * L, :] = jnp.where(lag == k, m_ref[here, k : k + 1], 0.0).astype(bf16)
            return carry
        lax.fori_loop(0, nc, make, 0)

    def chunk(c, carry):
        t0 = pl.multiple_of(c * L, L)
        here = pl.ds(t0, L)
        h0 = pl.multiple_of(jnp.maximum(t0 - 16, 0), 16)
        v = u_ref[here, :]
        moved = dot(move[c], jnp.concatenate([u_ref[pl.ds(h0, 16), :], v], axis=0))
        pre = taps[4:5] + taps[3:4] * v.astype(f32)
        for k in range(1, 4):
            pre = pre + taps[3 - k : 4 - k] * moved[(k - 1) * L : k * L]
        pre_ref[here, :] = pre.astype(bf16)
        x = pre * sigmoid(pre)
        s0 = pl.multiple_of(c * (3 * L), L)
        exp = dot(sc_ref[pl.ds(s0, 3 * L), :], onehot)
        dtx, einx, lvx = exp[:L], exp[L : 2 * L], exp[2 * L :]
        xd = x * dtx
        xdb = xd.astype(bf16)
        gm = gm_ref[c]
        cum4 = pltpu.roll(cum_ref[here, :], 128 - step * HG, 1)
        cumr = cumr_ref[0, :, here]
        sb = state[...].astype(bf16)
        st_ref[c] = sb
        inner = []
        for p in range(HG // 2):
            m0 = (decay(cum4, cumr, 2 * p) * gm).astype(bf16)
            m1 = (decay(cum4, cumr, 2 * p + 1) * gm).astype(bf16)
            xp = xdb[:, 2 * P * p : 2 * P * (p + 1)]
            inner.append(dot(jnp.concatenate([m0, m1], axis=1), jnp.concatenate([xp * ma, xp * mb], axis=0)))
        y = jnp.concatenate(inner, axis=1) + dot(c_ref[here, :], sb) * einx + skip * x
        state[...] = state[...] * einx[L - 1 : L] + dot(bt_ref[:, here], (xd * lvx).astype(bf16))
        gate = gate_ref[here, :].astype(f32)
        g = y * (gate * sigmoid(gate))
        gg_ref[here, :] = (g * gain).astype(bf16)
        g2 = g * g
        tot = g2[:, :128]
        for j in range(1, W // 128):
            tot = tot + g2[:, 128 * j : 128 * (j + 1)]
        ssq_ref[here, :] += tot
        return carry

    lax.fori_loop(0, nc, chunk, 0, unroll=4)

    @pl.when(step == pl.num_programs(0) - 1)
    def _():
        def root(c, carry):
            here = pl.ds(pl.multiple_of(c * L, L), L)
            total = jnp.sum(ssq_ref[here, :], axis=1, keepdims=True)
            r_ref[here, :] = lax.rsqrt(total / (W * pl.num_programs(0)) + EPS)
            return carry
        lax.fori_loop(0, nc, root, 0)


def fwd(u, gate, taps, masks, b, c, bt, gm, cum, cumr, sc):
    T, E = gate.shape
    N = b.shape[1]
    G = cumr.shape[0]
    W = E // G
    nc = T // L
    S = jax.ShapeDtypeStruct
    col = lambda off: pl.BlockSpec((T, W), lambda g: (0, g + off))
    full = lambda a: pl.BlockSpec(a.shape, lambda g: (0,) * a.ndim)
    grp = lambda a: pl.BlockSpec((1,) + a.shape[1:], lambda g: (g, 0, 0))
    return pl.pallas_call(
        fwd_kernel,
        grid=(G,),
        in_specs=[col(0), col(0), pl.BlockSpec((8, W), lambda g: (0, g)), full(masks), full(b), full(c), full(bt), full(gm),
                  full(cum), grp(cumr), full(sc)],
        out_specs=[col(0), pl.BlockSpec((T, 1), lambda g: (0, 0)), col(0), pl.BlockSpec((nc, N, W), lambda g: (0, 0, g))],
        out_shape=(S((T, E), bf16), S((T, 1), f32), S((T, E), bf16), S((nc, N, E), bf16)),
        scratch_shapes=[pltpu.VMEM((N, W), f32), pltpu.VMEM((nc, 3 * L, L + 16), bf16), pltpu.VMEM((T, 128), f32)],
        compiler_params=pltpu.CompilerParams(vmem_limit_bytes=60 << 20),
        cost_estimate=pl.CostEstimate(flops=T * E * (2 * L + 4 * N) * 2, bytes_accessed=T * E * 12, transcendentals=T * E * 4),
    )(u, gate, taps, masks, b, c, bt, gm, cum, cumr, sc)


def bwd_scatter_kernel(nd, nf, g0, Gh, nc, arrays, split, *refs):
    g_refs, ins, outs = refs[:arrays], refs[arrays : arrays + 16], refs[arrays + 16 : arrays + 23]
    refs = refs[arrays + 23 :]
    sums, own, comm = refs[: len(split)], refs[len(split) : len(split) + 4], refs[len(split) + 4 :]
    pipes = pipes_of(nd, nf, g_refs, sums, split, comm)
    nb = ins[15].shape[0] // MB
    pairs = nc // 2
    time_of = [20.0 * g + (3.7 * i if i < pairs else 3.7 * pairs + 1.7 * (i - pairs)) for g in range(Gh) for i in range(pairs + nb)]
    ticks = plan(pipes, pipes[0], time_of, BWD_SPOTS)
    last = len(time_of) - 1
    bwd_body(lambda i: run_ticks(ticks, pl.program_id(0) * (pairs + nb) + i, last), g0, *ins, *outs, *own)

    @pl.when(pl.program_id(0) == pl.num_programs(0) - 1)
    def _():
        run_rest(ticks, last)
        for p in pipes:
            p.finish()


def bwd_body(tick, g0, u_ref, gate_ref, pre_ref, dm_ref, rq_ref, taps_ref, m_ref, b_ref, c_ref, ct_ref, gm_ref, cum_ref, cumr_ref, sc_ref, st_ref, normt_ref,
             dz_ref, gw_ref, dg_ref, db_ref, dc_ref, rs_ref, small_ref, ds, nxt, acc, move):
    T, W = u_ref.shape
    P = W // HG
    nc = T // L
    step = pl.program_id(0)
    taps = taps_ref[...]
    gain = taps[5:6]
    skip = taps[6:7]
    onehot = lane_onehot(step + g0, W, P)
    ma, mb = half_masks(P)
    ds[...] = jnp.zeros_like(ds)
    nxt[...] = jnp.zeros_like(nxt)
    acc[...] = jnp.zeros_like(acc)

    @pl.when(step == 0)
    def _():
        dg_ref[...] = jnp.zeros_like(dg_ref)
        db_ref[...] = jnp.zeros_like(db_ref)
        dc_ref[...] = jnp.zeros_like(dc_ref)
        rs_ref[...] = jnp.zeros_like(rs_ref)

    @pl.when(step == 0)
    def _():
        def make(c, carry):
            mrows = m_ref[pl.ds(pl.multiple_of(c * L, L), L + 8), :]
            lag = lax.broadcasted_iota(jnp.int32, (2 * L, L), 0) - lax.broadcasted_iota(jnp.int32, (2 * L, L), 1)
            for k in range(1, 4):
                col = jnp.concatenate([mrows[:, k : k + 1], jnp.zeros((L - 8, 1), f32)], axis=0)
                move[c, (k - 1) * L : k * L, :] = jnp.where(lag == k, col, 0.0).T[:, : L + 16].astype(bf16)
            return carry
        lax.fori_loop(0, nc, make, 0)

    ri = lax.broadcasted_iota(jnp.int32, (4 * W, 128), 0)
    ci = lax.broadcasted_iota(jnp.int32, (4 * W, 128), 1)
    part = ri // W
    want = (jnp.maximum(part - 1, 0) * pl.num_programs(0) + step) * HG + (ri % W) // P
    fold = (want == ci).astype(bf16)

    def eight(z):
        return jnp.sum(z.reshape(L // 8, 8, W), axis=0)

    def chunk(i, carry):
        c = nc - 1 - i
        t0 = pl.multiple_of(c * L, L)
        here = pl.ds(t0, L)
        u = u_ref[here, :].astype(f32)
        pre = pre_ref[here, :].astype(f32)
        sig = sigmoid(pre)
        x = pre * sig
        dsilu = sig + x * (1.0 - sig)
        s0 = pl.multiple_of(c * (3 * L), L)
        exp = dot(sc_ref[pl.ds(s0, 3 * L), :], onehot)
        dtx, einx, lvx = exp[:L], exp[L : 2 * L], exp[2 * L :]
        xdb = (x * dtx).astype(bf16)
        xd = xdb.astype(f32)
        gm = gm_ref[c]
        cum4 = pltpu.roll(cum_ref[here, :], 128 - (step + g0) * HG, 1)
        cumr = cumr_ref[0, :, here]
        sb = st_ref[c]
        es, ms, inner = [], [], []
        for p in range(HG // 2):
            e0 = decay(cum4, cumr, 2 * p)
            e1 = decay(cum4, cumr, 2 * p + 1)
            m0 = (e0 * gm).astype(bf16)
            m1 = (e1 * gm).astype(bf16)
            xp = xdb[:, 2 * P * p : 2 * P * (p + 1)]
            inner.append(dot(jnp.concatenate([m0, m1], axis=1), jnp.concatenate([xp * ma, xp * mb], axis=0)))
            es.append((e0, e1))
            ms.append((m0, m1))
        yn = jnp.concatenate(inner, axis=1) + dot(c_ref[here, :], sb) * einx
        y = yn + skip * x
        gate = gate_ref[here, :].astype(f32)
        sgate = sigmoid(gate)
        silu_g = gate * sgate
        g = y * silu_g
        r = rq_ref[here, 0:1]
        q = rq_ref[here, 1:2]
        dmr = dm_ref[here, :].astype(f32) * r
        dgg = gain * dmr - g * q
        dyb = (dgg * silu_g).astype(bf16)
        dy = dyb.astype(f32)
        dz_ref[0, here, :] = (dgg * y * (sgate + silu_g * (1.0 - sgate))).astype(bf16)
        dxi = []
        dgc = dg_ref[c]
        for p in range(HG // 2):
            cols = slice(2 * P * p, 2 * P * (p + 1))
            dp = dyb[:, cols]
            dstack = jnp.concatenate([dp * ma, dp * mb], axis=0)
            dmm = dot(dstack, xdb[:, cols], ((1,), (1,)))
            dgc = dgc + dmm[:L] * es[p][0] + dmm[L:] * es[p][1]
            dxi.append(dot(jnp.concatenate(ms[p], axis=0), dstack, ((0,), (0,))))
        dg_ref[c] = dgc
        dxi = jnp.concatenate(dxi, axis=1)
        dsn = ds[...]
        dsb = dsn.astype(bf16)
        dye = (dy * einx).astype(bf16)
        dc_ref[here, :] += dot(dye, sb, ((1,), (1,)))
        kept = einx[L - 1 : L]
        through = kept * jnp.sum(sb.astype(f32) * dsn, axis=0, keepdims=True)
        db_ref[here, :] += dot((xd * lvx).astype(bf16), dsb, ((1,), (1,)))
        dxe = dot(b_ref[here, :], dsb) * lvx
        ds[...] = dsn * kept + dot(ct_ref[:, here], dye)
        dxd = dxi + dxe
        r1 = dy * yn - xd * dxi
        at_end = (lax.broadcasted_iota(jnp.int32, (8, 1), 0) == 7).astype(f32)
        r1 = jnp.concatenate([r1[: L - 8], r1[L - 8 :] + at_end * through], axis=0)
        r1h = r1.astype(bf16)
        r1l = (r1 - r1h.astype(f32)).astype(bf16)
        rs_ref[here, :] += dot(jnp.concatenate([r1h, r1l, (xd * dxe).astype(bf16), (x * dxd).astype(bf16)], axis=1), fold)
        dpre = (dxd * dtx + skip * dy) * dsilu
        dpb = dpre.astype(bf16)
        moved = dot(move[c], jnp.concatenate([dpb, nxt[...]], axis=0))
        nxt[...] = dpb[:16]
        du = taps[3:4] * dpre
        acc[0:8, :] += eight(dmr * g)
        acc[8:16, :] += eight(dy * x)
        acc[16:24, :] += eight(dpre)
        acc[24:32, :] += eight(dpre * u)
        for k in range(1, 4):
            sk = moved[(k - 1) * L : k * L]
            du = du + taps[3 - k : 4 - k] * sk
            acc[24 + 8 * k : 32 + 8 * k, :] += eight(sk * u)
        dz_ref[1, here, :] = du.astype(bf16)
        return carry

    def pair(i, carry):
        tick(i)
        chunk(2 * i, carry)
        return chunk(2 * i + 1, carry)

    lax.fori_loop(0, nc // 2, pair, 0)
    for j in range(7):
        small_ref[j : j + 1, :] = jnp.sum(acc[8 * j : 8 * j + 8, :], axis=0, keepdims=True)
    small_ref[7:8, :] = jnp.zeros((1, W), f32)

    def weights(i, carry):
        tick(nc // 2 + i)
        rows = pl.ds(pl.multiple_of(i * MB, MB), MB)
        for kind in range(2):
            gw_ref[kind, rows, :] = dot(normt_ref[rows, :], dz_ref[kind]).astype(bf16)
        return carry

    lax.fori_loop(0, normt_ref.shape[0] // MB, weights, 0)


def bwd(half, halves, u, gate, pre, dm, rq, taps, masks, b, c, ct, gm, cum, cumr, sc, st, normt, comm):
    T, E = gate.shape
    N = b.shape[1]
    G = cumr.shape[0]
    W = E // G
    nc = T // L
    Gh = G // halves
    Eh = E // halves
    g0 = half * Gh
    S = jax.ShapeDtypeStruct
    col = pl.BlockSpec((T, W), lambda g: (0, g + g0))
    full = lambda a: pl.BlockSpec(a.shape, lambda g: (0,) * a.ndim)
    whole = lambda s: pl.BlockSpec(s, lambda g: (0,) * len(s))
    grp = lambda a: pl.BlockSpec((1,) + a.shape[1:], lambda g: (g + g0, 0, 0))
    in_specs = [col, col, col, col, full(rq), pl.BlockSpec((8, W), lambda g: (0, g + g0)), full(masks), full(b), full(c),
                full(ct), full(gm), full(cum), grp(cumr), full(sc), pl.BlockSpec((nc, N, W), lambda g: (0, 0, g + g0)), full(normt)]
    D = normt.shape[0]
    out_specs = [pl.BlockSpec((2, T, W), lambda g: (0, 0, g)), pl.BlockSpec((2, D, W), lambda g: (0, 0, g)), whole((nc, L, L)), whole((T, N)), whole((T, N)),
                 whole((T, 128)), pl.BlockSpec((8, W), lambda g: (0, g))]
    out_shape = [S((2, T, Eh), bf16), S((2, D, Eh), bf16), S((nc, L, L), f32), S((T, N), f32), S((T, N), f32), S((T, 128), f32), S((8, Eh), f32)]
    scratch = [pltpu.VMEM((N, W), f32), pltpu.VMEM((16, W), bf16), pltpu.VMEM((56, W), f32), pltpu.VMEM((nc, 3 * L, L + 16), bf16)]
    nd, nf, cid, first, split = comm
    rows = first[0].shape[-2]
    return pl.pallas_call(
        functools.partial(bwd_scatter_kernel, nd, nf, g0, Gh, nc, len(first), split),
        grid=(Gh,),
        in_specs=[pl.BlockSpec(memory_space=pl.ANY)] * len(first) + in_specs,
        out_specs=out_specs + [whole((rows, w)) for w in widths(split)],
        out_shape=out_shape + [S((rows, w), f32) for w in widths(split)],
        scratch_shapes=scratch + pipes_scratch(nd, rows, split),
        compiler_params=pltpu.CompilerParams(vmem_limit_bytes=60 << 20, collective_id=cid, has_side_effects=True),
        cost_estimate=pl.CostEstimate(flops=T * Eh * (8 * L + 12 * N + 4 * D), bytes_accessed=T * Eh * 16, transcendentals=T * Eh * 4),
    )(*first, u, gate, pre, dm, rq, taps, masks, b, c, ct, gm, cum, cumr, sc, st, normt)


def post_kernel(bcdt_ref, pre_ref, taps_ref, heads_ref, m_ref, segc_ref, segr_ref, b_ref, c_ref, dg0_ref, db0_ref, dc0_ref, rs0_ref, dg1_ref, db1_ref, dc1_ref, rs1_ref, dt_ref,
                out_ref, small_ref, hs_ref, nxt, acc, hacc):
    T = bcdt_ref.shape[0]
    nc = T // L
    N = b_ref.shape[1]
    H = dt_ref.shape[1]
    taps = taps_ref[...]
    tri = (lax.broadcasted_iota(jnp.int32, (L, L), 0) >= lax.broadcasted_iota(jnp.int32, (L, L), 1))
    upper = (lax.broadcasted_iota(jnp.int32, (L, L), 0) <= lax.broadcasted_iota(jnp.int32, (L, L), 1)).astype(f32)
    strict = 1.0 - upper
    rate = -jnp.exp(heads_ref[0:1, :H])
    bias = heads_ref[1:2, :H]
    nxt[...] = jnp.zeros_like(nxt)
    acc[...] = jnp.zeros_like(acc)
    hacc[...] = jnp.zeros_like(hacc)

    def eight(z):
        return jnp.sum(z.reshape(L // 8, 8, z.shape[1]), axis=0)

    def chunk(i, carry):
        c = nc - 1 - i
        t0 = pl.multiple_of(c * L, L)
        here = pl.ds(t0, L)
        same = segc_ref[here, :] == segr_ref[:, here]
        dg = jnp.where(tri & same, dg0_ref[c] + dg1_ref[c], 0.0)
        dgb = dg.astype(bf16)
        dcv = dc0_ref[here, :] + dc1_ref[here, :] + dot(dgb, b_ref[here, :])
        dbv = db0_ref[here, :] + db1_ref[here, :] + dot(dg.T.astype(bf16), c_ref[here, :])
        pre = pre_ref[here, :]
        sig = sigmoid(pre)
        dpre = jnp.concatenate([dbv, dcv], axis=1) * (sig + pre * sig * (1.0 - sig))
        v = bcdt_ref[here, : 2 * N].astype(f32)
        ext = jnp.concatenate([dpre, nxt[...]], axis=0)
        nxt[...] = dpre[:8]
        dv = taps[3:4] * dpre
        acc[0:8, :] += eight(dpre)
        acc[8:16, :] += eight(dpre * v)
        mrows = m_ref[pl.ds(t0, L + 8), :]
        for k in range(1, 4):
            sk = pltpu.roll(ext * mrows[:, k : k + 1], L + 8 - k, 0)[:L]
            dv = dv + taps[3 - k : 4 - k] * sk
            acc[8 + 8 * k : 16 + 8 * k, :] += eight(sk * v)
        out_ref[here, : 2 * N] = dv.astype(bf16)
        q = H // 2
        r0, r1 = rs0_ref[here, :], rs1_ref[here, :]
        r1, r2, r3 = (jnp.concatenate([r0[:, m * q : (m + 1) * q], r1[:, m * q : (m + 1) * q]], axis=1) for m in range(3))
        da = dot(upper, r1, precision=HIGHEST) + dot(strict, r2, precision=HIGHEST)
        dt = dt_ref[here, :]
        raw = bcdt_ref[here, 2 * N : 2 * N + 128].astype(f32)[:, :H] + bias
        ddt = (r3 + da * rate) * sigmoid(raw)
        hacc[0:8, :] += eight(da * rate * dt)
        hacc[8:16, :] += eight(ddt)
        out_ref[here, 2 * N :] = jnp.concatenate([ddt, jnp.zeros((L, out_ref.shape[1] - 2 * N - H), f32)], axis=1).astype(bf16)
        return carry

    lax.fori_loop(0, nc, chunk, 0, unroll=2)
    for j in range(5):
        small_ref[j : j + 1, :] = jnp.sum(acc[8 * j : 8 * j + 8, :], axis=0, keepdims=True)
    small_ref[5:8, :] = jnp.zeros((3, 2 * N), f32)
    for j in range(2):
        hs_ref[j : j + 1, :] = jnp.sum(hacc[8 * j : 8 * j + 8, :], axis=0, keepdims=True)


def post(bcdt, pre, taps, heads, masks, segc, segr, b, c, first, second, dt):
    T = bcdt.shape[0]
    N = b.shape[1]
    H = dt.shape[1]
    S = jax.ShapeDtypeStruct
    wide = 2 * N + 128
    full = lambda a: pl.BlockSpec(a.shape, lambda i: (0,) * a.ndim)
    ins = (bcdt, pre, taps, heads, masks, segc, segr, b, c, *first, *second, dt)
    outs = (S((T, wide), bf16), S((8, 2 * N), f32), S((2, H), f32))
    return pl.pallas_call(
        post_kernel,
        grid=(1,),
        in_specs=[pl.BlockSpec((T, wide), lambda i: (0, bcdt.shape[1] // wide - 1))] + [full(a) for a in ins[1:]],
        out_specs=[full(o) for o in outs],
        out_shape=outs,
        scratch_shapes=[pltpu.VMEM((8, 2 * N), f32), pltpu.VMEM((40, 2 * N), f32), pltpu.VMEM((16, H), f32)],
        compiler_params=pltpu.CompilerParams(vmem_limit_bytes=60 << 20),
    )(*ins)


NT = 256


def tail_kernel(nd, nf, arrays, split, tiles, *refs):
    g_refs, refs = refs[:arrays], refs[arrays:]
    (wo_hbm, wg_hbm, wa_hbm, gg_ref, dz0_ref, dz1_ref, dbc_ref, hid_ref, go_ref, r_ref, gain_ref, mine_ref,
     suma_ref, sumb_ref, out_ref, gin_ref, small_ref) = refs[:17]
    wo, wg, wa, acc, sem = refs[17:22]
    mine = Spread(nd, nf, mine_ref, *refs[22:25])
    pipes = pipes_of(nd, nf, g_refs, (suma_ref, sumb_ref), split, refs[25:])
    D, E = wg.shape
    Eh = E // 2
    step = pl.program_id(0)
    early = tiles // 2
    blocks = D // NT
    mid = (early + tiles) * blocks
    scale = 4 / tiles
    time_of = [4 + 0.75 * scale * t if t < early * blocks else
               (13 + 1.65 * scale * (t - early * blocks) if t < mid else 52.6 + 0.65 * scale * (t - mid)) for t in range(2 * tiles * blocks)]
    ticks = plan(pipes, mine, time_of, TAIL_SPOTS)
    last = len(time_of) - 1
    ticks[1].append(mine.begin)
    fetch = [pltpu.make_async_copy(src, dst, sem.at[k]) for k, (src, dst) in enumerate(((wo_hbm, wo), (wg_hbm, wg), (wa_hbm, wa)))]

    @pl.when(step == 0)
    def _():
        for cp in fetch:
            cp.start()
        run_ticks(ticks, 0, 0)
        fetch[0].wait()

    @pl.when(step == early)
    def _():
        fetch[1].wait()
        fetch[2].wait()

    back = (step >= early) & (step < early + tiles)
    in_back = lambda t: early * blocks <= t < (early + tiles) * blocks

    @pl.when(jnp.logical_not(back))
    def _():
        def block(j, carry):
            run_ticks({t: f for t, f in ticks.items() if t and not in_back(t)}, step * blocks + j, last)
            cols = pl.ds(pl.multiple_of(j * NT, NT), NT)
            out_ref[:, cols] = (hid_ref[:, cols].astype(f32) + r_ref[...] * dot(gg_ref[...], wo[:, cols])).astype(bf16)
            return carry
        lax.fori_loop(0, blocks, block, 0)

    @pl.when(back)
    def _():
        def block(j, carry):
            run_ticks({t: f for t, f in ticks.items() if in_back(t)}, step * blocks + j, last)
            cols = pl.ds(pl.multiple_of(j * NT, NT), NT)
            part = dot(dz0_ref[0], wg[cols, :Eh], ((1,), (1,))) + dot(dz1_ref[0], wg[cols, Eh:], ((1,), (1,)))
            part = part + dot(dz0_ref[1], wa[cols, :Eh], ((1,), (1,))) + dot(dz1_ref[1], wa[cols, Eh:E], ((1,), (1,)))
            acc[:, cols] = part + dot(dbc_ref[...], wa[cols, E:], ((1,), (1,)))
            return carry
        lax.fori_loop(0, blocks, block, 0)
        gain = gain_ref[...]

        def rows_of(i, carry):
            here = pl.ds(pl.multiple_of(i * 64, 64), 64)
            rows = hid_ref[here, :].astype(f32)
            rinv = lax.rsqrt(jnp.mean(rows * rows, axis=-1, keepdims=True) + EPS)
            xhat = rows * rinv
            bn = acc[here, :]
            gb = bn * gain
            mean = jnp.mean(gb * xhat, axis=-1, keepdims=True)
            gin_ref[here, :] = (go_ref[here, :].astype(f32) + rinv * (gb - xhat * mean)).astype(bf16)
            return carry
        lax.fori_loop(0, hid_ref.shape[0] // 64, rows_of, 0)

    @pl.when(step == 2 * tiles - 1)
    def _():
        run_rest(ticks, last)
        for p in pipes:
            p.finish()
        small_ref[...] = mine.total()


def tail(nd, nf, cid, gs, split, dz0, dz1, dbcdt, full_gate, full_a, gg, full_out, hidden, grad_out, r, norm_gain, mine):
    T, D = hidden.shape
    E = full_out.shape[0]
    n = nd * nf
    rows = gs[0].shape[-2]
    MT = 256 if rows % 16 == 0 else 128
    tiles = T // MT
    early = tiles // 2
    wide = dbcdt.shape[1]
    S = jax.ShapeDtypeStruct
    any_ = pl.BlockSpec(memory_space=pl.ANY)
    whole = lambda s: pl.BlockSpec(s, lambda k: (0,) * len(s), pipeline_mode=pl.Buffered(1))
    at_out = lambda k: jnp.minimum(k, early - 1) + jnp.clip(k - tiles - early + 1, 0, tiles - early)
    at_back = lambda k: jnp.clip(k - early, 0, tiles - 1)
    at_row = lambda k: k - early * jnp.clip(k - early + 1, 0, 1) - (tiles - early) * jnp.clip(k - early - tiles + 1, 0, 1)
    out_tile = lambda w: pl.BlockSpec((MT, w), lambda k: (at_out(k), 0))
    back_tile = lambda w: pl.BlockSpec((MT, w), lambda k: (at_back(k), 0))
    half = pl.BlockSpec((2, MT, E // 2), lambda k: (0, at_back(k), 0))
    tile = mine.shape[1:]
    return pl.pallas_call(
        functools.partial(tail_kernel, nd, nf, len(gs), split, tiles),
        grid=(2 * tiles,),
        in_specs=[any_] * (len(gs) + 3) + [out_tile(E), half, half, back_tile(wide), pl.BlockSpec((MT, D), lambda k: (at_row(k), 0)), back_tile(D),
                                           out_tile(1), whole((1, D)), whole(mine.shape)],
        out_specs=[whole((rows, w)) for w in widths(split)] + [out_tile(D), back_tile(D), whole(tile)],
        out_shape=[S((rows, w), f32) for w in widths(split)] + [S((T, D), bf16), S((T, D), bf16), S(tile, f32)],
        scratch_shapes=[pltpu.VMEM((E, D), bf16), pltpu.VMEM((D, E), bf16), pltpu.VMEM((D, E + wide), bf16), pltpu.VMEM((MT, D), f32),
                        pltpu.SemaphoreType.DMA((3,))]
        + Spread.scratch(n, tile) + pipes_scratch(nd, rows, split),
        compiler_params=pltpu.CompilerParams(collective_id=cid, has_side_effects=True, vmem_limit_bytes=67043328),
        cost_estimate=pl.CostEstimate(flops=2 * T * D * 3 * E, bytes_accessed=8 * D * E, transcendentals=0),
    )(*gs, full_out, full_gate, full_a, gg, dz0, dz1, dbcdt, hidden, grad_out, r, norm_gain, mine)


def finish_kernel(gate0_ref, gate1_ref, u0_ref, u1_ref, oa_ref, ob_ref, tot_ref, wzx_ref, wbc_ref, wdt_ref, gain_ref, o_ref, gi_ref,
                  oo_ref, go_ref, zx_ref, bc_ref, dt_ref, out_ref, conv_ref, n_ref, gg_ref, heads_ref):
    oo_ref[...] = o_ref[...]
    go_ref[...] = gi_ref[...]

    @pl.when(pl.program_id(0) == 0)
    def _():
        Eh = gate0_ref.shape[1]
        for k, ref in enumerate((gate0_ref, gate1_ref, u0_ref)):
            zx_ref[:, k * Eh : (k + 1) * Eh] = ref[...]
        zx_ref[:, 3 * Eh :] = u1_ref[:, :Eh]
        wide = bc_ref.shape[1]
        bc_ref[...] = u1_ref[:, Eh : Eh + wide]
        dt_ref[...] = u1_ref[:, Eh + wide : Eh + wide + 128][:, : dt_ref.shape[1]]
        half = oa_ref.shape[1]
        out_ref[:, :half] = oa_ref[...]
        out_ref[:, half:] = ob_ref[...]
        k1 = conv_ref.shape[0]
        conv_ref[...] = tot_ref[:k1, : conv_ref.shape[1]]
        gg_ref[...] = tot_ref[k1 : k1 + 1, : gg_ref.shape[1]]
        heads_ref[...] = tot_ref[k1 + 1 : k1 + 1 + heads_ref.shape[0], : heads_ref.shape[1]]
        dots = lambda w, g: jnp.sum(w.astype(f32) * g, axis=1, keepdims=True)
        total = dots(wzx_ref[...], zx_ref[...]) + dots(wbc_ref[...], bc_ref[...]) + dots(wdt_ref[...], dt_ref[...])
        n_ref[...] = total / gain_ref[...].astype(f32)


def finish(gate0, gate1, u0, u1, s_out, tot, w_zx, w_bc, w_dt, gain, output, grad_in, shapes):
    S = jax.ShapeDtypeStruct
    tile = pl.BlockSpec((256, output.shape[1]), lambda i: (i, 0))
    return pl.pallas_call(
        finish_kernel,
        grid=(output.shape[0] // 256,),
        in_specs=[pl.BlockSpec(a.shape, lambda i: (0, 0)) for a in (gate0, gate1, u0, u1, *s_out, tot, w_zx, w_bc, w_dt, gain)] + [tile, tile],
        out_specs=[tile, tile] + [pl.BlockSpec(s, lambda i: (0, 0)) for s in shapes],
        out_shape=[S(output.shape, bf16), S(output.shape, bf16)] + [S(s, f32) for s in shapes],
        compiler_params=pltpu.CompilerParams(vmem_limit_bytes=63 << 20),
    )(gate0, gate1, u0, u1, *s_out, tot, w_zx, w_bc, w_dt, gain, output, grad_in)


def norm_kernel(hid_ref, gain_ref, normed_ref, normt_ref):
    rows = hid_ref[...].astype(f32)
    normed = rows * lax.rsqrt(jnp.mean(rows * rows, axis=-1, keepdims=True) + EPS) * gain_ref[...]
    normed_ref[...] = normed.astype(bf16)
    normt_ref[...] = normed.T.astype(bf16)


def norm(hidden, gain):
    T, D = hidden.shape
    S = jax.ShapeDtypeStruct
    row = pl.BlockSpec((256, D), lambda i: (i, 0))
    return pl.pallas_call(
        norm_kernel,
        grid=(T // 256,),
        in_specs=[row, pl.BlockSpec((1, D), lambda i: (0, 0))],
        out_specs=[row, pl.BlockSpec((D, 256), lambda i: (0, i))],
        out_shape=(S((T, D), bf16), S((D, T), bf16)),
        compiler_params=pltpu.CompilerParams(vmem_limit_bytes=40 << 20),
    )(hidden, gain)


def layer(nd, nf, hidden, grad_out, seg, shard_a, shard_gate, shard_out, head_params, owned, sizes):
    w_zx, w_bc, w_dt, own_gain = owned
    n = nd * nf
    E, N, H, K1, S = sizes
    T, D = hidden.shape
    wide = 2 * N + 128
    full_gate = lax.all_gather(shard_gate, AXES, axis=0, tiled=True)
    full_out = lax.all_gather(shard_out, AXES, axis=0, tiled=True)
    full_a = gather_rows(shard_a, nd, nf, 0)
    off = E + 2 * N + H
    flat = full_a[:, :, off : off + S].reshape(n, -1)
    ncol, nrow, ngate = (E + 2 * N) // n, D // n, E // n
    conv = flat[:, : K1 * ncol].reshape(n, K1, ncol).transpose(1, 0, 2).reshape(K1, n * ncol).astype(f32)
    norm_gain = flat[:, K1 * ncol : K1 * ncol + nrow].reshape(-1).astype(f32)
    gate_gain = flat[:, K1 * ncol + nrow : K1 * ncol + nrow + ngate].reshape(-1).astype(f32)
    full_a = full_a.reshape(D, E + wide)
    normed, normt = norm(hidden, norm_gain[None])
    ubc = dot(normed, full_a).astype(bf16)
    gate = dot(normed, full_gate).astype(bf16)
    segc, segr = seg[:, None], seg[None, :]
    taps_u = jnp.concatenate([conv[:, :E], gate_gain[None], jnp.repeat(head_params[2], E // H)[None], jnp.zeros((1, E), f32)], axis=0)
    taps_bc = jnp.concatenate([conv[:, E:], jnp.zeros((3, 2 * N), f32)], axis=0)
    masks, b, c, bt, ct, pre_bc, gm, cum, cumr, sc, dt = prep(ubc, taps_bc, head_params, segc, segr, N, H)
    gg, r, pre, st = fwd(ubc, gate, taps_u, masks, b, c, bt, gm, cum, cumr, sc)
    gos = (grad_out.astype(f32) * r).astype(bf16)
    g_out = dot(gg, gos, ((0,), (0,))).astype(bf16)
    g_out, full_out = lax.optimization_barrier((g_out, full_out))
    dm = dot(grad_out, full_out, ((1,), (1,))).astype(bf16)
    s = jnp.sum(gg.astype(f32) * dm.astype(f32), axis=1, keepdims=True)
    rq = jnp.concatenate([r, r * r * r * s / E], axis=1)
    back = functools.partial(bwd, u=ubc, gate=gate, pre=pre, dm=dm, rq=rq, taps=taps_u, masks=masks, b=b, c=c, ct=ct, gm=gm, cum=cum,
                             cumr=cumr, sc=sc, st=st, normt=normt)
    zn = max(nd // 2, 1)
    rows_of = lambda g: g.reshape(g.shape[:-2] + (zn, n // zn, g.shape[-2] // n, g.shape[-1]))
    Eh = E // 2
    dz0, gw0, dg0, db0, dc0, rs0, small0, *s_out = back(
        0, 2, comm=(nd, nf, 4, (rows_of(g_out),), (((0, None, 0, D // 2),), ((0, None, D // 2, D // 2),))))
    dz1, gw1, dg1, db1, dc1, rs1, small1, gate0, u0 = back(1, 2, comm=(nd, nf, 3, (rows_of(gw0),), (((0, 0, 0, Eh),), ((0, 1, 0, Eh),))))
    small = jnp.concatenate([small0, small1], axis=1)
    dbcdt, small_bc, hs = post(ubc, pre_bc, taps_bc, head_params, masks, segc, segr, b, c, (dg0, db0, dc0, rs0), (dg1, db1, dc1, rs1), dt)
    d_conv = jnp.concatenate([jnp.stack([small[6], small[5], small[4], small[3], small[2]]),
                              jnp.stack([small_bc[4], small_bc[3], small_bc[2], small_bc[1], small_bc[0]])], axis=1)
    d_heads = jnp.concatenate([hs, jnp.sum(small[1].reshape(1, H, E // H), axis=2)], axis=0)
    lanes = -(-max(ncol, ngate, H) // 128) * 128
    cols = lambda a: jnp.pad(a.reshape(-1, n, a.shape[1] // n).transpose(1, 0, 2), ((0, 0), (0, 0), (0, lanes - a.shape[1] // n)))
    heads_row = jnp.broadcast_to(jnp.pad(d_heads, ((0, 0), (0, lanes - H)))[None], (n, d_heads.shape[0], lanes))
    used = K1 + 1 + d_heads.shape[0]
    mine = jnp.concatenate([cols(d_conv), cols(small[:1]), heads_row, jnp.zeros((n, -(-used // 8) * 8 - used, lanes), f32)], axis=1)
    g_bcdt = dot(normt, dbcdt).astype(bf16)
    split = (((0, 0, 0, Eh),), ((0, 1, 0, Eh), (1, None, 0, wide)))
    gate1, u1, output, grad_in, tot = tail(nd, nf, 1, (rows_of(gw1), rows_of(g_bcdt)), split, dz0, dz1, dbcdt, full_gate, full_a, gg,
                                                   full_out, hidden, grad_out, r, norm_gain[None], mine)
    output, grad_in, s_zx, s_bc, s_dt, s_w, t_conv, t_norm, t_gate, t_heads = finish(
        gate0, gate1, u0, u1, s_out, tot, w_zx, w_bc, w_dt, own_gain, output, grad_in,
        ((nrow, 2 * E), (nrow, 2 * N), (nrow, H), (E // n, D), (K1, ncol), (nrow, 1), (1, ngate), d_heads.shape))
    return output, grad_in, s_zx, s_bc, s_dt, s_w, t_conv, t_norm.reshape(-1), t_gate.reshape(-1), t_heads


def per_device(nd, nf, hidden, grad_out, segment_ids, w_zx, w_bc, w_dt, w_out, conv_params, norm_gain, gate_gain, head_params):
    n = nd * nf
    E, N2, H = w_out.shape[0] * n, w_bc.shape[1], w_dt.shape[1]
    rows = w_zx.shape[0]
    small = jnp.concatenate([conv_params.reshape(-1), norm_gain, gate_gain])
    S = -(-small.shape[0] // rows)
    assert S + H <= 128
    small = jnp.pad(small, (0, S * rows - small.shape[0])).reshape(rows, S)
    shard_a = jnp.concatenate([w_zx[:, E:], w_bc, w_dt, small, jnp.zeros((rows, 128 - H - S), bf16)], axis=1)
    return layer(nd, nf, hidden, grad_out, segment_ids, shard_a, w_zx[:, :E], w_out, head_params, (w_zx, w_bc, w_dt, norm_gain[:, None]),
                 (E, N2 // 2, H, conv_params.shape[0], S))


def solution(mesh):
    row, col, vec, rep = P(AXES, None), P(None, AXES), P(AXES), P()
    return jax.shard_map(
        functools.partial(per_device, mesh.shape["dp"], mesh.shape["fsdp"]),
        mesh=mesh,
        in_specs=(row, row, vec, row, row, row, row, col, vec, vec, rep),
        out_specs=(row, row, row, row, row, row, col, vec, vec, rep),
        check_vma=False,
    )
```
